8 devices in a mesh: exam: 1 (over z), cols: 2 (over y), rows: 4 (over x, core).
Axes of the slice: x: 2, y: 2, z: 1, core: 2. Of those that a mesh axis runs over, the one named last changes fastest.
Arguments:
- kspace: float32 [2, 8, 32768], P(None, None, ('exam', 'rows', 'cols'))
- wts_y: float32 [6, 32768], P(None, ('exam', 'rows', 'cols'))
- wts_x: float32 [6, 32768], P(None, ('exam', 'rows', 'cols'))
- idx_y: int32 [32768], P(('exam', 'rows', 'cols'))
- idx_x: int32 [32768], P(('exam', 'rows', 'cols'))
- coil_maps: float32 [2, 8, 320, 320], P(None, ('exam', 'cols'), None, 'rows')
- deapod: float32 [320], replicated
Outputs:
- output: float32 [2, 320, 320], P(None, ('exam', 'cols'), 'rows')
All inputs are finite; a program needn't handle non-finite values.
Results may differ from the reference program's by a relative error of at most 0.001.
Values are sent between devices in bfloat16 or wider.
A program may use at most 1 GiB of HBM per device.

```python
import math
import jax
import jax.numpy as jnp
from jax import lax

IMG_SIZE = 320
NUM_COILS = 8
KERNEL_WIDTH = 6
ROW_BLOCKS = 4
COL_BLOCKS = 2
BLOCK_SLOTS = 4096


def setup_inputs(seed: int = 0, part: int = 0) -> dict:
    root_key = jax.random.key(seed)
    part_key = jax.random.fold_in(root_key, part)
    sub_keys = jax.random.split(part_key, 6)
    grid_size = 2 * IMG_SIZE
    row_blk = grid_size // ROW_BLOCKS
    col_blk = grid_size // COL_BLOCKS
    n_total = ROW_BLOCKS * COL_BLOCKS * BLOCK_SLOTS
    block_id = jnp.arange(n_total) // BLOCK_SLOTS
    idx_y = (block_id // COL_BLOCKS) * row_blk + jax.random.randint(sub_keys[0], (n_total,), 0, row_blk)
    idx_x = (block_id % COL_BLOCKS) * col_blk + jax.random.randint(sub_keys[1], (n_total,), 0, col_blk)
    centre = grid_size // 2
    dist_sq = ((idx_y - centre) ** 2 + (idx_x - centre) ** 2).astype(jnp.float32)
    blob_width = grid_size / 32.0
    envelope = 1.0 + 8.0 * jnp.exp(-dist_sq / (2.0 * blob_width * blob_width))
    samp_scale = grid_size / (KERNEL_WIDTH * math.sqrt(n_total))
    kspace = jax.random.normal(sub_keys[2], (2, NUM_COILS, n_total), jnp.float32) * (envelope * samp_scale)
    wts_y = jax.random.uniform(sub_keys[3], (KERNEL_WIDTH, n_total), jnp.float32, 0.2, 1.0)
    wts_x = jax.random.uniform(sub_keys[4], (KERNEL_WIDTH, n_total), jnp.float32, 0.2, 1.0)
    coil_maps = jax.random.normal(sub_keys[5], (2, NUM_COILS, IMG_SIZE, IMG_SIZE), jnp.float32) / math.sqrt(2.0 * NUM_COILS)
    shared_key = jax.random.key(seed + 99)
    deapod = jax.random.uniform(shared_key, (IMG_SIZE,), jnp.float32, 0.6, 1.4)
    return {'kspace': kspace, 'wts_y': wts_y, 'wts_x': wts_x, 'idx_y': idx_y, 'idx_x': idx_x, 'coil_maps': coil_maps, 'deapod': deapod}


def dft_matrix():
    grid_size = 2 * IMG_SIZE
    freq_idx = jnp.arange(grid_size) - grid_size // 2
    pos_idx = jnp.arange(IMG_SIZE) - IMG_SIZE // 2
    phase_int = (freq_idx[:, None] * pos_idx[None, :]) % grid_size
    phase_ang = phase_int.astype(jnp.float32) * (2.0 * math.pi / grid_size)
    dft_norm = 1.0 / math.sqrt(grid_size)
    cos_t = jnp.cos(phase_ang) * dft_norm
    sin_t = jnp.sin(phase_ang) * dft_norm
    upper_half = jnp.stack([cos_t, sin_t], axis=1)
    lower_half = jnp.stack([-sin_t, cos_t], axis=1)
    return jnp.stack([upper_half, lower_half], axis=0).astype(jnp.bfloat16)


def grid_spread(kspace, wts_y, wts_x, idx_y, idx_x):
    grid_size = 2 * IMG_SIZE
    half_w = KERNEL_WIDTH // 2
    tap_ids = jnp.arange(KERNEL_WIDTH)
    tap_pairs = (jnp.repeat(tap_ids, KERNEL_WIDTH), jnp.tile(tap_ids, KERNEL_WIDTH))

    def add_tap(k_grid, tap_pair):
        tap_a, tap_b = tap_pair
        rows_at = (idx_y + tap_a - half_w) % grid_size
        cols_at = (idx_x + tap_b - half_w) % grid_size
        weight = wts_y[tap_a] * wts_x[tap_b]
        return k_grid.at[:, :, rows_at, cols_at].add(kspace * weight), None

    start_grid = jnp.zeros((2, NUM_COILS, grid_size, grid_size), jnp.float32)
    k_grid, _ = lax.scan(add_tap, start_grid, tap_pairs)
    return k_grid


def reference(kspace, wts_y, wts_x, idx_y, idx_x, coil_maps, deapod):
    k_grid = grid_spread(kspace, wts_y, wts_x, idx_y, idx_x).astype(jnp.bfloat16)
    dft_mat = dft_matrix().astype(jnp.float32)
    half_img = jnp.einsum('scuv,svtq->tcuq', k_grid.astype(jnp.float32), dft_mat).astype(jnp.bfloat16)
    coil_img = jnp.einsum('tcuq,tuop->ocpq', half_img.astype(jnp.float32), dft_mat)
    out_re = jnp.sum(coil_maps[0] * coil_img[0] + coil_maps[1] * coil_img[1], axis=0)
    out_im = jnp.sum(coil_maps[0] * coil_img[1] - coil_maps[1] * coil_img[0], axis=0)
    apod_2d = deapod[:, None] * deapod[None, :]
    return jnp.stack([out_re, out_im]) * apod_2d
```

```python
import functools
import math

import jax
import jax.numpy as jnp
import numpy as np
from jax import lax
from jax.experimental import pallas as pl
from jax.experimental.pallas import tpu as pltpu
from jax.sharding import PartitionSpec as P

BF = jnp.bfloat16
F32 = jnp.float32
VMEM = pltpu.VMEM
LANES = 128
SUB, WIN, QTR, HALF = 8, 16, 32, 64
N_GRID, N_IMG, N_COILS, KW = 640, 320, 8, 6
ROWS, COLS = 4, 2
RB, CB, QB = N_GRID // ROWS, N_GRID // COLS, N_IMG // ROWS
PB = N_IMG // COLS
NS = 4096
NB = NS // LANES
NG = 21
CW = CB + WIN
T = 6
PS = 9
ORDER = (1, 2, 3, 0, 4)
GROUPS = ((0, 96), (96, 64))
MESH_ID = pl.DeviceIdType.MESH


def dft_parts():
    freq = np.arange(N_GRID) - N_GRID // 2
    pos = np.arange(N_IMG) - N_IMG // 2
    ang = ((freq[:, None] * pos[None, :]) % N_GRID).astype(np.float32) * np.float32(2.0 * math.pi / N_GRID)
    norm = np.float32(1.0 / math.sqrt(N_GRID))
    c, s = np.cos(ang) * norm, np.sin(ang) * norm
    return np.stack([np.stack([c, s], 1), np.stack([-s, c], 1)], 0)


def col_dft():
    e = dft_parts()
    out = np.zeros((2 * N_GRID, N_GRID), np.float32)
    for dp in range(2):
        for t in range(2):
            for h in range(2):
                q0 = QB * (2 * dp + h)
                l0 = LANES * (2 * dp + t) + HALF * h
                out[:, l0:l0 + HALF] = e[:, :, t, q0:q0 + HALF].reshape(2 * N_GRID, HALF)
    for t in range(2):
        for d in range(4):
            l0 = 4 * LANES + HALF * t + WIN * d
            out[:, l0:l0 + WIN] = e[:, :, t, QB * d + HALF:QB * d + 80].reshape(2 * N_GRID, WIN)
    return jnp.asarray(out, BF)


def row_dft():
    e = dft_parts()
    rows = np.concatenate([np.arange(QTR * l, QTR * l + QTR) for l in ORDER])
    parts = []
    for start, n in GROUPS:
        for t in range(2):
            for b in range(ROWS):
                u = b * RB + rows[start:start + n]
                parts.append(e[t, u].reshape(n, 2 * N_IMG))
    return jnp.asarray(np.concatenate(parts, 0).T, BF)


def unmix():
    m = np.zeros((256, 256), np.float32)
    for ch in range(SUB):
        for pp in range(2):
            for i in range(WIN):
                m[ch * QTR + WIN * pp + (i + SUB) % WIN, pp * 128 + i * SUB + ch] = 1.0
    return jnp.asarray(m, BF)


def prep_kernel(ks_ref, wy_ref, wx_ref, iy_ref, ix_ref, own_ref, far_ref, base_ref):
    k = lax.axis_index('cols')
    r = lax.axis_index('rows')
    iy = iy_ref[...]
    base_ref[...] = ((iy - r * RB + 5) >> 3) * CW + (ix_ref[...] - k * CB + 5)
    sh = ((iy + 5) & 15).astype(F32)
    lo = jnp.concatenate([ks_ref[0, 0:4, :], ks_ref[1, 0:4, :]], axis=0)
    hi = jnp.concatenate([ks_ref[0, 4:SUB, :], ks_ref[1, 4:SUB, :]], axis=0)
    own_ref[0:SUB, :] = jnp.where(k == 0, lo, hi)
    far_ref[0:SUB, :] = jnp.where(k == 0, hi, lo)
    zero2 = jnp.zeros((2, NS), F32)
    for ref in (own_ref, far_ref):
        ref[SUB:WIN, :] = jnp.concatenate([wx_ref[...], zero2], axis=0)
        ref[WIN:24, :] = jnp.concatenate([wy_ref[...], zero2], axis=0)
        for b in range(NB):
            ref[22:23, LANES * b:LANES * (b + 1)] = sh[b:b + 1, :]


def split3(x):
    hi = x.astype(BF).astype(F32)
    r = x - hi
    mid = r.astype(BF).astype(F32)
    return hi, mid, r - mid


def accumulate(base_ref, pay_ref, accs, us, xs, vs, r_ref):
    row_i = lax.broadcasted_iota(jnp.int32, (WIN, LANES), 0)

    def make_u(blk, k):
        off = pl.multiple_of(jnp.minimum(blk, NB - 1) * LANES, LANES)
        y8 = pay_ref[0:SUB, pl.ds(off, LANES)]
        wyp = pay_ref[WIN:24, pl.ds(off, LANES)]
        d = (row_i - wyp[6:7, :].astype(jnp.int32)) & 15
        p = jnp.zeros((WIN, LANES), F32)
        for a in range(KW):
            p = jnp.where(d == a, wyp[a:a + 1, :], p)
        us[k][...] = jnp.concatenate([y8 * p[i:i + 1, :] for i in range(WIN)], axis=0).T
        x3 = list(split3(pay_ref[SUB:WIN, pl.ds(off, LANES)])) + [jnp.zeros((104, LANES), F32)]
        xs[k][...] = jnp.concatenate(x3, axis=0).T

    def make_v(k):
        lhs = xs[k][...].astype(BF)
        u = us[k][...]
        for bp in range(3):
            w = jnp.dot(lhs, r_ref[:, 256 * bp:256 * bp + 256], preferred_element_type=F32)
            for c in range(2):
                v = w[:, LANES * c:LANES * (c + 1)] * u
                for g in range(WIN):
                    vs[k][pl.ds(SUB * PS * g + 2 * bp + c, SUB, stride=PS), :] = v[SUB * g:SUB * g + SUB, :]

    def add_tiles(blk, k):
        for j in range(LANES):
            acc = accs[j % T]
            b = base_ref[blk, j]
            acc[pl.ds(b, SUB), :] = acc[pl.ds(b, SUB), :] + vs[k][PS * j:PS * j + SUB, :]

    def clear(n, _):
        for a in accs:
            a[pl.ds(pl.multiple_of(n * CW, SUB), CW), :] = jnp.zeros((CW, LANES), F32)
        return 0

    lax.fori_loop(0, NG, clear, 0)
    kk = lax.broadcasted_iota(jnp.int32, (LANES, 768), 0)
    ll = lax.broadcasted_iota(jnp.int32, (LANES, 768), 1)
    r_ref[...] = jnp.where((kk < 24) & ((kk & 7) == (ll >> 7)), 1.0, 0.0).astype(BF)
    for v in vs:
        v[...] = jnp.zeros_like(v)
    make_u(0, 0)
    make_u(1, 1)
    make_v(0)

    def body(n, _):
        k = 2 * n
        make_v(1)
        add_tiles(k, 0)
        make_u(k + 2, 0)
        make_v(0)
        add_tiles(k + 1, 1)
        make_u(k + 3, 1)
        return 0

    lax.fori_loop(0, NB // 2, body, 0)


def folded(accs, off, n):
    def total(g):
        o = pl.multiple_of(g * CW + off, SUB)
        s = accs[0][pl.ds(o, n), :]
        for a in accs[1:]:
            s = s + a[pl.ds(o, n), :]
        return s

    high = lax.broadcasted_iota(jnp.int32, (n, LANES), 1) >= HALF
    even = [total(2 * p) for p in range(11)]
    tiles = [total(2 * p + 1) + jnp.where(high, even[p], even[p + 1]) for p in range(10)]
    return tiles + [jnp.where(high, even[10], even[0])]


def own_kernel(base_ref, pay_ref, out_ref, *scr):
    accs, us, xs, vs, r_ref = scr[:T], scr[T:T + 2], scr[T + 2:T + 4], scr[T + 4:T + 6], scr[T + 6]
    accumulate(base_ref, pay_ref, accs, us, xs, vs, r_ref)

    def fold(q, _):
        off = pl.multiple_of(q * SUB, SUB)
        for p, t in enumerate(folded(accs, off, SUB)):
            out_ref[p, pl.ds(off, SUB), :] = t
        return 0

    lax.fori_loop(0, CW // SUB, fold, 0)


def far_kernel(base_ref, pay_ref, a_ref, tb_ref, edge_ref, pack_ref, *scr):
    accs, us, xs, vs, r_ref, gh_ref = scr[:T], scr[T:T + 2], scr[T + 2:T + 4], scr[T + 4:T + 6], scr[T + 6], scr[T + 7]
    accumulate(base_ref, pay_ref, accs, us, xs, vs, r_ref)
    k = lax.axis_index('cols')
    own0 = k * CB
    far0 = CB - own0
    high = lax.broadcasted_iota(jnp.int32, (SUB, LANES), 1) >= HALF

    left = folded(accs, 0, SUB)
    right = folded(accs, CW - SUB, SUB)
    for src, dst in ((CW - SUB, SUB), (0, CB)):
        for p in range(10):
            rows = pl.ds((2 * p + 1) * CW + dst, SUB)
            accs[0][rows, :] = accs[0][rows, :] + a_ref[p, src:src + SUB, :]
        ghost = a_ref[10, src:src + SUB, :]
        accs[0][dst:dst + SUB, :] = accs[0][dst:dst + SUB, :] + jnp.where(high, 0.0, ghost)
        rows = pl.ds(20 * CW + dst, SUB)
        accs[0][rows, :] = accs[0][rows, :] + jnp.where(high, ghost, 0.0)

    high16 = lax.broadcasted_iota(jnp.int32, (WIN, LANES), 1) >= HALF

    def put(v, tiles):
        v = pl.multiple_of(v, WIN)
        for p in range(10):
            tb_ref[p, pl.ds(v, WIN), :] = tiles[p].astype(BF)
        edge_ref[pl.ds(v, WIN), :] = jnp.where(high16, tiles[0], tiles[9])
        gh_ref[pl.ds(v, WIN), :] = tiles[10]

    def far_part(s, _):
        put(far0 + WIN * s, folded(accs, pl.multiple_of(SUB + WIN * s, SUB), WIN))
        return 0

    lax.fori_loop(0, CB // WIN, far_part, 0)

    def own_part(s, _):
        put(own0 + WIN * s, [a_ref[p, pl.ds(pl.multiple_of(SUB + WIN * s, SUB), WIN), :] for p in range(11)])
        return 0

    lax.fori_loop(1, CB // WIN - 1, own_part, 0)
    put(own0, [jnp.concatenate([a_ref[p, SUB:WIN, :] + right[p], a_ref[p, WIN:24, :]], axis=0) for p in range(11)])
    put(own0 + CB - WIN, [jnp.concatenate([a_ref[p, CB - SUB:CB, :], a_ref[p, CB:CB + SUB, :] + left[p]], axis=0) for p in range(11)])

    slot = lax.broadcasted_iota(jnp.int32, (RB, LANES), 1) >> 5
    for side, lane0 in ((0, QTR), (1, HALF)):
        out = jnp.zeros((RB, LANES), F32)
        for j in range(4):
            piece = pltpu.roll(gh_ref[RB * j:RB * (j + 1), :], (QTR * j - lane0) % LANES, axis=1)
            out = jnp.where(slot == j, piece, out)
        pack_ref[side] = out


def image_kernel(tb_ref, edge_ref, pack_ref, s_ref, dd_ref, ev_hbm, eu_hbm, pm_ref, out_ref,
                 ev_ref, eu_ref, g_ref, halo, send_m, send_r, hm1, hm2, hr1, hr2, acc_m, acc_r, s_main, s_rem,
                 img_m, img_r, red_m, red_r,
                 load_sem, halo_ss, halo_rs, main_ss, main_rs, rem_ss, rem_rs, red_ss, red_rs):
    k = lax.axis_index('cols')
    r = lax.axis_index('rows')
    core = r % 2
    peers = (r + 1 - 2 * core, (r + 2) % 4, 3 - r)
    prev, nxt = (r + 3) % 4, (r + 1) % 4
    load_ev = pltpu.make_async_copy(ev_hbm, ev_ref, load_sem.at[0])
    load_eu = pltpu.make_async_copy(eu_hbm, eu_ref, load_sem.at[1])
    load_ev.start()
    load_eu.start()

    barrier = pltpu.get_barrier_semaphore()
    for d in peers:
        pl.semaphore_signal(barrier, inc=1, device_id={'rows': d}, device_id_type=MESH_ID)
    pl.semaphore_signal(barrier, inc=1, device_id={'cols': 1 - k}, device_id_type=MESH_ID)
    pl.semaphore_wait(barrier, 4)

    halos = []
    for side, dev in ((0, prev), (1, nxt)):
        cp = pltpu.make_async_remote_copy(src_ref=pack_ref.at[side], dst_ref=halo.at[side], send_sem=halo_ss.at[side],
                                          recv_sem=halo_rs.at[side], device_id={'rows': dev}, device_id_type=MESH_ID)
        cp.start()
        halos.append(cp)

    def to_rows(pos, t0, t1):
        a = jnp.concatenate([t0, t1], axis=1)
        g = lax.dot_general(pm_ref[...], a, (((1,), (1,)), ((), ())), preferred_element_type=F32).astype(BF)
        for ch in range(SUB):
            s, c = ch // 4, ch % 4
            g_ref[RB * c + QTR * pos:RB * c + QTR * pos + QTR, N_GRID * s:N_GRID * (s + 1)] = g[QTR * ch:QTR * ch + QTR, :]

    for pos in range(3):
        l = ORDER[pos]
        to_rows(pos, tb_ref[2 * l], tb_ref[2 * l + 1])
    load_ev.wait()

    hms, hrs = (hm1, hm2), (hr1, hr2)
    copies = {}

    def columns(grp):
        start, n = GROUPS[grp]
        lane = lax.broadcasted_iota(jnp.int32, (n, LANES), 1)
        low = lane < HALF
        block = (lane & 63) >> 4
        rems = []
        for cp in range(2):
            hs = []
            for c in (2 * cp, 2 * cp + 1):
                h = jnp.dot(g_ref[RB * c + start:RB * c + start + n, :], ev_ref[...], preferred_element_type=F32)
                hs.append([h[:, LANES * i:LANES * (i + 1)] for i in range(4)])
                rems.append(h[:, 4 * LANES:])
            for i in range(4):
                dp, t = i // 2, i % 2
                odd = pltpu.roll(hs[1][i], HALF, axis=1)
                send_m[2 * dp, cp, t, start:start + n, :] = jnp.where(low, hs[0][i], odd).astype(BF)
                send_m[2 * dp + 1, cp, t, start:start + n, :] = jnp.where(low, odd, hs[0][i]).astype(BF)
            for x in (1, 2, 0):
                i = 3 * (2 * grp + cp) + x
                rc = pltpu.make_async_remote_copy(
                    src_ref=send_m.at[peers[x], cp, :, pl.ds(start, n), :], dst_ref=hms[grp].at[cp, :, r],
                    send_sem=main_ss.at[i], recv_sem=main_rs.at[i], device_id={'rows': peers[x]}, device_id_type=MESH_ID)
                rc.start()
                copies['m', grp, cp, x] = rc
            hms[grp][cp, :, r] = send_m[r, cp, :, start:start + n, :]
        for d in range(4):
            out = jnp.zeros((n, LANES), F32)
            for c in range(4):
                piece = rems[c] if c == d else pltpu.roll(rems[c], (WIN * (c - d)) % LANES, axis=1)
                out = jnp.where(block == c, piece, out)
            send_r[d, start:start + n, :] = out.astype(BF)
        for x in (1, 2, 0):
            i = 3 * grp + x
            rc = pltpu.make_async_remote_copy(
                src_ref=send_r.at[peers[x], pl.ds(start, n), :], dst_ref=hrs[grp].at[r],
                send_sem=rem_ss.at[i], recv_sem=rem_rs.at[i], device_id={'rows': peers[x]}, device_id_type=MESH_ID)
            rc.start()
            copies['r', grp, x] = rc
        hrs[grp][r] = send_r[r, start:start + n, :]

    columns(0)

    for h in halos:
        h.wait()
    lane = lax.broadcasted_iota(jnp.int32, (RB, LANES), 1)
    high = lane >= HALF
    slot = lane >> 5
    t0s, t9s = [], []
    for j in range(4):
        rows = slice(RB * j, RB * (j + 1))
        add_first = pltpu.roll(halo[1], (HALF - QTR * j) % LANES, axis=1)
        add_last = pltpu.roll(halo[0], (QTR - QTR * j) % LANES, axis=1)
        e = edge_ref[rows, :] + jnp.where(slot == 2, add_first, jnp.where(slot == 1, add_last, 0.0))
        t0s.append(jnp.where(high, e, tb_ref[0, rows, :].astype(F32)).astype(BF))
        t9s.append(jnp.where(high, tb_ref[9, rows, :].astype(F32), e).astype(BF))
    to_rows(3, jnp.concatenate(t0s, axis=0), tb_ref[1])
    to_rows(4, tb_ref[SUB], jnp.concatenate(t9s, axis=0))
    columns(1)

    lane = lax.broadcasted_iota(jnp.int32, (N_IMG, LANES), 1)
    pad = jnp.zeros((N_IMG, LANES - QB), F32)
    for s in range(2):
        wide = [jnp.concatenate([s_ref[s, c], pad], axis=1) for c in range(4)]
        for cp in range(2):
            first = jnp.where(core == 0, wide[2 * cp], wide[2 * cp + 1])
            second = jnp.where(core == 0, wide[2 * cp + 1], wide[2 * cp])
            s_main[s, cp] = jnp.where(lane < HALF, first, pltpu.roll(second, HALF, axis=1))
        out = jnp.zeros((N_IMG, LANES), F32)
        for c in range(4):
            out = jnp.where((lane >> 4) == c, pltpu.roll(wide[c], (WIN * c - HALF) % LANES, axis=1), out)
        s_rem[s] = out
    load_eu.wait()

    k0 = (0, 2 * ROWS * 96)

    def rows_main(grp):
        n = GROUPS[grp][1]
        for cp in range(2):
            for x in range(3):
                copies['m', grp, cp, x].wait_recv()
        kk = 2 * ROWS * n
        rhs = jnp.concatenate([hms[grp][cp].reshape(kk, LANES) for cp in range(2)], axis=1)
        res = jnp.dot(eu_ref[:, k0[grp]:k0[grp] + kk], rhs, preferred_element_type=F32)
        return res

    def rows_rem(grp):
        n = GROUPS[grp][1]
        for x in range(3):
            copies['r', grp, x].wait_recv()
        kk = ROWS * n
        rhs = hrs[grp][...].reshape(kk, LANES)
        return [jnp.dot(eu_ref[:, k0[grp] + kk * t:k0[grp] + kk * (t + 1)], rhs, preferred_element_type=F32) for t in range(2)]

    acc_m[...] = rows_main(0)
    for t, v in enumerate(rows_rem(0)):
        acc_r[t] = v
    acc_m[...] = acc_m[...] + rows_main(1)

    low = lax.broadcasted_iota(jnp.int32, (PB, LANES), 1) < HALF

    def combine_main(p0):
        rows = pl.ds(pl.multiple_of(p0, SUB), PB)
        rows_im = pl.ds(pl.multiple_of(N_IMG + p0, SUB), PB)
        re = jnp.zeros((PB, LANES), F32)
        im = jnp.zeros((PB, LANES), F32)
        for cp in range(2):
            cols = slice(LANES * cp, LANES * (cp + 1))
            i_re, i_im = acc_m[rows, cols], acc_m[rows_im, cols]
            s_re, s_im = s_main[0, cp, rows, :], s_main[1, cp, rows, :]
            re = re + (s_re * i_re + s_im * i_im)
            im = im + (s_re * i_im - s_im * i_re)
        return jnp.where(low, re + pltpu.roll(re, HALF, axis=1), im + pltpu.roll(im, HALF, axis=1))

    lane = lax.broadcasted_iota(jnp.int32, (PB, LANES), 1)
    slot40 = lax.broadcasted_iota(jnp.int32, (PB // 4, LANES), 1) >> 5

    def combine_rem(p0):
        rows = pl.ds(pl.multiple_of(p0, SUB), PB)
        rows_im = pl.ds(pl.multiple_of(N_IMG + p0, SUB), PB)
        i_re = acc_r[0, rows, :] + pltpu.roll(acc_r[1, rows, :], HALF, axis=1)
        i_im = acc_r[0, rows_im, :] + pltpu.roll(acc_r[1, rows_im, :], HALF, axis=1)
        s_re, s_im = s_rem[0, rows, :], s_rem[1, rows, :]
        re = jnp.where(low, s_re * i_re + s_im * i_im, 0.0)
        im = jnp.where(low, s_re * i_im - s_im * i_re, 0.0)
        w = re + pltpu.roll(im, HALF, axis=1)
        w = w + pltpu.roll(w, LANES - QTR, axis=1)
        w = w + pltpu.roll(w, LANES - WIN, axis=1)
        w = jnp.where(lane < WIN, w, pltpu.roll(w, LANES - 48, axis=1))
        out = jnp.zeros((PB // 4, LANES), F32)
        for j in range(4):
            piece = w[PB // 4 * j:PB // 4 * (j + 1), :]
            out = jnp.where(slot40 == j, pltpu.roll(piece, QTR * j, axis=1) if j else piece, out)
        return out

    far_p, own_p = PB - k * PB, k * PB

    def reduce_copy(src, dst, i):
        return pltpu.make_async_remote_copy(src_ref=src, dst_ref=dst, send_sem=red_ss.at[i], recv_sem=red_rs.at[i],
                                            device_id={'cols': 1 - k}, device_id_type=MESH_ID)

    img_m[...] = combine_main(far_p)
    red_main = reduce_copy(img_m, red_m, 0)
    red_main.start()
    for t, v in enumerate(rows_rem(1)):
        acc_r[t] = acc_r[t] + v
    img_r[...] = combine_rem(far_p)
    red_rem = reduce_copy(img_r, red_r, 1)
    red_rem.start()
    own_main = combine_main(own_p)
    own_rem = combine_rem(own_p)
    red_main.wait_recv()
    main = own_main + red_m[...]
    red_rem.wait_recv()
    rem = own_rem + red_r[...]
    for o in range(2):
        m = main if o == 0 else pltpu.roll(main, HALF, axis=1)
        for j in range(4):
            rows = slice(PB // 4 * j, PB // 4 * (j + 1))
            piece = pltpu.roll(rem, (HALF - QTR * j - WIN * o) % LANES, axis=1)
            full = jnp.where(low[rows], m[rows], piece)
            out_ref[o, rows, :] = full[:, :QB] * dd_ref[rows, :]

    red_main.wait_send()
    red_rem.wait_send()
    for key in copies:
        copies[key].wait_send()


def solution(mesh):
    sample_spec = ('exam', 'rows', 'cols')
    vm = pl.BlockSpec(memory_space=pltpu.VMEM)
    sm = pl.BlockSpec(memory_space=pltpu.SMEM)
    anyspec = pl.BlockSpec(memory_space=pl.ANY)
    spread_scratch = ([VMEM((NG * CW, LANES), F32)] * T + [VMEM((LANES, LANES), F32)] * 4 + [VMEM((LANES * PS, LANES), F32)] * 2
                      + [VMEM((LANES, 768), BF)])
    big = 60 * 1024 * 1024

    def local_fn(kspace, wts_y, wts_x, idx_y, idx_x, coil_maps, deapod):
        k = lax.axis_index('cols')
        r = lax.axis_index('rows')
        own, far, base = pl.pallas_call(
            prep_kernel,
            out_shape=(jax.ShapeDtypeStruct((24, NS), F32), jax.ShapeDtypeStruct((24, NS), F32), jax.ShapeDtypeStruct((NB, LANES), jnp.int32)),
            in_specs=[vm] * 5, out_specs=(vm, vm, vm), name='prep',
        )(kspace, wts_y, wts_x, idx_y.reshape(NB, LANES), idx_x.reshape(NB, LANES))
        swap = [(0, 1), (1, 0)]
        far_in = lax.ppermute(far, 'cols', swap)
        base_in = lax.ppermute(base, 'cols', swap)
        half = pl.pallas_call(
            own_kernel, out_shape=jax.ShapeDtypeStruct((11, CW, LANES), F32), in_specs=[sm, vm], out_specs=vm,
            scratch_shapes=spread_scratch, compiler_params=pltpu.CompilerParams(vmem_limit_bytes=big), name='spread_own',
            cost_estimate=pl.CostEstimate(flops=4 * 10 ** 9, bytes_accessed=2 * 10 ** 6, transcendentals=0),
        )(base, own)
        tb, edge, pack = pl.pallas_call(
            far_kernel,
            out_shape=(jax.ShapeDtypeStruct((10, N_GRID, LANES), BF), jax.ShapeDtypeStruct((N_GRID, LANES), F32), jax.ShapeDtypeStruct((2, RB, LANES), F32)),
            in_specs=[sm, vm, vm], out_specs=(vm, vm, vm), scratch_shapes=spread_scratch + [VMEM((N_GRID, LANES), F32)],
            compiler_params=pltpu.CompilerParams(vmem_limit_bytes=big), name='spread_far',
            cost_estimate=pl.CostEstimate(flops=4 * 10 ** 9, bytes_accessed=4 * 10 ** 6, transcendentals=0),
        )(base_in, far_in, half)
        dd = lax.dynamic_slice(deapod, (k * PB,), (PB,))[:, None] * lax.dynamic_slice(deapod, (r * QB,), (QB,))[None, :]
        dma = pltpu.SemaphoreType.DMA
        return pl.pallas_call(
            image_kernel,
            out_shape=jax.ShapeDtypeStruct((2, PB, QB), F32),
            in_specs=[vm] * 5 + [anyspec] * 2 + [vm], out_specs=vm,
            scratch_shapes=[
                VMEM((2 * N_GRID, N_GRID), BF), VMEM((2 * N_IMG, 2 * N_GRID), BF), VMEM((4 * RB, 2 * N_GRID), BF), VMEM((2, RB, LANES), F32),
                VMEM((4, 2, 2, RB, LANES), BF), VMEM((4, RB, LANES), BF),
                VMEM((2, 2, ROWS, 96, LANES), BF), VMEM((2, 2, ROWS, HALF, LANES), BF), VMEM((ROWS, 96, LANES), BF), VMEM((ROWS, HALF, LANES), BF),
                VMEM((2 * N_IMG, 2 * LANES), F32), VMEM((2, 2 * N_IMG, LANES), F32), VMEM((2, 2, N_IMG, LANES), F32), VMEM((2, N_IMG, LANES), F32),
                VMEM((PB, LANES), F32), VMEM((PB // 4, LANES), F32), VMEM((PB, LANES), F32), VMEM((PB // 4, LANES), F32),
                dma((2,)), dma((2,)), dma((2,)), dma((12,)), dma((12,)), dma((6,)), dma((6,)), dma((2,)), dma((2,)),
            ],
            compiler_params=pltpu.CompilerParams(vmem_limit_bytes=40 * 1024 * 1024, collective_id=0, has_side_effects=True), name='image',
        )(tb, edge, pack, coil_maps, dd, col_dft(), row_dft(), unmix())

    return jax.shard_map(
        local_fn,
        mesh=mesh,
        in_specs=(P(None, None, sample_spec), P(None, sample_spec), P(None, sample_spec), P(sample_spec), P(sample_spec), P(None, ('exam', 'cols'), None, 'rows'), P()),
        out_specs=P(None, ('exam', 'cols'), 'rows'),
        check_vma=False,
    )
```

```python
import functools
import math

import jax
import jax.numpy as jnp
import numpy as np
from jax import lax
from jax.experimental import pallas as pl
from jax.experimental.pallas import tpu as pltpu
from jax.sharding import PartitionSpec as P

BF = jnp.bfloat16
F32 = jnp.float32
VMEM = pltpu.VMEM
LANES = 128
SUB, WIN, QTR, HALF = 8, 16, 32, 64
N_GRID, N_IMG, N_COILS, KW = 640, 320, 8, 6
ROWS, COLS = 4, 2
RB, CB, QB = N_GRID // ROWS, N_GRID // COLS, N_IMG // ROWS
PB = N_IMG // COLS
NS = 4096
NB = NS // LANES
NG = 21
CW = CB + WIN
T = 6
PS = 9
ORDER = (1, 2, 3, 0, 4)
GROUPS = ((0, 96), (96, 64))
MESH_ID = pl.DeviceIdType.MESH


def dft_parts():
    freq = np.arange(N_GRID) - N_GRID // 2
    pos = np.arange(N_IMG) - N_IMG // 2
    ang = ((freq[:, None] * pos[None, :]) % N_GRID).astype(np.float32) * np.float32(2.0 * math.pi / N_GRID)
    norm = np.float32(1.0 / math.sqrt(N_GRID))
    c, s = np.cos(ang) * norm, np.sin(ang) * norm
    return np.stack([np.stack([c, s], 1), np.stack([-s, c], 1)], 0)


def col_dft():
    e = dft_parts()
    out = np.zeros((2 * N_GRID, N_GRID), np.float32)
    for dp in range(2):
        for t in range(2):
            for h in range(2):
                q0 = QB * (2 * dp + h)
                l0 = LANES * (2 * dp + t) + HALF * h
                out[:, l0:l0 + HALF] = e[:, :, t, q0:q0 + HALF].reshape(2 * N_GRID, HALF)
    for t in range(2):
        for d in range(4):
            l0 = 4 * LANES + HALF * t + WIN * d
            out[:, l0:l0 + WIN] = e[:, :, t, QB * d + HALF:QB * d + 80].reshape(2 * N_GRID, WIN)
    return jnp.asarray(out, BF)


def row_dft():
    e = dft_parts()
    rows = np.concatenate([np.arange(QTR * l, QTR * l + QTR) for l in ORDER])
    parts = []
    for start, n in GROUPS:
        for t in range(2):
            for b in range(ROWS):
                u = b * RB + rows[start:start + n]
                parts.append(e[t, u].reshape(n, 2 * N_IMG))
    return jnp.asarray(np.concatenate(parts, 0).T, BF)


def unmix():
    m = np.zeros((256, 256), np.float32)
    for ch in range(SUB):
        for pp in range(2):
            for i in range(WIN):
                m[ch * QTR + WIN * pp + (i + SUB) % WIN, pp * 128 + i * SUB + ch] = 1.0
    return jnp.asarray(m, BF)


def prep_kernel(ks_hbm, wy_hbm, wx_hbm, iy_hbm, ix_hbm, own_ref, far_ref, base_ref, ks_ref, wy_ref, wx_ref, iy_ref, ix_ref, sem):
    k = lax.axis_index('cols')
    r = lax.axis_index('rows')
    loads = []
    for src, dst in ((iy_hbm, iy_ref), (ix_hbm, ix_ref), (wx_hbm, wx_ref), (wy_hbm, wy_ref), (ks_hbm, ks_ref)):
        cp = pltpu.make_async_copy(src, dst, sem.at[len(loads)])
        cp.start()
        loads.append(cp)
    loads[0].wait()
    loads[1].wait()
    iy = iy_ref[...]
    base_ref[...] = ((iy - r * RB + 5) >> 3) * CW + (ix_ref[...] - k * CB + 5)
    sh = ((iy + 5) & 15).astype(F32)
    loads[2].wait()
    loads[3].wait()
    zero2 = jnp.zeros((2, NS), F32)
    for ref in (own_ref, far_ref):
        ref[SUB:WIN, :] = jnp.concatenate([wx_ref[...], zero2], axis=0)
        ref[WIN:24, :] = jnp.concatenate([wy_ref[...], zero2], axis=0)
        for b in range(NB):
            ref[22:23, LANES * b:LANES * (b + 1)] = sh[b:b + 1, :]
    loads[4].wait()
    lo = jnp.concatenate([ks_ref[0, 0:4, :], ks_ref[1, 0:4, :]], axis=0)
    hi = jnp.concatenate([ks_ref[0, 4:SUB, :], ks_ref[1, 4:SUB, :]], axis=0)
    own_ref[0:SUB, :] = jnp.where(k == 0, lo, hi)
    far_ref[0:SUB, :] = jnp.where(k == 0, hi, lo)


def split3(x):
    hi = x.astype(BF).astype(F32)
    r = x - hi
    mid = r.astype(BF).astype(F32)
    return hi, mid, r - mid


def accumulate(base_ref, pay_ref, accs, us, xs, vs, r_ref):
    row_i = lax.broadcasted_iota(jnp.int32, (WIN, LANES), 0)

    def make_u(blk, k):
        off = pl.multiple_of(jnp.minimum(blk, NB - 1) * LANES, LANES)
        y8 = pay_ref[0:SUB, pl.ds(off, LANES)]
        wyp = pay_ref[WIN:24, pl.ds(off, LANES)]
        d = (row_i - wyp[6:7, :].astype(jnp.int32)) & 15
        p = jnp.zeros((WIN, LANES), F32)
        for a in range(KW):
            p = jnp.where(d == a, wyp[a:a + 1, :], p)
        us[k][...] = jnp.concatenate([y8 * p[i:i + 1, :] for i in range(WIN)], axis=0).T
        x3 = list(split3(pay_ref[SUB:WIN, pl.ds(off, LANES)])) + [jnp.zeros((104, LANES), F32)]
        xs[k][...] = jnp.concatenate(x3, axis=0).T

    def make_v(k):
        lhs = xs[k][...].astype(BF)
        u = us[k][...]
        for bp in range(3):
            w = jnp.dot(lhs, r_ref[:, 256 * bp:256 * bp + 256], preferred_element_type=F32)
            for c in range(2):
                v = w[:, LANES * c:LANES * (c + 1)] * u
                for g in range(WIN):
                    vs[k][pl.ds(SUB * PS * g + 2 * bp + c, SUB, stride=PS), :] = v[SUB * g:SUB * g + SUB, :]

    def add_tiles(blk, k):
        for j in range(LANES):
            acc = accs[j % T]
            b = base_ref[blk, j]
            acc[pl.ds(b, SUB), :] = acc[pl.ds(b, SUB), :] + vs[k][PS * j:PS * j + SUB, :]

    def clear(n, _):
        for a in accs:
            a[pl.ds(pl.multiple_of(n * CW, SUB), CW), :] = jnp.zeros((CW, LANES), F32)
        return 0

    lax.fori_loop(0, NG, clear, 0)
    kk = lax.broadcasted_iota(jnp.int32, (LANES, 768), 0)
    ll = lax.broadcasted_iota(jnp.int32, (LANES, 768), 1)
    r_ref[...] = jnp.where((kk < 24) & ((kk & 7) == (ll >> 7)), 1.0, 0.0).astype(BF)
    for v in vs:
        v[...] = jnp.zeros_like(v)
    make_u(0, 0)
    make_u(1, 1)
    make_v(0)

    def body(n, _):
        k = 2 * n
        make_v(1)
        add_tiles(k, 0)
        make_u(k + 2, 0)
        make_v(0)
        add_tiles(k + 1, 1)
        make_u(k + 3, 1)
        return 0

    lax.fori_loop(0, NB // 2, body, 0)


def folded(accs, off, n):
    def total(g):
        o = pl.multiple_of(g * CW + off, SUB)
        s = accs[0][pl.ds(o, n), :]
        for a in accs[1:]:
            s = s + a[pl.ds(o, n), :]
        return s

    high = lax.broadcasted_iota(jnp.int32, (n, LANES), 1) >= HALF
    even = [total(2 * p) for p in range(11)]
    tiles = [total(2 * p + 1) + jnp.where(high, even[p], even[p + 1]) for p in range(10)]
    return tiles + [jnp.where(high, even[10], even[0])]


def own_kernel(base_ref, pay_ref, out_ref, *scr):
    accs, us, xs, vs, r_ref = scr[:T], scr[T:T + 2], scr[T + 2:T + 4], scr[T + 4:T + 6], scr[T + 6]
    accumulate(base_ref, pay_ref, accs, us, xs, vs, r_ref)

    def fold(q, _):
        off = pl.multiple_of(q * SUB, SUB)
        for p, t in enumerate(folded(accs, off, SUB)):
            out_ref[p, pl.ds(off, SUB), :] = t
        return 0

    lax.fori_loop(0, CW // SUB, fold, 0)


def far_kernel(base_ref, pay_ref, a_ref, tb_ref, edge_ref, pack_ref, *scr):
    accs, us, xs, vs, r_ref, gh_ref = scr[:T], scr[T:T + 2], scr[T + 2:T + 4], scr[T + 4:T + 6], scr[T + 6], scr[T + 7]
    accumulate(base_ref, pay_ref, accs, us, xs, vs, r_ref)
    k = lax.axis_index('cols')
    own0 = k * CB
    far0 = CB - own0
    high = lax.broadcasted_iota(jnp.int32, (SUB, LANES), 1) >= HALF

    left = folded(accs, 0, SUB)
    right = folded(accs, CW - SUB, SUB)
    for src, dst in ((CW - SUB, SUB), (0, CB)):
        for p in range(10):
            rows = pl.ds((2 * p + 1) * CW + dst, SUB)
            accs[0][rows, :] = accs[0][rows, :] + a_ref[p, src:src + SUB, :]
        ghost = a_ref[10, src:src + SUB, :]
        accs[0][dst:dst + SUB, :] = accs[0][dst:dst + SUB, :] + jnp.where(high, 0.0, ghost)
        rows = pl.ds(20 * CW + dst, SUB)
        accs[0][rows, :] = accs[0][rows, :] + jnp.where(high, ghost, 0.0)

    high16 = lax.broadcasted_iota(jnp.int32, (WIN, LANES), 1) >= HALF

    def put(v, tiles):
        v = pl.multiple_of(v, WIN)
        for p in range(10):
            tb_ref[p, pl.ds(v, WIN), :] = tiles[p].astype(BF)
        edge_ref[pl.ds(v, WIN), :] = jnp.where(high16, tiles[0], tiles[9])
        gh_ref[pl.ds(v, WIN), :] = tiles[10]

    def far_part(s, _):
        put(far0 + WIN * s, folded(accs, pl.multiple_of(SUB + WIN * s, SUB), WIN))
        return 0

    lax.fori_loop(0, CB // WIN, far_part, 0)

    def own_part(s, _):
        put(own0 + WIN * s, [a_ref[p, pl.ds(pl.multiple_of(SUB + WIN * s, SUB), WIN), :] for p in range(11)])
        return 0

    lax.fori_loop(1, CB // WIN - 1, own_part, 0)
    put(own0, [jnp.concatenate([a_ref[p, SUB:WIN, :] + right[p], a_ref[p, WIN:24, :]], axis=0) for p in range(11)])
    put(own0 + CB - WIN, [jnp.concatenate([a_ref[p, CB - SUB:CB, :], a_ref[p, CB:CB + SUB, :] + left[p]], axis=0) for p in range(11)])

    slot = lax.broadcasted_iota(jnp.int32, (RB, LANES), 1) >> 5
    for side, lane0 in ((0, QTR), (1, HALF)):
        out = jnp.zeros((RB, LANES), F32)
        for j in range(4):
            piece = pltpu.roll(gh_ref[RB * j:RB * (j + 1), :], (QTR * j - lane0) % LANES, axis=1)
            out = jnp.where(slot == j, piece, out)
        pack_ref[side] = out


def image_kernel(tb_ref, edge_ref, pack_ref, s_ref, d_ref, ev_ref, eu_ref, pm_ref, out_ref,
                 g_ref, halo, send_m, send_r, hm1, hm2, hr1, hr2, acc_m, acc_r, s_main, s_rem,
                 img_m, img_r, red_m, red_r,
                 halo_ss, halo_rs, main_ss, main_rs, rem_ss, rem_rs, red_ss, red_rs):
    k = lax.axis_index('cols')
    r = lax.axis_index('rows')
    core = r % 2
    peers = (r + 1 - 2 * core, (r + 2) % 4, 3 - r)
    prev, nxt = (r + 3) % 4, (r + 1) % 4

    barrier = pltpu.get_barrier_semaphore()
    for d in peers:
        pl.semaphore_signal(barrier, inc=1, device_id={'rows': d}, device_id_type=MESH_ID)
    pl.semaphore_signal(barrier, inc=1, device_id={'cols': 1 - k}, device_id_type=MESH_ID)
    pl.semaphore_wait(barrier, 4)

    halos = []
    for side, dev in ((0, prev), (1, nxt)):
        cp = pltpu.make_async_remote_copy(src_ref=pack_ref.at[side], dst_ref=halo.at[side], send_sem=halo_ss.at[side],
                                          recv_sem=halo_rs.at[side], device_id={'rows': dev}, device_id_type=MESH_ID)
        cp.start()
        halos.append(cp)

    def to_rows(pos, t0, t1):
        a = jnp.concatenate([t0, t1], axis=1)
        g = lax.dot_general(pm_ref[...], a, (((1,), (1,)), ((), ())), preferred_element_type=F32).astype(BF)
        for ch in range(SUB):
            s, c = ch // 4, ch % 4
            g_ref[RB * c + QTR * pos:RB * c + QTR * pos + QTR, N_GRID * s:N_GRID * (s + 1)] = g[QTR * ch:QTR * ch + QTR, :]

    for pos in range(3):
        l = ORDER[pos]
        to_rows(pos, tb_ref[2 * l], tb_ref[2 * l + 1])

    hms, hrs = (hm1, hm2), (hr1, hr2)
    copies = {}

    def columns(grp):
        start, n = GROUPS[grp]
        lane = lax.broadcasted_iota(jnp.int32, (n, LANES), 1)
        low = lane < HALF
        block = (lane & 63) >> 4
        rems = []
        for cp in range(2):
            hs = []
            for c in (2 * cp, 2 * cp + 1):
                h = jnp.dot(g_ref[RB * c + start:RB * c + start + n, :], ev_ref[...], preferred_element_type=F32)
                hs.append([h[:, LANES * i:LANES * (i + 1)] for i in range(4)])
                rems.append(h[:, 4 * LANES:])
            for i in range(4):
                dp, t = i // 2, i % 2
                odd = pltpu.roll(hs[1][i], HALF, axis=1)
                send_m[2 * dp, cp, t, start:start + n, :] = jnp.where(low, hs[0][i], odd).astype(BF)
                send_m[2 * dp + 1, cp, t, start:start + n, :] = jnp.where(low, odd, hs[0][i]).astype(BF)
            for x in (1, 2, 0):
                i = 3 * (2 * grp + cp) + x
                rc = pltpu.make_async_remote_copy(
                    src_ref=send_m.at[peers[x], cp, :, pl.ds(start, n), :], dst_ref=hms[grp].at[cp, :, r],
                    send_sem=main_ss.at[i], recv_sem=main_rs.at[i], device_id={'rows': peers[x]}, device_id_type=MESH_ID)
                rc.start()
                copies['m', grp, cp, x] = rc
            hms[grp][cp, :, r] = send_m[r, cp, :, start:start + n, :]
        for d in range(4):
            out = jnp.zeros((n, LANES), F32)
            for c in range(4):
                piece = rems[c] if c == d else pltpu.roll(rems[c], (WIN * (c - d)) % LANES, axis=1)
                out = jnp.where(block == c, piece, out)
            send_r[d, start:start + n, :] = out.astype(BF)
        for x in (1, 2, 0):
            i = 3 * grp + x
            rc = pltpu.make_async_remote_copy(
                src_ref=send_r.at[peers[x], pl.ds(start, n), :], dst_ref=hrs[grp].at[r],
                send_sem=rem_ss.at[i], recv_sem=rem_rs.at[i], device_id={'rows': peers[x]}, device_id_type=MESH_ID)
            rc.start()
            copies['r', grp, x] = rc
        hrs[grp][r] = send_r[r, start:start + n, :]

    columns(0)

    for h in halos:
        h.wait()
    lane = lax.broadcasted_iota(jnp.int32, (RB, LANES), 1)
    high = lane >= HALF
    slot = lane >> 5
    t0s, t9s = [], []
    for j in range(4):
        rows = slice(RB * j, RB * (j + 1))
        add_first = pltpu.roll(halo[1], (HALF - QTR * j) % LANES, axis=1)
        add_last = pltpu.roll(halo[0], (QTR - QTR * j) % LANES, axis=1)
        e = edge_ref[rows, :] + jnp.where(slot == 2, add_first, jnp.where(slot == 1, add_last, 0.0))
        t0s.append(jnp.where(high, e, tb_ref[0, rows, :].astype(F32)).astype(BF))
        t9s.append(jnp.where(high, tb_ref[9, rows, :].astype(F32), e).astype(BF))
    to_rows(3, jnp.concatenate(t0s, axis=0), tb_ref[1])
    to_rows(4, tb_ref[SUB], jnp.concatenate(t9s, axis=0))
    columns(1)

    lane = lax.broadcasted_iota(jnp.int32, (N_IMG, LANES), 1)
    pad = jnp.zeros((LANES - QB, N_IMG), F32)
    for s in range(2):
        wide = [jnp.concatenate([s_ref[s, c], pad], axis=0).T for c in range(4)]
        for cp in range(2):
            first = jnp.where(core == 0, wide[2 * cp], wide[2 * cp + 1])
            second = jnp.where(core == 0, wide[2 * cp + 1], wide[2 * cp])
            s_main[s, cp] = jnp.where(lane < HALF, first, pltpu.roll(second, HALF, axis=1))
        out = jnp.zeros((N_IMG, LANES), F32)
        for c in range(4):
            out = jnp.where((lane >> 4) == c, pltpu.roll(wide[c], (WIN * c - HALF) % LANES, axis=1), out)
        s_rem[s] = out
    d8 = jnp.broadcast_to(jnp.concatenate([d_ref[...], jnp.zeros((1, HALF), F32)], axis=1), (SUB, N_IMG + HALF))
    dq = d8
    for j in range(1, ROWS):
        dq = jnp.where(r == j, pltpu.roll(d8, N_IMG + HALF - QB * j, axis=1), dq)
    dp = jnp.where(k == 0, d8, pltpu.roll(d8, N_IMG + HALF - PB, axis=1))[:, :2 * LANES]
    dd = jnp.concatenate([dp] * WIN, axis=0).T[:PB] * dq[:1, :LANES]

    k0 = (0, 2 * ROWS * 96)

    def rows_main(grp):
        n = GROUPS[grp][1]
        for cp in range(2):
            for x in range(3):
                copies['m', grp, cp, x].wait_recv()
        kk = 2 * ROWS * n
        rhs = jnp.concatenate([hms[grp][cp].reshape(kk, LANES) for cp in range(2)], axis=1)
        res = jnp.dot(eu_ref[:, k0[grp]:k0[grp] + kk], rhs, preferred_element_type=F32)
        return res

    def rows_rem(grp):
        n = GROUPS[grp][1]
        for x in range(3):
            copies['r', grp, x].wait_recv()
        kk = ROWS * n
        rhs = hrs[grp][...].reshape(kk, LANES)
        return [jnp.dot(eu_ref[:, k0[grp] + kk * t:k0[grp] + kk * (t + 1)], rhs, preferred_element_type=F32) for t in range(2)]

    acc_m[...] = rows_main(0)
    for t, v in enumerate(rows_rem(0)):
        acc_r[t] = v
    acc_m[...] = acc_m[...] + rows_main(1)

    low = lax.broadcasted_iota(jnp.int32, (PB, LANES), 1) < HALF

    def combine_main(p0):
        rows = pl.ds(pl.multiple_of(p0, SUB), PB)
        rows_im = pl.ds(pl.multiple_of(N_IMG + p0, SUB), PB)
        re = jnp.zeros((PB, LANES), F32)
        im = jnp.zeros((PB, LANES), F32)
        for cp in range(2):
            cols = slice(LANES * cp, LANES * (cp + 1))
            i_re, i_im = acc_m[rows, cols], acc_m[rows_im, cols]
            s_re, s_im = s_main[0, cp, rows, :], s_main[1, cp, rows, :]
            re = re + (s_re * i_re + s_im * i_im)
            im = im + (s_re * i_im - s_im * i_re)
        return jnp.where(low, re + pltpu.roll(re, HALF, axis=1), im + pltpu.roll(im, HALF, axis=1))

    lane = lax.broadcasted_iota(jnp.int32, (PB, LANES), 1)
    slot40 = lax.broadcasted_iota(jnp.int32, (PB // 4, LANES), 1) >> 5

    def combine_rem(p0):
        rows = pl.ds(pl.multiple_of(p0, SUB), PB)
        rows_im = pl.ds(pl.multiple_of(N_IMG + p0, SUB), PB)
        i_re = acc_r[0, rows, :] + pltpu.roll(acc_r[1, rows, :], HALF, axis=1)
        i_im = acc_r[0, rows_im, :] + pltpu.roll(acc_r[1, rows_im, :], HALF, axis=1)
        s_re, s_im = s_rem[0, rows, :], s_rem[1, rows, :]
        re = jnp.where(low, s_re * i_re + s_im * i_im, 0.0)
        im = jnp.where(low, s_re * i_im - s_im * i_re, 0.0)
        w = re + pltpu.roll(im, HALF, axis=1)
        w = w + pltpu.roll(w, LANES - QTR, axis=1)
        w = w + pltpu.roll(w, LANES - WIN, axis=1)
        w = jnp.where(lane < WIN, w, pltpu.roll(w, LANES - 48, axis=1))
        out = jnp.zeros((PB // 4, LANES), F32)
        for j in range(4):
            piece = w[PB // 4 * j:PB // 4 * (j + 1), :]
            out = jnp.where(slot40 == j, pltpu.roll(piece, QTR * j, axis=1) if j else piece, out)
        return out

    far_p, own_p = PB - k * PB, k * PB

    def reduce_copy(src, dst, i):
        return pltpu.make_async_remote_copy(src_ref=src, dst_ref=dst, send_sem=red_ss.at[i], recv_sem=red_rs.at[i],
                                            device_id={'cols': 1 - k}, device_id_type=MESH_ID)

    img_m[...] = combine_main(far_p)
    red_main = reduce_copy(img_m, red_m, 0)
    red_main.start()
    for t, v in enumerate(rows_rem(1)):
        acc_r[t] = acc_r[t] + v
    img_r[...] = combine_rem(far_p)
    red_rem = reduce_copy(img_r, red_r, 1)
    red_rem.start()
    own_main = combine_main(own_p)
    own_rem = combine_rem(own_p)
    red_main.wait_recv()
    main = own_main + red_m[...]
    red_rem.wait_recv()
    rem = own_rem + red_r[...]
    for o in range(2):
        m = main if o == 0 else pltpu.roll(main, HALF, axis=1)
        for j in range(4):
            rows = slice(PB // 4 * j, PB // 4 * (j + 1))
            piece = pltpu.roll(rem, (HALF - QTR * j - WIN * o) % LANES, axis=1)
            full = jnp.where(low[rows], m[rows], piece)
            out_ref[o, rows, :] = (full * dd[rows])[:, :QB]

    red_main.wait_send()
    red_rem.wait_send()
    for key in copies:
        copies[key].wait_send()


def solution(mesh):
    sample_spec = ('exam', 'rows', 'cols')
    vm = pl.BlockSpec(memory_space=pltpu.VMEM)
    sm = pl.BlockSpec(memory_space=pltpu.SMEM)
    hbm = pl.BlockSpec(memory_space=pltpu.HBM)
    spread_scratch = ([VMEM((NG * CW, LANES), F32)] * T + [VMEM((LANES, LANES), F32)] * 4 + [VMEM((LANES * PS, LANES), F32)] * 2
                      + [VMEM((LANES, 768), BF)])
    big = 28 * 1024 * 1024

    def local_fn(kspace, wts_y, wts_x, idx_y, idx_x, coil_maps, deapod):
        own, far, base = pl.pallas_call(
            prep_kernel,
            out_shape=(jax.ShapeDtypeStruct((24, NS), F32), jax.ShapeDtypeStruct((24, NS), F32), jax.ShapeDtypeStruct((NB, LANES), jnp.int32)),
            in_specs=[hbm] * 5, out_specs=(vm, vm, vm), name='prep',
            scratch_shapes=[VMEM((2, SUB, NS), F32), VMEM((KW, NS), F32), VMEM((KW, NS), F32), VMEM((NB, LANES), jnp.int32), VMEM((NB, LANES), jnp.int32), pltpu.SemaphoreType.DMA((5,))],
            compiler_params=pltpu.CompilerParams(vmem_limit_bytes=SUB * 1024 * 1024),
        )(kspace, wts_y, wts_x, idx_y.reshape(NB, LANES), idx_x.reshape(NB, LANES))
        swap = [(0, 1), (1, 0)]
        far_in = lax.ppermute(far, 'cols', swap)
        base_in = lax.ppermute(base, 'cols', swap)
        half = pl.pallas_call(
            own_kernel, out_shape=jax.ShapeDtypeStruct((11, CW, LANES), F32), in_specs=[sm, vm], out_specs=vm,
            scratch_shapes=spread_scratch, compiler_params=pltpu.CompilerParams(vmem_limit_bytes=big), name='spread_own',
            cost_estimate=pl.CostEstimate(flops=4 * 10 ** 9, bytes_accessed=2 * 10 ** 6, transcendentals=0),
        )(base, own)
        tb, edge, pack = pl.pallas_call(
            far_kernel,
            out_shape=(jax.ShapeDtypeStruct((10, N_GRID, LANES), BF), jax.ShapeDtypeStruct((N_GRID, LANES), F32), jax.ShapeDtypeStruct((2, RB, LANES), F32)),
            in_specs=[sm, vm, vm], out_specs=(vm, vm, vm), scratch_shapes=spread_scratch + [VMEM((N_GRID, LANES), F32)],
            compiler_params=pltpu.CompilerParams(vmem_limit_bytes=big), name='spread_far',
            cost_estimate=pl.CostEstimate(flops=4 * 10 ** 9, bytes_accessed=4 * 10 ** 6, transcendentals=0),
        )(base_in, far_in, half)
        dma = pltpu.SemaphoreType.DMA
        return pl.pallas_call(
            image_kernel,
            out_shape=jax.ShapeDtypeStruct((2, PB, QB), F32),
            in_specs=[vm] * 8, out_specs=vm,
            scratch_shapes=[
                VMEM((4 * RB, 2 * N_GRID), BF), VMEM((2, RB, LANES), F32),
                VMEM((4, 2, 2, RB, LANES), BF), VMEM((4, RB, LANES), BF),
                VMEM((2, 2, ROWS, 96, LANES), BF), VMEM((2, 2, ROWS, HALF, LANES), BF), VMEM((ROWS, 96, LANES), BF), VMEM((ROWS, HALF, LANES), BF),
                VMEM((2 * N_IMG, 2 * LANES), F32), VMEM((2, 2 * N_IMG, LANES), F32), VMEM((2, 2, N_IMG, LANES), F32), VMEM((2, N_IMG, LANES), F32),
                VMEM((PB, LANES), F32), VMEM((PB // 4, LANES), F32), VMEM((PB, LANES), F32), VMEM((PB // 4, LANES), F32),
                dma((2,)), dma((2,)), dma((12,)), dma((12,)), dma((6,)), dma((6,)), dma((2,)), dma((2,)),
            ],
            compiler_params=pltpu.CompilerParams(vmem_limit_bytes=20 * 1024 * 1024, collective_id=0, has_side_effects=True), name='image',
        )(tb, edge, pack, jnp.swapaxes(coil_maps, 2, 3), deapod.reshape(1, N_IMG), col_dft(), row_dft(), unmix())

    return jax.shard_map(
        local_fn,
        mesh=mesh,
        in_specs=(P(None, None, sample_spec), P(None, sample_spec), P(None, sample_spec), P(sample_spec), P(sample_spec), P(None, ('exam', 'cols'), None, 'rows'), P()),
        out_specs=P(None, ('exam', 'cols'), 'rows'),
        check_vma=False,
    )
```

```python
import functools
import math

import jax
import jax.numpy as jnp
import numpy as np
from jax import lax
from jax.experimental import pallas as pl
from jax.experimental.pallas import tpu as pltpu
from jax.sharding import PartitionSpec as P

BF = jnp.bfloat16
F32 = jnp.float32
VMEM = pltpu.VMEM
LANES = 128
SUB, WIN, QTR, HALF = 8, 16, 32, 64
N_GRID, N_IMG, N_COILS, KW = 640, 320, 8, 6
ROWS, COLS = 4, 2
RB, CB, QB = N_GRID // ROWS, N_GRID // COLS, N_IMG // ROWS
PB = N_IMG // COLS
NS = 4096
NB = NS // LANES
NG = 21
CW = CB + WIN
T = 6
PS = 9
ORDER = (1, 2, 3, 0, 4)
GROUPS = ((0, 96), (96, 64))
MESH_ID = pl.DeviceIdType.MESH


def dft_parts():
    freq = np.arange(N_GRID) - N_GRID // 2
    pos = np.arange(N_IMG) - N_IMG // 2
    ang = ((freq[:, None] * pos[None, :]) % N_GRID).astype(np.float32) * np.float32(2.0 * math.pi / N_GRID)
    norm = np.float32(1.0 / math.sqrt(N_GRID))
    c, s = np.cos(ang) * norm, np.sin(ang) * norm
    return np.stack([np.stack([c, s], 1), np.stack([-s, c], 1)], 0)


def col_dft():
    e = dft_parts()
    out = np.zeros((2 * N_GRID, N_GRID), np.float32)
    for dp in range(2):
        for t in range(2):
            for h in range(2):
                q0 = QB * (2 * dp + h)
                l0 = LANES * (2 * dp + t) + HALF * h
                out[:, l0:l0 + HALF] = e[:, :, t, q0:q0 + HALF].reshape(2 * N_GRID, HALF)
    for t in range(2):
        for d in range(4):
            l0 = 4 * LANES + HALF * (d // 2) + WIN * (2 * t + d % 2)
            out[:, l0:l0 + WIN] = e[:, :, t, QB * d + HALF:QB * (d + 1)].reshape(2 * N_GRID, WIN)
    return jnp.asarray(out, BF)


def row_dft():
    e = dft_parts()
    rows = np.concatenate([np.arange(QTR * l, QTR * (l + 1)) for l in ORDER])
    chips = []
    for x in range(2):
        parts = []
        for start, n in GROUPS:
            for t in range(2):
                for b in range(2):
                    parts.append(e[t, (2 * x + b) * RB + rows[start:start + n]])
        m = np.concatenate(parts, 0)
        chips.append([m[:, :, PB * h:PB * (h + 1)].reshape(N_GRID, N_IMG).T for h in range(2)])
    return jnp.asarray(np.array(chips), BF)


def unmix():
    m = np.zeros((256, 256), np.float32)
    for ch in range(SUB):
        for pp in range(2):
            for i in range(WIN):
                m[ch * QTR + WIN * pp + (i + SUB) % WIN, pp * 128 + i * SUB + ch] = 1.0
    return jnp.asarray(m, BF)


def prep_kernel(ks_hbm, wy_hbm, wx_hbm, iy_hbm, ix_hbm, own_ref, far_ref, base_ref, ks_ref, wy_ref, wx_ref, iy_ref, ix_ref, sem):
    k = lax.axis_index('cols')
    r = lax.axis_index('rows')
    loads = []
    for src, dst in ((iy_hbm, iy_ref), (ix_hbm, ix_ref), (wx_hbm, wx_ref), (wy_hbm, wy_ref), (ks_hbm, ks_ref)):
        cp = pltpu.make_async_copy(src, dst, sem.at[len(loads)])
        cp.start()
        loads.append(cp)
    loads[0].wait()
    loads[1].wait()
    iy = iy_ref[...]
    base_ref[...] = ((iy - r * RB + 5) >> 3) * CW + (ix_ref[...] - k * CB + 5)
    sh = ((iy + 5) & 15).astype(F32)
    loads[2].wait()
    loads[3].wait()
    zero2 = jnp.zeros((2, NS), F32)
    for ref in (own_ref, far_ref):
        ref[SUB:WIN, :] = jnp.concatenate([wx_ref[...], zero2], axis=0)
        ref[WIN:24, :] = jnp.concatenate([wy_ref[...], zero2], axis=0)
        for b in range(NB):
            ref[22:23, LANES * b:LANES * (b + 1)] = sh[b:b + 1, :]
    loads[4].wait()
    lo = jnp.concatenate([ks_ref[0, 0:4, :], ks_ref[1, 0:4, :]], axis=0)
    hi = jnp.concatenate([ks_ref[0, 4:SUB, :], ks_ref[1, 4:SUB, :]], axis=0)
    own_ref[0:SUB, :] = jnp.where(k == 0, lo, hi)
    far_ref[0:SUB, :] = jnp.where(k == 0, hi, lo)


def split3(x):
    hi = x.astype(BF).astype(F32)
    r = x - hi
    mid = r.astype(BF).astype(F32)
    return hi, mid, r - mid


def accumulate(base_ref, pay_ref, accs, us, xs, vs, r_ref):
    row_i = lax.broadcasted_iota(jnp.int32, (WIN, LANES), 0)

    def make_u(blk, k):
        off = pl.multiple_of(jnp.minimum(blk, NB - 1) * LANES, LANES)
        y8 = pay_ref[0:SUB, pl.ds(off, LANES)]
        wyp = pay_ref[WIN:24, pl.ds(off, LANES)]
        d = (row_i - wyp[6:7, :].astype(jnp.int32)) & 15
        p = jnp.zeros((WIN, LANES), F32)
        for a in range(KW):
            p = jnp.where(d == a, wyp[a:a + 1, :], p)
        us[k][...] = jnp.concatenate([y8 * p[i:i + 1, :] for i in range(WIN)], axis=0).T
        x3 = list(split3(pay_ref[SUB:WIN, pl.ds(off, LANES)])) + [jnp.zeros((104, LANES), F32)]
        xs[k][...] = jnp.concatenate(x3, axis=0).T

    def make_v(k):
        lhs = xs[k][...].astype(BF)
        u = us[k][...]
        for bp in range(3):
            w = jnp.dot(lhs, r_ref[:, 256 * bp:256 * bp + 256], preferred_element_type=F32)
            for c in range(2):
                v = w[:, LANES * c:LANES * (c + 1)] * u
                for g in range(WIN):
                    vs[k][pl.ds(SUB * PS * g + 2 * bp + c, SUB, stride=PS), :] = v[SUB * g:SUB * g + SUB, :]

    def add_tiles(blk, k):
        for j in range(LANES):
            acc = accs[j % T]
            b = base_ref[blk, j]
            acc[pl.ds(b, SUB), :] = acc[pl.ds(b, SUB), :] + vs[k][PS * j:PS * j + SUB, :]

    def clear(n, _):
        for a in accs:
            a[pl.ds(pl.multiple_of(n * CW, SUB), CW), :] = jnp.zeros((CW, LANES), F32)
        return 0

    lax.fori_loop(0, NG, clear, 0)
    kk = lax.broadcasted_iota(jnp.int32, (LANES, 768), 0)
    ll = lax.broadcasted_iota(jnp.int32, (LANES, 768), 1)
    r_ref[...] = jnp.where((kk < 24) & ((kk & 7) == (ll >> 7)), 1.0, 0.0).astype(BF)
    for v in vs:
        v[...] = jnp.zeros_like(v)
    make_u(0, 0)
    make_u(1, 1)
    make_v(0)

    def body(n, _):
        k = 2 * n
        make_v(1)
        add_tiles(k, 0)
        make_u(k + 2, 0)
        make_v(0)
        add_tiles(k + 1, 1)
        make_u(k + 3, 1)
        return 0

    lax.fori_loop(0, NB // 2, body, 0)


def folded(accs, off, n):
    def total(g):
        o = pl.multiple_of(g * CW + off, SUB)
        s = accs[0][pl.ds(o, n), :]
        for a in accs[1:]:
            s = s + a[pl.ds(o, n), :]
        return s

    high = lax.broadcasted_iota(jnp.int32, (n, LANES), 1) >= HALF
    even = [total(2 * p) for p in range(11)]
    tiles = [total(2 * p + 1) + jnp.where(high, even[p], even[p + 1]) for p in range(10)]
    return tiles + [jnp.where(high, even[10], even[0])]


def own_kernel(base_ref, pay_ref, out_ref, *scr):
    accs, us, xs, vs, r_ref = scr[:T], scr[T:T + 2], scr[T + 2:T + 4], scr[T + 4:T + 6], scr[T + 6]
    accumulate(base_ref, pay_ref, accs, us, xs, vs, r_ref)

    def fold(q, _):
        off = pl.multiple_of(q * SUB, SUB)
        for p, t in enumerate(folded(accs, off, SUB)):
            out_ref[p, pl.ds(off, SUB), :] = t
        return 0

    lax.fori_loop(0, CW // SUB, fold, 0)


def far_kernel(base_ref, pay_ref, a_ref, tb_ref, edge_ref, pack_ref, *scr):
    accs, us, xs, vs, r_ref, gh_ref = scr[:T], scr[T:T + 2], scr[T + 2:T + 4], scr[T + 4:T + 6], scr[T + 6], scr[T + 7]
    accumulate(base_ref, pay_ref, accs, us, xs, vs, r_ref)
    k = lax.axis_index('cols')
    own0 = k * CB
    far0 = CB - own0
    high = lax.broadcasted_iota(jnp.int32, (SUB, LANES), 1) >= HALF

    left = folded(accs, 0, SUB)
    right = folded(accs, CW - SUB, SUB)
    for src, dst in ((CW - SUB, SUB), (0, CB)):
        for p in range(10):
            rows = pl.ds((2 * p + 1) * CW + dst, SUB)
            accs[0][rows, :] = accs[0][rows, :] + a_ref[p, src:src + SUB, :]
        ghost = a_ref[10, src:src + SUB, :]
        accs[0][dst:dst + SUB, :] = accs[0][dst:dst + SUB, :] + jnp.where(high, 0.0, ghost)
        rows = pl.ds(20 * CW + dst, SUB)
        accs[0][rows, :] = accs[0][rows, :] + jnp.where(high, ghost, 0.0)

    high16 = lax.broadcasted_iota(jnp.int32, (WIN, LANES), 1) >= HALF

    def put(v, tiles):
        v = pl.multiple_of(v, WIN)
        for p in range(10):
            tb_ref[p, pl.ds(v, WIN), :] = tiles[p].astype(BF)
        edge_ref[pl.ds(v, WIN), :] = jnp.where(high16, tiles[0], tiles[9])
        gh_ref[pl.ds(v, WIN), :] = tiles[10]

    def far_part(s, _):
        put(far0 + WIN * s, folded(accs, pl.multiple_of(SUB + WIN * s, SUB), WIN))
        return 0

    lax.fori_loop(0, CB // WIN, far_part, 0)

    def own_part(s, _):
        put(own0 + WIN * s, [a_ref[p, pl.ds(pl.multiple_of(SUB + WIN * s, SUB), WIN), :] for p in range(11)])
        return 0

    lax.fori_loop(1, CB // WIN - 1, own_part, 0)
    put(own0, [jnp.concatenate([a_ref[p, SUB:WIN, :] + right[p], a_ref[p, WIN:24, :]], axis=0) for p in range(11)])
    put(own0 + CB - WIN, [jnp.concatenate([a_ref[p, CB - SUB:CB, :], a_ref[p, CB:CB + SUB, :] + left[p]], axis=0) for p in range(11)])

    slot = lax.broadcasted_iota(jnp.int32, (RB, LANES), 1) >> 5
    for side, lane0 in ((0, QTR), (1, HALF)):
        out = jnp.zeros((RB, LANES), F32)
        for j in range(4):
            piece = pltpu.roll(gh_ref[RB * j:RB * (j + 1), :], (QTR * j - lane0) % LANES, axis=1)
            out = jnp.where(slot == j, piece, out)
        pack_ref[side] = out


def image_kernel(tb_ref, edge_ref, pack_ref, so_ref, sx_ref, d_ref, ev_ref, eu_ref, pm_ref, out_ref,
                 g_ref, halo, sm1, sm2, sr1, sr2, hm1, hm2, hr1, hr2, s_main, s_rem, pieces, recvs,
                 halo_ss, halo_rs, swap_ss, swap_rs, red_ss, red_rs):
    k = lax.axis_index('cols')
    r = lax.axis_index('rows')
    core, x = r % 2, r // 2
    near = r + 1 - 2 * core
    across = (r + 2) % 4
    prev, nxt = (r + 3) % 4, (r + 1) % 4
    homes = ({'rows': across, 'cols': 1 - k}, {'cols': 1 - k}, {'rows': across})

    barrier = pltpu.get_barrier_semaphore()
    for dev in ({'rows': prev}, {'rows': nxt}) + homes:
        pl.semaphore_signal(barrier, inc=1, device_id=dev, device_id_type=MESH_ID)
    pl.semaphore_wait(barrier, 5)

    def remote(src, dst, ss, rs, i, dev):
        cp = pltpu.make_async_remote_copy(src_ref=src, dst_ref=dst, send_sem=ss.at[i], recv_sem=rs.at[i], device_id=dev, device_id_type=MESH_ID)
        cp.start()
        return cp

    halos = [remote(pack_ref.at[i], halo.at[i], halo_ss, halo_rs, i, {'rows': dev}) for i, dev in ((0, prev), (1, nxt))]

    def to_rows(pos, t0, t1):
        a = jnp.concatenate([t0, t1], axis=1)
        g = lax.dot_general(pm_ref[...], a, (((1,), (1,)), ((), ())), preferred_element_type=F32).astype(BF)
        for ch in range(SUB):
            s, c = ch // 4, ch % 4
            g_ref[RB * c + QTR * pos:RB * c + QTR * (pos + 1), N_GRID * s:N_GRID * (s + 1)] = g[QTR * ch:QTR * (ch + 1), :]

    for pos in range(3):
        l = ORDER[pos]
        to_rows(pos, tb_ref[2 * l], tb_ref[2 * l + 1])

    sms, srs, hms, hrs = (sm1, sm2), (sr1, sr2), (hm1, hm2), (hr1, hr2)
    swaps = []

    def columns(grp):
        start, n = GROUPS[grp]
        lane = lax.broadcasted_iota(jnp.int32, (n, LANES), 1)
        side = lane >> 6
        own_even, far_even = side == core, side != core
        block = (lane & (HALF - 1)) >> 4
        rems = []
        for cp in range(2):
            hs = []
            for c in (2 * cp, 2 * cp + 1):
                h = jnp.dot(g_ref[RB * c + start:RB * c + start + n, :], ev_ref[...], preferred_element_type=F32)
                hs.append([h[:, LANES * i:LANES * (i + 1)] for i in range(4)])
                rems.append(h[:, 4 * LANES:])
            for i in range(4):
                dp, t = i // 2, i % 2
                odd = pltpu.roll(hs[1][i], HALF, axis=1)
                sms[grp][dp, cp, t] = jnp.where(far_even, hs[0][i], odd).astype(BF)
                hms[grp][dp, cp, t, core] = jnp.where(own_even, hs[0][i], odd).astype(BF)
        for t in range(2):
            both = []
            for h in range(2):
                i = 2 * t + h
                out = rems[i]
                for c in range(4):
                    if c != i:
                        out = jnp.where(block == c, pltpu.roll(rems[c], (WIN * (c - i)) % LANES, axis=1), out)
                both.append(out)
            srs[grp][t] = jnp.where(core == 0, both[1], both[0]).astype(BF)
            hrs[grp][t, core] = jnp.where(core == 0, both[0], both[1]).astype(BF)
        swaps.append(remote(sms[grp], hms[grp].at[:, :, :, core], swap_ss, swap_rs, 2 * grp, {'rows': near}))
        swaps.append(remote(srs[grp], hrs[grp].at[:, core], swap_ss, swap_rs, 2 * grp + 1, {'rows': near}))

    columns(0)

    lane = lax.broadcasted_iota(jnp.int32, (N_IMG, LANES), 1)
    pad = jnp.zeros((LANES - QB, N_IMG), F32)
    for s in range(2):
        rem = []
        for j, ref in ((0, so_ref), (1, sx_ref)):
            wide = [jnp.concatenate([ref[s, c], pad], axis=0).T for c in range(4)]
            for cp in range(2):
                first = jnp.where(core == 0, wide[2 * cp], wide[2 * cp + 1])
                second = jnp.where(core == 0, wide[2 * cp + 1], wide[2 * cp])
                s_main[j, s, cp] = jnp.where(lane < HALF, first, pltpu.roll(second, HALF, axis=1))
            out = wide[0]
            for c in range(4):
                out = jnp.where((lane & (HALF - 1)) >> 4 == c, pltpu.roll(wide[c], (WIN * c + HALF) % LANES, axis=1), out)
            rem.append(out)
        flip = [pltpu.roll(v, HALF, axis=1) for v in rem]
        s_rem[s] = jnp.where(x == 0, jnp.where(lane < HALF, rem[0], flip[1]), jnp.where(lane < HALF, rem[1], flip[0]))
    d8 = jnp.broadcast_to(jnp.concatenate([d_ref[...], jnp.zeros((1, HALF), F32)], axis=1), (SUB, N_IMG + HALF))
    dq = d8
    for j in range(1, ROWS):
        dq = jnp.where(r == j, pltpu.roll(d8, N_IMG + HALF - QB * j, axis=1), dq)
    dp = jnp.where(k == 0, d8, pltpu.roll(d8, N_IMG + HALF - PB, axis=1))[:, :2 * LANES]
    dd = jnp.concatenate([dp] * WIN, axis=0).T[:PB] * dq[:1, :LANES]

    for h in halos:
        h.wait()
    lane = lax.broadcasted_iota(jnp.int32, (RB, LANES), 1)
    low = lane < HALF
    slot = lane >> 5
    t0s, t9s = [], []
    for j in range(4):
        rows = slice(RB * j, RB * (j + 1))
        add_first = pltpu.roll(halo[1], (HALF - QTR * j) % LANES, axis=1)
        add_last = pltpu.roll(halo[0], (QTR - QTR * j) % LANES, axis=1)
        e = edge_ref[rows, :] + jnp.where(slot == 2, add_first, jnp.where(slot == 1, add_last, 0.0))
        t0s.append(jnp.where(low, tb_ref[0, rows, :].astype(F32), e).astype(BF))
        t9s.append(jnp.where(low, e, tb_ref[9, rows, :].astype(F32)).astype(BF))
    to_rows(3, jnp.concatenate(t0s, axis=0), tb_ref[1])
    to_rows(4, tb_ref[SUB], jnp.concatenate(t9s, axis=0))
    columns(1)

    for cp in swaps:
        cp.wait_recv()

    def rows_dft(half, rhs):
        total, k0 = None, 0
        for grp in range(2):
            kk = 4 * GROUPS[grp][1]
            part = jnp.dot(eu_ref[x, half, :, k0:k0 + kk], rhs(grp), preferred_element_type=F32)
            total = part if total is None else total + part
            k0 += kk
        return total[:PB], total[PB:]

    quarter = lax.broadcasted_iota(jnp.int32, (PB // 4, LANES), 1) >> 5

    def rest(half):
        i_re, i_im = rows_dft(half, lambda g: hrs[g][...].reshape(4 * GROUPS[g][1], LANES))
        rows = pl.ds(pl.multiple_of(half * PB, SUB), PB)
        s_re, s_im = s_rem[0, rows, :], s_rem[1, rows, :]

        def fold(v):
            v = v + pltpu.roll(v, LANES - QTR, axis=1)
            return v + pltpu.roll(v, LANES - WIN, axis=1)

        re, im = fold(s_re * i_re + s_im * i_im), fold(s_re * i_im - s_im * i_re)
        return jnp.where(lane & (HALF - 1) < WIN, re, pltpu.roll(im, WIN, axis=1))

    def piece(half, j, tail):
        dp = (x + j) % 2
        i_re, i_im = rows_dft(half, lambda g: jnp.concatenate([hms[g][dp, cp].reshape(4 * GROUPS[g][1], LANES) for cp in range(2)], axis=1))
        rows = pl.ds(pl.multiple_of(half * PB, SUB), PB)
        re, im = None, None
        for cp in range(2):
            cols = slice(LANES * cp, LANES * (cp + 1))
            s_re, s_im = s_main[j, 0, cp, rows, :], s_main[j, 1, cp, rows, :]
            a = s_re * i_re[:, cols] + s_im * i_im[:, cols]
            b = s_re * i_im[:, cols] - s_im * i_re[:, cols]
            re, im = (a, b) if re is None else (re + a, im + b)
        main = jnp.where(low, re + pltpu.roll(re, HALF, axis=1), im + pltpu.roll(im, HALF, axis=1))
        y = jnp.where(dp == 0, tail, pltpu.roll(tail, HALF, axis=1))
        out = y[:PB // 4]
        for g in range(1, 4):
            out = jnp.where(quarter == g, pltpu.roll(y[PB // 4 * g:PB // 4 * (g + 1)], QTR * g, axis=1), out)
        return main, out

    sends = []
    far_tail = rest(1 - k)
    for i, (half, j) in enumerate(((1 - k, 1), (1 - k, 0), (k, 1))):
        if i == 2:
            own_tail = rest(k)
        pieces[i, :PB], pieces[i, PB:] = piece(half, j, own_tail if i == 2 else far_tail)
        sends.append(remote(pieces.at[i], recvs.at[i], red_ss, red_rs, i, homes[i]))
    main, rem = piece(k, 0, own_tail)
    for i in (2, 1, 0):
        sends[i].wait_recv()
        main = main + recvs[i, :PB]
        rem = rem + recvs[i, PB:]
    for o in range(2):
        m = pltpu.roll(main, HALF, axis=1) if o else main
        for j in range(4):
            rows = slice(PB // 4 * j, PB // 4 * (j + 1))
            tail = pltpu.roll(rem, (HALF - QTR * j - WIN * o) % LANES, axis=1)
            out_ref[o, rows, :] = (jnp.where(low[rows], m[rows], tail) * dd[rows])[:, :QB]

    for cp in sends + swaps:
        cp.wait_send()


def solution(mesh):
    sample_spec = ('exam', 'rows', 'cols')
    vm = pl.BlockSpec(memory_space=pltpu.VMEM)
    sm = pl.BlockSpec(memory_space=pltpu.SMEM)
    hbm = pl.BlockSpec(memory_space=pltpu.HBM)
    spread_scratch = ([VMEM((NG * CW, LANES), F32)] * T + [VMEM((LANES, LANES), F32)] * 4 + [VMEM((LANES * PS, LANES), F32)] * 2
                      + [VMEM((LANES, 768), BF)])
    big = 28 * 1024 * 1024

    def local_fn(kspace, wts_y, wts_x, idx_y, idx_x, coil_maps, deapod):
        own, far, base = pl.pallas_call(
            prep_kernel,
            out_shape=(jax.ShapeDtypeStruct((24, NS), F32), jax.ShapeDtypeStruct((24, NS), F32), jax.ShapeDtypeStruct((NB, LANES), jnp.int32)),
            in_specs=[hbm] * 5, out_specs=(vm, vm, vm), name='prep',
            scratch_shapes=[VMEM((2, SUB, NS), F32), VMEM((KW, NS), F32), VMEM((KW, NS), F32), VMEM((NB, LANES), jnp.int32), VMEM((NB, LANES), jnp.int32), pltpu.SemaphoreType.DMA((5,))],
            compiler_params=pltpu.CompilerParams(vmem_limit_bytes=SUB * 1024 * 1024),
        )(kspace, wts_y, wts_x, idx_y.reshape(NB, LANES), idx_x.reshape(NB, LANES))
        swap = [(0, 1), (1, 0)]
        far_in = lax.ppermute(far, 'cols', swap)
        base_in = lax.ppermute(base, 'cols', swap)
        half = pl.pallas_call(
            own_kernel, out_shape=jax.ShapeDtypeStruct((11, CW, LANES), F32), in_specs=[sm, vm], out_specs=vm,
            scratch_shapes=spread_scratch, compiler_params=pltpu.CompilerParams(vmem_limit_bytes=big), name='spread_own',
            cost_estimate=pl.CostEstimate(flops=4 * 10 ** 9, bytes_accessed=2 * 10 ** 6, transcendentals=0),
        )(base, own)
        tb, edge, pack = pl.pallas_call(
            far_kernel,
            out_shape=(jax.ShapeDtypeStruct((10, N_GRID, LANES), BF), jax.ShapeDtypeStruct((N_GRID, LANES), F32), jax.ShapeDtypeStruct((2, RB, LANES), F32)),
            in_specs=[sm, vm, vm], out_specs=(vm, vm, vm), scratch_shapes=spread_scratch + [VMEM((N_GRID, LANES), F32)],
            compiler_params=pltpu.CompilerParams(vmem_limit_bytes=big), name='spread_far',
            cost_estimate=pl.CostEstimate(flops=4 * 10 ** 9, bytes_accessed=4 * 10 ** 6, transcendentals=0),
        )(base_in, far_in, half)
        maps = jnp.swapaxes(coil_maps, 2, 3)
        maps_x = lax.ppermute(maps, 'rows', [(i, (i + 2) % ROWS) for i in range(ROWS)])
        dma = pltpu.SemaphoreType.DMA
        half_bufs = [VMEM((2, 2, 2, n, LANES), BF) for _, n in GROUPS] + [VMEM((2, n, LANES), BF) for _, n in GROUPS]
        full_bufs = [VMEM((2, 2, 2, 2, n, LANES), BF) for _, n in GROUPS] + [VMEM((2, 2, n, LANES), BF) for _, n in GROUPS]
        return pl.pallas_call(
            image_kernel,
            out_shape=jax.ShapeDtypeStruct((2, PB, QB), F32), in_specs=[vm] * 9, out_specs=vm,
            scratch_shapes=[VMEM((4 * RB, 2 * N_GRID), BF), VMEM((2, RB, LANES), F32)] + half_bufs + full_bufs + [
                VMEM((2, 2, 2, N_IMG, LANES), F32), VMEM((2, N_IMG, LANES), F32), VMEM((3, PB + PB // 4, LANES), F32), VMEM((3, PB + PB // 4, LANES), F32),
                dma((2,)), dma((2,)), dma((4,)), dma((4,)), dma((3,)), dma((3,)),
            ],
            compiler_params=pltpu.CompilerParams(vmem_limit_bytes=20 * 1024 * 1024, collective_id=0, has_side_effects=True), name='image',
        )(tb, edge, pack, maps, maps_x, deapod.reshape(1, N_IMG), col_dft(), row_dft(), unmix())

    return jax.shard_map(
        local_fn,
        mesh=mesh,
        in_specs=(P(None, None, sample_spec), P(None, sample_spec), P(None, sample_spec), P(sample_spec), P(sample_spec), P(None, ('exam', 'cols'), None, 'rows'), P()),
        out_specs=P(None, ('exam', 'cols'), 'rows'),
        check_vma=False,
    )
```

```python
import functools
import math

import jax
import jax.numpy as jnp
import numpy as np
from jax import lax
from jax.experimental import pallas as pl
from jax.experimental.pallas import tpu as pltpu
from jax.sharding import PartitionSpec as P

BF = jnp.bfloat16
F32 = jnp.float32
VMEM = pltpu.VMEM
LANES = 128
SUB, WIN, QTR, HALF = 8, 16, 32, 64
N_GRID, N_IMG, N_COILS, KW = 640, 320, 8, 6
ROWS, COLS = 4, 2
RB, CB, QB = N_GRID // ROWS, N_GRID // COLS, N_IMG // ROWS
PB = N_IMG // COLS
NS = 4096
NB = NS // LANES
NG = 21
CW = CB + WIN
T = 6
PS = 9
ORDER = (1, 2, 3, 0, 4)
GROUPS = ((0, 96), (96, 64))
MESH_ID = pl.DeviceIdType.MESH


def dft_parts():
    freq = np.arange(N_GRID) - N_GRID // 2
    pos = np.arange(N_IMG) - N_IMG // 2
    ang = ((freq[:, None] * pos[None, :]) % N_GRID).astype(np.float32) * np.float32(2.0 * math.pi / N_GRID)
    norm = np.float32(1.0 / math.sqrt(N_GRID))
    c, s = np.cos(ang) * norm, np.sin(ang) * norm
    return np.stack([np.stack([c, s], 1), np.stack([-s, c], 1)], 0)


def col_dft():
    e = dft_parts()
    out = np.zeros((2 * N_GRID, N_GRID), np.float32)
    for dp in range(2):
        for t in range(2):
            for h in range(2):
                q0 = QB * (2 * dp + h)
                l0 = LANES * (2 * dp + t) + HALF * h
                out[:, l0:l0 + HALF] = e[:, :, t, q0:q0 + HALF].reshape(2 * N_GRID, HALF)
    for t in range(2):
        for d in range(4):
            l0 = 4 * LANES + HALF * (d // 2) + WIN * (2 * t + d % 2)
            out[:, l0:l0 + WIN] = e[:, :, t, QB * d + HALF:QB * (d + 1)].reshape(2 * N_GRID, WIN)
    return jnp.asarray(out, BF)


def row_dft():
    e = dft_parts()
    rows = np.concatenate([np.arange(QTR * l, QTR * (l + 1)) for l in ORDER])
    chips = []
    for x in range(2):
        parts = []
        for start, n in GROUPS:
            for t in range(2):
                for b in range(2):
                    parts.append(e[t, (2 * x + b) * RB + rows[start:start + n]])
        m = np.concatenate(parts, 0)
        chips.append([m[:, :, PB * h:PB * (h + 1)].reshape(N_GRID, N_IMG).T for h in range(2)])
    return jnp.asarray(np.array(chips), BF)


def unmix():
    m = np.zeros((256, 256), np.float32)
    for ch in range(SUB):
        for pp in range(2):
            for i in range(WIN):
                m[ch * QTR + WIN * pp + (i + SUB) % WIN, pp * 128 + i * SUB + ch] = 1.0
    return jnp.asarray(m, BF)


def prep_kernel(ks_hbm, wy_hbm, wx_hbm, iy_hbm, ix_hbm, own_ref, far_ref, ks_ref, wy_ref, wx_ref, iy_ref, ix_ref, sem):
    k = lax.axis_index('cols')
    r = lax.axis_index('rows')
    loads = []
    for src, dst in ((iy_hbm, iy_ref), (ix_hbm, ix_ref), (wx_hbm, wx_ref), (wy_hbm, wy_ref), (ks_hbm, ks_ref)):
        cp = pltpu.make_async_copy(src, dst, sem.at[len(loads)])
        cp.start()
        loads.append(cp)
    loads[0].wait()
    loads[1].wait()
    iy = iy_ref[...]
    base = (((iy - r * RB + 5) >> 3) * CW + (ix_ref[...] - k * CB + 5)).astype(F32)
    sh = ((iy + 5) & 15).astype(F32)
    loads[2].wait()
    loads[3].wait()
    zero2 = jnp.zeros((2, NS), F32)
    for ref in (own_ref, far_ref):
        ref[SUB:WIN, :] = jnp.concatenate([wx_ref[...], zero2], axis=0)
        ref[WIN:24, :] = jnp.concatenate([wy_ref[...], zero2], axis=0)
        for b in range(NB):
            ref[22:24, LANES * b:LANES * (b + 1)] = jnp.concatenate([sh[b:b + 1, :], base[b:b + 1, :]], axis=0)
    loads[4].wait()
    lo = jnp.concatenate([ks_ref[0, 0:4, :], ks_ref[1, 0:4, :]], axis=0)
    hi = jnp.concatenate([ks_ref[0, 4:SUB, :], ks_ref[1, 4:SUB, :]], axis=0)
    own_ref[0:SUB, :] = jnp.where(k == 0, lo, hi)
    far_ref[0:SUB, :] = jnp.where(k == 0, hi, lo)


def split3(x):
    hi = x.astype(BF).astype(F32)
    r = x - hi
    mid = r.astype(BF).astype(F32)
    return hi, mid, r - mid


def accumulate(pay_ref, accs, us, xs, vs, r_ref, int_ref, base_ref, sem):
    row_i = lax.broadcasted_iota(jnp.int32, (WIN, LANES), 0)

    def make_u(blk, k):
        off = pl.multiple_of(jnp.minimum(blk, NB - 1) * LANES, LANES)
        y8 = pay_ref[0:SUB, pl.ds(off, LANES)]
        wyp = pay_ref[WIN:24, pl.ds(off, LANES)]
        d = (row_i - wyp[6:7, :].astype(jnp.int32)) & 15
        p = jnp.zeros((WIN, LANES), F32)
        for a in range(KW):
            p = jnp.where(d == a, wyp[a:a + 1, :], p)
        us[k][...] = jnp.concatenate([y8 * p[i:i + 1, :] for i in range(WIN)], axis=0).T
        x3 = list(split3(pay_ref[SUB:WIN, pl.ds(off, LANES)])) + [jnp.zeros((104, LANES), F32)]
        xs[k][...] = jnp.concatenate(x3, axis=0).T

    def make_v(k):
        lhs = xs[k][...].astype(BF)
        u = us[k][...]
        for bp in range(3):
            w = jnp.dot(lhs, r_ref[:, 256 * bp:256 * bp + 256], preferred_element_type=F32)
            for c in range(2):
                v = w[:, LANES * c:LANES * (c + 1)] * u
                for g in range(WIN):
                    vs[k][pl.ds(SUB * PS * g + 2 * bp + c, SUB, stride=PS), :] = v[SUB * g:SUB * g + SUB, :]

    def add_tiles(blk, k):
        for j in range(LANES):
            acc = accs[j % T]
            b = base_ref[blk, j]
            acc[pl.ds(b, SUB), :] = acc[pl.ds(b, SUB), :] + vs[k][PS * j:PS * j + SUB, :]

    def clear(n, _):
        for a in accs:
            a[pl.ds(pl.multiple_of(n * CW, SUB), CW), :] = jnp.zeros((CW, LANES), F32)
        return 0

    for b in range(NB):
        int_ref[b:b + 1, :] = pay_ref[23:24, LANES * b:LANES * (b + 1)].astype(jnp.int32)
    lax.fori_loop(0, NG, clear, 0)
    load = pltpu.make_async_copy(int_ref, base_ref, sem)
    load.start()
    kk = lax.broadcasted_iota(jnp.int32, (LANES, 768), 0)
    ll = lax.broadcasted_iota(jnp.int32, (LANES, 768), 1)
    r_ref[...] = jnp.where((kk < 24) & ((kk & 7) == (ll >> 7)), 1.0, 0.0).astype(BF)
    for v in vs:
        v[...] = jnp.zeros_like(v)
    make_u(0, 0)
    make_u(1, 1)
    make_v(0)
    load.wait()

    def body(n, _):
        k = 2 * n
        make_v(1)
        add_tiles(k, 0)
        make_u(k + 2, 0)
        make_v(0)
        add_tiles(k + 1, 1)
        make_u(k + 3, 1)
        return 0

    lax.fori_loop(0, NB // 2, body, 0)


def folded(accs, off, n):
    def total(g):
        o = pl.multiple_of(g * CW + off, SUB)
        s = accs[0][pl.ds(o, n), :]
        for a in accs[1:]:
            s = s + a[pl.ds(o, n), :]
        return s

    high = lax.broadcasted_iota(jnp.int32, (n, LANES), 1) >= HALF
    even = [total(2 * p) for p in range(11)]
    tiles = [total(2 * p + 1) + jnp.where(high, even[p], even[p + 1]) for p in range(10)]
    return tiles + [jnp.where(high, even[10], even[0])]


def own_kernel(pay_ref, out_ref, *scr):
    accs = scr[:T]
    accumulate(pay_ref, accs, scr[T:T + 2], scr[T + 2:T + 4], scr[T + 4:T + 6], *scr[T + 6:])

    def fold(q, _):
        off = pl.multiple_of(q * SUB, SUB)
        for p, t in enumerate(folded(accs, off, SUB)):
            out_ref[p, pl.ds(off, SUB), :] = t
        return 0

    lax.fori_loop(0, CW // SUB, fold, 0)


def far_kernel(pay_ref, a_ref, tb_ref, edge_ref, pack_ref, gh_ref, *scr):
    accs = scr[:T]
    accumulate(pay_ref, accs, scr[T:T + 2], scr[T + 2:T + 4], scr[T + 4:T + 6], *scr[T + 6:])
    k = lax.axis_index('cols')
    own0 = k * CB
    far0 = CB - own0
    high = lax.broadcasted_iota(jnp.int32, (SUB, LANES), 1) >= HALF

    left = folded(accs, 0, SUB)
    right = folded(accs, CW - SUB, SUB)
    for src, dst in ((CW - SUB, SUB), (0, CB)):
        for p in range(10):
            rows = pl.ds((2 * p + 1) * CW + dst, SUB)
            accs[0][rows, :] = accs[0][rows, :] + a_ref[p, src:src + SUB, :]
        ghost = a_ref[10, src:src + SUB, :]
        accs[0][dst:dst + SUB, :] = accs[0][dst:dst + SUB, :] + jnp.where(high, 0.0, ghost)
        rows = pl.ds(20 * CW + dst, SUB)
        accs[0][rows, :] = accs[0][rows, :] + jnp.where(high, ghost, 0.0)

    high16 = lax.broadcasted_iota(jnp.int32, (WIN, LANES), 1) >= HALF

    def put(v, tiles):
        v = pl.multiple_of(v, WIN)
        for p in range(10):
            tb_ref[p, pl.ds(v, WIN), :] = tiles[p].astype(BF)
        edge_ref[pl.ds(v, WIN), :] = jnp.where(high16, tiles[0], tiles[9])
        gh_ref[pl.ds(v, WIN), :] = tiles[10]

    def far_part(s, _):
        put(far0 + WIN * s, folded(accs, pl.multiple_of(SUB + WIN * s, SUB), WIN))
        return 0

    lax.fori_loop(0, CB // WIN, far_part, 0)

    def own_part(s, _):
        put(own0 + WIN * s, [a_ref[p, pl.ds(pl.multiple_of(SUB + WIN * s, SUB), WIN), :] for p in range(11)])
        return 0

    lax.fori_loop(1, CB // WIN - 1, own_part, 0)
    put(own0, [jnp.concatenate([a_ref[p, SUB:WIN, :] + right[p], a_ref[p, WIN:24, :]], axis=0) for p in range(11)])
    put(own0 + CB - WIN, [jnp.concatenate([a_ref[p, CB - SUB:CB, :], a_ref[p, CB:CB + SUB, :] + left[p]], axis=0) for p in range(11)])

    slot = lax.broadcasted_iota(jnp.int32, (RB, LANES), 1) >> 5
    for side, lane0 in ((0, QTR), (1, HALF)):
        out = jnp.zeros((RB, LANES), F32)
        for j in range(4):
            piece = pltpu.roll(gh_ref[RB * j:RB * (j + 1), :], (QTR * j - lane0) % LANES, axis=1)
            out = jnp.where(slot == j, piece, out)
        pack_ref[side] = out


def image_kernel(tb_ref, edge_ref, pack_ref, so_ref, sx_ref, d_ref, ev_ref, eu_ref, pm_ref, out_ref,
                 g_ref, halo, sm1, sm2, sr1, sr2, hm1, hm2, hr1, hr2, s_main, s_rem, pieces, recvs,
                 halo_ss, halo_rs, swap_ss, swap_rs, red_ss, red_rs):
    k = lax.axis_index('cols')
    r = lax.axis_index('rows')
    core, x = r % 2, r // 2
    near = r + 1 - 2 * core
    across = (r + 2) % 4
    prev, nxt = (r + 3) % 4, (r + 1) % 4
    homes = ({'rows': across, 'cols': 1 - k}, {'cols': 1 - k}, {'rows': across})

    barrier = pltpu.get_barrier_semaphore()
    for dev in ({'rows': prev}, {'rows': nxt}) + homes:
        pl.semaphore_signal(barrier, inc=1, device_id=dev, device_id_type=MESH_ID)
    pl.semaphore_wait(barrier, 5)

    def remote(src, dst, ss, rs, i, dev):
        cp = pltpu.make_async_remote_copy(src_ref=src, dst_ref=dst, send_sem=ss.at[i], recv_sem=rs.at[i], device_id=dev, device_id_type=MESH_ID)
        cp.start()
        return cp

    halos = [remote(pack_ref.at[i], halo.at[i], halo_ss, halo_rs, i, {'rows': dev}) for i, dev in ((0, prev), (1, nxt))]

    def to_rows(pos, t0, t1):
        a = jnp.concatenate([t0, t1], axis=1)
        g = lax.dot_general(pm_ref[...], a, (((1,), (1,)), ((), ())), preferred_element_type=F32).astype(BF)
        for ch in range(SUB):
            s, c = ch // 4, ch % 4
            g_ref[RB * c + QTR * pos:RB * c + QTR * (pos + 1), N_GRID * s:N_GRID * (s + 1)] = g[QTR * ch:QTR * (ch + 1), :]

    for pos in range(3):
        l = ORDER[pos]
        to_rows(pos, tb_ref[2 * l], tb_ref[2 * l + 1])

    sms, srs, hms, hrs = (sm1, sm2), (sr1, sr2), (hm1, hm2), (hr1, hr2)
    swaps = []

    def columns(grp):
        start, n = GROUPS[grp]
        lane = lax.broadcasted_iota(jnp.int32, (n, LANES), 1)
        side = lane >> 6
        own_even, far_even = side == core, side != core
        block = (lane & (HALF - 1)) >> 4
        rems = []
        for cp in range(2):
            hs = []
            for c in (2 * cp, 2 * cp + 1):
                h = jnp.dot(g_ref[RB * c + start:RB * c + start + n, :], ev_ref[...], preferred_element_type=F32)
                hs.append([h[:, LANES * i:LANES * (i + 1)] for i in range(4)])
                rems.append(h[:, 4 * LANES:])
            for i in range(4):
                dp, t = i // 2, i % 2
                odd = pltpu.roll(hs[1][i], HALF, axis=1)
                sms[grp][dp, cp, t] = jnp.where(far_even, hs[0][i], odd).astype(BF)
                hms[grp][dp, cp, t, core] = jnp.where(own_even, hs[0][i], odd).astype(BF)
        for t in range(2):
            both = []
            for h in range(2):
                i = 2 * t + h
                out = rems[i]
                for c in range(4):
                    if c != i:
                        out = jnp.where(block == c, pltpu.roll(rems[c], (WIN * (c - i)) % LANES, axis=1), out)
                both.append(out)
            srs[grp][t] = jnp.where(core == 0, both[1], both[0]).astype(BF)
            hrs[grp][t, core] = jnp.where(core == 0, both[0], both[1]).astype(BF)
        swaps.append(remote(sms[grp], hms[grp].at[:, :, :, core], swap_ss, swap_rs, 2 * grp, {'rows': near}))
        swaps.append(remote(srs[grp], hrs[grp].at[:, core], swap_ss, swap_rs, 2 * grp + 1, {'rows': near}))

    columns(0)

    lane = lax.broadcasted_iota(jnp.int32, (N_IMG, LANES), 1)
    pad = jnp.zeros((LANES - QB, N_IMG), F32)
    for s in range(2):
        rem = []
        for j, ref in ((0, so_ref), (1, sx_ref)):
            wide = [jnp.concatenate([ref[s, c], pad], axis=0).T for c in range(4)]
            for cp in range(2):
                first = jnp.where(core == 0, wide[2 * cp], wide[2 * cp + 1])
                second = jnp.where(core == 0, wide[2 * cp + 1], wide[2 * cp])
                s_main[j, s, cp] = jnp.where(lane < HALF, first, pltpu.roll(second, HALF, axis=1))
            out = wide[0]
            for c in range(4):
                out = jnp.where((lane & (HALF - 1)) >> 4 == c, pltpu.roll(wide[c], (WIN * c + HALF) % LANES, axis=1), out)
            rem.append(out)
        flip = [pltpu.roll(v, HALF, axis=1) for v in rem]
        s_rem[s] = jnp.where(x == 0, jnp.where(lane < HALF, rem[0], flip[1]), jnp.where(lane < HALF, rem[1], flip[0]))
    d8 = jnp.broadcast_to(jnp.concatenate([d_ref[...], jnp.zeros((1, HALF), F32)], axis=1), (SUB, N_IMG + HALF))
    dq = d8
    for j in range(1, ROWS):
        dq = jnp.where(r == j, pltpu.roll(d8, N_IMG + HALF - QB * j, axis=1), dq)
    dp = jnp.where(k == 0, d8, pltpu.roll(d8, N_IMG + HALF - PB, axis=1))[:, :2 * LANES]
    dd = jnp.concatenate([dp] * WIN, axis=0).T[:PB] * dq[:1, :LANES]

    for h in halos:
        h.wait()
    lane = lax.broadcasted_iota(jnp.int32, (RB, LANES), 1)
    low = lane < HALF
    slot = lane >> 5
    t0s, t9s = [], []
    for j in range(4):
        rows = slice(RB * j, RB * (j + 1))
        add_first = pltpu.roll(halo[1], (HALF - QTR * j) % LANES, axis=1)
        add_last = pltpu.roll(halo[0], (QTR - QTR * j) % LANES, axis=1)
        e = edge_ref[rows, :] + jnp.where(slot == 2, add_first, jnp.where(slot == 1, add_last, 0.0))
        t0s.append(jnp.where(low, tb_ref[0, rows, :].astype(F32), e).astype(BF))
        t9s.append(jnp.where(low, e, tb_ref[9, rows, :].astype(F32)).astype(BF))
    to_rows(3, jnp.concatenate(t0s, axis=0), tb_ref[1])
    to_rows(4, tb_ref[SUB], jnp.concatenate(t9s, axis=0))
    columns(1)

    for cp in swaps:
        cp.wait_recv()

    def rows_dft(half, rhs):
        total, k0 = None, 0
        for grp in range(2):
            kk = 4 * GROUPS[grp][1]
            part = jnp.dot(eu_ref[x, half, :, k0:k0 + kk], rhs(grp), preferred_element_type=F32)
            total = part if total is None else total + part
            k0 += kk
        return total[:PB], total[PB:]

    quarter = lax.broadcasted_iota(jnp.int32, (PB // 4, LANES), 1) >> 5

    def rest(half):
        i_re, i_im = rows_dft(half, lambda g: hrs[g][...].reshape(4 * GROUPS[g][1], LANES))
        rows = pl.ds(pl.multiple_of(half * PB, SUB), PB)
        s_re, s_im = s_rem[0, rows, :], s_rem[1, rows, :]

        def fold(v):
            v = v + pltpu.roll(v, LANES - QTR, axis=1)
            return v + pltpu.roll(v, LANES - WIN, axis=1)

        re, im = fold(s_re * i_re + s_im * i_im), fold(s_re * i_im - s_im * i_re)
        return jnp.where(lane & (HALF - 1) < WIN, re, pltpu.roll(im, WIN, axis=1))

    def piece(half, j, tail):
        dp = (x + j) % 2
        i_re, i_im = rows_dft(half, lambda g: jnp.concatenate([hms[g][dp, cp].reshape(4 * GROUPS[g][1], LANES) for cp in range(2)], axis=1))
        rows = pl.ds(pl.multiple_of(half * PB, SUB), PB)
        re, im = None, None
        for cp in range(2):
            cols = slice(LANES * cp, LANES * (cp + 1))
            s_re, s_im = s_main[j, 0, cp, rows, :], s_main[j, 1, cp, rows, :]
            a = s_re * i_re[:, cols] + s_im * i_im[:, cols]
            b = s_re * i_im[:, cols] - s_im * i_re[:, cols]
            re, im = (a, b) if re is None else (re + a, im + b)
        main = jnp.where(low, re + pltpu.roll(re, HALF, axis=1), im + pltpu.roll(im, HALF, axis=1))
        y = jnp.where(dp == 0, tail, pltpu.roll(tail, HALF, axis=1))
        out = y[:PB // 4]
        for g in range(1, 4):
            out = jnp.where(quarter == g, pltpu.roll(y[PB // 4 * g:PB // 4 * (g + 1)], QTR * g, axis=1), out)
        return main, out

    sends = []
    far_tail = rest(1 - k)
    for i, (half, j) in enumerate(((1 - k, 1), (1 - k, 0), (k, 1))):
        if i == 2:
            own_tail = rest(k)
        pieces[i, :PB], pieces[i, PB:] = piece(half, j, own_tail if i == 2 else far_tail)
        sends.append(remote(pieces.at[i], recvs.at[i], red_ss, red_rs, i, homes[i]))
    main, rem = piece(k, 0, own_tail)
    for i in (2, 1, 0):
        sends[i].wait_recv()
        main = main + recvs[i, :PB]
        rem = rem + recvs[i, PB:]
    for o in range(2):
        m = pltpu.roll(main, HALF, axis=1) if o else main
        for j in range(4):
            rows = slice(PB // 4 * j, PB // 4 * (j + 1))
            tail = pltpu.roll(rem, (HALF - QTR * j - WIN * o) % LANES, axis=1)
            out_ref[o, rows, :] = (jnp.where(low[rows], m[rows], tail) * dd[rows])[:, :QB]

    for cp in sends + swaps:
        cp.wait_send()


def solution(mesh):
    sample_spec = ('exam', 'rows', 'cols')
    vm = pl.BlockSpec(memory_space=pltpu.VMEM)
    hbm = pl.BlockSpec(memory_space=pltpu.HBM)
    spread_scratch = ([VMEM((NG * CW, LANES), F32)] * T + [VMEM((LANES, LANES), F32)] * 4 + [VMEM((LANES * PS, LANES), F32)] * 2
                      + [VMEM((LANES, 768), BF), VMEM((NB, LANES), jnp.int32), pltpu.SMEM((NB, LANES), jnp.int32), pltpu.SemaphoreType.DMA])
    big = 28 * 1024 * 1024

    def local_fn(kspace, wts_y, wts_x, idx_y, idx_x, coil_maps, deapod):
        own, far = pl.pallas_call(
            prep_kernel,
            out_shape=[jax.ShapeDtypeStruct((24, NS), F32)] * 2,
            in_specs=[hbm] * 5, out_specs=[vm] * 2, name='prep',
            scratch_shapes=[VMEM((2, SUB, NS), F32), VMEM((KW, NS), F32), VMEM((KW, NS), F32), VMEM((NB, LANES), jnp.int32), VMEM((NB, LANES), jnp.int32), pltpu.SemaphoreType.DMA((5,))],
            compiler_params=pltpu.CompilerParams(vmem_limit_bytes=SUB * 1024 * 1024),
        )(*[pltpu.with_memory_space_constraint(v, pltpu.HBM) for v in (kspace, wts_y, wts_x, idx_y.reshape(NB, LANES), idx_x.reshape(NB, LANES))])
        far_in = lax.ppermute(far, 'cols', [(0, 1), (1, 0)])
        maps, _ = lax.optimization_barrier((jnp.swapaxes(coil_maps, 2, 3), far))
        half = pl.pallas_call(
            own_kernel, out_shape=jax.ShapeDtypeStruct((11, CW, LANES), F32), in_specs=[vm], out_specs=vm,
            scratch_shapes=spread_scratch, compiler_params=pltpu.CompilerParams(vmem_limit_bytes=big), name='spread_own',
            cost_estimate=pl.CostEstimate(flops=4 * 10 ** 9, bytes_accessed=2 * 10 ** 6, transcendentals=0),
        )(own)
        tb, edge, pack = pl.pallas_call(
            far_kernel,
            out_shape=(jax.ShapeDtypeStruct((10, N_GRID, LANES), BF), jax.ShapeDtypeStruct((N_GRID, LANES), F32), jax.ShapeDtypeStruct((2, RB, LANES), F32)),
            in_specs=[vm, vm], out_specs=(vm, vm, vm), scratch_shapes=[VMEM((N_GRID, LANES), F32)] + spread_scratch,
            compiler_params=pltpu.CompilerParams(vmem_limit_bytes=big), name='spread_far',
            cost_estimate=pl.CostEstimate(flops=4 * 10 ** 9, bytes_accessed=4 * 10 ** 6, transcendentals=0),
        )(far_in, half)
        maps_x = lax.ppermute(maps, 'rows', [(i, (i + 2) % ROWS) for i in range(ROWS)])
        dma = pltpu.SemaphoreType.DMA
        half_bufs = [VMEM((2, 2, 2, n, LANES), BF) for _, n in GROUPS] + [VMEM((2, n, LANES), BF) for _, n in GROUPS]
        full_bufs = [VMEM((2, 2, 2, 2, n, LANES), BF) for _, n in GROUPS] + [VMEM((2, 2, n, LANES), BF) for _, n in GROUPS]
        return pl.pallas_call(
            image_kernel,
            out_shape=jax.ShapeDtypeStruct((2, PB, QB), F32), in_specs=[vm] * 9, out_specs=vm,
            scratch_shapes=[VMEM((4 * RB, 2 * N_GRID), BF), VMEM((2, RB, LANES), F32)] + half_bufs + full_bufs + [
                VMEM((2, 2, 2, N_IMG, LANES), F32), VMEM((2, N_IMG, LANES), F32), VMEM((3, PB + PB // 4, LANES), F32), VMEM((3, PB + PB // 4, LANES), F32),
                dma((2,)), dma((2,)), dma((4,)), dma((4,)), dma((3,)), dma((3,)),
            ],
            compiler_params=pltpu.CompilerParams(vmem_limit_bytes=20 * 1024 * 1024, collective_id=0, has_side_effects=True), name='image',
        )(tb, edge, pack, maps, maps_x, deapod.reshape(1, N_IMG), col_dft(), row_dft(), unmix())

    return jax.shard_map(
        local_fn,
        mesh=mesh,
        in_specs=(P(None, None, sample_spec), P(None, sample_spec), P(None, sample_spec), P(sample_spec), P(sample_spec), P(None, ('exam', 'cols'), None, 'rows'), P()),
        out_specs=P(None, ('exam', 'cols'), 'rows'),
        check_vma=False,
    )
```

```python
import functools
import math

import jax
import jax.numpy as jnp
import numpy as np
from jax import lax
from jax.experimental import pallas as pl
from jax.experimental.pallas import tpu as pltpu
from jax.sharding import PartitionSpec as P

BF = jnp.bfloat16
F32 = jnp.float32
VMEM = pltpu.VMEM
LANES = 128
MIB = 1 << 20
SUB, WIN, QTR, HALF, WIDE = 8, 16, 32, 64, 256
N_GRID, N_IMG, N_COILS, KW = 640, 320, 8, 6
ROWS, COLS = 4, 2
RB, CB, QB = N_GRID // ROWS, N_GRID // COLS, N_IMG // ROWS
PB = N_IMG // COLS
NS = 4096
NB = NS // LANES
NG = 21
CW = CB + WIN
T = 6
PS = 9
ORDER = tuple(range(1, 9)) + (0, 9)
GROUPS = ((0, 128), (128, 32))
MESH_ID = pl.DeviceIdType.MESH


def dft_parts():
    freq = np.arange(N_GRID) - N_GRID // 2
    pos = np.arange(N_IMG) - N_IMG // 2
    ang = ((freq[:, None] * pos[None, :]) % N_GRID).astype(np.float32) * np.float32(2.0 * math.pi / N_GRID)
    norm = np.float32(1.0 / math.sqrt(N_GRID))
    c, s = np.cos(ang) * norm, np.sin(ang) * norm
    return np.stack([np.stack([c, s], 1), np.stack([-s, c], 1)], 0)


def col_dft():
    e = dft_parts()
    out = np.zeros((2 * N_GRID, N_GRID), np.float32)
    for dp in range(2):
        for t in range(2):
            for h in range(2):
                q0 = QB * (2 * dp + h)
                l0 = LANES * (2 * dp + t) + HALF * h
                out[:, l0:l0 + HALF] = e[:, :, t, q0:q0 + HALF].reshape(2 * N_GRID, HALF)
    for t in range(2):
        for d in range(4):
            l0 = 4 * LANES + HALF * (d // 2) + WIN * (2 * t + d % 2)
            out[:, l0:l0 + WIN] = e[:, :, t, QB * d + HALF:QB * (d + 1)].reshape(2 * N_GRID, WIN)
    return jnp.asarray(out, BF)


def row_dft():
    e = dft_parts()
    rows = np.concatenate([np.arange(WIN * l, WIN * (l + 1)) for l in ORDER])
    chips = []
    for x in range(2):
        parts = []
        for start, n in GROUPS:
            for t in range(2):
                for b in range(2):
                    parts.append(e[t, (2 * x + b) * RB + rows[start:start + n]])
        m = np.concatenate(parts, 0)
        chips.append(np.concatenate([m[:, :, PB * h:PB * (h + 1)].reshape(N_GRID, N_IMG).T for h in range(2)], 0))
    return jnp.asarray(np.array(chips), BF)


def unmix():
    m = np.zeros((WIDE, WIDE), np.float32)
    for ch in range(SUB):
        for pp in range(2):
            for i in range(WIN):
                m[ch * QTR + WIN * pp + (i + SUB) % WIN, pp * 128 + i * SUB + ch] = 1.0
    return jnp.asarray(m, BF)


def prep_kernel(ks_hbm, wy_hbm, wx_hbm, iy_hbm, ix_hbm, maps_hbm, own_ref, far_ref, sp_ref, ks_ref, wy_ref, wx_ref, iy_ref, ix_ref, maps_ref, sem):
    k = lax.axis_index('cols')
    r = lax.axis_index('rows')
    loads = []
    for src, dst in ((iy_hbm, iy_ref), (ix_hbm, ix_ref), (wx_hbm, wx_ref), (wy_hbm, wy_ref), (ks_hbm, ks_ref), (maps_hbm, maps_ref)):
        cp = pltpu.make_async_copy(src, dst, sem.at[len(loads)])
        cp.start()
        loads.append(cp)
    loads[0].wait()
    loads[1].wait()
    iy = iy_ref[...]
    base = (((iy - r * RB + 5) >> 3) * CW + (ix_ref[...] - k * CB + 5)).astype(F32)
    sh = ((iy + 5) & 15).astype(F32)
    loads[2].wait()
    loads[3].wait()
    zero2 = jnp.zeros((2, NS), F32)
    for ref in (own_ref, far_ref):
        ref[SUB:WIN, :] = jnp.concatenate([wx_ref[...], zero2], axis=0)
        ref[WIN:24, :] = jnp.concatenate([wy_ref[...], zero2], axis=0)
        for b in range(NB):
            ref[22:24, LANES * b:LANES * (b + 1)] = jnp.concatenate([sh[b:b + 1, :], base[b:b + 1, :]], axis=0)
    loads[4].wait()
    lo = jnp.concatenate([ks_ref[0, 0:4, :], ks_ref[1, 0:4, :]], axis=0)
    hi = jnp.concatenate([ks_ref[0, 4:SUB, :], ks_ref[1, 4:SUB, :]], axis=0)
    own_ref[0:SUB, :] = jnp.where(k == 0, lo, hi)
    far_ref[0:SUB, :] = jnp.where(k == 0, hi, lo)
    loads[5].wait()
    for c in range(4):
        for i in range(2):
            sp_ref[c, :, WIDE * i:WIDE * (i + 1)] = maps_ref[i, c, :, :WIDE]
        sp_ref[c, :, 512:] = jnp.concatenate([maps_ref[i, c, :, WIDE:] for i in range(2)], axis=1)


def split3(x):
    hi = x.astype(BF).astype(F32)
    r = x - hi
    mid = r.astype(BF).astype(F32)
    return hi, mid, r - mid


def accumulate(pay_ref, accs, us, xs, vs, r_ref, int_ref, base_ref, sem):
    row_i = lax.broadcasted_iota(jnp.int32, (WIN, LANES), 0)

    def make_u(blk, k):
        off = pl.multiple_of(jnp.minimum(blk, NB - 1) * LANES, LANES)
        y8 = pay_ref[0:SUB, pl.ds(off, LANES)]
        wyp = pay_ref[WIN:24, pl.ds(off, LANES)]
        d = (row_i - wyp[6:7, :].astype(jnp.int32)) & 15
        p = jnp.zeros((WIN, LANES), F32)
        for a in range(KW):
            p = jnp.where(d == a, wyp[a:a + 1, :], p)
        us[k][...] = jnp.concatenate([y8 * p[i:i + 1, :] for i in range(WIN)], axis=0).T
        x3 = list(split3(pay_ref[SUB:WIN, pl.ds(off, LANES)])) + [jnp.zeros((104, LANES), F32)]
        xs[k][...] = jnp.concatenate(x3, axis=0).T

    def make_v(k):
        lhs = xs[k][...].astype(BF)
        u = us[k][...]
        for bp in range(3):
            w = jnp.dot(lhs, r_ref[:, WIDE * bp:WIDE * bp + WIDE], preferred_element_type=F32)
            for c in range(2):
                v = w[:, LANES * c:LANES * (c + 1)] * u
                for g in range(WIN):
                    vs[k][pl.ds(SUB * PS * g + 2 * bp + c, SUB, stride=PS), :] = v[SUB * g:SUB * g + SUB, :]

    def add_tiles(blk, k):
        for j in range(LANES):
            acc = accs[j % T]
            b = base_ref[blk, j]
            acc[pl.ds(b, SUB), :] = acc[pl.ds(b, SUB), :] + vs[k][PS * j:PS * j + SUB, :]

    def clear(n, _):
        for a in accs:
            a[pl.ds(pl.multiple_of(n * CW, SUB), CW), :] = jnp.zeros((CW, LANES), F32)
        return 0

    for b in range(NB):
        int_ref[b:b + 1, :] = pay_ref[23:24, LANES * b:LANES * (b + 1)].astype(jnp.int32)
    lax.fori_loop(0, NG, clear, 0)
    load = pltpu.make_async_copy(int_ref, base_ref, sem)
    load.start()
    kk = lax.broadcasted_iota(jnp.int32, (LANES, 768), 0)
    ll = lax.broadcasted_iota(jnp.int32, (LANES, 768), 1)
    r_ref[...] = jnp.where((kk < 24) & ((kk & 7) == (ll >> 7)), 1.0, 0.0).astype(BF)
    for v in vs:
        v[...] = jnp.zeros_like(v)
    make_u(0, 0)
    make_u(1, 1)
    make_v(0)
    load.wait()

    def body(n, _):
        k = 2 * n
        make_v(1)
        add_tiles(k, 0)
        make_u(k + 2, 0)
        make_v(0)
        add_tiles(k + 1, 1)
        make_u(k + 3, 1)
        return 0

    lax.fori_loop(0, NB // 2, body, 0)


def folded(accs, off, n):
    def total(g):
        o = pl.multiple_of(g * CW + off, SUB)
        s = accs[0][pl.ds(o, n), :]
        for a in accs[1:]:
            s = s + a[pl.ds(o, n), :]
        return s

    high = lax.broadcasted_iota(jnp.int32, (n, LANES), 1) >= HALF
    even = [total(2 * p) for p in range(11)]
    tiles = [total(2 * p + 1) + jnp.where(high, even[p], even[p + 1]) for p in range(10)]
    return tiles + [jnp.where(high, even[10], even[0])]


def own_kernel(pay_ref, out_ref, *scr):
    accs = scr[:T]
    accumulate(pay_ref, accs, scr[T:T + 2], scr[T + 2:T + 4], scr[T + 4:T + 6], *scr[T + 6:])

    def fold(q, _):
        off = pl.multiple_of(q * SUB, SUB)
        for p, t in enumerate(folded(accs, off, SUB)):
            out_ref[p, pl.ds(off, SUB), :] = t
        return 0

    lax.fori_loop(0, CW // SUB, fold, 0)


def far_kernel(pay_ref, a_ref, tb_ref, edge_ref, pack_ref, gh_ref, *scr):
    accs = scr[:T]
    accumulate(pay_ref, accs, scr[T:T + 2], scr[T + 2:T + 4], scr[T + 4:T + 6], *scr[T + 6:])
    k = lax.axis_index('cols')
    own0 = k * CB
    far0 = CB - own0
    high = lax.broadcasted_iota(jnp.int32, (SUB, LANES), 1) >= HALF

    left = folded(accs, 0, SUB)
    right = folded(accs, CW - SUB, SUB)
    for src, dst in ((CW - SUB, SUB), (0, CB)):
        for p in range(10):
            rows = pl.ds((2 * p + 1) * CW + dst, SUB)
            accs[0][rows, :] = accs[0][rows, :] + a_ref[p, src:src + SUB, :]
        ghost = a_ref[10, src:src + SUB, :]
        accs[0][dst:dst + SUB, :] = accs[0][dst:dst + SUB, :] + jnp.where(high, 0.0, ghost)
        rows = pl.ds(20 * CW + dst, SUB)
        accs[0][rows, :] = accs[0][rows, :] + jnp.where(high, ghost, 0.0)

    high16 = lax.broadcasted_iota(jnp.int32, (WIN, LANES), 1) >= HALF

    def put(v, tiles):
        v = pl.multiple_of(v, WIN)
        for p in range(10):
            tb_ref[p, pl.ds(v, WIN), :] = tiles[p].astype(BF)
        edge_ref[pl.ds(v, WIN), :] = jnp.where(high16, tiles[0], tiles[9])
        gh_ref[pl.ds(v, WIN), :] = tiles[10]

    def far_part(s, _):
        put(far0 + WIN * s, folded(accs, pl.multiple_of(SUB + WIN * s, SUB), WIN))
        return 0

    lax.fori_loop(0, CB // WIN, far_part, 0)

    def own_part(s, _):
        put(own0 + WIN * s, [a_ref[p, pl.ds(pl.multiple_of(SUB + WIN * s, SUB), WIN), :] for p in range(11)])
        return 0

    lax.fori_loop(1, CB // WIN - 1, own_part, 0)
    put(own0, [jnp.concatenate([a_ref[p, SUB:WIN, :] + right[p], a_ref[p, WIN:24, :]], axis=0) for p in range(11)])
    put(own0 + CB - WIN, [jnp.concatenate([a_ref[p, CB - SUB:CB, :], a_ref[p, CB:CB + SUB, :] + left[p]], axis=0) for p in range(11)])

    slot = lax.broadcasted_iota(jnp.int32, (RB, LANES), 1) >> 5
    for side, lane0 in ((0, QTR), (1, HALF)):
        out = jnp.zeros((RB, LANES), F32)
        for j in range(4):
            piece = pltpu.roll(gh_ref[RB * j:RB * (j + 1), :], (QTR * j - lane0) % LANES, axis=1)
            out = jnp.where(slot == j, piece, out)
        pack_ref[side] = out


def image_kernel(tb_ref, edge_ref, pack_ref, so_ref, sx_ref, d_ref, ev_ref, eu_ref, pm_ref, out_ref,
                 g_ref, halo, sm1, sm2, sr1, sr2, hm1, hm2, hr1, hr2, s_main, s_rem, acc_m, acc_r, pieces, recvs,
                 halo_ss, halo_rs, swap_ss, swap_rs, red_ss, red_rs):
    k = lax.axis_index('cols')
    r = lax.axis_index('rows')
    core, x = r % 2, r // 2
    near = r + 1 - 2 * core
    across = (r + 2) % 4
    prev, nxt = (r + 3) % 4, (r + 1) % 4
    homes = ({'rows': across, 'cols': 1 - k}, {'cols': 1 - k}, {'rows': across})

    barrier = pltpu.get_barrier_semaphore()
    for dev in ({'rows': prev}, {'rows': nxt}) + homes:
        pl.semaphore_signal(barrier, inc=1, device_id=dev, device_id_type=MESH_ID)
    pl.semaphore_wait(barrier, 5)

    def remote(src, dst, ss, rs, i, dev):
        cp = pltpu.make_async_remote_copy(src_ref=src, dst_ref=dst, send_sem=ss.at[i], recv_sem=rs.at[i], device_id=dev, device_id_type=MESH_ID)
        cp.start()
        return cp

    halos = [remote(pack_ref.at[i], halo.at[i], halo_ss, halo_rs, i, {'rows': dev}) for i, dev in ((0, prev), (1, nxt))]

    def to_rows(row0, n, t0, t1):
        a = jnp.concatenate([t0, t1], axis=1)
        g = lax.dot_general(pm_ref[...], a, (((1,), (1,)), ((), ())), preferred_element_type=F32).astype(BF)
        for ch in range(SUB):
            i, c = ch // 4, ch % 4
            g_ref[row0 + n * c:row0 + n * c + QTR, N_GRID * i:N_GRID * (i + 1)] = g[QTR * ch:QTR * (ch + 1), :]

    for m in range(4):
        to_rows(QTR * m, LANES, tb_ref[2 * m + 1], tb_ref[2 * m + 2])

    sms, srs, hms, hrs = (sm1, sm2), (sr1, sr2), (hm1, hm2), (hr1, hr2)
    swaps = []

    def columns(grp):
        start, n = GROUPS[grp]
        lane = lax.broadcasted_iota(jnp.int32, (n, LANES), 1)
        side = lane >> 6
        own_even, far_even = side == core, side != core
        block = (lane & (HALF - 1)) >> 4
        h = jnp.dot(g_ref[4 * start:4 * (start + n), :], ev_ref[...], preferred_element_type=F32)
        hc = [h[n * c:n * (c + 1)] for c in range(4)]
        rems = [v[:, 4 * LANES:] for v in hc]
        for cp in range(2):
            hs = [[v[:, LANES * i:LANES * (i + 1)] for i in range(4)] for v in hc[2 * cp:2 * cp + 2]]
            for i in range(4):
                dp, t = i // 2, i % 2
                odd = pltpu.roll(hs[1][i], HALF, axis=1)
                sms[grp][dp, cp, t] = jnp.where(far_even, hs[0][i], odd).astype(BF)
                hms[grp][dp, cp, t, core] = jnp.where(own_even, hs[0][i], odd).astype(BF)
        for t in range(2):
            both = []
            for h in range(2):
                i = 2 * t + h
                out = rems[i]
                for c in range(4):
                    if c != i:
                        out = jnp.where(block == c, pltpu.roll(rems[c], (WIN * (c - i)) % LANES, axis=1), out)
                both.append(out)
            srs[grp][t] = jnp.where(core == 0, both[1], both[0]).astype(BF)
            hrs[grp][t, core] = jnp.where(core == 0, both[0], both[1]).astype(BF)
        swaps.append(remote(sms[grp], hms[grp].at[:, :, :, core], swap_ss, swap_rs, 2 * grp, {'rows': near}))
        swaps.append(remote(srs[grp], hrs[grp].at[:, core], swap_ss, swap_rs, 2 * grp + 1, {'rows': near}))

    columns(0)

    def turn(rows):
        t = [rows[:, LANES * i:LANES * (i + 1)].T for i in range(5)]
        return [jnp.concatenate([t[2 * i], t[2 * i + 1], t[4][HALF * i:HALF * (i + 1)]], axis=0) for i in range(2)]

    for j, ref in enumerate((so_ref, sx_ref)):
        for cp in range(2):
            s_main[j, 0, cp], s_main[j, 1, cp] = turn(jnp.concatenate([ref[2 * cp + core, :HALF, :], ref[2 * cp + 1 - core, :HALF, :]], axis=0))
    last = [[ref[c, HALF:, :] for c in range(4)] for ref in (so_ref, sx_ref)]
    s_rem[0], s_rem[1] = turn(jnp.concatenate([jnp.where(x == j, last[0][c], last[1][c]) for j in range(2) for c in range(4)], axis=0))
    d8 = jnp.broadcast_to(jnp.concatenate([d_ref[...], jnp.zeros((1, HALF), F32)], axis=1), (SUB, N_IMG + HALF))
    dq = d8
    for j in range(1, ROWS):
        dq = jnp.where(r == j, pltpu.roll(d8, N_IMG + HALF - QB * j, axis=1), dq)
    dp = jnp.where(k == 0, d8, pltpu.roll(d8, N_IMG + HALF - PB, axis=1))[:, :2 * LANES]
    dd = jnp.concatenate([dp] * WIN, axis=0).T[:PB] * dq[:1, :LANES]

    for cp in swaps:
        cp.wait_recv()
    n0 = 4 * GROUPS[0][1]

    def block_of(grp, j):
        return jnp.concatenate([hms[grp][(x + j) % 2, cp].reshape(4 * GROUPS[grp][1], LANES) for cp in range(2)], axis=1)

    for j in range(2):
        acc_m[j] = jnp.dot(eu_ref[x, :, :n0], block_of(0, j), preferred_element_type=F32)
    acc_r[...] = jnp.dot(eu_ref[x, :, :n0], hrs[0][...].reshape(n0, LANES), preferred_element_type=F32)

    for h in halos:
        h.wait()
    lane = lax.broadcasted_iota(jnp.int32, (RB, LANES), 1)
    low = lane < HALF
    slot = lane >> 5
    t0s, t9s = [], []
    for j in range(4):
        rows = slice(RB * j, RB * (j + 1))
        add_first = pltpu.roll(halo[1], (HALF - QTR * j) % LANES, axis=1)
        add_last = pltpu.roll(halo[0], (QTR - QTR * j) % LANES, axis=1)
        e = edge_ref[rows, :] + jnp.where(slot == 2, add_first, jnp.where(slot == 1, add_last, 0.0))
        t0s.append(jnp.where(low, tb_ref[0, rows, :].astype(F32), e).astype(BF))
        t9s.append(jnp.where(low, e, tb_ref[9, rows, :].astype(F32)).astype(BF))
    to_rows(4 * LANES, QTR, jnp.concatenate(t0s, axis=0), jnp.concatenate(t9s, axis=0))
    columns(1)
    for cp in swaps[2:]:
        cp.wait_recv()

    def rows_dft(half, acc, rhs):
        rows = pl.ds(pl.multiple_of(half * N_IMG, WIN), N_IMG)
        total = acc[rows, :] + jnp.dot(eu_ref[x, rows, n0:], rhs, preferred_element_type=F32)
        return total[:PB], total[PB:]

    quarter = lax.broadcasted_iota(jnp.int32, (PB // 4, LANES), 1) >> 5

    def rest(half):
        i_re, i_im = rows_dft(half, acc_r, hrs[1][...].reshape(4 * GROUPS[1][1], LANES))
        rows = pl.ds(pl.multiple_of(half * PB, SUB), PB)
        s_re, s_im = s_rem[0, rows, :], s_rem[1, rows, :]

        def fold(v):
            v = v + pltpu.roll(v, LANES - QTR, axis=1)
            return v + pltpu.roll(v, LANES - WIN, axis=1)

        re, im = fold(s_re * i_re + s_im * i_im), fold(s_re * i_im - s_im * i_re)
        return jnp.where(lane & (HALF - 1) < WIN, re, pltpu.roll(im, WIN, axis=1))

    def piece(half, j, tail):
        dp = (x + j) % 2
        i_re, i_im = rows_dft(half, acc_m.at[j], block_of(1, j))
        rows = pl.ds(pl.multiple_of(half * PB, SUB), PB)
        re, im = None, None
        for cp in range(2):
            cols = slice(LANES * cp, LANES * (cp + 1))
            s_re, s_im = s_main[j, 0, cp, rows, :], s_main[j, 1, cp, rows, :]
            a = s_re * i_re[:, cols] + s_im * i_im[:, cols]
            b = s_re * i_im[:, cols] - s_im * i_re[:, cols]
            re, im = (a, b) if re is None else (re + a, im + b)
        main = jnp.where(low, re + pltpu.roll(re, HALF, axis=1), im + pltpu.roll(im, HALF, axis=1))
        y = jnp.where(dp == 0, tail, pltpu.roll(tail, HALF, axis=1))
        out = y[:PB // 4]
        for g in range(1, 4):
            out = jnp.where(quarter == g, pltpu.roll(y[PB // 4 * g:PB // 4 * (g + 1)], QTR * g, axis=1), out)
        return main, out

    sends = []
    far_tail = rest(1 - k)
    for i, (half, j) in enumerate(((1 - k, 1), (1 - k, 0), (k, 1))):
        if i == 2:
            own_tail = rest(k)
        pieces[i, :PB], pieces[i, PB:] = piece(half, j, own_tail if i == 2 else far_tail)
        sends.append(remote(pieces.at[i], recvs.at[i], red_ss, red_rs, i, homes[i]))
    main, rem = piece(k, 0, own_tail)
    for i in (2, 1, 0):
        sends[i].wait_recv()
        main = main + recvs[i, :PB]
        rem = rem + recvs[i, PB:]
    for o in range(2):
        m = pltpu.roll(main, HALF, axis=1) if o else main
        for j in range(4):
            rows = slice(PB // 4 * j, PB // 4 * (j + 1))
            tail = pltpu.roll(rem, (HALF - QTR * j - WIN * o) % LANES, axis=1)
            out_ref[o, rows, :] = (jnp.where(low[rows], m[rows], tail) * dd[rows])[:, :QB]

    for cp in sends + swaps:
        cp.wait_send()


def solution(mesh):
    sample_spec = ('exam', 'rows', 'cols')
    vm = pl.BlockSpec(memory_space=pltpu.VMEM)
    hbm = pl.BlockSpec(memory_space=pltpu.HBM)
    spread_scratch = ([VMEM((NG * CW, LANES), F32)] * T + [VMEM((LANES, LANES), F32)] * 4 + [VMEM((LANES * PS, LANES), F32)] * 2
                      + [VMEM((LANES, 768), BF), VMEM((NB, LANES), jnp.int32), pltpu.SMEM((NB, LANES), jnp.int32), pltpu.SemaphoreType.DMA])
    big = 28 * MIB

    def local_fn(kspace, wts_y, wts_x, idx_y, idx_x, coil_maps, deapod):
        own, far, maps = pl.pallas_call(
            prep_kernel,
            out_shape=[jax.ShapeDtypeStruct((24, NS), F32)] * 2 + [jax.ShapeDtypeStruct((4, QB, N_GRID), F32)],
            in_specs=[hbm] * 6, out_specs=[vm] * 3, name='prep',
            scratch_shapes=[VMEM((2, SUB, NS), F32), VMEM((KW, NS), F32), VMEM((KW, NS), F32), VMEM((NB, LANES), jnp.int32), VMEM((NB, LANES), jnp.int32), VMEM((2, 4, QB, N_IMG), F32), pltpu.SemaphoreType.DMA((6,))],
            compiler_params=pltpu.CompilerParams(vmem_limit_bytes=SUB * MIB),
        )(*[pltpu.with_memory_space_constraint(v, pltpu.HBM) for v in (kspace, wts_y, wts_x, idx_y.reshape(NB, LANES), idx_x.reshape(NB, LANES), jnp.swapaxes(coil_maps, 2, 3))])
        far_in = lax.ppermute(far, 'cols', [(0, 1), (1, 0)])
        half = pl.pallas_call(
            own_kernel, out_shape=jax.ShapeDtypeStruct((11, CW, LANES), F32), in_specs=[vm], out_specs=vm,
            scratch_shapes=spread_scratch, compiler_params=pltpu.CompilerParams(vmem_limit_bytes=big), name='spread_own',
            cost_estimate=pl.CostEstimate(flops=4 * 10 ** 9, bytes_accessed=2 * 10 ** 6, transcendentals=0),
        )(own)
        tb, edge, pack = pl.pallas_call(
            far_kernel,
            out_shape=(jax.ShapeDtypeStruct((10, N_GRID, LANES), BF), jax.ShapeDtypeStruct((N_GRID, LANES), F32), jax.ShapeDtypeStruct((2, RB, LANES), F32)),
            in_specs=[vm, vm], out_specs=(vm, vm, vm), scratch_shapes=[VMEM((N_GRID, LANES), F32)] + spread_scratch,
            compiler_params=pltpu.CompilerParams(vmem_limit_bytes=big), name='spread_far',
            cost_estimate=pl.CostEstimate(flops=4 * 10 ** 9, bytes_accessed=4 * 10 ** 6, transcendentals=0),
        )(far_in, half)
        maps_x = lax.ppermute(maps, 'rows', [(i, (i + 2) % ROWS) for i in range(ROWS)])
        dma = pltpu.SemaphoreType.DMA
        half_bufs = [VMEM((2, 2, 2, n, LANES), BF) for _, n in GROUPS] + [VMEM((2, n, LANES), BF) for _, n in GROUPS]
        full_bufs = [VMEM((2, 2, 2, 2, n, LANES), BF) for _, n in GROUPS] + [VMEM((2, 2, n, LANES), BF) for _, n in GROUPS]
        return pl.pallas_call(
            image_kernel,
            out_shape=jax.ShapeDtypeStruct((2, PB, QB), F32), in_specs=[vm] * 9, out_specs=vm,
            scratch_shapes=[VMEM((4 * RB, 2 * N_GRID), BF), VMEM((2, RB, LANES), F32)] + half_bufs + full_bufs + [
                VMEM((2, 2, 2, N_IMG, LANES), F32), VMEM((2, N_IMG, LANES), F32),
                VMEM((2, 2 * N_IMG, 2 * LANES), F32), VMEM((2 * N_IMG, LANES), F32), VMEM((3, PB + PB // 4, LANES), F32), VMEM((3, PB + PB // 4, LANES), F32),
                dma((2,)), dma((2,)), dma((4,)), dma((4,)), dma((3,)), dma((3,)),
            ],
            compiler_params=pltpu.CompilerParams(vmem_limit_bytes=20 * MIB, collective_id=0, has_side_effects=True), name='image',
        )(tb, edge, pack, maps, maps_x, deapod.reshape(1, N_IMG), col_dft(), row_dft(), unmix())

    return jax.shard_map(
        local_fn,
        mesh=mesh,
        in_specs=(P(None, None, sample_spec), P(None, sample_spec), P(None, sample_spec), P(sample_spec), P(sample_spec), P(None, ('exam', 'cols'), None, 'rows'), P()),
        out_specs=P(None, ('exam', 'cols'), 'rows'),
        check_vma=False,
    )
```

```python
import functools
import math

import jax
import jax.numpy as jnp
import numpy as np
from jax import lax
from jax.experimental import pallas as pl
from jax.experimental.pallas import tpu as pltpu
from jax.sharding import PartitionSpec as P

BF = jnp.bfloat16
F32 = jnp.float32
VMEM = pltpu.VMEM
LANES = 128
MIB = 1 << 20
SUB, WIN, QTR, HALF, WIDE = 8, 16, 32, 64, 256
N_GRID, N_IMG, N_COILS, KW = 640, 320, 8, 6
ROWS, COLS = 4, 2
RB, CB, QB = N_GRID // ROWS, N_GRID // COLS, N_IMG // ROWS
PB = N_IMG // COLS
NS = 4096
NB = NS // LANES
NG = 21
CW = CB + WIN
T = 6
PS = 9
PAY = 21
CODE = 512
HW = 24
ORDER = tuple(range(1, 9)) + (0, 9)
GROUPS = ((0, 128), (128, 32))
MESH_ID = pl.DeviceIdType.MESH


def dft_parts():
    freq = np.arange(N_GRID) - N_GRID // 2
    pos = np.arange(N_IMG) - N_IMG // 2
    ang = ((freq[:, None] * pos[None, :]) % N_GRID).astype(np.float32) * np.float32(2.0 * math.pi / N_GRID)
    norm = np.float32(1.0 / math.sqrt(N_GRID))
    c, s = np.cos(ang) * norm, np.sin(ang) * norm
    return np.stack([np.stack([c, s], 1), np.stack([-s, c], 1)], 0)


def col_dft():
    e = dft_parts()
    out = np.zeros((2 * N_GRID, N_GRID), np.float32)
    for dp in range(2):
        for t in range(2):
            for h in range(2):
                q0 = QB * (2 * dp + h)
                l0 = LANES * (2 * dp + t) + HALF * h
                out[:, l0:l0 + HALF] = e[:, :, t, q0:q0 + HALF].reshape(2 * N_GRID, HALF)
    for t in range(2):
        for d in range(4):
            l0 = 4 * LANES + HALF * (d // 2) + WIN * (2 * t + d % 2)
            out[:, l0:l0 + WIN] = e[:, :, t, QB * d + HALF:QB * (d + 1)].reshape(2 * N_GRID, WIN)
    return jnp.asarray(out, BF)


def row_dft():
    e = dft_parts()
    rows = np.concatenate([np.arange(WIN * l, WIN * (l + 1)) for l in ORDER])
    chips = []
    for x in range(2):
        parts = []
        for start, n in GROUPS:
            for t in range(2):
                for b in range(2):
                    parts.append(e[t, (2 * x + b) * RB + rows[start:start + n]])
        m = np.concatenate(parts, 0)
        chips.append(np.concatenate([m[:, :, PB * h:PB * (h + 1)].reshape(N_GRID, N_IMG).T for h in range(2)], 0))
    return jnp.asarray(np.array(chips), BF)


def unmix():
    m = np.zeros((WIDE, WIDE), np.float32)
    for ch in range(SUB):
        for pp in range(2):
            for i in range(WIN):
                m[ch * QTR + WIN * pp + (i + SUB) % WIN, pp * 128 + i * SUB + ch] = 1.0
    return jnp.asarray(m, BF)


def prep_kernel(ks_hbm, wy_hbm, wx_hbm, iy_hbm, ix_hbm, maps_hbm, own_ref, far_ref, sp_ref, ks_ref, wy_ref, wx_ref, iy_ref, ix_ref, maps_ref, sem):
    k = lax.axis_index('cols')
    r = lax.axis_index('rows')
    loads = []
    for src, dst in ((iy_hbm, iy_ref), (ix_hbm, ix_ref), (wx_hbm, wx_ref), (wy_hbm, wy_ref), (ks_hbm, ks_ref), (maps_hbm, maps_ref)):
        cp = pltpu.make_async_copy(src, dst, sem.at[len(loads)])
        cp.start()
        loads.append(cp)
    loads[0].wait()
    loads[1].wait()
    iy = iy_ref[...]
    code = ((iy - r * RB + 5) * CODE + ix_ref[...] - k * CB + 5).astype(F32)
    for i in range(2, 5):
        loads[i].wait()
    lo = jnp.concatenate([ks_ref[0, 0:4, :], ks_ref[1, 0:4, :]], axis=0)
    hi = jnp.concatenate([ks_ref[0, 4:SUB, :], ks_ref[1, 4:SUB, :]], axis=0)
    first = k == 0
    for ref, y in ((own_ref, jnp.where(first, lo, hi)), (far_ref, jnp.where(first, hi, lo))):
        for b in range(NB):
            cols = slice(LANES * b, LANES * (b + 1))
            ref[PAY * b:PAY * b + SUB, :] = y[:, cols]
            ref[PAY * b + SUB:PAY * b + SUB + KW, :] = wx_ref[:, cols]
            ref[PAY * (b + 1) - KW - 1:PAY * (b + 1) - 1, :] = wy_ref[:, cols]
            ref[PAY * (b + 1) - 1:PAY * (b + 1), :] = code[b:b + 1, :]
    loads[5].wait()
    for c in range(4):
        for i in range(2):
            sp_ref[c, :, WIDE * i:WIDE * (i + 1)] = maps_ref[i, c, :, :WIDE]
        sp_ref[c, :, 512:] = jnp.concatenate([maps_ref[i, c, :, WIDE:] for i in range(2)], axis=1)


def split3(x):
    hi = x.astype(BF).astype(F32)
    r = x - hi
    mid = r.astype(BF).astype(F32)
    return hi, mid, r - mid


def accumulate(pay_ref, accs, us, xs, vs, r_ref, int_ref, base_ref, sem):
    row_i = lax.broadcasted_iota(jnp.int32, (WIN, LANES), 0)

    def make_u(blk, k):
        off = jnp.minimum(blk, NB - 1) * PAY
        y8 = pay_ref[pl.ds(off, SUB), :]
        wx = pay_ref[pl.ds(off + SUB, SUB), :]
        wyp = pay_ref[pl.ds(off + PAY - SUB, SUB), :]
        d = (row_i - (wyp[7:, :].astype(jnp.int32) // CODE)) & (WIN - 1)
        p = jnp.zeros((WIN, LANES), F32)
        for a in range(KW):
            p = jnp.where(d == a, wyp[a + 1:a + 2, :], p)
        us[k][...] = jnp.concatenate([y8 * p[i:i + 1, :] for i in range(WIN)], axis=0).T
        x3 = list(split3(wx)) + [jnp.zeros((LANES - HW, LANES), F32)]
        xs[k][...] = jnp.concatenate(x3, axis=0).T

    def make_v(k):
        lhs = xs[k][...].astype(BF)
        u = us[k][...]
        for bp in range(3):
            w = jnp.dot(lhs, r_ref[:, WIDE * bp:WIDE * bp + WIDE], preferred_element_type=F32)
            for c in range(2):
                v = w[:, LANES * c:LANES * (c + 1)] * u
                for g in range(WIN):
                    vs[k][pl.ds(SUB * PS * g + 2 * bp + c, SUB, stride=PS), :] = v[SUB * g:SUB * g + SUB, :]

    def add_tiles(blk, k):
        for j in range(LANES):
            acc = accs[j % T]
            b = base_ref[blk, j]
            acc[pl.ds(b, SUB), :] = acc[pl.ds(b, SUB), :] + vs[k][PS * j:PS * j + SUB, :]

    code = jnp.concatenate([pay_ref[PAY * (b + 1) - 1:PAY * (b + 1), :] for b in range(NB)], axis=0).astype(jnp.int32)
    int_ref[...] = (code // (CODE * SUB)) * CW + (code & (CODE - 1))
    kk = lax.broadcasted_iota(jnp.int32, (LANES, WIDE * 3), 0)
    ll = lax.broadcasted_iota(jnp.int32, (LANES, WIDE * 3), 1)
    r_ref[...] = jnp.where((kk < HW) & ((kk & 7) == (ll >> 7)), 1.0, 0.0).astype(BF)
    for v in vs:
        v[...] = jnp.zeros_like(v)
    load = pltpu.make_async_copy(int_ref, base_ref, sem)
    load.start()
    make_u(0, 0)
    make_u(1, 1)
    make_v(0)
    load.wait()

    def body(n, _):
        k = 2 * n
        make_v(1)
        add_tiles(k, 0)
        make_u(k + 2, 0)
        make_v(0)
        add_tiles(k + 1, 1)
        make_u(k + 3, 1)
        return 0

    lax.fori_loop(0, NB // 2, body, 0)


def folded(accs, off, n, clear=False):
    def total(g):
        rows = pl.ds(pl.multiple_of(g * CW + off, SUB), n)
        v = accs[0][rows, :]
        for a in accs[1:]:
            v = v + a[rows, :]
        if clear:
            for a in accs:
                a[rows, :] = jnp.zeros((n, LANES), F32)
        return v

    high = lax.broadcasted_iota(jnp.int32, (n, LANES), 1) >= HALF
    even = [total(2 * p) for p in range(11)]
    tiles = [total(2 * p + 1) + jnp.where(high, even[p], even[p + 1]) for p in range(10)]
    return tiles + [jnp.where(high, even[10], even[0])]


def own_kernel(pay_ref, out_ref, *refs):
    accs, scr = refs[:T], refs[T:]

    def clear(n, _):
        for a in accs:
            a[pl.ds(pl.multiple_of(n * CW, SUB), CW), :] = jnp.zeros((CW, LANES), F32)
        return 0

    lax.fori_loop(0, NG, clear, 0)
    accumulate(pay_ref, accs, scr[:2], scr[2:4], scr[4:6], *scr[6:])

    def fold(q, _):
        off = pl.multiple_of(q * WIN, WIN)
        for p, t in enumerate(folded(accs, off, WIN, clear=True)):
            out_ref[p, pl.ds(off, WIN), :] = t
        return 0

    lax.fori_loop(0, CW // WIN, fold, 0)


def far_kernel(pay_ref, a_ref, *refs):
    accs, pack_ref, gh_ref, scr = refs[T:2 * T], refs[2 * T], refs[2 * T + 1], refs[2 * T + 2:]
    accumulate(pay_ref, accs, scr[:2], scr[2:4], scr[4:6], *scr[6:])
    own0 = lax.axis_index('cols') * CB
    far0 = CB - own0

    def ghost(off, n):
        high = lax.broadcasted_iota(jnp.int32, (n, LANES), 1) >= HALF
        ends = []
        for g in (0, NG - 1):
            rows = pl.ds(pl.multiple_of(g * CW + off, SUB), n)
            v = accs[0][rows, :]
            for a in accs[1:]:
                v = v + a[rows, :]
            ends.append(v)
        return jnp.where(high, ends[1], ends[0])

    def copy(n, _):
        o = pl.multiple_of(n * QTR, SUB)
        gh_ref[pl.ds(pl.multiple_of(far0 + o, SUB), QTR), :] = ghost(SUB + o, QTR)
        gh_ref[pl.ds(pl.multiple_of(own0 + o, SUB), QTR), :] = a_ref[10, pl.ds(pl.multiple_of(SUB + o, SUB), QTR), :]
        return 0

    lax.fori_loop(0, CB // QTR, copy, 0)
    for dst, add in ((own0, ghost(CW - SUB, SUB)), (own0 + CB - SUB, ghost(0, SUB)), (far0, a_ref[10, CW - SUB:, :]), (far0 + CB - SUB, a_ref[10, :SUB, :])):
        rows = pl.ds(pl.multiple_of(dst, SUB), SUB)
        gh_ref[rows, :] = gh_ref[rows, :] + add

    lane = lax.broadcasted_iota(jnp.int32, (LANES, LANES), 1)
    for side, lane0 in ((0, HALF - HW), (1, HALF)):
        out = jnp.zeros((LANES, LANES), F32)
        for j in range(5):
            piece = pltpu.roll(gh_ref[LANES * j:LANES * (j + 1), :], (HW * j - lane0) % LANES, axis=1)
            out = jnp.where(lane >= HW * j, piece, out)
        pack_ref[side] = out


def image_kernel(*refs):
    accs = refs[:T]
    (a_ref, pack_ref, so_ref, sx_ref, d_ref, ev_ref, eu_ref, pm_ref, out_ref,
     tb_ref, edge_ref, g_ref, halo, sm1, sm2, sr1, sr2, hm1, hm2, hr1, hr2, s_main, s_rem, acc_m, acc_r, pieces, recvs,
     halo_ss, halo_rs, swap_ss, swap_rs, red_ss, red_rs) = refs[T:]
    k = lax.axis_index('cols')
    r = lax.axis_index('rows')
    core, x = r % 2, r // 2
    near = r + 1 - 2 * core
    across = (r + 2) % 4
    prev, nxt = (r + 3) % 4, (r + 1) % 4
    homes = ({'rows': across, 'cols': 1 - k}, {'cols': 1 - k}, {'rows': across})

    barrier = pltpu.get_barrier_semaphore()
    for dev in ({'rows': prev}, {'rows': nxt}) + homes:
        pl.semaphore_signal(barrier, inc=1, device_id=dev, device_id_type=MESH_ID)

    own0 = k * CB
    far0 = CB - own0
    high16 = lax.broadcasted_iota(jnp.int32, (WIN, LANES), 1) >= HALF

    def put(v, tiles):
        rows = pl.ds(pl.multiple_of(v, WIN), WIN)
        for p in range(10):
            tb_ref[p, rows, :] = tiles[p].astype(BF)
        edge_ref[rows, :] = jnp.where(high16, tiles[0], tiles[9])

    def far_part(n, _):
        put(far0 + WIN * n, folded(accs, pl.multiple_of(SUB + WIN * n, SUB), WIN))
        return 0

    def own_part(n, _):
        put(own0 + WIN * n, [a_ref[p, pl.ds(pl.multiple_of(SUB + WIN * n, SUB), WIN), :] for p in range(10)])
        return 0

    last = CB // WIN - 1
    lax.fori_loop(1, last, far_part, 0)
    pl.semaphore_wait(barrier, 5)

    def remote(src, dst, ss, rs, i, dev):
        cp = pltpu.make_async_remote_copy(src_ref=src, dst_ref=dst, send_sem=ss.at[i], recv_sem=rs.at[i], device_id=dev, device_id_type=MESH_ID)
        cp.start()
        return cp

    halos = [remote(pack_ref.at[i], halo.at[i], halo_ss, halo_rs, i, {'rows': dev}) for i, dev in ((0, prev), (1, nxt))]

    lax.fori_loop(1, last, own_part, 0)
    none = jnp.zeros((SUB, LANES), F32)
    for n, side in ((0, CW - SUB), (last, 0)):
        off = SUB + WIN * n
        near_tiles = folded(accs, off, WIN)
        far_ends = folded(accs, side, SUB)
        order = (lambda v: [v, none]) if n == 0 else (lambda v: [none, v])
        put(far0 + WIN * n, [near_tiles[p] + jnp.concatenate(order(a_ref[p, side:side + SUB, :]), axis=0) for p in range(10)])
        put(own0 + WIN * n, [a_ref[p, off:off + WIN, :] + jnp.concatenate(order(far_ends[p]), axis=0) for p in range(10)])

    def to_rows(row0, n, t0, t1):
        a = jnp.concatenate([t0, t1], axis=1)
        g = lax.dot_general(pm_ref[...], a, (((1,), (1,)), ((), ())), preferred_element_type=F32).astype(BF)
        for ch in range(SUB):
            i, c = ch // 4, ch % 4
            g_ref[row0 + n * c:row0 + n * c + QTR, N_GRID * i:N_GRID * (i + 1)] = g[QTR * ch:QTR * (ch + 1), :]

    for m in range(4):
        to_rows(QTR * m, LANES, tb_ref[2 * m + 1], tb_ref[2 * m + 2])

    sms, srs, hms, hrs = (sm1, sm2), (sr1, sr2), (hm1, hm2), (hr1, hr2)
    swaps = []

    def columns(grp):
        start, n = GROUPS[grp]
        lane = lax.broadcasted_iota(jnp.int32, (n, LANES), 1)
        side = lane >> 6
        own_even, far_even = side == core, side != core
        block = (lane & (HALF - 1)) >> 4
        h = jnp.dot(g_ref[4 * start:4 * (start + n), :], ev_ref[...], preferred_element_type=F32)
        hc = [h[n * c:n * (c + 1)] for c in range(4)]
        rems = [v[:, 4 * LANES:] for v in hc]
        for cp in range(2):
            hs = [[v[:, LANES * i:LANES * (i + 1)] for i in range(4)] for v in hc[2 * cp:2 * cp + 2]]
            for i in range(4):
                dp, t = i // 2, i % 2
                odd = pltpu.roll(hs[1][i], HALF, axis=1)
                sms[grp][dp, cp, t] = jnp.where(far_even, hs[0][i], odd).astype(BF)
                hms[grp][dp, cp, t, core] = jnp.where(own_even, hs[0][i], odd).astype(BF)
        for t in range(2):
            both = []
            for h in range(2):
                i = 2 * t + h
                out = rems[i]
                for c in range(4):
                    if c != i:
                        out = jnp.where(block == c, pltpu.roll(rems[c], (WIN * (c - i)) % LANES, axis=1), out)
                both.append(out)
            srs[grp][t] = jnp.where(core == 0, both[1], both[0]).astype(BF)
            hrs[grp][t, core] = jnp.where(core == 0, both[0], both[1]).astype(BF)
        swaps.append(remote(sms[grp], hms[grp].at[:, :, :, core], swap_ss, swap_rs, 2 * grp, {'rows': near}))
        swaps.append(remote(srs[grp], hrs[grp].at[:, core], swap_ss, swap_rs, 2 * grp + 1, {'rows': near}))

    columns(0)

    def turn(rows):
        t = [rows[:, LANES * i:LANES * (i + 1)].T for i in range(5)]
        return [jnp.concatenate([t[2 * i], t[2 * i + 1], t[4][HALF * i:HALF * (i + 1)]], axis=0) for i in range(2)]

    for j, ref in enumerate((so_ref, sx_ref)):
        for cp in range(2):
            s_main[j, 0, cp], s_main[j, 1, cp] = turn(jnp.concatenate([ref[2 * cp + core, :HALF, :], ref[2 * cp + 1 - core, :HALF, :]], axis=0))
    tails = [[ref[c, HALF:, :] for c in range(4)] for ref in (so_ref, sx_ref)]
    s_rem[0], s_rem[1] = turn(jnp.concatenate([jnp.where(x == j, tails[0][c], tails[1][c]) for j in range(2) for c in range(4)], axis=0))
    d8 = jnp.broadcast_to(jnp.concatenate([d_ref[...][None, :], jnp.zeros((1, HALF), F32)], axis=1), (SUB, N_IMG + HALF))
    dq = d8
    for j in range(1, ROWS):
        dq = jnp.where(r == j, pltpu.roll(d8, N_IMG + HALF - QB * j, axis=1), dq)
    dp = jnp.where(k == 0, d8, pltpu.roll(d8, N_IMG + HALF - PB, axis=1))[:, :2 * LANES]
    dd = jnp.concatenate([dp] * WIN, axis=0).T[:PB] * dq[:1, :LANES]

    for cp in swaps:
        cp.wait_recv()
    n0 = 4 * GROUPS[0][1]

    def block_of(grp, j):
        return jnp.concatenate([hms[grp][(x + j) % 2, cp].reshape(4 * GROUPS[grp][1], LANES) for cp in range(2)], axis=1)

    for j in range(2):
        acc_m[j] = jnp.dot(eu_ref[x, :, :n0], block_of(0, j), preferred_element_type=F32)
    acc_r[...] = jnp.dot(eu_ref[x, :, :n0], hrs[0][...].reshape(n0, LANES), preferred_element_type=F32)

    for h in halos:
        h.wait()
    lane = lax.broadcasted_iota(jnp.int32, (LANES, LANES), 1)
    low = lane < HALF
    t0s, t9s = [], []
    for j in range(5):
        rows = slice(LANES * j, LANES * (j + 1))
        add_first = pltpu.roll(halo[1], (HALF - HW * j) % LANES, axis=1)
        add_last = pltpu.roll(halo[0], (HALF - HW - HW * j) % LANES, axis=1)
        e = edge_ref[rows, :] + jnp.where(low, jnp.where(lane >= HALF - HW, add_last, 0.0), jnp.where(lane < HALF + HW, add_first, 0.0))
        t0s.append(jnp.where(low, tb_ref[0, rows, :].astype(F32), e).astype(BF))
        t9s.append(jnp.where(low, e, tb_ref[9, rows, :].astype(F32)).astype(BF))
    lane = lax.broadcasted_iota(jnp.int32, (PB, LANES), 1)
    low = lane < HALF
    to_rows(4 * LANES, QTR, jnp.concatenate(t0s, axis=0), jnp.concatenate(t9s, axis=0))
    columns(1)
    for cp in swaps[2:]:
        cp.wait_recv()

    def rows_dft(half, acc, rhs):
        rows = pl.ds(pl.multiple_of(half * N_IMG, WIN), N_IMG)
        total = acc[rows, :] + jnp.dot(eu_ref[x, rows, n0:], rhs, preferred_element_type=F32)
        return total[:PB], total[PB:]

    quarter = lax.broadcasted_iota(jnp.int32, (PB // 4, LANES), 1) >> 5

    def rest(half):
        i_re, i_im = rows_dft(half, acc_r, hrs[1][...].reshape(4 * GROUPS[1][1], LANES))
        rows = pl.ds(pl.multiple_of(half * PB, SUB), PB)
        s_re, s_im = s_rem[0, rows, :], s_rem[1, rows, :]

        def fold(v):
            v = v + pltpu.roll(v, LANES - QTR, axis=1)
            return v + pltpu.roll(v, LANES - WIN, axis=1)

        re, im = fold(s_re * i_re + s_im * i_im), fold(s_re * i_im - s_im * i_re)
        return jnp.where(lane & (HALF - 1) < WIN, re, pltpu.roll(im, WIN, axis=1))

    def piece(half, j, tail):
        dp = (x + j) % 2
        i_re, i_im = rows_dft(half, acc_m.at[j], block_of(1, j))
        rows = pl.ds(pl.multiple_of(half * PB, SUB), PB)
        re, im = None, None
        for cp in range(2):
            cols = slice(LANES * cp, LANES * (cp + 1))
            s_re, s_im = s_main[j, 0, cp, rows, :], s_main[j, 1, cp, rows, :]
            a = s_re * i_re[:, cols] + s_im * i_im[:, cols]
            b = s_re * i_im[:, cols] - s_im * i_re[:, cols]
            re, im = (a, b) if re is None else (re + a, im + b)
        main = jnp.where(low, re + pltpu.roll(re, HALF, axis=1), im + pltpu.roll(im, HALF, axis=1))
        y = jnp.where(dp == 0, tail, pltpu.roll(tail, HALF, axis=1))
        out = y[:PB // 4]
        for g in range(1, 4):
            out = jnp.where(quarter == g, pltpu.roll(y[PB // 4 * g:PB // 4 * (g + 1)], QTR * g, axis=1), out)
        return main, out

    sends = []
    far_tail = rest(1 - k)
    for i, (half, j) in enumerate(((1 - k, 1), (1 - k, 0), (k, 1))):
        if i == 2:
            own_tail = rest(k)
        pieces[i, :PB], pieces[i, PB:] = piece(half, j, own_tail if i == 2 else far_tail)
        sends.append(remote(pieces.at[i], recvs.at[i], red_ss, red_rs, i, homes[i]))
    main, rem = piece(k, 0, own_tail)
    for i in (2, 1, 0):
        sends[i].wait_recv()
        main = main + recvs[i, :PB]
        rem = rem + recvs[i, PB:]
    for o in range(2):
        m = pltpu.roll(main, HALF, axis=1) if o else main
        for j in range(4):
            rows = slice(PB // 4 * j, PB // 4 * (j + 1))
            tail = pltpu.roll(rem, (HALF - QTR * j - WIN * o) % LANES, axis=1)
            out_ref[o, rows, :] = (jnp.where(low[rows], m[rows], tail) * dd[rows])[:, :QB]

    for cp in sends + swaps:
        cp.wait_send()


def solution(mesh):
    sample_spec = ('exam', 'rows', 'cols')
    vm = pl.BlockSpec(memory_space=pltpu.VMEM)
    hbm = pl.BlockSpec(memory_space=pltpu.HBM)
    spread_scratch = ([VMEM((LANES, LANES), F32)] * 4 + [VMEM((LANES * PS, LANES), F32)] * 2
                      + [VMEM((LANES, WIDE * 3), BF), VMEM((NB, LANES), jnp.int32), pltpu.SMEM((NB, LANES), jnp.int32), pltpu.SemaphoreType.DMA])
    acc_shape = [jax.ShapeDtypeStruct((NG * CW, LANES), F32)] * T
    big = 6 * MIB

    def local_fn(kspace, wts_y, wts_x, idx_y, idx_x, coil_maps, deapod):
        own, far, maps = pl.pallas_call(
            prep_kernel,
            out_shape=[jax.ShapeDtypeStruct((PAY * NB, LANES), F32)] * 2 + [jax.ShapeDtypeStruct((4, QB, N_GRID), F32)],
            in_specs=[hbm] * 6, out_specs=[vm] * 3, name='prep',
            scratch_shapes=[VMEM((2, SUB, NS), F32), VMEM((KW, NS), F32), VMEM((KW, NS), F32), VMEM((NB, LANES), jnp.int32), VMEM((NB, LANES), jnp.int32), VMEM((2, 4, QB, N_IMG), F32), pltpu.SemaphoreType.DMA((6,))],
            compiler_params=pltpu.CompilerParams(vmem_limit_bytes=SUB * MIB),
        )(*[pltpu.with_memory_space_constraint(v, pltpu.HBM) for v in (kspace, wts_y, wts_x, idx_y.reshape(NB, LANES), idx_x.reshape(NB, LANES), jnp.swapaxes(coil_maps, 2, 3))])
        far_in = lax.ppermute(far, 'cols', [(0, 1), (1, 0)])
        half, *accs = pl.pallas_call(
            own_kernel, out_shape=[jax.ShapeDtypeStruct((11, CW, LANES), F32)] + acc_shape, in_specs=[vm], out_specs=[vm] * (T + 1),
            scratch_shapes=spread_scratch, compiler_params=pltpu.CompilerParams(vmem_limit_bytes=big), name='spread_own',
            cost_estimate=pl.CostEstimate(flops=4 * 10 ** 9, bytes_accessed=2 * 10 ** 6, transcendentals=0),
        )(own)
        *accs, pack = pl.pallas_call(
            far_kernel, out_shape=acc_shape + [jax.ShapeDtypeStruct((2, LANES, LANES), F32)],
            in_specs=[vm] * (T + 2), out_specs=[vm] * (T + 1), scratch_shapes=[VMEM((N_GRID, LANES), F32)] + spread_scratch,
            input_output_aliases={i + 2: i for i in range(T)},
            compiler_params=pltpu.CompilerParams(vmem_limit_bytes=big), name='spread_far',
            cost_estimate=pl.CostEstimate(flops=4 * 10 ** 9, bytes_accessed=4 * 10 ** 6, transcendentals=0),
        )(far_in, half, *accs)
        maps_x = lax.ppermute(maps, 'rows', [(i, (i + 2) % ROWS) for i in range(ROWS)])
        dma = pltpu.SemaphoreType.DMA
        half_bufs = [VMEM((2, 2, 2, n, LANES), BF) for _, n in GROUPS] + [VMEM((2, n, LANES), BF) for _, n in GROUPS]
        full_bufs = [VMEM((2, 2, 2, 2, n, LANES), BF) for _, n in GROUPS] + [VMEM((2, 2, n, LANES), BF) for _, n in GROUPS]
        return pl.pallas_call(
            image_kernel,
            out_shape=jax.ShapeDtypeStruct((2, PB, QB), F32), in_specs=[vm] * (T + 8), out_specs=vm,
            scratch_shapes=[VMEM((10, N_GRID, LANES), BF), VMEM((N_GRID, LANES), F32), VMEM((4 * RB, 2 * N_GRID), BF), VMEM((2, LANES, LANES), F32)] + half_bufs + full_bufs + [
                VMEM((2, 2, 2, N_IMG, LANES), F32), VMEM((2, N_IMG, LANES), F32),
                VMEM((2, 2 * N_IMG, 2 * LANES), F32), VMEM((2 * N_IMG, LANES), F32), VMEM((3, PB + PB // 4, LANES), F32), VMEM((3, PB + PB // 4, LANES), F32),
                dma((2,)), dma((2,)), dma((4,)), dma((4,)), dma((3,)), dma((3,)),
            ],
            compiler_params=pltpu.CompilerParams(vmem_limit_bytes=20 * MIB, collective_id=0, has_side_effects=True), name='image',
        )(*accs, half, pack, maps, maps_x, deapod, col_dft(), row_dft(), unmix())

    return jax.shard_map(
        local_fn,
        mesh=mesh,
        in_specs=(P(None, None, sample_spec), P(None, sample_spec), P(None, sample_spec), P(sample_spec), P(sample_spec), P(None, ('exam', 'cols'), None, 'rows'), P()),
        out_specs=P(None, ('exam', 'cols'), 'rows'),
        check_vma=False,
    )
```

```python
import functools
import math

import jax
import jax.numpy as jnp
import numpy as np
from jax import lax
from jax.experimental import pallas as pl
from jax.experimental.pallas import tpu as pltpu
from jax.sharding import PartitionSpec as P

BF = jnp.bfloat16
F32 = jnp.float32
VMEM = pltpu.VMEM
LANES = 128
MIB = 1 << 20
GIGA = 4000 * MIB
TILES = 10
SUB, WIN, QTR, HALF, WIDE = 8, 16, 32, 64, 256
N_GRID, N_IMG, N_COILS, KW = 640, 320, 8, 6
ROWS, COLS = 4, 2
RB, CB, QB = N_GRID // ROWS, N_GRID // COLS, N_IMG // ROWS
PB = N_IMG // COLS
NS = 4096
NB = NS // LANES
NG = 21
CW = CB + WIN
T = 7
PS = 9
PAY = 21
CODE = 512
HW = 24
ORDER = tuple(range(1, 9)) + (0, 9)
GROUPS = ((0, 128), (128, 32))
MESH_ID = pl.DeviceIdType.MESH


def dft_parts():
    freq = np.arange(N_GRID) - N_GRID // 2
    pos = np.arange(N_IMG) - N_IMG // 2
    ang = ((freq[:, None] * pos[None, :]) % N_GRID).astype(np.float32) * np.float32(2.0 * math.pi / N_GRID)
    norm = np.float32(1.0 / math.sqrt(N_GRID))
    c, s = np.cos(ang) * norm, np.sin(ang) * norm
    return np.stack([np.stack([c, s], 1), np.stack([-s, c], 1)], 0)


def col_dft():
    e = dft_parts()
    out = np.zeros((2 * N_GRID, N_GRID), np.float32)
    for dp in range(2):
        for t in range(2):
            for h in range(2):
                q0 = QB * (2 * dp + h)
                l0 = LANES * (2 * dp + t) + HALF * h
                out[:, l0:l0 + HALF] = e[:, :, t, q0:q0 + HALF].reshape(2 * N_GRID, HALF)
    for t in range(2):
        for d in range(4):
            l0 = 4 * LANES + HALF * (d // 2) + WIN * (2 * t + d % 2)
            out[:, l0:l0 + WIN] = e[:, :, t, QB * d + HALF:QB * (d + 1)].reshape(2 * N_GRID, WIN)
    return jnp.asarray(out, BF)


def row_dft():
    e = dft_parts()
    rows = np.concatenate([np.arange(WIN * l, WIN * (l + 1)) for l in ORDER])
    chips = []
    for x in range(2):
        parts = []
        for start, n in GROUPS:
            for t in range(2):
                for b in range(2):
                    parts.append(e[t, (2 * x + b) * RB + rows[start:start + n]])
        m = np.concatenate(parts, 0)
        chips.append(np.concatenate([m[:, :, PB * h:PB * (h + 1)].reshape(N_GRID, N_IMG).T for h in range(2)], 0))
    return jnp.asarray(np.array(chips), BF)


def unmix():
    m = np.zeros((WIDE, WIDE), np.float32)
    for ch in range(SUB):
        for pp in range(2):
            for i in range(WIN):
                m[ch * QTR + WIN * pp + (i + SUB) % WIN, pp * 128 + i * SUB + ch] = 1.0
    return jnp.asarray(m, BF)


def prep_kernel(ks_hbm, wy_hbm, wx_hbm, iy_hbm, ix_hbm, maps_hbm, own_ref, far_ref, sp_ref, sq_ref, ks_ref, wy_ref, wx_ref, iy_ref, ix_ref, maps_ref, sem):
    k = lax.axis_index('cols')
    r = lax.axis_index('rows')
    loads = []
    for src, dst in ((iy_hbm, iy_ref), (ix_hbm, ix_ref), (wx_hbm, wx_ref), (wy_hbm, wy_ref), (ks_hbm, ks_ref), (maps_hbm, maps_ref)):
        cp = pltpu.make_async_copy(src, dst, sem.at[len(loads)])
        cp.start()
        loads.append(cp)
    loads[0].wait()
    loads[1].wait()
    iy = iy_ref[...]
    code = ((iy - r * RB + 5) * CODE + ix_ref[...] - k * CB + 5).astype(F32)
    for i in range(2, 5):
        loads[i].wait()
    lo = jnp.concatenate([ks_ref[0, 0:4, :], ks_ref[1, 0:4, :]], axis=0)
    hi = jnp.concatenate([ks_ref[0, 4:SUB, :], ks_ref[1, 4:SUB, :]], axis=0)
    first = k == 0
    for ref, y in ((own_ref, jnp.where(first, lo, hi)), (far_ref, jnp.where(first, hi, lo))):
        for b in range(NB):
            cols = slice(LANES * b, LANES * (b + 1))
            ref[PAY * b:PAY * b + SUB, :] = y[:, cols]
            ref[PAY * b + SUB:PAY * b + SUB + KW, :] = wx_ref[:, cols]
            ref[PAY * (b + 1) - KW - 1:PAY * (b + 1) - 1, :] = wy_ref[:, cols]
            ref[PAY * (b + 1) - 1:PAY * (b + 1), :] = code[b:b + 1, :]
    loads[5].wait()
    for c in range(4):
        for ref, q in ((sp_ref, slice(0, HALF)), (sq_ref, slice(HALF, QB))):
            for i in range(2):
                ref[c, :, WIDE * i:WIDE * (i + 1)] = maps_ref[i, c, q, :WIDE]
            ref[c, :, 2 * WIDE:] = jnp.concatenate([maps_ref[i, c, q, WIDE:] for i in range(2)], axis=1)


def split3(x):
    hi = x.astype(BF).astype(F32)
    r = x - hi
    mid = r.astype(BF).astype(F32)
    return hi, mid, r - mid


def accumulate(pay_ref, accs, us, xs, vs, r_ref, int_ref, base_ref, sem):
    row_i = lax.broadcasted_iota(jnp.int32, (WIN, LANES), 0)

    def make_u(blk, k):
        off = jnp.minimum(blk, NB - 1) * PAY
        y8 = pay_ref[pl.ds(off, SUB), :]
        wx = pay_ref[pl.ds(off + SUB, SUB), :]
        wyp = pay_ref[pl.ds(off + PAY - SUB, SUB), :]
        d = (row_i - (wyp[7:, :].astype(jnp.int32) // CODE)) & (WIN - 1)
        p = jnp.zeros((WIN, LANES), F32)
        for a in range(KW):
            p = jnp.where(d == a, wyp[a + 1:a + 2, :], p)
        us[k][...] = jnp.concatenate([y8 * p[i:i + 1, :] for i in range(WIN)], axis=0).T
        x3 = list(split3(wx)) + [jnp.zeros((LANES - HW, LANES), F32)]
        xs[k][...] = jnp.concatenate(x3, axis=0).T

    def make_v(k):
        lhs = xs[k][...].astype(BF)
        u = us[k][...]
        for bp in range(3):
            w = jnp.dot(lhs, r_ref[:, WIDE * bp:WIDE * bp + WIDE], preferred_element_type=F32)
            for c in range(2):
                v = w[:, LANES * c:LANES * (c + 1)] * u
                for g in range(WIN):
                    vs[k][pl.ds(SUB * PS * g + 2 * bp + c, SUB, stride=PS), :] = v[SUB * g:SUB * g + SUB, :]

    def add_tiles(blk, k):
        for j in range(LANES):
            acc = accs[j % T]
            b = base_ref[blk, j]
            acc[pl.ds(b, SUB), :] = acc[pl.ds(b, SUB), :] + vs[k][PS * j:PS * j + SUB, :]

    code = jnp.concatenate([pay_ref[PAY * (b + 1) - 1:PAY * (b + 1), :] for b in range(NB)], axis=0).astype(jnp.int32)
    int_ref[...] = (code // (CODE * SUB)) * CW + (code & (CODE - 1))
    kk = lax.broadcasted_iota(jnp.int32, (LANES, WIDE * 3), 0)
    ll = lax.broadcasted_iota(jnp.int32, (LANES, WIDE * 3), 1)
    r_ref[...] = jnp.where((kk < HW) & ((kk & 7) == (ll >> 7)), 1.0, 0.0).astype(BF)
    for v in vs:
        v[...] = jnp.zeros_like(v)
    load = pltpu.make_async_copy(int_ref, base_ref, sem)
    load.start()
    make_u(0, 0)
    make_u(1, 1)
    make_v(0)
    load.wait()

    def body(n, _):
        k = 2 * n
        make_v(1)
        add_tiles(k, 0)
        make_u(k + 2, 0)
        make_v(0)
        add_tiles(k + 1, 1)
        make_u(k + 3, 1)
        return 0

    lax.fori_loop(0, NB // 2, body, 0)


def folded(accs, off, n, clear=False):
    def total(g):
        rows = pl.ds(pl.multiple_of(g * CW + off, SUB), n)
        v = accs[0][rows, :]
        for a in accs[1:]:
            v = v + a[rows, :]
        if clear:
            for a in accs:
                a[rows, :] = jnp.zeros((n, LANES), F32)
        return v

    high = lax.broadcasted_iota(jnp.int32, (n, LANES), 1) >= HALF
    even = [total(2 * p) for p in range(11)]
    tiles = [total(2 * p + 1) + jnp.where(high, even[p], even[p + 1]) for p in range(TILES)]
    return tiles + [jnp.where(high, even[TILES], even[0])]


def own_kernel(pay_ref, out_ref, *refs):
    accs, scr = refs[:T], refs[T:]

    def clear(n, _):
        for a in accs:
            a[pl.ds(pl.multiple_of(n * CW, SUB), CW), :] = jnp.zeros((CW, LANES), F32)
        return 0

    lax.fori_loop(0, NG, clear, 0)
    accumulate(pay_ref, accs, scr[:2], scr[2:4], scr[4:6], *scr[6:])

    def fold(q, _):
        off = pl.multiple_of(q * WIN, WIN)
        for p, t in enumerate(folded(accs, off, WIN, clear=True)):
            out_ref[p, pl.ds(off, WIN), :] = t
        return 0

    lax.fori_loop(0, CW // WIN, fold, 0)


def far_kernel(pay_ref, a_ref, *refs):
    accs, pack_ref, gh_ref, scr = refs[T:2 * T], refs[2 * T], refs[2 * T + 1], refs[2 * T + 2:]
    accumulate(pay_ref, accs, scr[:2], scr[2:4], scr[4:6], *scr[6:])
    own0 = lax.axis_index('cols') * CB
    far0 = CB - own0

    def ghost(off, n):
        high = lax.broadcasted_iota(jnp.int32, (n, LANES), 1) >= HALF
        ends = []
        for g in (0, NG - 1):
            rows = pl.ds(pl.multiple_of(g * CW + off, SUB), n)
            v = accs[0][rows, :]
            for a in accs[1:]:
                v = v + a[rows, :]
            ends.append(v)
        return jnp.where(high, ends[1], ends[0])

    def copy(n, _):
        o = pl.multiple_of(n * QTR, SUB)
        gh_ref[pl.ds(pl.multiple_of(far0 + o, SUB), QTR), :] = ghost(SUB + o, QTR)
        gh_ref[pl.ds(pl.multiple_of(own0 + o, SUB), QTR), :] = a_ref[TILES, pl.ds(pl.multiple_of(SUB + o, SUB), QTR), :]
        return 0

    lax.fori_loop(0, CB // QTR, copy, 0)
    for dst, add in ((own0, ghost(CW - SUB, SUB)), (own0 + CB - SUB, ghost(0, SUB)), (far0, a_ref[TILES, CW - SUB:, :]), (far0 + CB - SUB, a_ref[TILES, :SUB, :])):
        rows = pl.ds(pl.multiple_of(dst, SUB), SUB)
        gh_ref[rows, :] = gh_ref[rows, :] + add

    lane = lax.broadcasted_iota(jnp.int32, (LANES, LANES), 1)
    for side, lane0 in ((0, HALF - HW), (1, HALF)):
        out = jnp.zeros((LANES, LANES), F32)
        for j in range(5):
            piece = pltpu.roll(gh_ref[LANES * j:LANES * (j + 1), :], (HW * j - lane0) % LANES, axis=1)
            out = jnp.where(lane >= HW * j, piece, out)
        pack_ref[side] = out


def image_kernel(*refs):
    accs = refs[:T]
    (a_ref, pack_ref, so_ref, sx_ref, se_ref, d_ref, ev_ref, eu_ref, pm_ref, out_ref,
     tb_ref, edge_ref, g_ref, halo, sm1, sm2, sr1, sr2, hm1, hm2, hr1, hr2, s_main, s_rem, acc_m, acc_r, sx_end, pieces, recvs, tails, recvs_t,
     halo_ss, halo_rs, swap_ss, swap_rs, red_ss, red_rs) = refs[T:]
    k = lax.axis_index('cols')
    r = lax.axis_index('rows')
    core, x = r % 2, r // 2
    near = r + 1 - 2 * core
    across = (r + 2) % 4
    prev, nxt = (r + 3) % 4, (r + 1) % 4
    homes = ({'rows': across, 'cols': 1 - k}, {'cols': 1 - k}, {'rows': across})

    barrier = pltpu.get_barrier_semaphore()
    for dev in ({'rows': prev}, {'rows': nxt}) + homes:
        pl.semaphore_signal(barrier, inc=1, device_id=dev, device_id_type=MESH_ID)

    own0 = k * CB
    far0 = CB - own0
    high16 = lax.broadcasted_iota(jnp.int32, (WIN, LANES), 1) >= HALF

    def put(v, tiles):
        rows = pl.ds(pl.multiple_of(v, WIN), WIN)
        for p in range(TILES):
            tb_ref[p, rows, :] = tiles[p].astype(BF)
        edge_ref[rows, :] = jnp.where(high16, tiles[0], tiles[9])

    def far_part(n, _):
        put(far0 + WIN * n, folded(accs, pl.multiple_of(SUB + WIN * n, SUB), WIN))
        return 0

    def own_part(n, _):
        put(own0 + WIN * n, [a_ref[p, pl.ds(pl.multiple_of(SUB + WIN * n, SUB), WIN), :] for p in range(TILES)])
        return 0

    last = CB // WIN - 1
    lax.fori_loop(1, last, far_part, 0)
    pl.semaphore_wait(barrier, 5)

    def remote(src, dst, ss, rs, i, dev):
        cp = pltpu.make_async_remote_copy(src_ref=src, dst_ref=dst, send_sem=ss.at[i], recv_sem=rs.at[i], device_id=dev, device_id_type=MESH_ID)
        cp.start()
        return cp

    halos = [remote(pack_ref.at[i], halo.at[i], halo_ss, halo_rs, i, {'rows': dev}) for i, dev in ((0, prev), (1, nxt))]

    lax.fori_loop(1, last, own_part, 0)
    none = jnp.zeros((SUB, LANES), F32)
    for n, side in ((0, CW - SUB), (last, 0)):
        off = SUB + WIN * n
        near_tiles = folded(accs, off, WIN)
        far_ends = folded(accs, side, SUB)
        order = (lambda v: [v, none]) if n == 0 else (lambda v: [none, v])
        put(far0 + WIN * n, [near_tiles[p] + jnp.concatenate(order(a_ref[p, side:side + SUB, :]), axis=0) for p in range(TILES)])
        put(own0 + WIN * n, [a_ref[p, off:off + WIN, :] + jnp.concatenate(order(far_ends[p]), axis=0) for p in range(TILES)])

    end_copy = remote(se_ref, sx_end, halo_ss, halo_rs, 2, {'rows': across})

    def to_rows(row0, n, t0, t1):
        a = jnp.concatenate([t0, t1], axis=1)
        g = lax.dot_general(pm_ref[...], a, (((1,), (1,)), ((), ())), preferred_element_type=F32).astype(BF)
        for ch in range(SUB):
            i, c = ch // 4, ch % 4
            g_ref[row0 + n * c:row0 + n * c + QTR, N_GRID * i:N_GRID * (i + 1)] = g[QTR * ch:QTR * (ch + 1), :]

    for m in range(4):
        to_rows(QTR * m, LANES, tb_ref[2 * m + 1], tb_ref[2 * m + 2])

    sms, srs, hms, hrs = (sm1, sm2), (sr1, sr2), (hm1, hm2), (hr1, hr2)
    swaps = []

    def columns(grp):
        start, n = GROUPS[grp]
        lane = lax.broadcasted_iota(jnp.int32, (n, LANES), 1)
        side = lane >> 6
        own_even, far_even = side == core, side != core
        block = (lane & (HALF - 1)) >> 4
        h = jnp.dot(g_ref[4 * start:4 * (start + n), :], ev_ref[...], preferred_element_type=F32)
        hc = [h[n * c:n * (c + 1)] for c in range(4)]
        rems = [v[:, 4 * LANES:] for v in hc]
        for cp in range(2):
            hs = [[v[:, LANES * i:LANES * (i + 1)] for i in range(4)] for v in hc[2 * cp:2 * cp + 2]]
            for i in range(4):
                dp, t = i // 2, i % 2
                odd = pltpu.roll(hs[1][i], HALF, axis=1)
                sms[grp][dp, cp, t] = jnp.where(far_even, hs[0][i], odd).astype(BF)
                hms[grp][dp, cp, t, core] = jnp.where(own_even, hs[0][i], odd).astype(BF)
        for t in range(2):
            both = []
            for h in range(2):
                i = 2 * t + h
                out = rems[i]
                for c in range(4):
                    if c != i:
                        out = jnp.where(block == c, pltpu.roll(rems[c], (WIN * (c - i)) % LANES, axis=1), out)
                both.append(out)
            srs[grp][t] = jnp.where(core == 0, both[1], both[0]).astype(BF)
            hrs[grp][t, core] = jnp.where(core == 0, both[0], both[1]).astype(BF)
        swaps.append(remote(sms[grp], hms[grp].at[:, :, :, core], swap_ss, swap_rs, 2 * grp, {'rows': near}))
        swaps.append(remote(srs[grp], hrs[grp].at[:, core], swap_ss, swap_rs, 2 * grp + 1, {'rows': near}))

    columns(0)

    def turn(rows):
        t = [rows[:, LANES * i:LANES * (i + 1)].T for i in range(5)]
        return [jnp.concatenate([t[2 * i], t[2 * i + 1], t[4][HALF * i:HALF * (i + 1)]], axis=0) for i in range(2)]

    for j, ref in enumerate((so_ref, sx_ref)):
        for cp in range(2):
            s_main[j, 0, cp], s_main[j, 1, cp] = turn(jnp.concatenate([ref[2 * cp + core], ref[2 * cp + 1 - core]], axis=0))
    d8 = jnp.broadcast_to(jnp.concatenate([d_ref[...][None, :], jnp.zeros((1, HALF), F32)], axis=1), (SUB, N_IMG + HALF))
    dq = d8
    for j in range(1, ROWS):
        dq = jnp.where(r == j, pltpu.roll(d8, N_IMG + HALF - QB * j, axis=1), dq)
    dp = jnp.where(k == 0, d8, pltpu.roll(d8, N_IMG + HALF - PB, axis=1))[:, :2 * LANES]
    dd = jnp.concatenate([dp] * WIN, axis=0).T[:PB] * dq[:1, :LANES]

    for h in halos:
        h.wait()
    lane = lax.broadcasted_iota(jnp.int32, (LANES, LANES), 1)
    low = lane < HALF
    t0s, t9s = [], []
    for j in range(5):
        rows = slice(LANES * j, LANES * (j + 1))
        add_first = pltpu.roll(halo[1], (HALF - HW * j) % LANES, axis=1)
        add_last = pltpu.roll(halo[0], (HALF - HW - HW * j) % LANES, axis=1)
        e = edge_ref[rows, :] + jnp.where(low, jnp.where(lane >= HALF - HW, add_last, 0.0), jnp.where(lane < HALF + HW, add_first, 0.0))
        t0s.append(jnp.where(low, tb_ref[0, rows, :].astype(F32), e).astype(BF))
        t9s.append(jnp.where(low, e, tb_ref[9, rows, :].astype(F32)).astype(BF))
    lane = lax.broadcasted_iota(jnp.int32, (PB, LANES), 1)
    low = lane < HALF
    to_rows(4 * LANES, QTR, jnp.concatenate(t0s, axis=0), jnp.concatenate(t9s, axis=0))
    columns(1)

    for cp in swaps[:2]:
        cp.wait_recv()
    n0 = 4 * GROUPS[0][1]

    def block_of(grp, j):
        return jnp.concatenate([hms[grp][(x + j) % 2, cp].reshape(4 * GROUPS[grp][1], LANES) for cp in range(2)], axis=1)

    for j in range(2):
        acc_m[j] = jnp.dot(eu_ref[x, :, :n0], block_of(0, j), preferred_element_type=F32)
    acc_r[...] = jnp.dot(eu_ref[x, :, :n0], hrs[0][...].reshape(n0, LANES), preferred_element_type=F32)

    for cp in swaps[2:]:
        cp.wait_recv()

    def rows_dft(half, acc, rhs):
        rows = pl.ds(pl.multiple_of(half * N_IMG, WIN), N_IMG)
        total = acc[rows, :] + jnp.dot(eu_ref[x, rows, n0:], rhs, preferred_element_type=F32)
        return total[:PB], total[PB:]

    quarter = lax.broadcasted_iota(jnp.int32, (PB // 4, LANES), 1) >> 5

    def piece(half, j):
        i_re, i_im = rows_dft(half, acc_m.at[j], block_of(1, j))
        rows = pl.ds(pl.multiple_of(half * PB, SUB), PB)
        re, im = None, None
        for cp in range(2):
            cols = slice(LANES * cp, LANES * (cp + 1))
            s_re, s_im = s_main[j, 0, cp, rows, :], s_main[j, 1, cp, rows, :]
            a = s_re * i_re[:, cols] + s_im * i_im[:, cols]
            b = s_re * i_im[:, cols] - s_im * i_re[:, cols]
            re, im = (a, b) if re is None else (re + a, im + b)
        return jnp.where(low, re + pltpu.roll(re, HALF, axis=1), im + pltpu.roll(im, HALF, axis=1))

    def rest(half):
        i_re, i_im = rows_dft(half, acc_r, hrs[1][...].reshape(4 * GROUPS[1][1], LANES))
        rows = pl.ds(pl.multiple_of(half * PB, SUB), PB)
        s_re, s_im = s_rem[0, rows, :], s_rem[1, rows, :]

        def fold(v):
            v = v + pltpu.roll(v, LANES - QTR, axis=1)
            return v + pltpu.roll(v, LANES - WIN, axis=1)

        re, im = fold(s_re * i_re + s_im * i_im), fold(s_re * i_im - s_im * i_re)
        both = jnp.where(lane & (HALF - 1) < WIN, re, pltpu.roll(im, WIN, axis=1))
        outs = []
        for dp in range(2):
            out = None
            for g in range(4):
                v = both[PB // 4 * g:PB // 4 * (g + 1)]
                if g + 2 * dp:
                    v = pltpu.roll(v, (QTR * g + HALF * dp) % LANES, axis=1)
                out = v if out is None else jnp.where(quarter == g, v, out)
            outs.append(out)
        return jnp.where(x == 0, outs[0], outs[1]), jnp.where(x == 0, outs[1], outs[0])

    sends = []
    for i, (half, j) in enumerate(((1 - k, 1), (1 - k, 0), (k, 1))):
        pieces[i] = piece(half, j)
        sends.append(remote(pieces.at[i], recvs.at[i], red_ss, red_rs, i, homes[i]))
    end_copy.wait_recv()
    s_rem[0], s_rem[1] = turn(jnp.concatenate([jnp.where(x == j, se_ref[c], sx_end[c]) for j in range(2) for c in range(4)], axis=0))
    tails[1], tails[0] = rest(1 - k)
    for i in range(2):
        sends.append(remote(tails.at[i], recvs_t.at[i], red_ss, red_rs, 3 + i, homes[i]))
    rem, tails[2] = rest(k)
    sends.append(remote(tails.at[2], recvs_t.at[2], red_ss, red_rs, 5, homes[2]))
    main = piece(k, 0)
    for i in (1, 0, 2):
        sends[i].wait_recv()
        main = main + recvs[i]
    for i in (1, 0, 2):
        sends[3 + i].wait_recv()
        rem = rem + recvs_t[i]
    for o in range(2):
        m = pltpu.roll(main, HALF, axis=1) if o else main
        for j in range(4):
            rows = slice(PB // 4 * j, PB // 4 * (j + 1))
            tail = pltpu.roll(rem, (HALF - QTR * j - WIN * o) % LANES, axis=1)
            out_ref[o, rows, :] = (jnp.where(low[rows], m[rows], tail) * dd[rows])[:, :QB]

    for cp in sends + swaps + [end_copy]:
        cp.wait_send()


def solution(mesh):
    sample_spec = ('exam', 'rows', 'cols')
    vm = pl.BlockSpec(memory_space=pltpu.VMEM)
    hbm = pl.BlockSpec(memory_space=pltpu.HBM)
    spread_scratch = ([VMEM((LANES, LANES), F32)] * 4 + [VMEM((LANES * PS, LANES), F32)] * 2
                      + [VMEM((LANES, WIDE * 3), BF), VMEM((NB, LANES), jnp.int32), pltpu.SMEM((NB, LANES), jnp.int32), pltpu.SemaphoreType.DMA])
    acc_shape = [jax.ShapeDtypeStruct((NG * CW, LANES), F32)] * T
    big = 6 * MIB

    def local_fn(kspace, wts_y, wts_x, idx_y, idx_x, coil_maps, deapod):
        own, far, maps, maps_end = pl.pallas_call(
            prep_kernel,
            out_shape=[jax.ShapeDtypeStruct((PAY * NB, LANES), F32)] * 2 + [jax.ShapeDtypeStruct((4, n, N_GRID), F32) for n in (HALF, WIN)],
            in_specs=[hbm] * 6, out_specs=[vm] * 4, name='prep',
            scratch_shapes=[VMEM((2, SUB, NS), F32), VMEM((KW, NS), F32), VMEM((KW, NS), F32), VMEM((NB, LANES), jnp.int32), VMEM((NB, LANES), jnp.int32), VMEM((2, 4, QB, N_IMG), F32), pltpu.SemaphoreType.DMA((6,))],
            compiler_params=pltpu.CompilerParams(vmem_limit_bytes=SUB * MIB),
        )(*[pltpu.with_memory_space_constraint(v, pltpu.HBM) for v in (kspace, wts_y, wts_x, idx_y.reshape(NB, LANES), idx_x.reshape(NB, LANES), jnp.swapaxes(coil_maps, 2, 3))])
        far_in = lax.ppermute(far, 'cols', [(0, 1), (1, 0)])
        half, *accs = pl.pallas_call(
            own_kernel, out_shape=[jax.ShapeDtypeStruct((11, CW, LANES), F32)] + acc_shape, in_specs=[vm], out_specs=[vm] * (T + 1),
            scratch_shapes=spread_scratch, compiler_params=pltpu.CompilerParams(vmem_limit_bytes=big), name='spread_own',
            cost_estimate=pl.CostEstimate(flops=GIGA, bytes_accessed=4 * MIB, transcendentals=0),
        )(own)
        *accs, pack = pl.pallas_call(
            far_kernel, out_shape=acc_shape + [jax.ShapeDtypeStruct((2, LANES, LANES), F32)],
            in_specs=[vm] * (T + 2), out_specs=[vm] * (T + 1), scratch_shapes=[VMEM((N_GRID, LANES), F32)] + spread_scratch,
            input_output_aliases={i + 2: i for i in range(T)},
            compiler_params=pltpu.CompilerParams(vmem_limit_bytes=big), name='spread_far',
            cost_estimate=pl.CostEstimate(flops=GIGA, bytes_accessed=4 * MIB, transcendentals=0),
        )(far_in, half, *accs)
        maps_x = lax.ppermute(maps, 'rows', [(i, (i + 2) % ROWS) for i in range(ROWS)])
        dma = pltpu.SemaphoreType.DMA
        half_bufs = [VMEM((2, 2, 2, n, LANES), BF) for _, n in GROUPS] + [VMEM((2, n, LANES), BF) for _, n in GROUPS]
        full_bufs = [VMEM((2, 2, 2, 2, n, LANES), BF) for _, n in GROUPS] + [VMEM((2, 2, n, LANES), BF) for _, n in GROUPS]
        return pl.pallas_call(
            image_kernel,
            out_shape=jax.ShapeDtypeStruct((2, PB, QB), F32), in_specs=[vm] * (T + 9), out_specs=vm,
            scratch_shapes=[VMEM((TILES, N_GRID, LANES), BF), VMEM((N_GRID, LANES), F32), VMEM((4 * RB, 2 * N_GRID), BF), VMEM((2, LANES, LANES), F32)] + half_bufs + full_bufs + [
                VMEM((2, 2, 2, N_IMG, LANES), F32), VMEM((2, N_IMG, LANES), F32),
                VMEM((2, 2 * N_IMG, 2 * LANES), F32), VMEM((2 * N_IMG, LANES), F32), VMEM((4, WIN, N_GRID), F32),
                VMEM((3, PB, LANES), F32), VMEM((3, PB, LANES), F32), VMEM((3, PB // 4, LANES), F32), VMEM((3, PB // 4, LANES), F32),
                dma((3,)), dma((3,)), dma((4,)), dma((4,)), dma((6,)), dma((6,)),
            ],
            compiler_params=pltpu.CompilerParams(vmem_limit_bytes=11 * MIB, collective_id=0, has_side_effects=True), name='image',
        )(*accs, half, pack, maps, maps_x, maps_end, deapod, col_dft(), row_dft(), unmix())

    return jax.shard_map(
        local_fn,
        mesh=mesh,
        in_specs=(P(None, None, sample_spec), P(None, sample_spec), P(None, sample_spec), P(sample_spec), P(sample_spec), P(None, ('exam', 'cols'), None, 'rows'), P()),
        out_specs=P(None, ('exam', 'cols'), 'rows'),
        check_vma=False,
    )
```

```python
import functools
import math

import jax
import jax.numpy as jnp
import numpy as np
from jax import lax
from jax.experimental import pallas as pl
from jax.experimental.pallas import tpu as pltpu
from jax.sharding import PartitionSpec as P

BF = jnp.bfloat16
F32 = jnp.float32
VMEM = pltpu.VMEM
LANES = 128
MIB = 1 << 20
GIGA = 4000 * MIB
TILES = 10
SUB, WIN, QTR, HALF, WIDE = 8, 16, 32, 64, 256
N_GRID, N_IMG, N_COILS, KW = 640, 320, 8, 6
ROWS, COLS = 4, 2
RB, CB, QB = N_GRID // ROWS, N_GRID // COLS, N_IMG // ROWS
PB = N_IMG // COLS
NS = 4096
NB = NS // LANES
NG = 21
CW = CB + WIN
T = 6
PS = 9
PAY = 21
CODE = 512
HW = 24
ORDER = tuple(range(1, 9)) + (0, 9)
GROUPS = ((0, 128), (128, 32))
MESH_ID = pl.DeviceIdType.MESH


def dft_parts():
    freq = np.arange(N_GRID) - N_GRID // 2
    pos = np.arange(N_IMG) - N_IMG // 2
    ang = ((freq[:, None] * pos[None, :]) % N_GRID).astype(np.float32) * np.float32(2.0 * math.pi / N_GRID)
    norm = np.float32(1.0 / math.sqrt(N_GRID))
    c, s = np.cos(ang) * norm, np.sin(ang) * norm
    return np.stack([np.stack([c, s], 1), np.stack([-s, c], 1)], 0)


def col_dft():
    e = dft_parts()
    out = np.zeros((2 * N_GRID, N_GRID), np.float32)
    for dp in range(2):
        for t in range(2):
            for h in range(2):
                q0 = QB * (2 * dp + h)
                l0 = LANES * (2 * dp + t) + HALF * h
                out[:, l0:l0 + HALF] = e[:, :, t, q0:q0 + HALF].reshape(2 * N_GRID, HALF)
    for t in range(2):
        for d in range(4):
            l0 = 4 * LANES + HALF * (d // 2) + WIN * (2 * t + d % 2)
            out[:, l0:l0 + WIN] = e[:, :, t, QB * d + HALF:QB * (d + 1)].reshape(2 * N_GRID, WIN)
    return jnp.asarray(out, BF)


def row_dft():
    e = dft_parts()
    rows = np.concatenate([np.arange(WIN * l, WIN * (l + 1)) for l in ORDER])
    chips = []
    for x in range(2):
        parts = []
        for start, n in GROUPS:
            for t in range(2):
                for b in range(2):
                    parts.append(e[t, (2 * x + b) * RB + rows[start:start + n]])
        m = np.concatenate(parts, 0)
        chips.append(np.concatenate([m[:, :, PB * h:PB * (h + 1)].reshape(N_GRID, N_IMG).T for h in range(2)], 0))
    return jnp.asarray(np.array(chips), BF)


def unmix():
    m = np.zeros((WIDE, WIDE), np.float32)
    for ch in range(SUB):
        for pp in range(2):
            for i in range(WIN):
                m[ch * QTR + WIN * pp + (i + SUB) % WIN, pp * 128 + i * SUB + ch] = 1.0
    return jnp.asarray(m, BF)


def prep_kernel(ks_hbm, wy_hbm, wx_hbm, iy_hbm, ix_hbm, maps_hbm, own_ref, far_ref, sp_ref, sq_ref, ks_ref, wy_ref, wx_ref, iy_ref, ix_ref, maps_ref, sem):
    k = lax.axis_index('cols')
    r = lax.axis_index('rows')
    loads = []
    for src, dst in ((iy_hbm, iy_ref), (ix_hbm, ix_ref), (wx_hbm, wx_ref), (wy_hbm, wy_ref), (ks_hbm, ks_ref), (maps_hbm, maps_ref)):
        cp = pltpu.make_async_copy(src, dst, sem.at[len(loads)])
        cp.start()
        loads.append(cp)
    loads[0].wait()
    loads[1].wait()
    iy = iy_ref[...]
    code = ((iy - r * RB + 5) * CODE + ix_ref[...] - k * CB + 5).astype(F32)
    for i in range(2, 5):
        loads[i].wait()
    lo = jnp.concatenate([ks_ref[0, 0:4, :], ks_ref[1, 0:4, :]], axis=0)
    hi = jnp.concatenate([ks_ref[0, 4:SUB, :], ks_ref[1, 4:SUB, :]], axis=0)
    first = k == 0
    for ref, y in ((own_ref, jnp.where(first, lo, hi)), (far_ref, jnp.where(first, hi, lo))):
        for b in range(NB):
            cols = slice(LANES * b, LANES * (b + 1))
            ref[PAY * b:PAY * b + SUB, :] = y[:, cols]
            ref[PAY * b + SUB:PAY * b + SUB + KW, :] = wx_ref[:, cols]
            ref[PAY * (b + 1) - KW - 1:PAY * (b + 1) - 1, :] = wy_ref[:, cols]
            ref[PAY * (b + 1) - 1:PAY * (b + 1), :] = code[b:b + 1, :]
    loads[5].wait()
    for c in range(4):
        for ref, q in ((sp_ref, slice(0, HALF)), (sq_ref, slice(HALF, QB))):
            for i in range(2):
                ref[c, :, WIDE * i:WIDE * (i + 1)] = maps_ref[i, c, q, :WIDE]
            ref[c, :, 2 * WIDE:] = jnp.concatenate([maps_ref[i, c, q, WIDE:] for i in range(2)], axis=1)


def split3(x):
    hi = x.astype(BF).astype(F32)
    r = x - hi
    mid = r.astype(BF).astype(F32)
    return hi, mid, r - mid


def accumulate(pay_ref, accs, us, xs, vs, r_ref, int_ref, base_ref, sem):
    row_i = lax.broadcasted_iota(jnp.int32, (WIN, LANES), 0)

    def make_u(blk, k):
        off = jnp.minimum(blk, NB - 1) * PAY
        y8 = pay_ref[pl.ds(off, SUB), :]
        wx = pay_ref[pl.ds(off + SUB, SUB), :]
        wyp = pay_ref[pl.ds(off + PAY - SUB, SUB), :]
        d = (row_i - (wyp[7:, :].astype(jnp.int32) // CODE)) & (WIN - 1)
        p = jnp.zeros((WIN, LANES), F32)
        for a in range(KW):
            p = jnp.where(d == a, wyp[a + 1:a + 2, :], p)
        us[k][...] = jnp.concatenate([y8 * p[i:i + 1, :] for i in range(WIN)], axis=0).T
        x3 = list(split3(wx)) + [jnp.zeros((LANES - HW, LANES), F32)]
        xs[k][...] = jnp.concatenate(x3, axis=0).T

    def make_v(k):
        lhs = xs[k][...].astype(BF)
        u = us[k][...]
        for bp in range(3):
            w = jnp.dot(lhs, r_ref[:, WIDE * bp:WIDE * bp + WIDE], preferred_element_type=F32)
            for c in range(2):
                v = w[:, LANES * c:LANES * (c + 1)] * u
                for g in range(WIN):
                    vs[k][pl.ds(SUB * PS * g + 2 * bp + c, SUB, stride=PS), :] = v[SUB * g:SUB * g + SUB, :]

    def add_tiles(blk, k):
        row = base_ref.at[blk]
        for j in range(LANES):
            acc = accs[j % T]
            b = row[j]
            acc[pl.ds(b, SUB), :] = acc[pl.ds(b, SUB), :] + vs[k][PS * j:PS * j + SUB, :]

    code = jnp.concatenate([pay_ref[PAY * (b + 1) - 1:PAY * (b + 1), :] for b in range(NB)], axis=0).astype(jnp.int32)
    int_ref[...] = (code // (CODE * SUB)) * CW + (code & (CODE - 1))
    kk = lax.broadcasted_iota(jnp.int32, (LANES, WIDE * 3), 0)
    ll = lax.broadcasted_iota(jnp.int32, (LANES, WIDE * 3), 1)
    r_ref[...] = jnp.where((kk < HW) & ((kk & 7) == (ll >> 7)), 1.0, 0.0).astype(BF)
    for v in vs:
        v[...] = jnp.zeros_like(v)
    load = pltpu.make_async_copy(int_ref, base_ref, sem)
    load.start()
    make_u(0, 0)
    make_u(1, 1)
    make_v(0)
    load.wait()

    def body(n, _):
        k = 2 * n
        make_v(1)
        add_tiles(k, 0)
        make_u(k + 2, 0)
        make_v(0)
        add_tiles(k + 1, 1)
        make_u(k + 3, 1)
        return 0

    lax.fori_loop(0, NB // 2, body, 0)


def folded(accs, off, n, clear=False):
    def total(g):
        rows = pl.ds(pl.multiple_of(g * CW + off, SUB), n)
        v = accs[0][rows, :]
        for a in accs[1:]:
            v = v + a[rows, :]
        if clear:
            for a in accs:
                a[rows, :] = jnp.zeros((n, LANES), F32)
        return v

    high = lax.broadcasted_iota(jnp.int32, (n, LANES), 1) >= HALF
    even = [total(2 * p) for p in range(11)]
    tiles = [total(2 * p + 1) + jnp.where(high, even[p], even[p + 1]) for p in range(TILES)]
    return tiles + [jnp.where(high, even[TILES], even[0])]


def own_kernel(pay_ref, out_ref, *refs):
    accs, scr = refs[:T], refs[T:]

    def clear(n, _):
        for a in accs:
            a[pl.ds(pl.multiple_of(n * CW, SUB), CW), :] = jnp.zeros((CW, LANES), F32)
        return 0

    lax.fori_loop(0, NG, clear, 0)
    accumulate(pay_ref, accs, scr[:2], scr[2:4], scr[4:6], *scr[6:])

    def fold(q, _):
        off = pl.multiple_of(q * WIN, WIN)
        for p, t in enumerate(folded(accs, off, WIN, clear=True)):
            out_ref[p, pl.ds(off, WIN), :] = t
        return 0

    lax.fori_loop(0, CW // WIN, fold, 0)


def far_kernel(pay_ref, a_ref, *refs):
    accs, pack_ref, gh_ref, scr = refs[T:2 * T], refs[2 * T], refs[2 * T + 1], refs[2 * T + 2:]
    accumulate(pay_ref, accs, scr[:2], scr[2:4], scr[4:6], *scr[6:])
    own0 = lax.axis_index('cols') * CB
    far0 = CB - own0

    def ghost(off, n):
        high = lax.broadcasted_iota(jnp.int32, (n, LANES), 1) >= HALF
        ends = []
        for g in (0, NG - 1):
            rows = pl.ds(pl.multiple_of(g * CW + off, SUB), n)
            v = accs[0][rows, :]
            for a in accs[1:]:
                v = v + a[rows, :]
            ends.append(v)
        return jnp.where(high, ends[1], ends[0])

    def copy(n, _):
        o = pl.multiple_of(n * QTR, SUB)
        gh_ref[pl.ds(pl.multiple_of(far0 + o, SUB), QTR), :] = ghost(SUB + o, QTR)
        gh_ref[pl.ds(pl.multiple_of(own0 + o, SUB), QTR), :] = a_ref[TILES, pl.ds(pl.multiple_of(SUB + o, SUB), QTR), :]
        return 0

    lax.fori_loop(0, CB // QTR, copy, 0)
    for dst, add in ((own0, ghost(CW - SUB, SUB)), (own0 + CB - SUB, ghost(0, SUB)), (far0, a_ref[TILES, CW - SUB:, :]), (far0 + CB - SUB, a_ref[TILES, :SUB, :])):
        rows = pl.ds(pl.multiple_of(dst, SUB), SUB)
        gh_ref[rows, :] = gh_ref[rows, :] + add

    lane = lax.broadcasted_iota(jnp.int32, (LANES, LANES), 1)
    for side, lane0 in ((0, HALF - HW), (1, HALF)):
        out = jnp.zeros((LANES, LANES), F32)
        for j in range(5):
            piece = pltpu.roll(gh_ref[LANES * j:LANES * (j + 1), :], (HW * j - lane0) % LANES, axis=1)
            out = jnp.where(lane >= HW * j, piece, out)
        pack_ref[side] = out


def image_kernel(*refs):
    accs = refs[:T]
    (a_ref, pack_ref, so_ref, sx_ref, se_ref, d_ref, ev_ref, eu_ref, pm_ref, out_ref,
     tb_ref, edge_ref, g_ref, halo, sm1, sm2, sr1, sr2, hm1, hm2, hr1, hr2, s_main, s_rem, acc_m, acc_r, sx_end, pieces, recvs, tails, recvs_t,
     halo_ss, halo_rs, swap_ss, swap_rs, red_ss, red_rs) = refs[T:]
    k = lax.axis_index('cols')
    r = lax.axis_index('rows')
    core, x = r % 2, r // 2
    near = r + 1 - 2 * core
    across = (r + 2) % 4
    prev, nxt = (r + 3) % 4, (r + 1) % 4
    homes = ({'rows': across, 'cols': 1 - k}, {'rows': across}, {'cols': 1 - k})

    barrier = pltpu.get_barrier_semaphore()
    for dev in ({'rows': prev}, {'rows': nxt}) + homes:
        pl.semaphore_signal(barrier, inc=1, device_id=dev, device_id_type=MESH_ID)

    own0 = k * CB
    far0 = CB - own0
    high16 = lax.broadcasted_iota(jnp.int32, (WIN, LANES), 1) >= HALF

    def put(v, tiles):
        rows = pl.ds(pl.multiple_of(v, WIN), WIN)
        for p in range(TILES):
            tb_ref[p, rows, :] = tiles[p].astype(BF)
        edge_ref[rows, :] = jnp.where(high16, tiles[0], tiles[9])

    def far_part(n, _):
        put(far0 + WIN * n, folded(accs, pl.multiple_of(SUB + WIN * n, SUB), WIN))
        return 0

    def own_part(n, _):
        put(own0 + WIN * n, [a_ref[p, pl.ds(pl.multiple_of(SUB + WIN * n, SUB), WIN), :] for p in range(TILES)])
        return 0

    last = CB // WIN - 1
    lax.fori_loop(1, last, far_part, 0)
    pl.semaphore_wait(barrier, 5)

    def remote(src, dst, ss, rs, i, dev):
        cp = pltpu.make_async_remote_copy(src_ref=src, dst_ref=dst, send_sem=ss.at[i], recv_sem=rs.at[i], device_id=dev, device_id_type=MESH_ID)
        cp.start()
        return cp

    halos = [remote(pack_ref.at[i], halo.at[i], halo_ss, halo_rs, i, {'rows': dev}) for i, dev in ((0, prev), (1, nxt))]

    lax.fori_loop(1, last, own_part, 0)
    none = jnp.zeros((SUB, LANES), F32)
    for n, side in ((0, CW - SUB), (last, 0)):
        off = SUB + WIN * n
        near_tiles = folded(accs, off, WIN)
        far_ends = folded(accs, side, SUB)
        order = (lambda v: [v, none]) if n == 0 else (lambda v: [none, v])
        put(far0 + WIN * n, [near_tiles[p] + jnp.concatenate(order(a_ref[p, side:side + SUB, :]), axis=0) for p in range(TILES)])
        put(own0 + WIN * n, [a_ref[p, off:off + WIN, :] + jnp.concatenate(order(far_ends[p]), axis=0) for p in range(TILES)])

    end_copy = remote(se_ref, sx_end, halo_ss, halo_rs, 2, {'rows': across})

    def to_rows(row0, n, t0, t1):
        a = jnp.concatenate([t0, t1], axis=1)
        g = lax.dot_general(pm_ref[...], a, (((1,), (1,)), ((), ())), preferred_element_type=F32).astype(BF)
        for ch in range(SUB):
            i, c = ch // 4, ch % 4
            g_ref[row0 + n * c:row0 + n * c + QTR, N_GRID * i:N_GRID * (i + 1)] = g[QTR * ch:QTR * (ch + 1), :]

    for m in range(4):
        to_rows(QTR * m, LANES, tb_ref[2 * m + 1], tb_ref[2 * m + 2])

    sms, srs, hms, hrs = (sm1, sm2), (sr1, sr2), (hm1, hm2), (hr1, hr2)
    swaps = []

    def columns(grp):
        start, n = GROUPS[grp]
        lane = lax.broadcasted_iota(jnp.int32, (n, LANES), 1)
        side = lane >> 6
        own_even, far_even = side == core, side != core
        block = (lane & (HALF - 1)) >> 4
        h = jnp.dot(g_ref[4 * start:4 * (start + n), :], ev_ref[...], preferred_element_type=F32)
        hc = [h[n * c:n * (c + 1)] for c in range(4)]
        rems = [v[:, 4 * LANES:] for v in hc]
        for cp in range(2):
            hs = [[v[:, LANES * i:LANES * (i + 1)] for i in range(4)] for v in hc[2 * cp:2 * cp + 2]]
            for i in range(4):
                dp, t = i // 2, i % 2
                odd = pltpu.roll(hs[1][i], HALF, axis=1)
                sms[grp][dp, cp, t] = jnp.where(far_even, hs[0][i], odd).astype(BF)
                hms[grp][dp, cp, t, core] = jnp.where(own_even, hs[0][i], odd).astype(BF)
        for t in range(2):
            both = []
            for h in range(2):
                i = 2 * t + h
                out = rems[i]
                for c in range(4):
                    if c != i:
                        out = jnp.where(block == c, pltpu.roll(rems[c], (WIN * (c - i)) % LANES, axis=1), out)
                both.append(out)
            srs[grp][t] = jnp.where(core == 0, both[1], both[0]).astype(BF)
            hrs[grp][t, core] = jnp.where(core == 0, both[0], both[1]).astype(BF)
        swaps.append(remote(sms[grp], hms[grp].at[:, :, :, core], swap_ss, swap_rs, 2 * grp, {'rows': near}))
        swaps.append(remote(srs[grp], hrs[grp].at[:, core], swap_ss, swap_rs, 2 * grp + 1, {'rows': near}))

    columns(0)

    for h in halos:
        h.wait()
    lane = lax.broadcasted_iota(jnp.int32, (LANES, LANES), 1)
    low = lane < HALF
    t0s, t9s = [], []
    for j in range(5):
        rows = slice(LANES * j, LANES * (j + 1))
        add_first = pltpu.roll(halo[1], (HALF - HW * j) % LANES, axis=1)
        add_last = pltpu.roll(halo[0], (HALF - HW - HW * j) % LANES, axis=1)
        e = edge_ref[rows, :] + jnp.where(low, jnp.where(lane >= HALF - HW, add_last, 0.0), jnp.where(lane < HALF + HW, add_first, 0.0))
        t0s.append(jnp.where(low, tb_ref[0, rows, :].astype(F32), e).astype(BF))
        t9s.append(jnp.where(low, e, tb_ref[9, rows, :].astype(F32)).astype(BF))
    lane = lax.broadcasted_iota(jnp.int32, (PB, LANES), 1)
    low = lane < HALF
    to_rows(4 * LANES, QTR, jnp.concatenate(t0s, axis=0), jnp.concatenate(t9s, axis=0))
    columns(1)

    def turn(rows):
        t = [rows[:, LANES * i:LANES * (i + 1)].T for i in range(5)]
        return [jnp.concatenate([t[2 * i], t[2 * i + 1], t[4][HALF * i:HALF * (i + 1)]], axis=0) for i in range(2)]


    for cp in swaps[:2]:
        cp.wait_recv()
    n0 = 4 * GROUPS[0][1]

    def block_of(grp, j):
        return jnp.concatenate([hms[grp][(x + j) % 2, cp].reshape(4 * GROUPS[grp][1], LANES) for cp in range(2)], axis=1)

    for j, ref in ((1, sx_ref), (0, so_ref)):
        acc_m[j] = jnp.dot(eu_ref[x, :, :n0], block_of(0, j), preferred_element_type=F32)
        for cp in range(2):
            s_main[j, 0, cp], s_main[j, 1, cp] = turn(jnp.concatenate([ref[2 * cp + core], ref[2 * cp + 1 - core]], axis=0))
    acc_r[...] = jnp.dot(eu_ref[x, :, :n0], hrs[0][...].reshape(n0, LANES), preferred_element_type=F32)

    for cp in swaps[2:]:
        cp.wait_recv()

    def rows_dft(half, acc, rhs):
        rows = pl.ds(pl.multiple_of(half * N_IMG, WIN), N_IMG)
        total = acc[rows, :] + jnp.dot(eu_ref[x, rows, n0:], rhs, preferred_element_type=F32)
        return total[:PB], total[PB:]

    quarter = lax.broadcasted_iota(jnp.int32, (PB // 4, LANES), 1) >> 5

    def piece(half, j):
        i_re, i_im = rows_dft(half, acc_m.at[j], block_of(1, j))
        rows = pl.ds(pl.multiple_of(half * PB, SUB), PB)
        re, im = None, None
        for cp in range(2):
            cols = slice(LANES * cp, LANES * (cp + 1))
            s_re, s_im = s_main[j, 0, cp, rows, :], s_main[j, 1, cp, rows, :]
            a = s_re * i_re[:, cols] + s_im * i_im[:, cols]
            b = s_re * i_im[:, cols] - s_im * i_re[:, cols]
            re, im = (a, b) if re is None else (re + a, im + b)
        return jnp.where(low, re + pltpu.roll(re, HALF, axis=1), im + pltpu.roll(im, HALF, axis=1))

    def rest(half):
        i_re, i_im = rows_dft(half, acc_r, hrs[1][...].reshape(4 * GROUPS[1][1], LANES))
        rows = pl.ds(pl.multiple_of(half * PB, SUB), PB)
        s_re, s_im = s_rem[0, rows, :], s_rem[1, rows, :]

        def fold(v):
            v = v + pltpu.roll(v, LANES - QTR, axis=1)
            return v + pltpu.roll(v, LANES - WIN, axis=1)

        re, im = fold(s_re * i_re + s_im * i_im), fold(s_re * i_im - s_im * i_re)
        both = jnp.where(lane & (HALF - 1) < WIN, re, pltpu.roll(im, WIN, axis=1))
        outs = []
        for dp in range(2):
            out = None
            for g in range(4):
                v = both[PB // 4 * g:PB // 4 * (g + 1)]
                if g + 2 * dp:
                    v = pltpu.roll(v, (QTR * g + HALF * dp) % LANES, axis=1)
                out = v if out is None else jnp.where(quarter == g, v, out)
            outs.append(out)
        return jnp.where(x == 0, outs[0], outs[1]), jnp.where(x == 0, outs[1], outs[0])

    sends = []
    for i, (half, j) in enumerate(((1 - k, 1), (k, 1), (1 - k, 0))):
        pieces[i] = piece(half, j)
        sends.append(remote(pieces.at[i], recvs.at[i], red_ss, red_rs, i, homes[i]))
    end_copy.wait_recv()
    s_rem[0], s_rem[1] = turn(jnp.concatenate([jnp.where(x == j, se_ref[c], sx_end[c]) for j in range(2) for c in range(4)], axis=0))
    tails[2], tails[0] = rest(1 - k)
    sends.append(remote(tails.at[0], recvs_t.at[0], red_ss, red_rs, 3, homes[0]))
    rem, tails[1] = rest(k)
    for i in (1, 2):
        sends.append(remote(tails.at[i], recvs_t.at[i], red_ss, red_rs, 3 + i, homes[i]))
    main = piece(k, 0)
    d8 = jnp.broadcast_to(jnp.concatenate([d_ref[...][None, :], jnp.zeros((1, HALF), F32)], axis=1), (SUB, N_IMG + HALF))
    dq = d8
    for j in range(1, ROWS):
        dq = jnp.where(r == j, pltpu.roll(d8, N_IMG + HALF - QB * j, axis=1), dq)
    dp = jnp.where(k == 0, d8, pltpu.roll(d8, N_IMG + HALF - PB, axis=1))[:, :2 * LANES]
    dd = jnp.concatenate([dp] * WIN, axis=0).T[:PB] * dq[:1, :LANES]

    for i in (2, 0, 1):
        sends[i].wait_recv()
        main = main + recvs[i]
    for i in (2, 0, 1):
        sends[3 + i].wait_recv()
        rem = rem + recvs_t[i]
    for o in range(2):
        m = pltpu.roll(main, HALF, axis=1) if o else main
        for j in range(4):
            rows = slice(PB // 4 * j, PB // 4 * (j + 1))
            tail = pltpu.roll(rem, (HALF - QTR * j - WIN * o) % LANES, axis=1)
            out_ref[o, rows, :] = (jnp.where(low[rows], m[rows], tail) * dd[rows])[:, :QB]

    for cp in sends + swaps + [end_copy]:
        cp.wait_send()


def solution(mesh):
    sample_spec = ('exam', 'rows', 'cols')
    vm = pl.BlockSpec(memory_space=pltpu.VMEM)
    hbm = pl.BlockSpec(memory_space=pltpu.HBM)
    spread_scratch = ([VMEM((LANES, LANES), F32)] * 4 + [VMEM((LANES * PS, LANES), F32)] * 2
                      + [VMEM((LANES, WIDE * 3), BF), VMEM((NB, LANES), jnp.int32), pltpu.SMEM((NB, LANES), jnp.int32), pltpu.SemaphoreType.DMA])
    acc_shape = [jax.ShapeDtypeStruct((NG * CW, LANES), F32)] * T
    big = 6 * MIB

    def local_fn(kspace, wts_y, wts_x, idx_y, idx_x, coil_maps, deapod):
        own, far, maps, maps_end = pl.pallas_call(
            prep_kernel,
            out_shape=[jax.ShapeDtypeStruct((PAY * NB, LANES), F32)] * 2 + [jax.ShapeDtypeStruct((4, n, N_GRID), F32) for n in (HALF, WIN)],
            in_specs=[hbm] * 6, out_specs=[vm] * 4, name='prep',
            scratch_shapes=[VMEM((2, SUB, NS), F32), VMEM((KW, NS), F32), VMEM((KW, NS), F32), VMEM((NB, LANES), jnp.int32), VMEM((NB, LANES), jnp.int32), VMEM((2, 4, QB, N_IMG), F32), pltpu.SemaphoreType.DMA((6,))],
            compiler_params=pltpu.CompilerParams(vmem_limit_bytes=SUB * MIB),
        )(*[pltpu.with_memory_space_constraint(v, pltpu.HBM) for v in (kspace, wts_y, wts_x, idx_y.reshape(NB, LANES), idx_x.reshape(NB, LANES), jnp.swapaxes(coil_maps, 2, 3))])
        far_in = lax.ppermute(far, 'cols', [(0, 1), (1, 0)])
        half, *accs = pl.pallas_call(
            own_kernel, out_shape=[jax.ShapeDtypeStruct((11, CW, LANES), F32)] + acc_shape, in_specs=[vm], out_specs=[vm] * (T + 1),
            scratch_shapes=spread_scratch, compiler_params=pltpu.CompilerParams(vmem_limit_bytes=big), name='spread_own',
            cost_estimate=pl.CostEstimate(flops=GIGA, bytes_accessed=4 * MIB, transcendentals=0),
        )(own)
        *accs, pack = pl.pallas_call(
            far_kernel, out_shape=acc_shape + [jax.ShapeDtypeStruct((2, LANES, LANES), F32)],
            in_specs=[vm] * (T + 2), out_specs=[vm] * (T + 1), scratch_shapes=[VMEM((N_GRID, LANES), F32)] + spread_scratch,
            input_output_aliases={i + 2: i for i in range(T)},
            compiler_params=pltpu.CompilerParams(vmem_limit_bytes=big), name='spread_far',
            cost_estimate=pl.CostEstimate(flops=GIGA, bytes_accessed=4 * MIB, transcendentals=0),
        )(far_in, half, *accs)
        maps_x = lax.ppermute(maps, 'rows', [(i, (i + 2) % ROWS) for i in range(ROWS)])
        dma = pltpu.SemaphoreType.DMA
        half_bufs = [VMEM((2, 2, 2, n, LANES), BF) for _, n in GROUPS] + [VMEM((2, n, LANES), BF) for _, n in GROUPS]
        full_bufs = [VMEM((2, 2, 2, 2, n, LANES), BF) for _, n in GROUPS] + [VMEM((2, 2, n, LANES), BF) for _, n in GROUPS]
        return pl.pallas_call(
            image_kernel,
            out_shape=jax.ShapeDtypeStruct((2, PB, QB), F32), in_specs=[vm] * (T + 9), out_specs=vm,
            scratch_shapes=[VMEM((TILES, N_GRID, LANES), BF), VMEM((N_GRID, LANES), F32), VMEM((4 * RB, 2 * N_GRID), BF), VMEM((2, LANES, LANES), F32)] + half_bufs + full_bufs + [
                VMEM((2, 2, 2, N_IMG, LANES), F32), VMEM((2, N_IMG, LANES), F32),
                VMEM((2, 2 * N_IMG, 2 * LANES), F32), VMEM((2 * N_IMG, LANES), F32), VMEM((4, WIN, N_GRID), F32),
                VMEM((3, PB, LANES), F32), VMEM((3, PB, LANES), F32), VMEM((3, PB // 4, LANES), F32), VMEM((3, PB // 4, LANES), F32),
                dma((3,)), dma((3,)), dma((4,)), dma((4,)), dma((6,)), dma((6,)),
            ],
            compiler_params=pltpu.CompilerParams(vmem_limit_bytes=11 * MIB, collective_id=0, has_side_effects=True), name='image',
        )(*accs, half, pack, maps, maps_x, maps_end, deapod, col_dft(), row_dft(), unmix())

    return jax.shard_map(
        local_fn,
        mesh=mesh,
        in_specs=(P(None, None, sample_spec), P(None, sample_spec), P(None, sample_spec), P(sample_spec), P(sample_spec), P(None, ('exam', 'cols'), None, 'rows'), P()),
        out_specs=P(None, ('exam', 'cols'), 'rows'),
        check_vma=False,
    )
```

```python
import functools
import math

import jax
import jax.numpy as jnp
import numpy as np
from jax import lax
from jax.experimental import pallas as pl
from jax.experimental.pallas import tpu as pltpu
from jax.sharding import PartitionSpec as P

BF = jnp.bfloat16
F32 = jnp.float32
VMEM = pltpu.VMEM
LANES = 128
MIB = 1 << 20
GIGA = 4000 * MIB
TILES = 10
SUB, WIN, QTR, HALF, WIDE = 8, 16, 32, 64, 256
N_GRID, N_IMG, N_COILS, KW = 640, 320, 8, 6
ROWS, COLS = 4, 2
RB, CB, QB = N_GRID // ROWS, N_GRID // COLS, N_IMG // ROWS
PB = N_IMG // COLS
NS = 4096
NB = NS // LANES
STEP = 11
NG = 15
CW = CB + WIN
T = 6
PS = 9
PAY = 21
CODE = 512
HW = 24
ORDER = tuple(range(1, 9)) + (0, 9)
GROUPS = ((0, 128), (128, 32))
MESH_ID = pl.DeviceIdType.MESH


def dft_parts():
    freq = np.arange(N_GRID) - N_GRID // 2
    pos = np.arange(N_IMG) - N_IMG // 2
    ang = ((freq[:, None] * pos[None, :]) % N_GRID).astype(np.float32) * np.float32(2.0 * math.pi / N_GRID)
    norm = np.float32(1.0 / math.sqrt(N_GRID))
    c, s = np.cos(ang) * norm, np.sin(ang) * norm
    return np.stack([np.stack([c, s], 1), np.stack([-s, c], 1)], 0)


def col_dft():
    e = dft_parts()
    out = np.zeros((2 * N_GRID, N_GRID), np.float32)
    for dp in range(2):
        for t in range(2):
            for h in range(2):
                q0 = QB * (2 * dp + h)
                l0 = LANES * (2 * dp + t) + HALF * h
                out[:, l0:l0 + HALF] = e[:, :, t, q0:q0 + HALF].reshape(2 * N_GRID, HALF)
    for t in range(2):
        for d in range(4):
            l0 = 4 * LANES + HALF * (d // 2) + WIN * (2 * t + d % 2)
            out[:, l0:l0 + WIN] = e[:, :, t, QB * d + HALF:QB * (d + 1)].reshape(2 * N_GRID, WIN)
    return jnp.asarray(out, BF)


def row_dft():
    e = dft_parts()
    rows = np.concatenate([np.arange(WIN * l, WIN * (l + 1)) for l in ORDER])
    chips = []
    for x in range(2):
        parts = []
        for start, n in GROUPS:
            for t in range(2):
                for b in range(2):
                    parts.append(e[t, (2 * x + b) * RB + rows[start:start + n]])
        m = np.concatenate(parts, 0)
        chips.append(np.concatenate([m[:, :, PB * h:PB * (h + 1)].reshape(N_GRID, N_IMG).T for h in range(2)], 0))
    return jnp.asarray(np.array(chips), BF)


def unmix():
    m = np.zeros((WIDE, WIDE), np.float32)
    for ch in range(SUB):
        for pp in range(2):
            for i in range(WIN):
                m[ch * QTR + WIN * pp + (i + SUB) % WIN, pp * 128 + i * SUB + ch] = 1.0
    return jnp.asarray(m, BF)


def prep_kernel(ks_hbm, wy_hbm, wx_hbm, iy_hbm, ix_hbm, maps_hbm, own_ref, far_ref, sp_ref, sq_ref, ks_ref, wy_ref, wx_ref, iy_ref, ix_ref, maps_ref, sem):
    k = lax.axis_index('cols')
    r = lax.axis_index('rows')
    loads = []
    for src, dst in ((iy_hbm, iy_ref), (ix_hbm, ix_ref), (wx_hbm, wx_ref), (wy_hbm, wy_ref), (ks_hbm, ks_ref), (maps_hbm, maps_ref)):
        cp = pltpu.make_async_copy(src, dst, sem.at[len(loads)])
        cp.start()
        loads.append(cp)
    loads[0].wait()
    loads[1].wait()
    iy = iy_ref[...]
    code = ((iy - r * RB + 5) * CODE + ix_ref[...] - k * CB + 5).astype(F32)
    for i in range(2, 5):
        loads[i].wait()
    lo = jnp.concatenate([ks_ref[0, 0:4, :], ks_ref[1, 0:4, :]], axis=0)
    hi = jnp.concatenate([ks_ref[0, 4:SUB, :], ks_ref[1, 4:SUB, :]], axis=0)
    first = k == 0
    for ref, y in ((own_ref, jnp.where(first, lo, hi)), (far_ref, jnp.where(first, hi, lo))):
        for b in range(NB):
            cols = slice(LANES * b, LANES * (b + 1))
            ref[PAY * b:PAY * b + SUB, :] = y[:, cols]
            ref[PAY * b + SUB:PAY * b + SUB + KW, :] = wx_ref[:, cols]
            ref[PAY * (b + 1) - KW - 1:PAY * (b + 1) - 1, :] = wy_ref[:, cols]
            ref[PAY * (b + 1) - 1:PAY * (b + 1), :] = code[b:b + 1, :]
    loads[5].wait()
    for c in range(4):
        for ref, q in ((sp_ref, slice(0, HALF)), (sq_ref, slice(HALF, QB))):
            for i in range(2):
                ref[c, :, WIDE * i:WIDE * (i + 1)] = maps_ref[i, c, q, :WIDE]
            ref[c, :, 2 * WIDE:] = jnp.concatenate([maps_ref[i, c, q, WIDE:] for i in range(2)], axis=1)


def split3(x):
    hi = x.astype(BF).astype(F32)
    r = x - hi
    mid = r.astype(BF).astype(F32)
    return hi, mid, r - mid


def accumulate(pay_ref, accs, us, xs, vs, r_ref, int_ref, base_ref, sem):
    row_i = lax.broadcasted_iota(jnp.int32, (WIN, LANES), 0)

    def make_u(blk, k):
        off = jnp.minimum(blk, NB - 1) * PAY
        y8 = pay_ref[pl.ds(off, SUB), :]
        wx = pay_ref[pl.ds(off + SUB, SUB), :]
        wyp = pay_ref[pl.ds(off + PAY - SUB, SUB), :]
        d = (row_i - (wyp[7:, :].astype(jnp.int32) // CODE)) & (WIN - 1)
        p = jnp.zeros((WIN, LANES), F32)
        for a in range(KW):
            p = jnp.where(d == a, wyp[a + 1:a + 2, :], p)
        us[k][...] = jnp.concatenate([y8 * p[i:i + 1, :] for i in range(WIN)], axis=0).T
        x3 = list(split3(wx)) + [jnp.zeros((LANES - HW, LANES), F32)]
        xs[k][...] = jnp.concatenate(x3, axis=0).T

    def make_v(k):
        lhs = xs[k][...].astype(BF)
        u = us[k][...]
        for bp in range(3):
            w = jnp.dot(lhs, r_ref[:, WIDE * bp:WIDE * bp + WIDE], preferred_element_type=F32)
            for c in range(2):
                v = w[:, LANES * c:LANES * (c + 1)] * u
                for g in range(WIN):
                    vs[k][pl.ds(SUB * PS * g + 2 * bp + c, SUB, stride=PS), :] = v[SUB * g:SUB * g + SUB, :]

    def add_tiles(blk, k):
        row = base_ref.at[blk]
        for j in range(LANES):
            acc = accs[j % T]
            b = row[j]
            acc[pl.ds(b, SUB), :] = acc[pl.ds(b, SUB), :] + vs[k][PS * j:PS * j + SUB, :]

    code = jnp.concatenate([pay_ref[PAY * (b + 1) - 1:PAY * (b + 1), :] for b in range(NB)], axis=0).astype(jnp.int32)
    int_ref[...] = (((code // CODE - 5) * 187) >> STEP) * CW + (code & (CODE - 1))
    kk = lax.broadcasted_iota(jnp.int32, (LANES, WIDE * 3), 0)
    ll = lax.broadcasted_iota(jnp.int32, (LANES, WIDE * 3), 1)
    r_ref[...] = jnp.where((kk < HW) & ((kk & 7) == (ll >> 7)), 1.0, 0.0).astype(BF)
    for v in vs:
        v[...] = jnp.zeros_like(v)
    load = pltpu.make_async_copy(int_ref, base_ref, sem)
    load.start()
    make_u(0, 0)
    make_u(1, 1)
    make_v(0)
    load.wait()

    def body(n, _):
        k = 2 * n
        make_v(1)
        add_tiles(k, 0)
        make_u(k + 2, 0)
        make_v(0)
        add_tiles(k + 1, 1)
        make_u(k + 3, 1)
        return 0

    lax.fori_loop(0, NB // 2, body, 0)


def folded(accs, off, n, clear=False):
    def total(g):
        rows = pl.ds(pl.multiple_of(g * CW + off, SUB), n)
        v = accs[0][rows, :]
        for a in accs[1:]:
            v = v + a[rows, :]
        if clear:
            for a in accs:
                a[rows, :] = jnp.zeros((n, LANES), F32)
        return v

    row = lax.broadcasted_iota(jnp.int32, (n, LANES), 1) >> 3
    tiles = [None] * TILES
    for g in range(NG):
        v = total(g)
        if g == 0:
            ghost = v
        first = 5 + STEP * g
        for p in range(TILES):
            lo, hi = max(first, SUB + WIN * p), min(first + WIN, SUB + WIN * (p + 1))
            if lo < hi:
                part = jnp.where((row - lo & (WIN - 1)) < hi - lo, v, 0.0)
                tiles[p] = part if tiles[p] is None else tiles[p] + part
    return tiles + [jnp.where(row >= SUB, v, ghost)]


def own_kernel(pay_ref, out_ref, *refs):
    accs, scr = refs[:T], refs[T:]

    def clear(n, _):
        for a in accs:
            a[pl.ds(pl.multiple_of(n * CW, SUB), CW), :] = jnp.zeros((CW, LANES), F32)
        return 0

    lax.fori_loop(0, NG, clear, 0)
    accumulate(pay_ref, accs, scr[:2], scr[2:4], scr[4:6], *scr[6:])

    def fold(q, _):
        off = pl.multiple_of(q * WIN, WIN)
        for p, t in enumerate(folded(accs, off, WIN, clear=True)):
            out_ref[p, pl.ds(off, WIN), :] = t
        return 0

    lax.fori_loop(0, CW // WIN, fold, 0)


def far_kernel(pay_ref, a_ref, *refs):
    accs, pack_ref, gh_ref, scr = refs[T:2 * T], refs[2 * T], refs[2 * T + 1], refs[2 * T + 2:]
    accumulate(pay_ref, accs, scr[:2], scr[2:4], scr[4:6], *scr[6:])
    own0 = lax.axis_index('cols') * CB
    far0 = CB - own0

    def ghost(off, n):
        high = lax.broadcasted_iota(jnp.int32, (n, LANES), 1) >= HALF
        ends = []
        for g in (0, NG - 1):
            rows = pl.ds(pl.multiple_of(g * CW + off, SUB), n)
            v = accs[0][rows, :]
            for a in accs[1:]:
                v = v + a[rows, :]
            ends.append(v)
        return jnp.where(high, ends[1], ends[0])

    def copy(n, _):
        o = pl.multiple_of(n * QTR, SUB)
        gh_ref[pl.ds(pl.multiple_of(far0 + o, SUB), QTR), :] = ghost(SUB + o, QTR)
        gh_ref[pl.ds(pl.multiple_of(own0 + o, SUB), QTR), :] = a_ref[TILES, pl.ds(pl.multiple_of(SUB + o, SUB), QTR), :]
        return 0

    lax.fori_loop(0, CB // QTR, copy, 0)
    for dst, add in ((own0, ghost(CW - SUB, SUB)), (own0 + CB - SUB, ghost(0, SUB)), (far0, a_ref[TILES, CW - SUB:, :]), (far0 + CB - SUB, a_ref[TILES, :SUB, :])):
        rows = pl.ds(pl.multiple_of(dst, SUB), SUB)
        gh_ref[rows, :] = gh_ref[rows, :] + add

    lane = lax.broadcasted_iota(jnp.int32, (LANES, LANES), 1)
    for side, lane0 in ((0, HALF - HW), (1, HALF)):
        out = jnp.zeros((LANES, LANES), F32)
        for j in range(5):
            piece = pltpu.roll(gh_ref[LANES * j:LANES * (j + 1), :], (HW * j - lane0) % LANES, axis=1)
            out = jnp.where(lane >= HW * j, piece, out)
        pack_ref[side] = out


def image_kernel(*refs):
    accs = refs[:T]
    (a_ref, pack_ref, so_ref, sx_ref, se_ref, d_ref, ev_ref, eu_ref, pm_ref, out_ref,
     tb_ref, edge_ref, g_ref, halo, sm1, sm2, sr1, sr2, hm1, hm2, hr1, hr2, s_main, s_rem, acc_m, acc_r, sx_end, pieces, recvs, tails, recvs_t,
     halo_ss, halo_rs, swap_ss, swap_rs, red_ss, red_rs) = refs[T:]
    k = lax.axis_index('cols')
    r = lax.axis_index('rows')
    core, x = r % 2, r // 2
    near = r + 1 - 2 * core
    across = (r + 2) % 4
    prev, nxt = (r + 3) % 4, (r + 1) % 4
    homes = ({'rows': across, 'cols': 1 - k}, {'rows': across}, {'cols': 1 - k})

    barrier = pltpu.get_barrier_semaphore()
    for dev in ({'rows': prev}, {'rows': nxt}) + homes:
        pl.semaphore_signal(barrier, inc=1, device_id=dev, device_id_type=MESH_ID)

    own0 = k * CB
    far0 = CB - own0
    high16 = lax.broadcasted_iota(jnp.int32, (WIN, LANES), 1) >= HALF

    def put(v, tiles):
        rows = pl.ds(pl.multiple_of(v, WIN), WIN)
        for p in range(TILES):
            tb_ref[p, rows, :] = tiles[p].astype(BF)
        edge_ref[rows, :] = jnp.where(high16, tiles[0], tiles[9])

    def far_part(n, _):
        put(far0 + WIN * n, folded(accs, pl.multiple_of(SUB + WIN * n, SUB), WIN))
        return 0

    def own_part(n, _):
        put(own0 + WIN * n, [a_ref[p, pl.ds(pl.multiple_of(SUB + WIN * n, SUB), WIN), :] for p in range(TILES)])
        return 0

    last = CB // WIN - 1
    lax.fori_loop(1, last, far_part, 0)
    pl.semaphore_wait(barrier, 5)

    def remote(src, dst, ss, rs, i, dev):
        cp = pltpu.make_async_remote_copy(src_ref=src, dst_ref=dst, send_sem=ss.at[i], recv_sem=rs.at[i], device_id=dev, device_id_type=MESH_ID)
        cp.start()
        return cp

    halos = [remote(pack_ref.at[i], halo.at[i], halo_ss, halo_rs, i, {'rows': dev}) for i, dev in ((0, prev), (1, nxt))]

    lax.fori_loop(1, last, own_part, 0)
    none = jnp.zeros((SUB, LANES), F32)
    for n, side in ((0, CW - SUB), (last, 0)):
        off = SUB + WIN * n
        near_tiles = folded(accs, off, WIN)
        far_ends = folded(accs, side, SUB)
        order = (lambda v: [v, none]) if n == 0 else (lambda v: [none, v])
        put(far0 + WIN * n, [near_tiles[p] + jnp.concatenate(order(a_ref[p, side:side + SUB, :]), axis=0) for p in range(TILES)])
        put(own0 + WIN * n, [a_ref[p, off:off + WIN, :] + jnp.concatenate(order(far_ends[p]), axis=0) for p in range(TILES)])

    end_copy = remote(se_ref, sx_end, halo_ss, halo_rs, 2, {'rows': across})

    def to_rows(row0, n, t0, t1):
        a = jnp.concatenate([t0, t1], axis=1)
        g = lax.dot_general(pm_ref[...], a, (((1,), (1,)), ((), ())), preferred_element_type=F32).astype(BF)
        for ch in range(SUB):
            i, c = ch // 4, ch % 4
            g_ref[row0 + n * c:row0 + n * c + QTR, N_GRID * i:N_GRID * (i + 1)] = g[QTR * ch:QTR * (ch + 1), :]

    for m in range(4):
        to_rows(QTR * m, LANES, tb_ref[2 * m + 1], tb_ref[2 * m + 2])

    sms, srs, hms, hrs = (sm1, sm2), (sr1, sr2), (hm1, hm2), (hr1, hr2)
    swaps = []

    def columns(grp):
        start, n = GROUPS[grp]
        lane = lax.broadcasted_iota(jnp.int32, (n, LANES), 1)
        side = lane >> 6
        own_even, far_even = side == core, side != core
        block = (lane & (HALF - 1)) >> 4
        h = jnp.dot(g_ref[4 * start:4 * (start + n), :], ev_ref[...], preferred_element_type=F32)
        hc = [h[n * c:n * (c + 1)] for c in range(4)]
        rems = [v[:, 4 * LANES:] for v in hc]
        for cp in range(2):
            hs = [[v[:, LANES * i:LANES * (i + 1)] for i in range(4)] for v in hc[2 * cp:2 * cp + 2]]
            for i in range(4):
                dp, t = i // 2, i % 2
                odd = pltpu.roll(hs[1][i], HALF, axis=1)
                sms[grp][dp, cp, t] = jnp.where(far_even, hs[0][i], odd).astype(BF)
                hms[grp][dp, cp, t, core] = jnp.where(own_even, hs[0][i], odd).astype(BF)
        for t in range(2):
            both = []
            for h in range(2):
                i = 2 * t + h
                out = rems[i]
                for c in range(4):
                    if c != i:
                        out = jnp.where(block == c, pltpu.roll(rems[c], (WIN * (c - i)) % LANES, axis=1), out)
                both.append(out)
            srs[grp][t] = jnp.where(core == 0, both[1], both[0]).astype(BF)
            hrs[grp][t, core] = jnp.where(core == 0, both[0], both[1]).astype(BF)
        swaps.append(remote(sms[grp], hms[grp].at[:, :, :, core], swap_ss, swap_rs, 2 * grp, {'rows': near}))
        swaps.append(remote(srs[grp], hrs[grp].at[:, core], swap_ss, swap_rs, 2 * grp + 1, {'rows': near}))

    columns(0)

    for h in halos:
        h.wait()
    lane = lax.broadcasted_iota(jnp.int32, (LANES, LANES), 1)
    low = lane < HALF
    t0s, t9s = [], []
    for j in range(5):
        rows = slice(LANES * j, LANES * (j + 1))
        add_first = pltpu.roll(halo[1], (HALF - HW * j) % LANES, axis=1)
        add_last = pltpu.roll(halo[0], (HALF - HW - HW * j) % LANES, axis=1)
        e = edge_ref[rows, :] + jnp.where(low, jnp.where(lane >= HALF - HW, add_last, 0.0), jnp.where(lane < HALF + HW, add_first, 0.0))
        t0s.append(jnp.where(low, tb_ref[0, rows, :].astype(F32), e).astype(BF))
        t9s.append(jnp.where(low, e, tb_ref[9, rows, :].astype(F32)).astype(BF))
    lane = lax.broadcasted_iota(jnp.int32, (PB, LANES), 1)
    low = lane < HALF
    to_rows(4 * LANES, QTR, jnp.concatenate(t0s, axis=0), jnp.concatenate(t9s, axis=0))
    columns(1)

    def turn(rows):
        t = [rows[:, LANES * i:LANES * (i + 1)].T for i in range(5)]
        return [jnp.concatenate([t[2 * i], t[2 * i + 1], t[4][HALF * i:HALF * (i + 1)]], axis=0) for i in range(2)]


    for cp in swaps[:2]:
        cp.wait_recv()
    n0 = 4 * GROUPS[0][1]

    def block_of(grp, j):
        return jnp.concatenate([hms[grp][(x + j) % 2, cp].reshape(4 * GROUPS[grp][1], LANES) for cp in range(2)], axis=1)

    for j, ref in ((1, sx_ref), (0, so_ref)):
        acc_m[j] = jnp.dot(eu_ref[x, :, :n0], block_of(0, j), preferred_element_type=F32)
        for cp in range(2):
            s_main[j, 0, cp], s_main[j, 1, cp] = turn(jnp.concatenate([ref[2 * cp + core], ref[2 * cp + 1 - core]], axis=0))
    acc_r[...] = jnp.dot(eu_ref[x, :, :n0], hrs[0][...].reshape(n0, LANES), preferred_element_type=F32)

    for cp in swaps[2:]:
        cp.wait_recv()

    def rows_dft(half, acc, rhs):
        rows = pl.ds(pl.multiple_of(half * N_IMG, WIN), N_IMG)
        total = acc[rows, :] + jnp.dot(eu_ref[x, rows, n0:], rhs, preferred_element_type=F32)
        return total[:PB], total[PB:]

    quarter = lax.broadcasted_iota(jnp.int32, (PB // 4, LANES), 1) >> 5

    def piece(half, j):
        i_re, i_im = rows_dft(half, acc_m.at[j], block_of(1, j))
        rows = pl.ds(pl.multiple_of(half * PB, SUB), PB)
        re, im = None, None
        for cp in range(2):
            cols = slice(LANES * cp, LANES * (cp + 1))
            s_re, s_im = s_main[j, 0, cp, rows, :], s_main[j, 1, cp, rows, :]
            a = s_re * i_re[:, cols] + s_im * i_im[:, cols]
            b = s_re * i_im[:, cols] - s_im * i_re[:, cols]
            re, im = (a, b) if re is None else (re + a, im + b)
        return jnp.where(low, re + pltpu.roll(re, HALF, axis=1), im + pltpu.roll(im, HALF, axis=1))

    def rest(half):
        i_re, i_im = rows_dft(half, acc_r, hrs[1][...].reshape(4 * GROUPS[1][1], LANES))
        rows = pl.ds(pl.multiple_of(half * PB, SUB), PB)
        s_re, s_im = s_rem[0, rows, :], s_rem[1, rows, :]

        def fold(v):
            v = v + pltpu.roll(v, LANES - QTR, axis=1)
            return v + pltpu.roll(v, LANES - WIN, axis=1)

        re, im = fold(s_re * i_re + s_im * i_im), fold(s_re * i_im - s_im * i_re)
        both = jnp.where(lane & (HALF - 1) < WIN, re, pltpu.roll(im, WIN, axis=1))
        outs = []
        for dp in range(2):
            out = None
            for g in range(4):
                v = both[PB // 4 * g:PB // 4 * (g + 1)]
                if g + 2 * dp:
                    v = pltpu.roll(v, (QTR * g + HALF * dp) % LANES, axis=1)
                out = v if out is None else jnp.where(quarter == g, v, out)
            outs.append(out)
        return jnp.where(x == 0, outs[0], outs[1]), jnp.where(x == 0, outs[1], outs[0])

    sends = []
    for i, (half, j) in enumerate(((1 - k, 1), (k, 1), (1 - k, 0))):
        pieces[i] = piece(half, j)
        sends.append(remote(pieces.at[i], recvs.at[i], red_ss, red_rs, i, homes[i]))
    end_copy.wait_recv()
    s_rem[0], s_rem[1] = turn(jnp.concatenate([jnp.where(x == j, se_ref[c], sx_end[c]) for j in range(2) for c in range(4)], axis=0))
    tails[2], tails[0] = rest(1 - k)
    sends.append(remote(tails.at[0], recvs_t.at[0], red_ss, red_rs, 3, homes[0]))
    rem, tails[1] = rest(k)
    for i in (1, 2):
        sends.append(remote(tails.at[i], recvs_t.at[i], red_ss, red_rs, 3 + i, homes[i]))
    main = piece(k, 0)
    d8 = jnp.broadcast_to(jnp.concatenate([d_ref[...][None, :], jnp.zeros((1, HALF), F32)], axis=1), (SUB, N_IMG + HALF))
    dq = d8
    for j in range(1, ROWS):
        dq = jnp.where(r == j, pltpu.roll(d8, N_IMG + HALF - QB * j, axis=1), dq)
    dp = jnp.where(k == 0, d8, pltpu.roll(d8, N_IMG + HALF - PB, axis=1))[:, :2 * LANES]
    dd = jnp.concatenate([dp] * WIN, axis=0).T[:PB] * dq[:1, :LANES]

    for i in (2, 0, 1):
        sends[i].wait_recv()
        main = main + recvs[i]
    for i in (2, 0, 1):
        sends[3 + i].wait_recv()
        rem = rem + recvs_t[i]
    for o in range(2):
        m = pltpu.roll(main, HALF, axis=1) if o else main
        for j in range(4):
            rows = slice(PB // 4 * j, PB // 4 * (j + 1))
            tail = pltpu.roll(rem, (HALF - QTR * j - WIN * o) % LANES, axis=1)
            out_ref[o, rows, :] = (jnp.where(low[rows], m[rows], tail) * dd[rows])[:, :QB]

    for cp in sends + swaps + [end_copy]:
        cp.wait_send()


def solution(mesh):
    sample_spec = ('exam', 'rows', 'cols')
    vm = pl.BlockSpec(memory_space=pltpu.VMEM)
    hbm = pl.BlockSpec(memory_space=pltpu.HBM)
    spread_scratch = ([VMEM((LANES, LANES), F32)] * 4 + [VMEM((LANES * PS, LANES), F32)] * 2
                      + [VMEM((LANES, WIDE * 3), BF), VMEM((NB, LANES), jnp.int32), pltpu.SMEM((NB, LANES), jnp.int32), pltpu.SemaphoreType.DMA])
    acc_shape = [jax.ShapeDtypeStruct((NG * CW, LANES), F32)] * T
    big = 6 * MIB

    def local_fn(kspace, wts_y, wts_x, idx_y, idx_x, coil_maps, deapod):
        own, far, maps, maps_end = pl.pallas_call(
            prep_kernel,
            out_shape=[jax.ShapeDtypeStruct((PAY * NB, LANES), F32)] * 2 + [jax.ShapeDtypeStruct((4, n, N_GRID), F32) for n in (HALF, WIN)],
            in_specs=[hbm] * 6, out_specs=[vm] * 4, name='prep',
            scratch_shapes=[VMEM((2, SUB, NS), F32), VMEM((KW, NS), F32), VMEM((KW, NS), F32), VMEM((NB, LANES), jnp.int32), VMEM((NB, LANES), jnp.int32), VMEM((2, 4, QB, N_IMG), F32), pltpu.SemaphoreType.DMA((6,))],
            compiler_params=pltpu.CompilerParams(vmem_limit_bytes=SUB * MIB),
        )(*[pltpu.with_memory_space_constraint(v, pltpu.HBM) for v in (kspace, wts_y, wts_x, idx_y.reshape(NB, LANES), idx_x.reshape(NB, LANES), jnp.swapaxes(coil_maps, 2, 3))])
        far_in = lax.ppermute(far, 'cols', [(0, 1), (1, 0)])
        half, *accs = pl.pallas_call(
            own_kernel, out_shape=[jax.ShapeDtypeStruct((11, CW, LANES), F32)] + acc_shape, in_specs=[vm], out_specs=[vm] * (T + 1),
            scratch_shapes=spread_scratch, compiler_params=pltpu.CompilerParams(vmem_limit_bytes=big), name='spread_own',
            cost_estimate=pl.CostEstimate(flops=GIGA, bytes_accessed=4 * MIB, transcendentals=0),
        )(own)
        *accs, pack = pl.pallas_call(
            far_kernel, out_shape=acc_shape + [jax.ShapeDtypeStruct((2, LANES, LANES), F32)],
            in_specs=[vm] * (T + 2), out_specs=[vm] * (T + 1), scratch_shapes=[VMEM((N_GRID, LANES), F32)] + spread_scratch,
            input_output_aliases={i + 2: i for i in range(T)},
            compiler_params=pltpu.CompilerParams(vmem_limit_bytes=big), name='spread_far',
            cost_estimate=pl.CostEstimate(flops=GIGA, bytes_accessed=4 * MIB, transcendentals=0),
        )(far_in, half, *accs)
        maps_x = lax.ppermute(maps, 'rows', [(i, (i + 2) % ROWS) for i in range(ROWS)])
        dma = pltpu.SemaphoreType.DMA
        half_bufs = [VMEM((2, 2, 2, n, LANES), BF) for _, n in GROUPS] + [VMEM((2, n, LANES), BF) for _, n in GROUPS]
        full_bufs = [VMEM((2, 2, 2, 2, n, LANES), BF) for _, n in GROUPS] + [VMEM((2, 2, n, LANES), BF) for _, n in GROUPS]
        return pl.pallas_call(
            image_kernel,
            out_shape=jax.ShapeDtypeStruct((2, PB, QB), F32), in_specs=[vm] * (T + 9), out_specs=vm,
            scratch_shapes=[VMEM((TILES, N_GRID, LANES), BF), VMEM((N_GRID, LANES), F32), VMEM((4 * RB, 2 * N_GRID), BF), VMEM((2, LANES, LANES), F32)] + half_bufs + full_bufs + [
                VMEM((2, 2, 2, N_IMG, LANES), F32), VMEM((2, N_IMG, LANES), F32),
                VMEM((2, 2 * N_IMG, 2 * LANES), F32), VMEM((2 * N_IMG, LANES), F32), VMEM((4, WIN, N_GRID), F32),
                VMEM((3, PB, LANES), F32), VMEM((3, PB, LANES), F32), VMEM((3, PB // 4, LANES), F32), VMEM((3, PB // 4, LANES), F32),
                dma((3,)), dma((3,)), dma((4,)), dma((4,)), dma((6,)), dma((6,)),
            ],
            compiler_params=pltpu.CompilerParams(vmem_limit_bytes=11 * MIB, collective_id=0, has_side_effects=True), name='image',
        )(*accs, half, pack, maps, maps_x, maps_end, deapod, col_dft(), row_dft(), unmix())

    return jax.shard_map(
        local_fn,
        mesh=mesh,
        in_specs=(P(None, None, sample_spec), P(None, sample_spec), P(None, sample_spec), P(sample_spec), P(sample_spec), P(None, ('exam', 'cols'), None, 'rows'), P()),
        out_specs=P(None, ('exam', 'cols'), 'rows'),
        check_vma=False,
    )
```

```python
import functools
import math

import jax
import jax.numpy as jnp
import numpy as np
from jax import lax
from jax.experimental import pallas as pl
from jax.experimental.pallas import tpu as pltpu
from jax.sharding import PartitionSpec as P

BF = jnp.bfloat16
F32 = jnp.float32
VMEM = pltpu.VMEM
LANES = 128
MIB = 1 << 20
GIGA = 4000 * MIB
TILES = 10
SUB, WIN, QTR, HALF, WIDE = 8, 16, 32, 64, 256
N_GRID, N_IMG, N_COILS, KW = 640, 320, 8, 6
ROWS, COLS = 4, 2
RB, CB, QB = N_GRID // ROWS, N_GRID // COLS, N_IMG // ROWS
PB = N_IMG // COLS
NS = 4096
NB = NS // LANES
STEP = 11
NG = 15
CW = CB + WIN
T = 7
PS = 9
PAY = 21
CODE = 512
HW = 24
ORDER = tuple(range(1, 9)) + (0, 9)
GROUPS = ((0, 128), (128, 32))
MESH_ID = pl.DeviceIdType.MESH


def dft_parts():
    freq = np.arange(N_GRID) - N_GRID // 2
    pos = np.arange(N_IMG) - N_IMG // 2
    ang = ((freq[:, None] * pos[None, :]) % N_GRID).astype(np.float32) * np.float32(2.0 * math.pi / N_GRID)
    norm = np.float32(1.0 / math.sqrt(N_GRID))
    c, s = np.cos(ang) * norm, np.sin(ang) * norm
    return np.stack([np.stack([c, s], 1), np.stack([-s, c], 1)], 0)


def col_dft():
    e = dft_parts()
    out = np.zeros((2 * N_GRID, N_GRID), np.float32)
    for dp in range(2):
        for t in range(2):
            for h in range(2):
                q0 = QB * (2 * dp + h)
                l0 = LANES * (2 * dp + t) + HALF * h
                out[:, l0:l0 + HALF] = e[:, :, t, q0:q0 + HALF].reshape(2 * N_GRID, HALF)
    for t in range(2):
        for d in range(4):
            l0 = 4 * LANES + HALF * (d // 2) + WIN * (2 * t + d % 2)
            out[:, l0:l0 + WIN] = e[:, :, t, QB * d + HALF:QB * (d + 1)].reshape(2 * N_GRID, WIN)
    return jnp.asarray(out, BF)


def row_dft():
    e = dft_parts()
    rows = np.concatenate([np.arange(WIN * l, WIN * (l + 1)) for l in ORDER])
    chips = []
    for x in range(2):
        parts = []
        for start, n in GROUPS:
            for t in range(2):
                for b in range(2):
                    parts.append(e[t, (2 * x + b) * RB + rows[start:start + n]])
        m = np.concatenate(parts, 0)
        chips.append(np.concatenate([m[:, :, PB * h:PB * (h + 1)].reshape(N_GRID, N_IMG).T for h in range(2)], 0))
    return jnp.asarray(np.array(chips), BF)


def unmix():
    m = np.zeros((WIDE, WIDE), np.float32)
    for ch in range(SUB):
        for pp in range(2):
            for i in range(WIN):
                m[ch * QTR + WIN * pp + (i + SUB) % WIN, pp * 128 + i * SUB + ch] = 1.0
    return jnp.asarray(m, BF)


def prep_kernel(ks_hbm, wy_hbm, wx_hbm, iy_hbm, ix_hbm, maps_hbm, own_ref, far_ref, sp_ref, sq_ref, ks_ref, wy_ref, wx_ref, iy_ref, ix_ref, maps_ref, sem):
    k = lax.axis_index('cols')
    r = lax.axis_index('rows')
    loads = []
    for src, dst in ((iy_hbm, iy_ref), (ix_hbm, ix_ref), (wx_hbm, wx_ref), (wy_hbm, wy_ref), (ks_hbm, ks_ref), (maps_hbm, maps_ref)):
        cp = pltpu.make_async_copy(src, dst, sem.at[len(loads)])
        cp.start()
        loads.append(cp)
    loads[0].wait()
    loads[1].wait()
    iy = iy_ref[...]
    code = ((iy - r * RB + 5) * CODE + ix_ref[...] - k * CB + 5).astype(F32)
    for i in range(2, 5):
        loads[i].wait()
    lo = jnp.concatenate([ks_ref[0, 0:4, :], ks_ref[1, 0:4, :]], axis=0)
    hi = jnp.concatenate([ks_ref[0, 4:SUB, :], ks_ref[1, 4:SUB, :]], axis=0)
    first = k == 0
    for ref, y in ((own_ref, jnp.where(first, lo, hi)), (far_ref, jnp.where(first, hi, lo))):
        for b in range(NB):
            cols = slice(LANES * b, LANES * (b + 1))
            ref[PAY * b:PAY * b + SUB, :] = y[:, cols]
            ref[PAY * b + SUB:PAY * b + SUB + KW, :] = wx_ref[:, cols]
            ref[PAY * (b + 1) - KW - 1:PAY * (b + 1) - 1, :] = wy_ref[:, cols]
            ref[PAY * (b + 1) - 1:PAY * (b + 1), :] = code[b:b + 1, :]
    loads[5].wait()
    for c in range(4):
        for ref, q in ((sp_ref, slice(0, HALF)), (sq_ref, slice(HALF, QB))):
            for i in range(2):
                ref[c, :, WIDE * i:WIDE * (i + 1)] = maps_ref[i, c, q, :WIDE]
            ref[c, :, 2 * WIDE:] = jnp.concatenate([maps_ref[i, c, q, WIDE:] for i in range(2)], axis=1)


def split3(x):
    hi = x.astype(BF).astype(F32)
    r = x - hi
    mid = r.astype(BF).astype(F32)
    return hi, mid, r - mid


def accumulate(pay_ref, accs, us, xs, vs, r_ref, int_ref, base_ref, sem):
    row_i = lax.broadcasted_iota(jnp.int32, (WIN, LANES), 0)

    def make_u(blk, k):
        off = jnp.minimum(blk, NB - 1) * PAY
        y8 = pay_ref[pl.ds(off, SUB), :]
        wx = pay_ref[pl.ds(off + SUB, SUB), :]
        wyp = pay_ref[pl.ds(off + PAY - SUB, SUB), :]
        d = (row_i - (wyp[7:, :].astype(jnp.int32) // CODE)) & (WIN - 1)
        p = jnp.zeros((WIN, LANES), F32)
        for a in range(KW):
            p = jnp.where(d == a, wyp[a + 1:a + 2, :], p)
        us[k][...] = jnp.concatenate([y8 * p[i:i + 1, :] for i in range(WIN)], axis=0).T
        x3 = list(split3(wx)) + [jnp.zeros((LANES - HW, LANES), F32)]
        xs[k][...] = jnp.concatenate(x3, axis=0).T

    def make_v(k):
        lhs = xs[k][...].astype(BF)
        u = us[k][...]
        for bp in range(3):
            w = jnp.dot(lhs, r_ref[:, WIDE * bp:WIDE * bp + WIDE], preferred_element_type=F32)
            for c in range(2):
                v = w[:, LANES * c:LANES * (c + 1)] * u
                for g in range(WIN):
                    vs[k][pl.ds(SUB * PS * g + 2 * bp + c, SUB, stride=PS), :] = v[SUB * g:SUB * g + SUB, :]

    def add_tiles(blk, k):
        row = base_ref.at[blk]
        for j in range(LANES):
            acc = accs[j % T]
            b = row[j]
            acc[pl.ds(b, SUB), :] = acc[pl.ds(b, SUB), :] + vs[k][PS * j:PS * j + SUB, :]

    code = jnp.concatenate([pay_ref[PAY * (b + 1) - 1:PAY * (b + 1), :] for b in range(NB)], axis=0).astype(jnp.int32)
    int_ref[...] = (((code // CODE - 5) * 187) >> STEP) * CW + (code & (CODE - 1))
    kk = lax.broadcasted_iota(jnp.int32, (LANES, WIDE * 3), 0)
    ll = lax.broadcasted_iota(jnp.int32, (LANES, WIDE * 3), 1)
    r_ref[...] = jnp.where((kk < HW) & ((kk & 7) == (ll >> 7)), 1.0, 0.0).astype(BF)
    for v in vs:
        v[...] = jnp.zeros_like(v)
    load = pltpu.make_async_copy(int_ref, base_ref, sem)
    load.start()
    make_u(0, 0)
    make_u(1, 1)
    make_v(0)
    load.wait()

    def body(n, _):
        k = 2 * n
        make_v(1)
        add_tiles(k, 0)
        make_u(k + 2, 0)
        make_v(0)
        add_tiles(k + 1, 1)
        make_u(k + 3, 1)
        return 0

    lax.fori_loop(0, NB // 2, body, 0)


def folded(accs, off, n, clear=False):
    def total(g):
        rows = pl.ds(pl.multiple_of(g * CW + off, SUB), n)
        v = accs[0][rows, :]
        for a in accs[1:]:
            v = v + a[rows, :]
        if clear:
            for a in accs:
                a[rows, :] = jnp.zeros((n, LANES), F32)
        return v

    row = lax.broadcasted_iota(jnp.int32, (n, LANES), 1) >> 3
    tiles = [None] * TILES
    for g in range(NG):
        v = total(g)
        if g == 0:
            ghost = v
        first = 5 + STEP * g
        for p in range(TILES):
            lo, hi = max(first, SUB + WIN * p), min(first + WIN, SUB + WIN * (p + 1))
            if lo < hi:
                part = jnp.where((row - lo & (WIN - 1)) < hi - lo, v, 0.0)
                tiles[p] = part if tiles[p] is None else tiles[p] + part
    return tiles + [jnp.where(row >= SUB, v, ghost)]


def own_kernel(pay_ref, out_ref, *refs):
    accs, scr = refs[:T], refs[T:]

    def clear(n, _):
        for a in accs:
            a[pl.ds(pl.multiple_of(n * CW, SUB), CW), :] = jnp.zeros((CW, LANES), F32)
        return 0

    lax.fori_loop(0, NG, clear, 0)
    accumulate(pay_ref, accs, scr[:2], scr[2:4], scr[4:6], *scr[6:])

    def fold(q, _):
        off = pl.multiple_of(q * WIN, WIN)
        for p, t in enumerate(folded(accs, off, WIN, clear=True)):
            out_ref[p, pl.ds(off, WIN), :] = t
        return 0

    lax.fori_loop(0, CW // WIN, fold, 0)


def far_kernel(pay_ref, a_ref, *refs):
    accs, pack_ref, gh_ref, scr = refs[T:2 * T], refs[2 * T], refs[2 * T + 1], refs[2 * T + 2:]
    accumulate(pay_ref, accs, scr[:2], scr[2:4], scr[4:6], *scr[6:])
    own0 = lax.axis_index('cols') * CB
    far0 = CB - own0

    def ghost(off, n):
        high = lax.broadcasted_iota(jnp.int32, (n, LANES), 1) >= HALF
        ends = []
        for g in (0, NG - 1):
            rows = pl.ds(pl.multiple_of(g * CW + off, SUB), n)
            v = accs[0][rows, :]
            for a in accs[1:]:
                v = v + a[rows, :]
            ends.append(v)
        return jnp.where(high, ends[1], ends[0])

    def copy(n, _):
        o = pl.multiple_of(n * QTR, SUB)
        gh_ref[pl.ds(pl.multiple_of(far0 + o, SUB), QTR), :] = ghost(SUB + o, QTR)
        gh_ref[pl.ds(pl.multiple_of(own0 + o, SUB), QTR), :] = a_ref[TILES, pl.ds(pl.multiple_of(SUB + o, SUB), QTR), :]
        return 0

    lax.fori_loop(0, CB // QTR, copy, 0)
    for dst, add in ((own0, ghost(CW - SUB, SUB)), (own0 + CB - SUB, ghost(0, SUB)), (far0, a_ref[TILES, CW - SUB:, :]), (far0 + CB - SUB, a_ref[TILES, :SUB, :])):
        rows = pl.ds(pl.multiple_of(dst, SUB), SUB)
        gh_ref[rows, :] = gh_ref[rows, :] + add

    lane = lax.broadcasted_iota(jnp.int32, (LANES, LANES), 1)
    for side, lane0 in ((0, HALF - HW), (1, HALF)):
        out = jnp.zeros((LANES, LANES), F32)
        for j in range(5):
            piece = pltpu.roll(gh_ref[LANES * j:LANES * (j + 1), :], (HW * j - lane0) % LANES, axis=1)
            out = jnp.where(lane >= HW * j, piece, out)
        pack_ref[side] = out


def image_kernel(*refs):
    accs = refs[:T]
    (a_ref, pack_ref, so_ref, sx_ref, se_ref, d_ref, ev_ref, eu_ref, pm_ref, out_ref,
     tb_ref, edge_ref, g_ref, halo, sm1, sm2, sr1, sr2, hm1, hm2, hr1, hr2, s_main, s_rem, acc_m, acc_r, sx_end, pieces, recvs, tails, recvs_t,
     halo_ss, halo_rs, swap_ss, swap_rs, red_ss, red_rs) = refs[T:]
    k = lax.axis_index('cols')
    r = lax.axis_index('rows')
    core, x = r % 2, r // 2
    near = r + 1 - 2 * core
    across = (r + 2) % 4
    prev, nxt = (r + 3) % 4, (r + 1) % 4
    homes = ({'rows': across, 'cols': 1 - k}, {'rows': across}, {'cols': 1 - k})

    barrier = pltpu.get_barrier_semaphore()
    for dev in ({'rows': prev}, {'rows': nxt}) + homes:
        pl.semaphore_signal(barrier, inc=1, device_id=dev, device_id_type=MESH_ID)

    own0 = k * CB
    far0 = CB - own0
    high16 = lax.broadcasted_iota(jnp.int32, (WIN, LANES), 1) >= HALF

    def put(v, tiles):
        rows = pl.ds(pl.multiple_of(v, WIN), WIN)
        for p in range(TILES):
            tb_ref[p, rows, :] = tiles[p].astype(BF)
        edge_ref[rows, :] = jnp.where(high16, tiles[0], tiles[9])

    def far_part(n, _):
        put(far0 + WIN * n, folded(accs, pl.multiple_of(SUB + WIN * n, SUB), WIN))
        return 0

    def own_part(n, _):
        put(own0 + WIN * n, [a_ref[p, pl.ds(pl.multiple_of(SUB + WIN * n, SUB), WIN), :] for p in range(TILES)])
        return 0

    last = CB // WIN - 1
    lax.fori_loop(1, last, far_part, 0)
    pl.semaphore_wait(barrier, 5)

    def remote(src, dst, ss, rs, i, dev):
        cp = pltpu.make_async_remote_copy(src_ref=src, dst_ref=dst, send_sem=ss.at[i], recv_sem=rs.at[i], device_id=dev, device_id_type=MESH_ID)
        cp.start()
        return cp

    halos = [remote(pack_ref.at[i], halo.at[i], halo_ss, halo_rs, i, {'rows': dev}) for i, dev in ((0, prev), (1, nxt))]

    lax.fori_loop(1, last, own_part, 0)
    none = jnp.zeros((SUB, LANES), F32)
    for n, side in ((0, CW - SUB), (last, 0)):
        off = SUB + WIN * n
        near_tiles = folded(accs, off, WIN)
        far_ends = folded(accs, side, SUB)
        order = (lambda v: [v, none]) if n == 0 else (lambda v: [none, v])
        put(far0 + WIN * n, [near_tiles[p] + jnp.concatenate(order(a_ref[p, side:side + SUB, :]), axis=0) for p in range(TILES)])
        put(own0 + WIN * n, [a_ref[p, off:off + WIN, :] + jnp.concatenate(order(far_ends[p]), axis=0) for p in range(TILES)])


    def to_rows(row0, n, t0, t1):
        a = jnp.concatenate([t0, t1], axis=1)
        g = lax.dot_general(pm_ref[...], a, (((1,), (1,)), ((), ())), preferred_element_type=F32).astype(BF)
        for ch in range(SUB):
            i, c = ch // 4, ch % 4
            g_ref[row0 + n * c:row0 + n * c + QTR, N_GRID * i:N_GRID * (i + 1)] = g[QTR * ch:QTR * (ch + 1), :]

    for m in range(4):
        to_rows(QTR * m, LANES, tb_ref[2 * m + 1], tb_ref[2 * m + 2])

    sms, srs, hms, hrs = (sm1, sm2), (sr1, sr2), (hm1, hm2), (hr1, hr2)
    swaps = []

    def columns(grp):
        start, n = GROUPS[grp]
        lane = lax.broadcasted_iota(jnp.int32, (n, LANES), 1)
        side = lane >> 6
        own_even, far_even = side == core, side != core
        block = (lane & (HALF - 1)) >> 4
        h = jnp.dot(g_ref[4 * start:4 * (start + n), :], ev_ref[...], preferred_element_type=F32)
        hc = [h[n * c:n * (c + 1)] for c in range(4)]
        rems = [v[:, 4 * LANES:] for v in hc]
        for cp in range(2):
            hs = [[v[:, LANES * i:LANES * (i + 1)] for i in range(4)] for v in hc[2 * cp:2 * cp + 2]]
            for i in range(4):
                dp, t = i // 2, i % 2
                odd = pltpu.roll(hs[1][i], HALF, axis=1)
                sms[grp][dp, cp, t] = jnp.where(far_even, hs[0][i], odd).astype(BF)
                hms[grp][dp, cp, t, core] = jnp.where(own_even, hs[0][i], odd).astype(BF)
        for t in range(2):
            both = []
            for h in range(2):
                i = 2 * t + h
                out = rems[i]
                for c in range(4):
                    if c != i:
                        out = jnp.where(block == c, pltpu.roll(rems[c], (WIN * (c - i)) % LANES, axis=1), out)
                both.append(out)
            srs[grp][t] = jnp.where(core == 0, both[1], both[0]).astype(BF)
            hrs[grp][t, core] = jnp.where(core == 0, both[0], both[1]).astype(BF)
        swaps.append(remote(sms[grp], hms[grp].at[:, :, :, core], swap_ss, swap_rs, 2 * grp, {'rows': near}))
        swaps.append(remote(srs[grp], hrs[grp].at[:, core], swap_ss, swap_rs, 2 * grp + 1, {'rows': near}))

    columns(0)
    end_copy = remote(se_ref, sx_end, halo_ss, halo_rs, 2, {'rows': across})

    for h in halos:
        h.wait()
    lane = lax.broadcasted_iota(jnp.int32, (LANES, LANES), 1)
    low = lane < HALF
    t0s, t9s = [], []
    for j in range(5):
        rows = slice(LANES * j, LANES * (j + 1))
        add_first = pltpu.roll(halo[1], (HALF - HW * j) % LANES, axis=1)
        add_last = pltpu.roll(halo[0], (HALF - HW - HW * j) % LANES, axis=1)
        e = edge_ref[rows, :] + jnp.where(low, jnp.where(lane >= HALF - HW, add_last, 0.0), jnp.where(lane < HALF + HW, add_first, 0.0))
        t0s.append(jnp.where(low, tb_ref[0, rows, :].astype(F32), e).astype(BF))
        t9s.append(jnp.where(low, e, tb_ref[9, rows, :].astype(F32)).astype(BF))
    lane = lax.broadcasted_iota(jnp.int32, (PB, LANES), 1)
    low = lane < HALF
    to_rows(4 * LANES, QTR, jnp.concatenate(t0s, axis=0), jnp.concatenate(t9s, axis=0))
    columns(1)

    def turn(rows):
        t = [rows[:, LANES * i:LANES * (i + 1)].T for i in range(5)]
        return [jnp.concatenate([t[2 * i], t[2 * i + 1], t[4][HALF * i:HALF * (i + 1)]], axis=0) for i in range(2)]


    for cp in swaps[:2]:
        cp.wait_recv()
    n0 = 4 * GROUPS[0][1]

    def block_of(grp, j):
        return jnp.concatenate([hms[grp][(x + j) % 2, cp].reshape(4 * GROUPS[grp][1], LANES) for cp in range(2)], axis=1)

    for j, ref in ((1, sx_ref), (0, so_ref)):
        acc_m[j] = jnp.dot(eu_ref[x, :, :n0], block_of(0, j), preferred_element_type=F32)
        for cp in range(2):
            s_main[j, 0, cp], s_main[j, 1, cp] = turn(jnp.concatenate([ref[2 * cp + core], ref[2 * cp + 1 - core]], axis=0))
    acc_r[...] = jnp.dot(eu_ref[x, :, :n0], hrs[0][...].reshape(n0, LANES), preferred_element_type=F32)

    for cp in swaps[2:]:
        cp.wait_recv()

    def rows_dft(half, acc, rhs):
        rows = pl.ds(pl.multiple_of(half * N_IMG, WIN), N_IMG)
        total = acc[rows, :] + jnp.dot(eu_ref[x, rows, n0:], rhs, preferred_element_type=F32)
        return total[:PB], total[PB:]

    quarter = lax.broadcasted_iota(jnp.int32, (PB // 4, LANES), 1) >> 5

    def piece(half, j):
        i_re, i_im = rows_dft(half, acc_m.at[j], block_of(1, j))
        rows = pl.ds(pl.multiple_of(half * PB, SUB), PB)
        re, im = None, None
        for cp in range(2):
            cols = slice(LANES * cp, LANES * (cp + 1))
            s_re, s_im = s_main[j, 0, cp, rows, :], s_main[j, 1, cp, rows, :]
            a = s_re * i_re[:, cols] + s_im * i_im[:, cols]
            b = s_re * i_im[:, cols] - s_im * i_re[:, cols]
            re, im = (a, b) if re is None else (re + a, im + b)
        return jnp.where(low, re + pltpu.roll(re, HALF, axis=1), im + pltpu.roll(im, HALF, axis=1))

    def rest(half):
        i_re, i_im = rows_dft(half, acc_r, hrs[1][...].reshape(4 * GROUPS[1][1], LANES))
        rows = pl.ds(pl.multiple_of(half * PB, SUB), PB)
        s_re, s_im = s_rem[0, rows, :], s_rem[1, rows, :]

        def fold(v):
            v = v + pltpu.roll(v, LANES - QTR, axis=1)
            return v + pltpu.roll(v, LANES - WIN, axis=1)

        re, im = fold(s_re * i_re + s_im * i_im), fold(s_re * i_im - s_im * i_re)
        both = jnp.where(lane & (HALF - 1) < WIN, re, pltpu.roll(im, WIN, axis=1))
        outs = []
        for dp in range(2):
            out = None
            for g in range(4):
                v = both[PB // 4 * g:PB // 4 * (g + 1)]
                if g + 2 * dp:
                    v = pltpu.roll(v, (QTR * g + HALF * dp) % LANES, axis=1)
                out = v if out is None else jnp.where(quarter == g, v, out)
            outs.append(out)
        return jnp.where(x == 0, outs[0], outs[1]), jnp.where(x == 0, outs[1], outs[0])

    sends = []
    for i, (half, j) in enumerate(((1 - k, 1), (k, 1), (1 - k, 0))):
        pieces[i] = piece(half, j)
        sends.append(remote(pieces.at[i], recvs.at[i], red_ss, red_rs, i, homes[i]))
    end_copy.wait_recv()
    s_rem[0], s_rem[1] = turn(jnp.concatenate([jnp.where(x == j, se_ref[c], sx_end[c]) for j in range(2) for c in range(4)], axis=0))
    tails[2], tails[0] = rest(1 - k)
    sends.append(remote(tails.at[0], recvs_t.at[0], red_ss, red_rs, 3, homes[0]))
    rem, tails[1] = rest(k)
    for i in (1, 2):
        sends.append(remote(tails.at[i], recvs_t.at[i], red_ss, red_rs, 3 + i, homes[i]))
    main = piece(k, 0)
    d8 = jnp.broadcast_to(jnp.concatenate([d_ref[...][None, :], jnp.zeros((1, HALF), F32)], axis=1), (SUB, N_IMG + HALF))
    dq = d8
    for j in range(1, ROWS):
        dq = jnp.where(r == j, pltpu.roll(d8, N_IMG + HALF - QB * j, axis=1), dq)
    dp = jnp.where(k == 0, d8, pltpu.roll(d8, N_IMG + HALF - PB, axis=1))[:, :2 * LANES]
    dd = jnp.concatenate([dp] * WIN, axis=0).T[:PB] * dq[:1, :LANES]

    for i in (2, 0, 1):
        sends[i].wait_recv()
        main = main + recvs[i]
    for i in (2, 0, 1):
        sends[3 + i].wait_recv()
        rem = rem + recvs_t[i]
    for o in range(2):
        m = pltpu.roll(main, HALF, axis=1) if o else main
        for j in range(4):
            rows = slice(PB // 4 * j, PB // 4 * (j + 1))
            tail = pltpu.roll(rem, (HALF - QTR * j - WIN * o) % LANES, axis=1)
            out_ref[o, rows, :] = (jnp.where(low[rows], m[rows], tail) * dd[rows])[:, :QB]

    for cp in sends + swaps + [end_copy]:
        cp.wait_send()


def solution(mesh):
    sample_spec = ('exam', 'rows', 'cols')
    vm = pl.BlockSpec(memory_space=pltpu.VMEM)
    hbm = pl.BlockSpec(memory_space=pltpu.HBM)
    spread_scratch = ([VMEM((LANES, LANES), F32)] * 4 + [VMEM((LANES * PS, LANES), F32)] * 2
                      + [VMEM((LANES, WIDE * 3), BF), VMEM((NB, LANES), jnp.int32), pltpu.SMEM((NB, LANES), jnp.int32), pltpu.SemaphoreType.DMA])
    acc_shape = [jax.ShapeDtypeStruct((NG * CW, LANES), F32)] * T
    big = 6 * MIB

    def local_fn(kspace, wts_y, wts_x, idx_y, idx_x, coil_maps, deapod):
        own, far, maps, maps_end = pl.pallas_call(
            prep_kernel,
            out_shape=[jax.ShapeDtypeStruct((PAY * NB, LANES), F32)] * 2 + [jax.ShapeDtypeStruct((4, n, N_GRID), F32) for n in (HALF, WIN)],
            in_specs=[hbm] * 6, out_specs=[vm] * 4, name='prep',
            scratch_shapes=[VMEM((2, SUB, NS), F32), VMEM((KW, NS), F32), VMEM((KW, NS), F32), VMEM((NB, LANES), jnp.int32), VMEM((NB, LANES), jnp.int32), VMEM((2, 4, QB, N_IMG), F32), pltpu.SemaphoreType.DMA((6,))],
            compiler_params=pltpu.CompilerParams(vmem_limit_bytes=SUB * MIB),
        )(*[pltpu.with_memory_space_constraint(v, pltpu.HBM) for v in (kspace, wts_y, wts_x, idx_y.reshape(NB, LANES), idx_x.reshape(NB, LANES), jnp.swapaxes(coil_maps, 2, 3))])
        far_in = lax.ppermute(far, 'cols', [(0, 1), (1, 0)])
        half, *accs = pl.pallas_call(
            own_kernel, out_shape=[jax.ShapeDtypeStruct((11, CW, LANES), F32)] + acc_shape, in_specs=[vm], out_specs=[vm] * (T + 1),
            scratch_shapes=spread_scratch, compiler_params=pltpu.CompilerParams(vmem_limit_bytes=big), name='spread_own',
            cost_estimate=pl.CostEstimate(flops=GIGA, bytes_accessed=4 * MIB, transcendentals=0),
        )(own)
        *accs, pack = pl.pallas_call(
            far_kernel, out_shape=acc_shape + [jax.ShapeDtypeStruct((2, LANES, LANES), F32)],
            in_specs=[vm] * (T + 2), out_specs=[vm] * (T + 1), scratch_shapes=[VMEM((N_GRID, LANES), F32)] + spread_scratch,
            input_output_aliases={i + 2: i for i in range(T)},
            compiler_params=pltpu.CompilerParams(vmem_limit_bytes=big), name='spread_far',
            cost_estimate=pl.CostEstimate(flops=GIGA, bytes_accessed=4 * MIB, transcendentals=0),
        )(far_in, half, *accs)
        maps_x = lax.ppermute(maps, 'rows', [(i, (i + 2) % ROWS) for i in range(ROWS)])
        dma = pltpu.SemaphoreType.DMA
        half_bufs = [VMEM((2, 2, 2, n, LANES), BF) for _, n in GROUPS] + [VMEM((2, n, LANES), BF) for _, n in GROUPS]
        full_bufs = [VMEM((2, 2, 2, 2, n, LANES), BF) for _, n in GROUPS] + [VMEM((2, 2, n, LANES), BF) for _, n in GROUPS]
        return pl.pallas_call(
            image_kernel,
            out_shape=jax.ShapeDtypeStruct((2, PB, QB), F32), in_specs=[vm] * (T + 9), out_specs=vm,
            scratch_shapes=[VMEM((TILES, N_GRID, LANES), BF), VMEM((N_GRID, LANES), F32), VMEM((4 * RB, 2 * N_GRID), BF), VMEM((2, LANES, LANES), F32)] + half_bufs + full_bufs + [
                VMEM((2, 2, 2, N_IMG, LANES), F32), VMEM((2, N_IMG, LANES), F32),
                VMEM((2, 2 * N_IMG, 2 * LANES), F32), VMEM((2 * N_IMG, LANES), F32), VMEM((4, WIN, N_GRID), F32),
                VMEM((3, PB, LANES), F32), VMEM((3, PB, LANES), F32), VMEM((3, PB // 4, LANES), F32), VMEM((3, PB // 4, LANES), F32),
                dma((3,)), dma((3,)), dma((4,)), dma((4,)), dma((6,)), dma((6,)),
            ],
            compiler_params=pltpu.CompilerParams(vmem_limit_bytes=11 * MIB, collective_id=0, has_side_effects=True), name='image',
        )(*accs, half, pack, maps, maps_x, maps_end, deapod, col_dft(), row_dft(), unmix())

    return jax.shard_map(
        local_fn,
        mesh=mesh,
        in_specs=(P(None, None, sample_spec), P(None, sample_spec), P(None, sample_spec), P(sample_spec), P(sample_spec), P(None, ('exam', 'cols'), None, 'rows'), P()),
        out_specs=P(None, ('exam', 'cols'), 'rows'),
        check_vma=False,
    )
```

```python
import functools
import math

import jax
import jax.numpy as jnp
import numpy as np
from jax import lax
from jax.experimental import pallas as pl
from jax.experimental.pallas import tpu as pltpu
from jax.sharding import PartitionSpec as P

BF = jnp.bfloat16
F32 = jnp.float32
VMEM = pltpu.VMEM
LANES = 128
MIB = 1 << 20
GIGA = 4000 * MIB
TILES = 10
SUB, WIN, QTR, HALF, WIDE = 8, 16, 32, 64, 256
N_GRID, N_IMG, N_COILS, KW = 640, 320, 8, 6
ROWS, COLS = 4, 2
RB, CB, QB = N_GRID // ROWS, N_GRID // COLS, N_IMG // ROWS
PB = N_IMG // COLS
NS = 4096
NB = NS // LANES
STEP = 11
NG = 15
CW = CB + WIN
T = 7
PS = 9
PAY = 21
CODE = 512
HW = 24
ORDER = tuple(range(1, 9)) + (0, 9)
GROUPS = ((0, 128), (128, 32))
MESH_ID = pl.DeviceIdType.MESH


def dft_parts():
    freq = np.arange(N_GRID) - N_GRID // 2
    pos = np.arange(N_IMG) - N_IMG // 2
    ang = ((freq[:, None] * pos[None, :]) % N_GRID).astype(np.float32) * np.float32(2.0 * math.pi / N_GRID)
    norm = np.float32(1.0 / math.sqrt(N_GRID))
    c, s = np.cos(ang) * norm, np.sin(ang) * norm
    return np.stack([np.stack([c, s], 1), np.stack([-s, c], 1)], 0)


def col_dft():
    e = dft_parts()
    out = np.zeros((2 * N_GRID, N_GRID), np.float32)
    for dp in range(2):
        for t in range(2):
            for h in range(2):
                q0 = QB * (2 * dp + h)
                l0 = LANES * (2 * dp + t) + HALF * h
                out[:, l0:l0 + HALF] = e[:, :, t, q0:q0 + HALF].reshape(2 * N_GRID, HALF)
    for t in range(2):
        for d in range(4):
            l0 = 4 * LANES + HALF * t + WIN * d
            out[:, l0:l0 + WIN] = e[:, :, t, QB * d + HALF:QB * (d + 1)].reshape(2 * N_GRID, WIN)
    return jnp.asarray(out, BF)


def row_dft():
    e = dft_parts()
    rows = np.concatenate([np.arange(WIN * l, WIN * (l + 1)) for l in ORDER])
    chips = []
    for x in range(2):
        parts = []
        for start, n in GROUPS:
            for t in range(2):
                for b in range(2):
                    parts.append(e[t, (2 * x + b) * RB + rows[start:start + n]])
        m = np.concatenate(parts, 0)
        chips.append(np.concatenate([m[:, :, PB * h:PB * (h + 1)].reshape(N_GRID, N_IMG).T for h in range(2)], 0))
    return jnp.asarray(np.array(chips), BF)


def unmix():
    m = np.zeros((WIDE, WIDE), np.float32)
    for ch in range(SUB):
        for pp in range(2):
            for i in range(WIN):
                m[ch * QTR + WIN * pp + (i + SUB) % WIN, pp * 128 + i * SUB + ch] = 1.0
    return jnp.asarray(m, BF)


def prep_kernel(ks_hbm, wy_hbm, wx_hbm, iy_hbm, ix_hbm, maps_hbm, own_ref, far_ref, sp_ref, sq_ref, ks_ref, wy_ref, wx_ref, iy_ref, ix_ref, maps_ref, sem):
    k = lax.axis_index('cols')
    r = lax.axis_index('rows')
    loads = []
    for src, dst in ((iy_hbm, iy_ref), (ix_hbm, ix_ref), (wx_hbm, wx_ref), (wy_hbm, wy_ref), (ks_hbm, ks_ref), (maps_hbm, maps_ref)):
        cp = pltpu.make_async_copy(src, dst, sem.at[len(loads)])
        cp.start()
        loads.append(cp)
    loads[0].wait()
    loads[1].wait()
    iy = iy_ref[...]
    code = ((iy - r * RB + 5) * CODE + ix_ref[...] - k * CB + 5).astype(F32)
    for i in range(2, 5):
        loads[i].wait()
    lo = jnp.concatenate([ks_ref[0, 0:4, :], ks_ref[1, 0:4, :]], axis=0)
    hi = jnp.concatenate([ks_ref[0, 4:SUB, :], ks_ref[1, 4:SUB, :]], axis=0)
    first = k == 0
    for ref, y in ((own_ref, jnp.where(first, lo, hi)), (far_ref, jnp.where(first, hi, lo))):
        for b in range(NB):
            cols = slice(LANES * b, LANES * (b + 1))
            ref[PAY * b:PAY * b + SUB, :] = y[:, cols]
            ref[PAY * b + SUB:PAY * b + SUB + KW, :] = wx_ref[:, cols]
            ref[PAY * (b + 1) - KW - 1:PAY * (b + 1) - 1, :] = wy_ref[:, cols]
            ref[PAY * (b + 1) - 1:PAY * (b + 1), :] = code[b:b + 1, :]
    loads[5].wait()
    for c in range(4):
        for ref, q in ((sp_ref, slice(0, HALF)), (sq_ref, slice(HALF, QB))):
            for i in range(2):
                ref[c, :, WIDE * i:WIDE * (i + 1)] = maps_ref[i, c, q, :WIDE]
            ref[c, :, 2 * WIDE:] = jnp.concatenate([maps_ref[i, c, q, WIDE:] for i in range(2)], axis=1)


def split3(x):
    hi = x.astype(BF).astype(F32)
    r = x - hi
    mid = r.astype(BF).astype(F32)
    return hi, mid, r - mid


def accumulate(pay_ref, accs, us, xs, vs, r_ref, int_ref, base_ref, sem):
    row_i = lax.broadcasted_iota(jnp.int32, (WIN, LANES), 0)

    def make_u(blk, k):
        off = jnp.minimum(blk, NB - 1) * PAY
        y8 = pay_ref[pl.ds(off, SUB), :]
        wx = pay_ref[pl.ds(off + SUB, SUB), :]
        wyp = pay_ref[pl.ds(off + PAY - SUB, SUB), :]
        d = (row_i - (wyp[7:, :].astype(jnp.int32) // CODE)) & (WIN - 1)
        p = jnp.zeros((WIN, LANES), F32)
        for a in range(KW):
            p = jnp.where(d == a, wyp[a + 1:a + 2, :], p)
        us[k][...] = jnp.concatenate([y8 * p[i:i + 1, :] for i in range(WIN)], axis=0).T
        x3 = list(split3(wx)) + [jnp.zeros((LANES - HW, LANES), F32)]
        xs[k][...] = jnp.concatenate(x3, axis=0).T

    def make_v(k):
        lhs = xs[k][...].astype(BF)
        u = us[k][...]
        for bp in range(3):
            w = jnp.dot(lhs, r_ref[:, WIDE * bp:WIDE * bp + WIDE], preferred_element_type=F32)
            for c in range(2):
                v = w[:, LANES * c:LANES * (c + 1)] * u
                for g in range(WIN):
                    vs[k][pl.ds(SUB * PS * g + 2 * bp + c, SUB, stride=PS), :] = v[SUB * g:SUB * g + SUB, :]

    def add_tiles(blk, k):
        row = base_ref.at[blk]
        for j in range(LANES):
            acc = accs[j % T]
            b = row[j]
            acc[pl.ds(b, SUB), :] = acc[pl.ds(b, SUB), :] + vs[k][PS * j:PS * j + SUB, :]

    code = jnp.concatenate([pay_ref[PAY * (b + 1) - 1:PAY * (b + 1), :] for b in range(NB)], axis=0).astype(jnp.int32)
    int_ref[...] = (((code // CODE - 5) * 187) >> STEP) * CW + (code & (CODE - 1))
    kk = lax.broadcasted_iota(jnp.int32, (LANES, WIDE * 3), 0)
    ll = lax.broadcasted_iota(jnp.int32, (LANES, WIDE * 3), 1)
    r_ref[...] = jnp.where((kk < HW) & ((kk & 7) == (ll >> 7)), 1.0, 0.0).astype(BF)
    for v in vs:
        v[...] = jnp.zeros_like(v)
    load = pltpu.make_async_copy(int_ref, base_ref, sem)
    load.start()
    make_u(0, 0)
    make_u(1, 1)
    make_v(0)
    load.wait()

    def body(n, _):
        k = 2 * n
        make_v(1)
        add_tiles(k, 0)
        make_u(k + 2, 0)
        make_v(0)
        add_tiles(k + 1, 1)
        make_u(k + 3, 1)
        return 0

    lax.fori_loop(0, NB // 2, body, 0)


def folded(accs, off, n, clear=False):
    def total(g):
        rows = pl.ds(pl.multiple_of(g * CW + off, SUB), n)
        v = accs[0][rows, :]
        for a in accs[1:]:
            v = v + a[rows, :]
        if clear:
            for a in accs:
                a[rows, :] = jnp.zeros((n, LANES), F32)
        return v

    row = lax.broadcasted_iota(jnp.int32, (n, LANES), 1) >> 3
    tiles = [None] * TILES
    for g in range(NG):
        v = total(g)
        if g == 0:
            ghost = v
        first = 5 + STEP * g
        for p in range(TILES):
            lo, hi = max(first, SUB + WIN * p), min(first + WIN, SUB + WIN * (p + 1))
            if lo < hi:
                part = jnp.where((row - lo & (WIN - 1)) < hi - lo, v, 0.0)
                tiles[p] = part if tiles[p] is None else tiles[p] + part
    return tiles + [jnp.where(row >= SUB, v, ghost)]


def own_kernel(pay_ref, out_ref, *refs):
    accs, scr = refs[:T], refs[T:]

    def clear(n, _):
        for a in accs:
            a[pl.ds(pl.multiple_of(n * CW, SUB), CW), :] = jnp.zeros((CW, LANES), F32)
        return 0

    lax.fori_loop(0, NG, clear, 0)
    accumulate(pay_ref, accs, scr[:2], scr[2:4], scr[4:6], *scr[6:])

    def fold(q, _):
        off = pl.multiple_of(q * WIN, WIN)
        for p, t in enumerate(folded(accs, off, WIN, clear=True)):
            out_ref[p, pl.ds(off, WIN), :] = t
        return 0

    lax.fori_loop(0, CW // WIN, fold, 0)


def far_kernel(pay_ref, a_ref, *refs):
    accs, pack_ref, gh_ref, scr = refs[T:2 * T], refs[2 * T], refs[2 * T + 1], refs[2 * T + 2:]
    accumulate(pay_ref, accs, scr[:2], scr[2:4], scr[4:6], *scr[6:])
    own0 = lax.axis_index('cols') * CB
    far0 = CB - own0

    def ghost(off, n):
        high = lax.broadcasted_iota(jnp.int32, (n, LANES), 1) >= HALF
        ends = []
        for g in (0, NG - 1):
            rows = pl.ds(pl.multiple_of(g * CW + off, SUB), n)
            v = accs[0][rows, :]
            for a in accs[1:]:
                v = v + a[rows, :]
            ends.append(v)
        return jnp.where(high, ends[1], ends[0])

    def copy(n, _):
        o = pl.multiple_of(n * QTR, SUB)
        gh_ref[pl.ds(pl.multiple_of(far0 + o, SUB), QTR), :] = ghost(SUB + o, QTR)
        gh_ref[pl.ds(pl.multiple_of(own0 + o, SUB), QTR), :] = a_ref[TILES, pl.ds(pl.multiple_of(SUB + o, SUB), QTR), :]
        return 0

    lax.fori_loop(0, CB // QTR, copy, 0)
    for dst, add in ((own0, ghost(CW - SUB, SUB)), (own0 + CB - SUB, ghost(0, SUB)), (far0, a_ref[TILES, CW - SUB:, :]), (far0 + CB - SUB, a_ref[TILES, :SUB, :])):
        rows = pl.ds(pl.multiple_of(dst, SUB), SUB)
        gh_ref[rows, :] = gh_ref[rows, :] + add

    lane = lax.broadcasted_iota(jnp.int32, (LANES, LANES), 1)
    for side, lane0 in ((0, HALF - HW), (1, HALF)):
        out = jnp.zeros((LANES, LANES), F32)
        for j in range(5):
            piece = pltpu.roll(gh_ref[LANES * j:LANES * (j + 1), :], (HW * j - lane0) % LANES, axis=1)
            out = jnp.where(lane >= HW * j, piece, out)
        pack_ref[side] = out


def image_kernel(*refs):
    accs = refs[:T]
    (a_ref, pack_ref, so_ref, sx_ref, se_ref, d_ref, ev_ref, eu_ref, pm_ref, out_ref,
     tb_ref, edge_ref, g_ref, halo, sm1, sm2, sr1, sr2, hm1, hm2, hr1, hr2, s_main, s_rem, acc_m, acc_r, pieces, recvs, tails, recvs_t,
     halo_ss, halo_rs, swap_ss, swap_rs, red_ss, red_rs) = refs[T:]
    k = lax.axis_index('cols')
    r = lax.axis_index('rows')
    core, x = r % 2, r // 2
    near = r + 1 - 2 * core
    across = (r + 2) % 4
    prev, nxt = (r + 3) % 4, (r + 1) % 4
    homes = ({'rows': across, 'cols': 1 - k}, {'rows': across}, {'cols': 1 - k})

    barrier = pltpu.get_barrier_semaphore()
    for dev in ({'rows': prev}, {'rows': nxt}) + homes:
        pl.semaphore_signal(barrier, inc=1, device_id=dev, device_id_type=MESH_ID)

    own0 = k * CB
    far0 = CB - own0
    high16 = lax.broadcasted_iota(jnp.int32, (WIN, LANES), 1) >= HALF

    def put(v, tiles):
        rows = pl.ds(pl.multiple_of(v, WIN), WIN)
        for p in range(TILES):
            tb_ref[p, rows, :] = tiles[p].astype(BF)
        edge_ref[rows, :] = jnp.where(high16, tiles[0], tiles[9])

    def far_part(n, _):
        put(far0 + WIN * n, folded(accs, pl.multiple_of(SUB + WIN * n, SUB), WIN))
        return 0

    def own_part(n, _):
        put(own0 + WIN * n, [a_ref[p, pl.ds(pl.multiple_of(SUB + WIN * n, SUB), WIN), :] for p in range(TILES)])
        return 0

    last = CB // WIN - 1
    lax.fori_loop(1, last, far_part, 0)
    pl.semaphore_wait(barrier, 5)

    def remote(src, dst, ss, rs, i, dev):
        cp = pltpu.make_async_remote_copy(src_ref=src, dst_ref=dst, send_sem=ss.at[i], recv_sem=rs.at[i], device_id=dev, device_id_type=MESH_ID)
        cp.start()
        return cp

    halos = [remote(pack_ref.at[i], halo.at[i], halo_ss, halo_rs, i, {'rows': dev}) for i, dev in ((0, prev), (1, nxt))]

    lax.fori_loop(1, last, own_part, 0)
    none = jnp.zeros((SUB, LANES), F32)
    for n, side in ((0, CW - SUB), (last, 0)):
        off = SUB + WIN * n
        near_tiles = folded(accs, off, WIN)
        far_ends = folded(accs, side, SUB)
        order = (lambda v: [v, none]) if n == 0 else (lambda v: [none, v])
        put(far0 + WIN * n, [near_tiles[p] + jnp.concatenate(order(a_ref[p, side:side + SUB, :]), axis=0) for p in range(TILES)])
        put(own0 + WIN * n, [a_ref[p, off:off + WIN, :] + jnp.concatenate(order(far_ends[p]), axis=0) for p in range(TILES)])


    def to_rows(row0, n, t0, t1):
        a = jnp.concatenate([t0, t1], axis=1)
        g = lax.dot_general(pm_ref[...], a, (((1,), (1,)), ((), ())), preferred_element_type=F32).astype(BF)
        for ch in range(SUB):
            i, c = ch // 4, ch % 4
            g_ref[row0 + n * c:row0 + n * c + QTR, N_GRID * i:N_GRID * (i + 1)] = g[QTR * ch:QTR * (ch + 1), :]

    for m in range(4):
        to_rows(QTR * m, LANES, tb_ref[2 * m + 1], tb_ref[2 * m + 2])

    sms, srs, hms, hrs = (sm1, sm2), (sr1, sr2), (hm1, hm2), (hr1, hr2)
    swaps, trades = [], []

    def columns(grp):
        start, n = GROUPS[grp]
        lane = lax.broadcasted_iota(jnp.int32, (n, LANES), 1)
        side = lane >> 6
        own_even, far_even = side == core, side != core
        block = (lane & (HALF - 1)) >> 4
        h = jnp.dot(g_ref[4 * start:4 * (start + n), :], ev_ref[...], preferred_element_type=F32)
        hc = [h[n * c:n * (c + 1)] for c in range(4)]
        rems = [v[:, 4 * LANES:] for v in hc]
        for cp in range(2):
            hs = [[v[:, LANES * i:LANES * (i + 1)] for i in range(4)] for v in hc[2 * cp:2 * cp + 2]]
            for i in range(4):
                dp, t = i // 2, i % 2
                odd = pltpu.roll(hs[1][i], HALF, axis=1)
                sms[grp][dp, cp, t] = jnp.where(far_even, hs[0][i], odd).astype(BF)
                hms[grp][dp, cp, t, core] = jnp.where(own_even, hs[0][i], odd).astype(BF)
        for d in range(ROWS):
            out = rems[d]
            for c in range(4):
                if c != d:
                    out = jnp.where(block == c, pltpu.roll(rems[c], (WIN * (c - d)) % LANES, axis=1), out)
            srs[grp][d] = out.astype(BF)
        hrs[grp][r] = srs[grp][r]
        swaps.append(remote(sms[grp], hms[grp].at[:, :, :, core], swap_ss, swap_rs, grp, {'rows': near}))
        for i, dev in enumerate((across, 3 - r, near)):
            trades.append(remote(srs[grp].at[dev], hrs[grp].at[r], swap_ss, swap_rs, 2 + 3 * grp + i, {'rows': dev}))

    columns(0)

    for h in halos:
        h.wait()
    lane = lax.broadcasted_iota(jnp.int32, (LANES, LANES), 1)
    low = lane < HALF
    t0s, t9s = [], []
    for j in range(5):
        rows = slice(LANES * j, LANES * (j + 1))
        add_first = pltpu.roll(halo[1], (HALF - HW * j) % LANES, axis=1)
        add_last = pltpu.roll(halo[0], (HALF - HW - HW * j) % LANES, axis=1)
        e = edge_ref[rows, :] + jnp.where(low, jnp.where(lane >= HALF - HW, add_last, 0.0), jnp.where(lane < HALF + HW, add_first, 0.0))
        t0s.append(jnp.where(low, tb_ref[0, rows, :].astype(F32), e).astype(BF))
        t9s.append(jnp.where(low, e, tb_ref[9, rows, :].astype(F32)).astype(BF))
    lane = lax.broadcasted_iota(jnp.int32, (PB, LANES), 1)
    low = lane < HALF
    to_rows(4 * LANES, QTR, jnp.concatenate(t0s, axis=0), jnp.concatenate(t9s, axis=0))
    columns(1)

    def turn(rows):
        t = [rows[:, LANES * i:LANES * (i + 1)].T for i in range(5)]
        return [jnp.concatenate([t[2 * i], t[2 * i + 1], t[4][HALF * i:HALF * (i + 1)]], axis=0) for i in range(2)]


    for cp in swaps[:1]:
        cp.wait_recv()
    n0 = 4 * GROUPS[0][1]

    def block_of(grp, j):
        return jnp.concatenate([hms[grp][(x + j) % 2, cp].reshape(4 * GROUPS[grp][1], LANES) for cp in range(2)], axis=1)

    for j, ref in ((1, sx_ref), (0, so_ref)):
        acc_m[j] = jnp.dot(eu_ref[x, :, :n0], block_of(0, j), preferred_element_type=F32)
        for cp in range(2):
            s_main[j, 0, cp], s_main[j, 1, cp] = turn(jnp.concatenate([ref[2 * cp + core], ref[2 * cp + 1 - core]], axis=0))

    for cp in swaps[1:]:
        cp.wait_recv()

    def rows_dft(half, acc, rhs):
        rows = pl.ds(pl.multiple_of(half * N_IMG, WIN), N_IMG)
        total = acc[rows, :] + jnp.dot(eu_ref[x, rows, n0:], rhs, preferred_element_type=F32)
        return total[:PB], total[PB:]

    quarter = lax.broadcasted_iota(jnp.int32, (PB // 4, LANES), 1) >> 5

    def piece(half, j):
        i_re, i_im = rows_dft(half, acc_m.at[j], block_of(1, j))
        rows = pl.ds(pl.multiple_of(half * PB, SUB), PB)
        re, im = None, None
        for cp in range(2):
            cols = slice(LANES * cp, LANES * (cp + 1))
            s_re, s_im = s_main[j, 0, cp, rows, :], s_main[j, 1, cp, rows, :]
            a = s_re * i_re[:, cols] + s_im * i_im[:, cols]
            b = s_re * i_im[:, cols] - s_im * i_re[:, cols]
            re, im = (a, b) if re is None else (re + a, im + b)
        return jnp.where(low, re + pltpu.roll(re, HALF, axis=1), im + pltpu.roll(im, HALF, axis=1))

    def rest(half):
        parts = []
        for o in range(2):
            rows = pl.ds(pl.multiple_of(half * N_IMG + PB * o, WIN), PB)
            parts.append(acc_r[0, rows, :] + pltpu.roll(acc_r[1, rows, :], HALF, axis=1))
        i_re, i_im = parts
        rows = pl.ds(pl.multiple_of(half * PB, SUB), PB)
        s_re, s_im = s_rem[0, rows, :], s_rem[1, rows, :]
        w = s_re * i_re + s_im * i_im + pltpu.roll(s_re * i_im - s_im * i_re, HALF, axis=1)
        w = w + pltpu.roll(w, LANES - QTR, axis=1)
        w = w + pltpu.roll(w, LANES - WIN, axis=1)
        w = jnp.where(lane < WIN, w, pltpu.roll(w, LANES - HALF + WIN, axis=1))
        out = w[:PB // 4]
        for g in range(1, 4):
            out = jnp.where(quarter == g, pltpu.roll(w[PB // 4 * g:PB // 4 * (g + 1)], QTR * g, axis=1), out)
        return out

    sends = []
    for i, (half, j) in enumerate(((1 - k, 1), (k, 1), (1 - k, 0))):
        pieces[i] = piece(half, j)
        sends.append(remote(pieces.at[i], recvs.at[i], red_ss, red_rs, i, homes[i]))
    for cp in trades:
        cp.wait_recv()
    for t in range(2):
        total = None
        for grp in range(2):
            kk = 2 * GROUPS[grp][1]
            for c in range(2):
                part = jnp.dot(eu_ref[c, :, n0 * grp + kk * t:n0 * grp + kk * (t + 1)], hrs[grp][2 * c:2 * c + 2].reshape(kk, LANES), preferred_element_type=F32)
                total = part if total is None else total + part
        acc_r[t] = total
    s_rem[0], s_rem[1] = turn(jnp.concatenate([se_ref[c] for c in range(4)] + [jnp.zeros((HALF, N_GRID), F32)], axis=0))
    tails[...] = rest(1 - k)
    tail = remote(tails, recvs_t, red_ss, red_rs, 3, homes[2])
    rem = rest(k)
    main = piece(k, 0)
    d8 = jnp.broadcast_to(jnp.concatenate([d_ref[...][None, :], jnp.zeros((1, HALF), F32)], axis=1), (SUB, N_IMG + HALF))
    dq = d8
    for j in range(1, ROWS):
        dq = jnp.where(r == j, pltpu.roll(d8, N_IMG + HALF - QB * j, axis=1), dq)
    dp = jnp.where(k == 0, d8, pltpu.roll(d8, N_IMG + HALF - PB, axis=1))[:, :2 * LANES]
    dd = jnp.concatenate([dp] * WIN, axis=0).T[:PB] * dq[:1, :LANES]

    for i in (2, 0, 1):
        sends[i].wait_recv()
        main = main + recvs[i]
    tail.wait_recv()
    rem = rem + recvs_t[...]
    for o in range(2):
        m = pltpu.roll(main, HALF, axis=1) if o else main
        for j in range(4):
            rows = slice(PB // 4 * j, PB // 4 * (j + 1))
            end = pltpu.roll(rem, (HALF - QTR * j - WIN * o) % LANES, axis=1)
            out_ref[o, rows, :] = (jnp.where(low[rows], m[rows], end) * dd[rows])[:, :QB]

    for cp in sends + swaps + trades + [tail]:
        cp.wait_send()


def solution(mesh):
    sample_spec = ('exam', 'rows', 'cols')
    vm = pl.BlockSpec(memory_space=pltpu.VMEM)
    hbm = pl.BlockSpec(memory_space=pltpu.HBM)
    spread_scratch = ([VMEM((LANES, LANES), F32)] * 4 + [VMEM((LANES * PS, LANES), F32)] * 2
                      + [VMEM((LANES, WIDE * 3), BF), VMEM((NB, LANES), jnp.int32), pltpu.SMEM((NB, LANES), jnp.int32), pltpu.SemaphoreType.DMA])
    acc_shape = [jax.ShapeDtypeStruct((NG * CW, LANES), F32)] * T
    big = 6 * MIB

    def local_fn(kspace, wts_y, wts_x, idx_y, idx_x, coil_maps, deapod):
        own, far, maps, maps_end = pl.pallas_call(
            prep_kernel,
            out_shape=[jax.ShapeDtypeStruct((PAY * NB, LANES), F32)] * 2 + [jax.ShapeDtypeStruct((4, n, N_GRID), F32) for n in (HALF, WIN)],
            in_specs=[hbm] * 6, out_specs=[vm] * 4, name='prep',
            scratch_shapes=[VMEM((2, SUB, NS), F32), VMEM((KW, NS), F32), VMEM((KW, NS), F32), VMEM((NB, LANES), jnp.int32), VMEM((NB, LANES), jnp.int32), VMEM((2, 4, QB, N_IMG), F32), pltpu.SemaphoreType.DMA((6,))],
            compiler_params=pltpu.CompilerParams(vmem_limit_bytes=SUB * MIB),
        )(*[pltpu.with_memory_space_constraint(v, pltpu.HBM) for v in (kspace, wts_y, wts_x, idx_y.reshape(NB, LANES), idx_x.reshape(NB, LANES), jnp.swapaxes(coil_maps, 2, 3))])
        far_in = lax.ppermute(far, 'cols', [(0, 1), (1, 0)])
        half, *accs = pl.pallas_call(
            own_kernel, out_shape=[jax.ShapeDtypeStruct((11, CW, LANES), F32)] + acc_shape, in_specs=[vm], out_specs=[vm] * (T + 1),
            scratch_shapes=spread_scratch, compiler_params=pltpu.CompilerParams(vmem_limit_bytes=big), name='spread_own',
            cost_estimate=pl.CostEstimate(flops=GIGA, bytes_accessed=4 * MIB, transcendentals=0),
        )(own)
        *accs, pack = pl.pallas_call(
            far_kernel, out_shape=acc_shape + [jax.ShapeDtypeStruct((2, LANES, LANES), F32)],
            in_specs=[vm] * (T + 2), out_specs=[vm] * (T + 1), scratch_shapes=[VMEM((N_GRID, LANES), F32)] + spread_scratch,
            input_output_aliases={i + 2: i for i in range(T)},
            compiler_params=pltpu.CompilerParams(vmem_limit_bytes=big), name='spread_far',
            cost_estimate=pl.CostEstimate(flops=GIGA, bytes_accessed=4 * MIB, transcendentals=0),
        )(far_in, half, *accs)
        maps_x = lax.ppermute(maps, 'rows', [(i, (i + 2) % ROWS) for i in range(ROWS)])
        dma = pltpu.SemaphoreType.DMA
        half_bufs = [VMEM((2, 2, 2, n, LANES), BF) for _, n in GROUPS] + [VMEM((ROWS, n, LANES), BF) for _, n in GROUPS]
        full_bufs = [VMEM((2, 2, 2, 2, n, LANES), BF) for _, n in GROUPS] + [VMEM((ROWS, n, LANES), BF) for _, n in GROUPS]
        return pl.pallas_call(
            image_kernel,
            out_shape=jax.ShapeDtypeStruct((2, PB, QB), F32), in_specs=[vm] * (T + 9), out_specs=vm,
            scratch_shapes=[VMEM((TILES, N_GRID, LANES), BF), VMEM((N_GRID, LANES), F32), VMEM((4 * RB, 2 * N_GRID), BF), VMEM((2, LANES, LANES), F32)] + half_bufs + full_bufs + [
                VMEM((2, 2, 2, N_IMG, LANES), F32), VMEM((2, N_IMG, LANES), F32),
                VMEM((2, 2 * N_IMG, 2 * LANES), F32), VMEM((2, 2 * N_IMG, LANES), F32),
                VMEM((3, PB, LANES), F32), VMEM((3, PB, LANES), F32), VMEM((PB // 4, LANES), F32), VMEM((PB // 4, LANES), F32),
                dma((2,)), dma((2,)), dma((8,)), dma((8,)), dma((4,)), dma((4,)),
            ],
            compiler_params=pltpu.CompilerParams(vmem_limit_bytes=11 * MIB, collective_id=0, has_side_effects=True), name='image',
        )(*accs, half, pack, maps, maps_x, maps_end, deapod, col_dft(), row_dft(), unmix())

    return jax.shard_map(
        local_fn,
        mesh=mesh,
        in_specs=(P(None, None, sample_spec), P(None, sample_spec), P(None, sample_spec), P(sample_spec), P(sample_spec), P(None, ('exam', 'cols'), None, 'rows'), P()),
        out_specs=P(None, ('exam', 'cols'), 'rows'),
        check_vma=False,
    )
```

```python
import functools
import math

import jax
import jax.numpy as jnp
import numpy as np
from jax import lax
from jax.experimental import pallas as pl
from jax.experimental.pallas import tpu as pltpu
from jax.sharding import PartitionSpec as P

BF = jnp.bfloat16
F32 = jnp.float32
VMEM = pltpu.VMEM
LANES = 128
MIB = 1 << 20
GIGA = 4000 * MIB
TILES = 10
SUB, WIN, QTR, HALF, WIDE = 8, 16, 32, 64, 256
N_GRID, N_IMG, N_COILS, KW = 640, 320, 8, 6
ROWS, COLS = 4, 2
RB, CB, QB = N_GRID // ROWS, N_GRID // COLS, N_IMG // ROWS
PB = N_IMG // COLS
NS = 4096
NB = NS // LANES
STEP = 11
NG = 15
CW = CB + WIN
T = 7
PS = 9
PAY = 21
CODE = 512
HW = 24
ORDER = tuple(range(1, 9)) + (0, 9)
GROUPS = ((0, 128), (128, 32))
MESH_ID = pl.DeviceIdType.MESH


def dft_parts():
    freq = np.arange(N_GRID) - N_GRID // 2
    pos = np.arange(N_IMG) - N_IMG // 2
    ang = ((freq[:, None] * pos[None, :]) % N_GRID).astype(np.float32) * np.float32(2.0 * math.pi / N_GRID)
    norm = np.float32(1.0 / math.sqrt(N_GRID))
    c, s = np.cos(ang) * norm, np.sin(ang) * norm
    return np.stack([np.stack([c, s], 1), np.stack([-s, c], 1)], 0)


def col_dft():
    e = dft_parts()
    out = np.zeros((2 * N_GRID, N_GRID), np.float32)
    for dp in range(2):
        for t in range(2):
            for h in range(2):
                q0 = QB * (2 * dp + h)
                l0 = LANES * (2 * dp + t) + HALF * h
                out[:, l0:l0 + HALF] = e[:, :, t, q0:q0 + HALF].reshape(2 * N_GRID, HALF)
    for t in range(2):
        for d in range(4):
            l0 = 4 * LANES + HALF * t + WIN * d
            out[:, l0:l0 + WIN] = e[:, :, t, QB * d + HALF:QB * (d + 1)].reshape(2 * N_GRID, WIN)
    return jnp.asarray(out, BF)


def row_dft():
    e = dft_parts()
    rows = np.concatenate([np.arange(WIN * l, WIN * (l + 1)) for l in ORDER])
    chips = []
    for x in range(2):
        parts = []
        for start, n in GROUPS:
            for t in range(2):
                for b in range(2):
                    parts.append(e[t, (2 * x + b) * RB + rows[start:start + n]])
        m = np.concatenate(parts, 0)
        chips.append(np.concatenate([m[:, :, PB * h:PB * (h + 1)].reshape(N_GRID, N_IMG).T for h in range(2)], 0))
    return jnp.asarray(np.array(chips), BF)


def unmix():
    m = np.zeros((WIDE, WIDE), np.float32)
    for ch in range(SUB):
        for pp in range(2):
            for i in range(WIN):
                m[ch * QTR + WIN * pp + (i + SUB) % WIN, pp * 128 + i * SUB + ch] = 1.0
    return jnp.asarray(m, BF)


def prep_kernel(ks_hbm, wy_hbm, wx_hbm, iy_hbm, ix_hbm, maps_hbm, own_ref, far_ref, sp_ref, sq_ref, ks_ref, wy_ref, wx_ref, iy_ref, ix_ref, maps_ref, sem):
    k = lax.axis_index('cols')
    r = lax.axis_index('rows')
    loads = []
    for src, dst in ((iy_hbm, iy_ref), (ix_hbm, ix_ref), (wx_hbm, wx_ref), (wy_hbm, wy_ref), (ks_hbm, ks_ref), (maps_hbm, maps_ref)):
        cp = pltpu.make_async_copy(src, dst, sem.at[len(loads)])
        cp.start()
        loads.append(cp)
    loads[0].wait()
    loads[1].wait()
    iy = iy_ref[...]
    code = ((iy - r * RB + 5) * CODE + ix_ref[...] - k * CB + 5).astype(F32)
    for i in range(2, 5):
        loads[i].wait()
    lo = jnp.concatenate([ks_ref[0, 0:4, :], ks_ref[1, 0:4, :]], axis=0)
    hi = jnp.concatenate([ks_ref[0, 4:SUB, :], ks_ref[1, 4:SUB, :]], axis=0)
    first = k == 0
    for ref, y in ((own_ref, jnp.where(first, lo, hi)), (far_ref, jnp.where(first, hi, lo))):
        for b in range(NB):
            cols = slice(LANES * b, LANES * (b + 1))
            ref[PAY * b:PAY * b + SUB, :] = y[:, cols]
            ref[PAY * b + SUB:PAY * b + SUB + KW, :] = wx_ref[:, cols]
            ref[PAY * (b + 1) - KW - 1:PAY * (b + 1) - 1, :] = wy_ref[:, cols]
            ref[PAY * (b + 1) - 1:PAY * (b + 1), :] = code[b:b + 1, :]
    loads[5].wait()
    for c in range(4):
        for ref, q in ((sp_ref, slice(0, HALF)), (sq_ref, slice(HALF, QB))):
            for i in range(2):
                ref[c, :, WIDE * i:WIDE * (i + 1)] = maps_ref[i, c, q, :WIDE]
            ref[c, :, 2 * WIDE:] = jnp.concatenate([maps_ref[i, c, q, WIDE:] for i in range(2)], axis=1)


def split3(x):
    hi = x.astype(BF).astype(F32)
    r = x - hi
    mid = r.astype(BF).astype(F32)
    return hi, mid, r - mid


def accumulate(pay_ref, accs, us, xs, vs, r_ref, int_ref, base_ref, sem):
    row_i = lax.broadcasted_iota(jnp.int32, (WIN, LANES), 0)

    def make_u(blk, k):
        off = jnp.minimum(blk, NB - 1) * PAY
        y8 = pay_ref[pl.ds(off, SUB), :]
        wx = pay_ref[pl.ds(off + SUB, SUB), :]
        wyp = pay_ref[pl.ds(off + PAY - SUB, SUB), :]
        d = (row_i - (wyp[7:, :].astype(jnp.int32) // CODE)) & (WIN - 1)
        p = jnp.zeros((WIN, LANES), F32)
        for a in range(KW):
            p = jnp.where(d == a, wyp[a + 1:a + 2, :], p)
        us[k][...] = jnp.concatenate([y8 * p[i:i + 1, :] for i in range(WIN)], axis=0).T
        x3 = list(split3(wx)) + [jnp.zeros((LANES - HW, LANES), F32)]
        xs[k][...] = jnp.concatenate(x3, axis=0).T

    def make_v(k):
        lhs = xs[k][...].astype(BF)
        u = us[k][...]
        for bp in range(3):
            w = jnp.dot(lhs, r_ref[:, WIDE * bp:WIDE * bp + WIDE], preferred_element_type=F32)
            for c in range(2):
                v = w[:, LANES * c:LANES * (c + 1)] * u
                for g in range(WIN):
                    vs[k][pl.ds(SUB * PS * g + 2 * bp + c, SUB, stride=PS), :] = v[SUB * g:SUB * g + SUB, :]

    def add_tiles(blk, k):
        row = base_ref.at[blk]
        for j in range(LANES):
            acc = accs[j % T]
            b = row[j]
            acc[pl.ds(b, SUB), :] = acc[pl.ds(b, SUB), :] + vs[k][PS * j:PS * j + SUB, :]

    code = jnp.concatenate([pay_ref[PAY * (b + 1) - 1:PAY * (b + 1), :] for b in range(NB)], axis=0).astype(jnp.int32)
    int_ref[...] = (((code // CODE - 5) * 187) >> STEP) * CW + (code & (CODE - 1))
    kk = lax.broadcasted_iota(jnp.int32, (LANES, WIDE * 3), 0)
    ll = lax.broadcasted_iota(jnp.int32, (LANES, WIDE * 3), 1)
    r_ref[...] = jnp.where((kk < HW) & ((kk & 7) == (ll >> 7)), 1.0, 0.0).astype(BF)
    for v in vs:
        v[...] = jnp.zeros_like(v)
    load = pltpu.make_async_copy(int_ref, base_ref, sem)
    load.start()
    make_u(0, 0)
    make_u(1, 1)
    make_v(0)
    load.wait()

    def body(n, _):
        k = 2 * n
        make_v(1)
        add_tiles(k, 0)
        make_u(k + 2, 0)
        make_v(0)
        add_tiles(k + 1, 1)
        make_u(k + 3, 1)
        return 0

    lax.fori_loop(0, NB // 2, body, 0)


def folded(accs, off, n, clear=False):
    def total(g):
        rows = pl.ds(pl.multiple_of(g * CW + off, SUB), n)
        v = accs[0][rows, :]
        for a in accs[1:]:
            v = v + a[rows, :]
        if clear:
            for a in accs:
                a[rows, :] = jnp.zeros((n, LANES), F32)
        return v

    row = lax.broadcasted_iota(jnp.int32, (n, LANES), 1) >> 3
    tiles = [None] * TILES
    for g in range(NG):
        v = total(g)
        if g == 0:
            ghost = v
        first = 5 + STEP * g
        for p in range(TILES):
            lo, hi = max(first, SUB + WIN * p), min(first + WIN, SUB + WIN * (p + 1))
            if lo < hi:
                part = jnp.where((row - lo & (WIN - 1)) < hi - lo, v, 0.0)
                tiles[p] = part if tiles[p] is None else tiles[p] + part
    return tiles + [jnp.where(row >= SUB, v, ghost)]


def own_kernel(pay_ref, out_ref, *refs):
    accs, scr = refs[:T], refs[T:]

    def clear(n, _):
        for a in accs:
            a[pl.ds(pl.multiple_of(n * CW, SUB), CW), :] = jnp.zeros((CW, LANES), F32)
        return 0

    lax.fori_loop(0, NG, clear, 0)
    accumulate(pay_ref, accs, scr[:2], scr[2:4], scr[4:6], *scr[6:])

    def fold(q, _):
        off = pl.multiple_of(q * WIN, WIN)
        for p, t in enumerate(folded(accs, off, WIN, clear=True)):
            out_ref[p, pl.ds(off, WIN), :] = t
        return 0

    lax.fori_loop(0, CW // WIN, fold, 0)


def far_kernel(pay_ref, a_ref, *refs):
    accs, pack_ref, gh_ref, scr = refs[T:2 * T], refs[2 * T], refs[2 * T + 1], refs[2 * T + 2:]
    accumulate(pay_ref, accs, scr[:2], scr[2:4], scr[4:6], *scr[6:])
    own0 = lax.axis_index('cols') * CB
    far0 = CB - own0

    def ghost(off, n):
        high = lax.broadcasted_iota(jnp.int32, (n, LANES), 1) >= HALF
        ends = []
        for g in (0, NG - 1):
            rows = pl.ds(pl.multiple_of(g * CW + off, SUB), n)
            v = accs[0][rows, :]
            for a in accs[1:]:
                v = v + a[rows, :]
            ends.append(v)
        return jnp.where(high, ends[1], ends[0])

    def copy(n, _):
        o = pl.multiple_of(n * QTR, SUB)
        gh_ref[pl.ds(pl.multiple_of(far0 + o, SUB), QTR), :] = ghost(SUB + o, QTR)
        gh_ref[pl.ds(pl.multiple_of(own0 + o, SUB), QTR), :] = a_ref[TILES, pl.ds(pl.multiple_of(SUB + o, SUB), QTR), :]
        return 0

    lax.fori_loop(0, CB // QTR, copy, 0)
    for dst, add in ((own0, ghost(CW - SUB, SUB)), (own0 + CB - SUB, ghost(0, SUB)), (far0, a_ref[TILES, CW - SUB:, :]), (far0 + CB - SUB, a_ref[TILES, :SUB, :])):
        rows = pl.ds(pl.multiple_of(dst, SUB), SUB)
        gh_ref[rows, :] = gh_ref[rows, :] + add

    lane = lax.broadcasted_iota(jnp.int32, (LANES, LANES), 1)
    for side, lane0 in ((0, HALF - HW), (1, HALF)):
        out = jnp.zeros((LANES, LANES), F32)
        for j in range(5):
            piece = pltpu.roll(gh_ref[LANES * j:LANES * (j + 1), :], (HW * j - lane0) % LANES, axis=1)
            out = jnp.where(lane >= HW * j, piece, out)
        pack_ref[side] = out


def image_kernel(*refs):
    accs = refs[:T]
    (a_ref, pack_ref, so_ref, sx_ref, se_ref, d_ref, ev_ref, eu_ref, pm_ref, out_ref,
     tb_ref, edge_ref, g_ref, halo, sm1, sm2, sr1, sr2, hm1, hm2, hr1, hr2, s_main, s_rem, acc_m, acc_r, pieces, recvs, tails, recvs_t,
     halo_ss, halo_rs, swap_ss, swap_rs, red_ss, red_rs) = refs[T:]
    k = lax.axis_index('cols')
    r = lax.axis_index('rows')
    core, x = r % 2, r // 2
    near = r + 1 - 2 * core
    across = (r + 2) % 4
    prev, nxt = (r + 3) % 4, (r + 1) % 4
    homes = ({'rows': across, 'cols': 1 - k}, {'rows': across}, {'cols': 1 - k})

    barrier = pltpu.get_barrier_semaphore()
    for dev in ({'rows': prev}, {'rows': nxt}) + homes:
        pl.semaphore_signal(barrier, inc=1, device_id=dev, device_id_type=MESH_ID)

    own0 = k * CB
    far0 = CB - own0
    high16 = lax.broadcasted_iota(jnp.int32, (WIN, LANES), 1) >= HALF

    def put(v, tiles):
        rows = pl.ds(pl.multiple_of(v, WIN), WIN)
        for p in range(TILES):
            tb_ref[p, rows, :] = tiles[p].astype(BF)
        edge_ref[rows, :] = jnp.where(high16, tiles[0], tiles[9])

    def far_part(n, _):
        put(far0 + WIN * n, folded(accs, pl.multiple_of(SUB + WIN * n, SUB), WIN))
        return 0

    def own_part(n, _):
        put(own0 + WIN * n, [a_ref[p, pl.ds(pl.multiple_of(SUB + WIN * n, SUB), WIN), :] for p in range(TILES)])
        return 0

    last = CB // WIN - 1
    lax.fori_loop(1, last, far_part, 0)
    pl.semaphore_wait(barrier, 5)

    def remote(src, dst, ss, rs, i, dev):
        cp = pltpu.make_async_remote_copy(src_ref=src, dst_ref=dst, send_sem=ss.at[i], recv_sem=rs.at[i], device_id=dev, device_id_type=MESH_ID)
        cp.start()
        return cp

    halos = [remote(pack_ref.at[i], halo.at[i], halo_ss, halo_rs, i, {'rows': dev}) for i, dev in ((0, prev), (1, nxt))]

    lax.fori_loop(1, last, own_part, 0)
    none = jnp.zeros((SUB, LANES), F32)
    for n, side in ((0, CW - SUB), (last, 0)):
        off = SUB + WIN * n
        near_tiles = folded(accs, off, WIN)
        far_ends = folded(accs, side, SUB)
        order = (lambda v: [v, none]) if n == 0 else (lambda v: [none, v])
        put(far0 + WIN * n, [near_tiles[p] + jnp.concatenate(order(a_ref[p, side:side + SUB, :]), axis=0) for p in range(TILES)])
        put(own0 + WIN * n, [a_ref[p, off:off + WIN, :] + jnp.concatenate(order(far_ends[p]), axis=0) for p in range(TILES)])


    def to_rows(row0, n, t0, t1):
        a = jnp.concatenate([t0, t1], axis=1)
        g = lax.dot_general(pm_ref[...], a, (((1,), (1,)), ((), ())), preferred_element_type=F32).astype(BF)
        for ch in range(SUB):
            i, c = ch // 4, ch % 4
            g_ref[row0 + n * c:row0 + n * c + QTR, N_GRID * i:N_GRID * (i + 1)] = g[QTR * ch:QTR * (ch + 1), :]

    for m in range(4):
        to_rows(QTR * m, LANES, tb_ref[2 * m + 1], tb_ref[2 * m + 2])

    sms, srs, hms, hrs = (sm1, sm2), (sr1, sr2), (hm1, hm2), (hr1, hr2)
    swaps, trades = [], []

    def columns(grp):
        start, n = GROUPS[grp]
        lane = lax.broadcasted_iota(jnp.int32, (n, LANES), 1)
        side = lane >> 6
        own_even, far_even = side == core, side != core
        block = (lane & (HALF - 1)) >> 4
        h = jnp.dot(g_ref[4 * start:4 * (start + n), :], ev_ref[...], preferred_element_type=F32)
        hc = [h[n * c:n * (c + 1)] for c in range(4)]
        rems = [v[:, 4 * LANES:] for v in hc]
        for cp in range(2):
            hs = [[v[:, LANES * i:LANES * (i + 1)] for i in range(4)] for v in hc[2 * cp:2 * cp + 2]]
            for i in range(4):
                dp, t = i // 2, i % 2
                odd = pltpu.roll(hs[1][i], HALF, axis=1)
                sms[grp][dp, cp, t] = jnp.where(far_even, hs[0][i], odd).astype(BF)
                hms[grp][dp, cp, t, core] = jnp.where(own_even, hs[0][i], odd).astype(BF)
        for d in range(ROWS):
            out = rems[d]
            for c in range(4):
                if c != d:
                    out = jnp.where(block == c, pltpu.roll(rems[c], (WIN * (c - d)) % LANES, axis=1), out)
            srs[grp][d] = out.astype(BF)
        hrs[grp][r] = srs[grp][r]
        swaps.append(remote(sms[grp], hms[grp].at[:, :, :, core], swap_ss, swap_rs, grp, {'rows': near}))
        for i, dev in enumerate((across, 3 - r, near)):
            trades.append(remote(srs[grp].at[dev], hrs[grp].at[r], swap_ss, swap_rs, 2 + 3 * grp + i, {'rows': dev}))

    columns(0)

    for h in halos:
        h.wait()
    lane = lax.broadcasted_iota(jnp.int32, (LANES, LANES), 1)
    low = lane < HALF
    t0s, t9s = [], []
    for j in range(5):
        rows = slice(LANES * j, LANES * (j + 1))
        add_first = pltpu.roll(halo[1], (HALF - HW * j) % LANES, axis=1)
        add_last = pltpu.roll(halo[0], (HALF - HW - HW * j) % LANES, axis=1)
        e = edge_ref[rows, :] + jnp.where(low, jnp.where(lane >= HALF - HW, add_last, 0.0), jnp.where(lane < HALF + HW, add_first, 0.0))
        t0s.append(jnp.where(low, tb_ref[0, rows, :].astype(F32), e).astype(BF))
        t9s.append(jnp.where(low, e, tb_ref[9, rows, :].astype(F32)).astype(BF))
    lane = lax.broadcasted_iota(jnp.int32, (PB, LANES), 1)
    low = lane < HALF
    to_rows(4 * LANES, QTR, jnp.concatenate(t0s, axis=0), jnp.concatenate(t9s, axis=0))
    columns(1)

    def turn(rows):
        t = [rows[:, LANES * i:LANES * (i + 1)].T for i in range(5)]
        return [jnp.concatenate([t[2 * i], t[2 * i + 1], t[4][HALF * i:HALF * (i + 1)]], axis=0) for i in range(2)]


    for cp in swaps[:1]:
        cp.wait_recv()
    n0 = 4 * GROUPS[0][1]

    def block_of(grp, j):
        return jnp.concatenate([hms[grp][(x + j) % 2, cp].reshape(4 * GROUPS[grp][1], LANES) for cp in range(2)], axis=1)

    for j, ref in ((1, sx_ref), (0, so_ref)):
        acc_m[j] = jnp.dot(eu_ref[x, :, :n0], block_of(0, j), preferred_element_type=F32)
        for cp in range(2):
            s_main[j, 0, cp], s_main[j, 1, cp] = turn(jnp.concatenate([ref[2 * cp + core], ref[2 * cp + 1 - core]], axis=0))

    for cp in swaps[1:]:
        cp.wait_recv()

    def rows_dft(half, acc, rhs):
        rows = pl.ds(pl.multiple_of(half * N_IMG, WIN), N_IMG)
        total = acc[rows, :] + jnp.dot(eu_ref[x, rows, n0:], rhs, preferred_element_type=F32)
        return total[:PB], total[PB:]

    quarter = lax.broadcasted_iota(jnp.int32, (PB // 4, LANES), 1) >> 5

    def piece(half, j):
        i_re, i_im = rows_dft(half, acc_m.at[j], block_of(1, j))
        rows = pl.ds(pl.multiple_of(half * PB, SUB), PB)
        re, im = None, None
        for cp in range(2):
            cols = slice(LANES * cp, LANES * (cp + 1))
            s_re, s_im = s_main[j, 0, cp, rows, :], s_main[j, 1, cp, rows, :]
            a = s_re * i_re[:, cols] + s_im * i_im[:, cols]
            b = s_re * i_im[:, cols] - s_im * i_re[:, cols]
            re, im = (a, b) if re is None else (re + a, im + b)
        return jnp.where(low, re + pltpu.roll(re, HALF, axis=1), im + pltpu.roll(im, HALF, axis=1))

    def rest(half):
        parts = []
        for o in range(2):
            rows = pl.ds(pl.multiple_of(half * N_IMG + PB * o, WIN), PB)
            parts.append(acc_r[0, rows, :] + pltpu.roll(acc_r[1, rows, :], HALF, axis=1))
        i_re, i_im = parts
        rows = pl.ds(pl.multiple_of(half * PB, SUB), PB)
        s_re, s_im = s_rem[0, rows, :], s_rem[1, rows, :]
        w = s_re * i_re + s_im * i_im + pltpu.roll(s_re * i_im - s_im * i_re, HALF, axis=1)
        w = w + pltpu.roll(w, LANES - QTR, axis=1)
        w = w + pltpu.roll(w, LANES - WIN, axis=1)
        w = jnp.where(lane < WIN, w, pltpu.roll(w, LANES - HALF + WIN, axis=1))
        out = w[:PB // 4]
        for g in range(1, 4):
            out = jnp.where(quarter == g, pltpu.roll(w[PB // 4 * g:PB // 4 * (g + 1)], QTR * g, axis=1), out)
        return out

    first, other = pl.ds(0, HALF), pl.ds(HALF, PB - HALF)
    pieces[0] = piece(1 - k, 1)
    joined = remote(pieces.at[0, first], recvs.at[0, first], red_ss, red_rs, 0, homes[1])
    sends = [remote(pieces.at[0, other], recvs.at[0, other], red_ss, red_rs, 1, homes[0])]
    pieces[1] = piece(k, 1)
    sends.append(remote(pieces.at[1], recvs.at[1], red_ss, red_rs, 2, homes[1]))
    across_y = piece(1 - k, 0)
    pieces[2, HALF:] = across_y[HALF:]
    sends.append(remote(pieces.at[2, other], recvs.at[2, other], red_ss, red_rs, 4, homes[2]))
    for cp in trades:
        cp.wait_recv()
    for t in range(2):
        total = None
        for grp in range(2):
            kk = 2 * GROUPS[grp][1]
            for c in range(2):
                part = jnp.dot(eu_ref[c, :, n0 * grp + kk * t:n0 * grp + kk * (t + 1)], hrs[grp][2 * c:2 * c + 2].reshape(kk, LANES), preferred_element_type=F32)
                total = part if total is None else total + part
        acc_r[t] = total
    s_rem[0], s_rem[1] = turn(jnp.concatenate([se_ref[c] for c in range(4)] + [jnp.zeros((HALF, N_GRID), F32)], axis=0))
    tails[...] = rest(1 - k)
    tail = remote(tails, recvs_t, red_ss, red_rs, 3, homes[2])
    rem = rest(k)
    joined.wait_recv()
    pieces[2, :HALF] = across_y[:HALF] + recvs[0, :HALF]
    sends.append(remote(pieces.at[2, first], recvs.at[2, first], red_ss, red_rs, 5, homes[2]))
    main = piece(k, 0)
    d8 = jnp.broadcast_to(jnp.concatenate([d_ref[...][None, :], jnp.zeros((1, HALF), F32)], axis=1), (SUB, N_IMG + HALF))
    dq = d8
    for j in range(1, ROWS):
        dq = jnp.where(r == j, pltpu.roll(d8, N_IMG + HALF - QB * j, axis=1), dq)
    dp = jnp.where(k == 0, d8, pltpu.roll(d8, N_IMG + HALF - PB, axis=1))[:, :2 * LANES]
    dd = jnp.concatenate([dp] * WIN, axis=0).T[:PB] * dq[:1, :LANES]

    for cp in sends:
        cp.wait_recv()
    main = main + recvs[1] + recvs[2]
    main = jnp.concatenate([main[:HALF], main[HALF:] + recvs[0, HALF:]], axis=0)
    tail.wait_recv()
    rem = rem + recvs_t[...]
    for o in range(2):
        m = pltpu.roll(main, HALF, axis=1) if o else main
        for j in range(4):
            rows = slice(PB // 4 * j, PB // 4 * (j + 1))
            end = pltpu.roll(rem, (HALF - QTR * j - WIN * o) % LANES, axis=1)
            out_ref[o, rows, :] = (jnp.where(low[rows], m[rows], end) * dd[rows])[:, :QB]

    for cp in sends + swaps + trades + [tail, joined]:
        cp.wait_send()


def solution(mesh):
    sample_spec = ('exam', 'rows', 'cols')
    vm = pl.BlockSpec(memory_space=pltpu.VMEM)
    hbm = pl.BlockSpec(memory_space=pltpu.HBM)
    spread_scratch = ([VMEM((LANES, LANES), F32)] * 4 + [VMEM((LANES * PS, LANES), F32)] * 2
                      + [VMEM((LANES, WIDE * 3), BF), VMEM((NB, LANES), jnp.int32), pltpu.SMEM((NB, LANES), jnp.int32), pltpu.SemaphoreType.DMA])
    acc_shape = [jax.ShapeDtypeStruct((NG * CW, LANES), F32)] * T
    big = 6 * MIB

    def local_fn(kspace, wts_y, wts_x, idx_y, idx_x, coil_maps, deapod):
        own, far, maps, maps_end = pl.pallas_call(
            prep_kernel,
            out_shape=[jax.ShapeDtypeStruct((PAY * NB, LANES), F32)] * 2 + [jax.ShapeDtypeStruct((4, n, N_GRID), F32) for n in (HALF, WIN)],
            in_specs=[hbm] * 6, out_specs=[vm] * 4, name='prep',
            scratch_shapes=[VMEM((2, SUB, NS), F32), VMEM((KW, NS), F32), VMEM((KW, NS), F32), VMEM((NB, LANES), jnp.int32), VMEM((NB, LANES), jnp.int32), VMEM((2, 4, QB, N_IMG), F32), pltpu.SemaphoreType.DMA((6,))],
            compiler_params=pltpu.CompilerParams(vmem_limit_bytes=SUB * MIB),
        )(*[pltpu.with_memory_space_constraint(v, pltpu.HBM) for v in (kspace, wts_y, wts_x, idx_y.reshape(NB, LANES), idx_x.reshape(NB, LANES), jnp.swapaxes(coil_maps, 2, 3))])
        far_in = lax.ppermute(far, 'cols', [(0, 1), (1, 0)])
        half, *accs = pl.pallas_call(
            own_kernel, out_shape=[jax.ShapeDtypeStruct((11, CW, LANES), F32)] + acc_shape, in_specs=[vm], out_specs=[vm] * (T + 1),
            scratch_shapes=spread_scratch, compiler_params=pltpu.CompilerParams(vmem_limit_bytes=big), name='spread_own',
            cost_estimate=pl.CostEstimate(flops=GIGA, bytes_accessed=4 * MIB, transcendentals=0),
        )(own)
        *accs, pack = pl.pallas_call(
            far_kernel, out_shape=acc_shape + [jax.ShapeDtypeStruct((2, LANES, LANES), F32)],
            in_specs=[vm] * (T + 2), out_specs=[vm] * (T + 1), scratch_shapes=[VMEM((N_GRID, LANES), F32)] + spread_scratch,
            input_output_aliases={i + 2: i for i in range(T)},
            compiler_params=pltpu.CompilerParams(vmem_limit_bytes=big), name='spread_far',
            cost_estimate=pl.CostEstimate(flops=GIGA, bytes_accessed=4 * MIB, transcendentals=0),
        )(far_in, half, *accs)
        maps_x = lax.ppermute(maps, 'rows', [(i, (i + 2) % ROWS) for i in range(ROWS)])
        dma = pltpu.SemaphoreType.DMA
        half_bufs = [VMEM((2, 2, 2, n, LANES), BF) for _, n in GROUPS] + [VMEM((ROWS, n, LANES), BF) for _, n in GROUPS]
        full_bufs = [VMEM((2, 2, 2, 2, n, LANES), BF) for _, n in GROUPS] + [VMEM((ROWS, n, LANES), BF) for _, n in GROUPS]
        return pl.pallas_call(
            image_kernel,
            out_shape=jax.ShapeDtypeStruct((2, PB, QB), F32), in_specs=[vm] * (T + 9), out_specs=vm,
            scratch_shapes=[VMEM((TILES, N_GRID, LANES), BF), VMEM((N_GRID, LANES), F32), VMEM((4 * RB, 2 * N_GRID), BF), VMEM((2, LANES, LANES), F32)] + half_bufs + full_bufs + [
                VMEM((2, 2, 2, N_IMG, LANES), F32), VMEM((2, N_IMG, LANES), F32),
                VMEM((2, 2 * N_IMG, 2 * LANES), F32), VMEM((2, 2 * N_IMG, LANES), F32),
                VMEM((3, PB, LANES), F32), VMEM((3, PB, LANES), F32), VMEM((PB // 4, LANES), F32), VMEM((PB // 4, LANES), F32),
                dma((2,)), dma((2,)), dma((8,)), dma((8,)), dma((6,)), dma((6,)),
            ],
            compiler_params=pltpu.CompilerParams(vmem_limit_bytes=11 * MIB, collective_id=0, has_side_effects=True), name='image',
        )(*accs, half, pack, maps, maps_x, maps_end, deapod, col_dft(), row_dft(), unmix())

    return jax.shard_map(
        local_fn,
        mesh=mesh,
        in_specs=(P(None, None, sample_spec), P(None, sample_spec), P(None, sample_spec), P(sample_spec), P(sample_spec), P(None, ('exam', 'cols'), None, 'rows'), P()),
        out_specs=P(None, ('exam', 'cols'), 'rows'),
        check_vma=False,
    )
```

```python
import functools
import math

import jax
import jax.numpy as jnp
import numpy as np
from jax import lax
from jax.experimental import pallas as pl
from jax.experimental.pallas import tpu as pltpu
from jax.sharding import PartitionSpec as P

BF = jnp.bfloat16
F32 = jnp.float32
VMEM = pltpu.VMEM
LANES = 128
MIB = 1 << 20
GIGA = 4000 * MIB
TILES = 10
SUB, WIN, QTR, HALF, WIDE = 8, 16, 32, 64, 256
N_GRID, N_IMG, N_COILS, KW = 640, 320, 8, 6
ROWS, COLS = 4, 2
RB, CB, QB = N_GRID // ROWS, N_GRID // COLS, N_IMG // ROWS
PB = N_IMG // COLS
NS = 4096
NB = NS // LANES
STEP = 11
NG = 15
CW = CB + WIN
T = 7
PS = 9
PAY = 21
CODE = 512
HW = 24
ORDER = tuple(range(1, 9)) + (0, 9)
GROUPS = ((0, 128), (128, 32))
MESH_ID = pl.DeviceIdType.MESH


def dft_parts():
    freq = np.arange(N_GRID) - N_GRID // 2
    pos = np.arange(N_IMG) - N_IMG // 2
    ang = ((freq[:, None] * pos[None, :]) % N_GRID).astype(np.float32) * np.float32(2.0 * math.pi / N_GRID)
    norm = np.float32(1.0 / math.sqrt(N_GRID))
    c, s = np.cos(ang) * norm, np.sin(ang) * norm
    return np.stack([np.stack([c, s], 1), np.stack([-s, c], 1)], 0)


def col_dft():
    e = dft_parts()
    out = np.zeros((2 * N_GRID, N_GRID), np.float32)
    for dp in range(2):
        for t in range(2):
            for h in range(2):
                q0 = QB * (2 * dp + h)
                l0 = LANES * (2 * dp + t) + HALF * h
                out[:, l0:l0 + HALF] = e[:, :, t, q0:q0 + HALF].reshape(2 * N_GRID, HALF)
    for t in range(2):
        for d in range(4):
            l0 = 4 * LANES + HALF * t + WIN * d
            out[:, l0:l0 + WIN] = e[:, :, t, QB * d + HALF:QB * (d + 1)].reshape(2 * N_GRID, WIN)
    return jnp.asarray(out, BF)


def row_dft():
    e = dft_parts()
    rows = np.concatenate([np.arange(WIN * l, WIN * (l + 1)) for l in ORDER])
    chips = []
    for x in range(2):
        parts = []
        for start, n in GROUPS:
            for t in range(2):
                for b in range(2):
                    parts.append(e[t, (2 * x + b) * RB + rows[start:start + n]])
        m = np.concatenate(parts, 0)
        chips.append(np.concatenate([m[:, :, PB * h:PB * (h + 1)].reshape(N_GRID, N_IMG).T for h in range(2)], 0))
    return jnp.asarray(np.array(chips), BF)


def unmix():
    m = np.zeros((WIDE, WIDE), np.float32)
    for ch in range(SUB):
        for pp in range(2):
            for i in range(WIN):
                m[ch * QTR + WIN * pp + (i + SUB) % WIN, pp * 128 + i * SUB + ch] = 1.0
    return jnp.asarray(m, BF)


def prep_kernel(ks_hbm, wy_hbm, wx_hbm, iy_hbm, ix_hbm, maps_hbm, own_ref, far_ref, sp_ref, sq_ref, ks_ref, wy_ref, wx_ref, iy_ref, ix_ref, maps_ref, sem):
    k = lax.axis_index('cols')
    r = lax.axis_index('rows')
    loads = []
    for src, dst in ((iy_hbm, iy_ref), (ix_hbm, ix_ref), (wx_hbm, wx_ref), (wy_hbm, wy_ref), (ks_hbm, ks_ref), (maps_hbm, maps_ref)):
        cp = pltpu.make_async_copy(src, dst, sem.at[len(loads)])
        cp.start()
        loads.append(cp)
    loads[0].wait()
    loads[1].wait()
    iy = iy_ref[...]
    code = ((iy - r * RB + 5) * CODE + ix_ref[...] - k * CB + 5).astype(F32)
    for i in range(2, 5):
        loads[i].wait()
    lo = jnp.concatenate([ks_ref[0, 0:4, :], ks_ref[1, 0:4, :]], axis=0)
    hi = jnp.concatenate([ks_ref[0, 4:SUB, :], ks_ref[1, 4:SUB, :]], axis=0)
    first = k == 0
    for ref, y in ((own_ref, jnp.where(first, lo, hi)), (far_ref, jnp.where(first, hi, lo))):
        for b in range(NB):
            cols = slice(LANES * b, LANES * (b + 1))
            ref[PAY * b:PAY * b + SUB, :] = y[:, cols]
            ref[PAY * b + SUB:PAY * b + SUB + KW, :] = wx_ref[:, cols]
            ref[PAY * (b + 1) - KW - 1:PAY * (b + 1) - 1, :] = wy_ref[:, cols]
            ref[PAY * (b + 1) - 1:PAY * (b + 1), :] = code[b:b + 1, :]
    loads[5].wait()
    for c in range(4):
        for ref, q in ((sp_ref, slice(0, HALF)), (sq_ref, slice(HALF, QB))):
            for i in range(2):
                ref[c, :, WIDE * i:WIDE * (i + 1)] = maps_ref[i, c, q, :WIDE]
            ref[c, :, 2 * WIDE:] = jnp.concatenate([maps_ref[i, c, q, WIDE:] for i in range(2)], axis=1)


def split3(x):
    hi = x.astype(BF).astype(F32)
    r = x - hi
    mid = r.astype(BF).astype(F32)
    return hi, mid, r - mid


def accumulate(pay_ref, accs, us, xs, vs, r_ref, int_ref, base_ref, sem):
    row_i = lax.broadcasted_iota(jnp.int32, (WIN, LANES), 0)

    def make_u(blk, k):
        off = jnp.minimum(blk, NB - 1) * PAY
        y8 = pay_ref[pl.ds(off, SUB), :]
        wx = pay_ref[pl.ds(off + SUB, SUB), :]
        wyp = pay_ref[pl.ds(off + PAY - SUB, SUB), :]
        d = (row_i - (wyp[7:, :].astype(jnp.int32) // CODE)) & (WIN - 1)
        p = jnp.zeros((WIN, LANES), F32)
        for a in range(KW):
            p = jnp.where(d == a, wyp[a + 1:a + 2, :], p)
        us[k][...] = jnp.concatenate([y8 * p[i:i + 1, :] for i in range(WIN)], axis=0).T
        x3 = list(split3(wx)) + [jnp.zeros((LANES - HW, LANES), F32)]
        xs[k][...] = jnp.concatenate(x3, axis=0).T

    def make_v(k):
        lhs = xs[k][...].astype(BF)
        u = us[k][...]
        for bp in range(3):
            w = jnp.dot(lhs, r_ref[:, WIDE * bp:WIDE * bp + WIDE], preferred_element_type=F32)
            for c in range(2):
                v = w[:, LANES * c:LANES * (c + 1)] * u
                for g in range(WIN):
                    vs[k][pl.ds(SUB * PS * g + 2 * bp + c, SUB, stride=PS), :] = v[SUB * g:SUB * g + SUB, :]

    def add_tiles(blk, k):
        row = base_ref.at[blk]
        for j in range(LANES):
            acc = accs[j % T]
            b = row[j]
            acc[pl.ds(b, SUB), :] = acc[pl.ds(b, SUB), :] + vs[k][PS * j:PS * j + SUB, :]

    code = jnp.concatenate([pay_ref[PAY * (b + 1) - 1:PAY * (b + 1), :] for b in range(NB)], axis=0).astype(jnp.int32)
    int_ref[...] = (((code // CODE - 5) * 187) >> STEP) * CW + (code & (CODE - 1))
    kk = lax.broadcasted_iota(jnp.int32, (LANES, WIDE * 3), 0)
    ll = lax.broadcasted_iota(jnp.int32, (LANES, WIDE * 3), 1)
    r_ref[...] = jnp.where((kk < HW) & ((kk & 7) == (ll >> 7)), 1.0, 0.0).astype(BF)
    for v in vs:
        v[...] = jnp.zeros_like(v)
    load = pltpu.make_async_copy(int_ref, base_ref, sem)
    load.start()
    make_u(0, 0)
    make_u(1, 1)
    make_v(0)
    load.wait()

    def body(n, _):
        k = 2 * n
        make_v(1)
        add_tiles(k, 0)
        make_u(k + 2, 0)
        make_v(0)
        add_tiles(k + 1, 1)
        make_u(k + 3, 1)
        return 0

    lax.fori_loop(0, NB // 2, body, 0)


def folded(accs, off, n, clear=False):
    def total(g):
        rows = pl.ds(pl.multiple_of(g * CW + off, SUB), n)
        v = accs[0][rows, :]
        for a in accs[1:]:
            v = v + a[rows, :]
        if clear:
            for a in accs:
                a[rows, :] = jnp.zeros((n, LANES), F32)
        return v

    row = lax.broadcasted_iota(jnp.int32, (n, LANES), 1) >> 3
    tiles = [None] * TILES
    for g in range(NG):
        v = total(g)
        if g == 0:
            ghost = v
        first = 5 + STEP * g
        for p in range(TILES):
            lo, hi = max(first, SUB + WIN * p), min(first + WIN, SUB + WIN * (p + 1))
            if lo < hi:
                part = jnp.where((row - lo & (WIN - 1)) < hi - lo, v, 0.0)
                tiles[p] = part if tiles[p] is None else tiles[p] + part
    return tiles + [jnp.where(row >= SUB, v, ghost)]


def own_kernel(pay_ref, out_ref, *refs):
    accs, scr = refs[:T], refs[T:]

    def clear(n, _):
        for a in accs:
            a[pl.ds(pl.multiple_of(n * CW, SUB), CW), :] = jnp.zeros((CW, LANES), F32)
        return 0

    lax.fori_loop(0, NG, clear, 0)
    accumulate(pay_ref, accs, scr[:2], scr[2:4], scr[4:6], *scr[6:])

    def fold(q, _):
        off = pl.multiple_of(q * WIN, WIN)
        for p, t in enumerate(folded(accs, off, WIN, clear=True)):
            out_ref[p, pl.ds(off, WIN), :] = t
        return 0

    lax.fori_loop(0, CW // WIN, fold, 0)


def far_kernel(pay_ref, a_ref, *refs):
    accs, pack_ref, gh_ref, scr = refs[T:2 * T], refs[2 * T], refs[2 * T + 1], refs[2 * T + 2:]
    accumulate(pay_ref, accs, scr[:2], scr[2:4], scr[4:6], *scr[6:])
    own0 = lax.axis_index('cols') * CB
    far0 = CB - own0

    def ghost(off, n):
        high = lax.broadcasted_iota(jnp.int32, (n, LANES), 1) >= HALF
        ends = []
        for g in (0, NG - 1):
            rows = pl.ds(pl.multiple_of(g * CW + off, SUB), n)
            v = accs[0][rows, :]
            for a in accs[1:]:
                v = v + a[rows, :]
            ends.append(v)
        return jnp.where(high, ends[1], ends[0])

    def copy(n, _):
        o = pl.multiple_of(n * QTR, SUB)
        gh_ref[pl.ds(pl.multiple_of(far0 + o, SUB), QTR), :] = ghost(SUB + o, QTR)
        gh_ref[pl.ds(pl.multiple_of(own0 + o, SUB), QTR), :] = a_ref[TILES, pl.ds(pl.multiple_of(SUB + o, SUB), QTR), :]
        return 0

    lax.fori_loop(0, CB // QTR, copy, 0)
    for dst, add in ((own0, ghost(CW - SUB, SUB)), (own0 + CB - SUB, ghost(0, SUB)), (far0, a_ref[TILES, CW - SUB:, :]), (far0 + CB - SUB, a_ref[TILES, :SUB, :])):
        rows = pl.ds(pl.multiple_of(dst, SUB), SUB)
        gh_ref[rows, :] = gh_ref[rows, :] + add

    lane = lax.broadcasted_iota(jnp.int32, (LANES, LANES), 1)
    for side, lane0 in ((0, HALF - HW), (1, HALF)):
        out = jnp.zeros((LANES, LANES), F32)
        for j in range(5):
            piece = pltpu.roll(gh_ref[LANES * j:LANES * (j + 1), :], (HW * j - lane0) % LANES, axis=1)
            out = jnp.where(lane >= HW * j, piece, out)
        pack_ref[side] = out


def image_kernel(*refs):
    accs = refs[:T]
    (a_ref, pack_ref, so_ref, sx_ref, se_ref, d_ref, ev_ref, eu_ref, pm_ref, out_ref,
     tb_ref, edge_ref, g_ref, halo, sm1, sm2, sr1, sr2, hm1, hm2, hr1, hr2, s_main, s_rem, acc_m, acc_r, pieces, recvs, tails, recvs_t,
     halo_ss, halo_rs, swap_ss, swap_rs, red_ss, red_rs) = refs[T:]
    k = lax.axis_index('cols')
    r = lax.axis_index('rows')
    core, x = r % 2, r // 2
    near = r + 1 - 2 * core
    across = (r + 2) % 4
    prev, nxt = (r + 3) % 4, (r + 1) % 4
    homes = ({'rows': across, 'cols': 1 - k}, {'rows': across}, {'cols': 1 - k})

    barrier = pltpu.get_barrier_semaphore()
    for dev in ({'rows': prev}, {'rows': nxt}) + homes:
        pl.semaphore_signal(barrier, inc=1, device_id=dev, device_id_type=MESH_ID)

    own0 = k * CB
    far0 = CB - own0
    high16 = lax.broadcasted_iota(jnp.int32, (WIN, LANES), 1) >= HALF

    def put(v, tiles):
        rows = pl.ds(pl.multiple_of(v, WIN), WIN)
        for p in range(TILES):
            tb_ref[p, rows, :] = tiles[p].astype(BF)
        edge_ref[rows, :] = jnp.where(high16, tiles[0], tiles[9])

    def far_part(n, _):
        put(far0 + WIN * n, folded(accs, pl.multiple_of(SUB + WIN * n, SUB), WIN))
        return 0

    def own_part(n, _):
        put(own0 + WIN * n, [a_ref[p, pl.ds(pl.multiple_of(SUB + WIN * n, SUB), WIN), :] for p in range(TILES)])
        return 0

    last = CB // WIN - 1
    lax.fori_loop(1, last, far_part, 0)
    pl.semaphore_wait(barrier, 5)

    def remote(src, dst, ss, rs, i, dev):
        cp = pltpu.make_async_remote_copy(src_ref=src, dst_ref=dst, send_sem=ss.at[i], recv_sem=rs.at[i], device_id=dev, device_id_type=MESH_ID)
        cp.start()
        return cp

    halos = [remote(pack_ref.at[i], halo.at[i], halo_ss, halo_rs, i, {'rows': dev}) for i, dev in ((0, prev), (1, nxt))]

    lax.fori_loop(1, last, own_part, 0)
    none = jnp.zeros((SUB, LANES), F32)
    for n, side in ((0, CW - SUB), (last, 0)):
        off = SUB + WIN * n
        near_tiles = folded(accs, off, WIN)
        far_ends = folded(accs, side, SUB)
        order = (lambda v: [v, none]) if n == 0 else (lambda v: [none, v])
        put(far0 + WIN * n, [near_tiles[p] + jnp.concatenate(order(a_ref[p, side:side + SUB, :]), axis=0) for p in range(TILES)])
        put(own0 + WIN * n, [a_ref[p, off:off + WIN, :] + jnp.concatenate(order(far_ends[p]), axis=0) for p in range(TILES)])


    def to_rows(row0, n, t0, t1):
        a = jnp.concatenate([t0, t1], axis=1)
        g = lax.dot_general(pm_ref[...], a, (((1,), (1,)), ((), ())), preferred_element_type=F32).astype(BF)
        for ch in range(SUB):
            i, c = ch // 4, ch % 4
            g_ref[row0 + n * c:row0 + n * c + QTR, N_GRID * i:N_GRID * (i + 1)] = g[QTR * ch:QTR * (ch + 1), :]

    for m in range(4):
        to_rows(QTR * m, LANES, tb_ref[2 * m + 1], tb_ref[2 * m + 2])

    sms, srs, hms, hrs = (sm1, sm2), (sr1, sr2), (hm1, hm2), (hr1, hr2)
    swaps, trades = [], []

    def columns(grp):
        start, n = GROUPS[grp]
        lane = lax.broadcasted_iota(jnp.int32, (n, LANES), 1)
        side = lane >> 6
        own_even, far_even = side == core, side != core
        block = (lane & (HALF - 1)) >> 4
        h = jnp.dot(g_ref[4 * start:4 * (start + n), :], ev_ref[...], preferred_element_type=F32)
        hc = [h[n * c:n * (c + 1)] for c in range(4)]
        rems = [v[:, 4 * LANES:] for v in hc]
        for cp in range(2):
            hs = [[v[:, LANES * i:LANES * (i + 1)] for i in range(4)] for v in hc[2 * cp:2 * cp + 2]]
            for i in range(4):
                dp, t = i // 2, i % 2
                odd = pltpu.roll(hs[1][i], HALF, axis=1)
                sms[grp][dp, cp, t] = jnp.where(far_even, hs[0][i], odd).astype(BF)
                hms[grp][dp, cp, t, core] = jnp.where(own_even, hs[0][i], odd).astype(BF)
        for d in range(ROWS):
            out = rems[d]
            for c in range(4):
                if c != d:
                    out = jnp.where(block == c, pltpu.roll(rems[c], (WIN * (c - d)) % LANES, axis=1), out)
            srs[grp][d] = out.astype(BF)
        hrs[grp][r] = srs[grp][r]
        swaps.append(remote(sms[grp], hms[grp].at[:, :, :, core], swap_ss, swap_rs, grp, {'rows': near}))
        for i, dev in enumerate((across, 3 - r, near)):
            trades.append(remote(srs[grp].at[dev], hrs[grp].at[r], swap_ss, swap_rs, 2 + 3 * grp + i, {'rows': dev}))

    columns(0)

    def turn(rows):
        t = [rows[:, LANES * i:LANES * (i + 1)].T for i in range(5)]
        return [jnp.concatenate([t[2 * i], t[2 * i + 1], t[4][HALF * i:HALF * (i + 1)]], axis=0) for i in range(2)]


    def turn_main(j, ref):
        for cp in range(2):
            s_main[j, 0, cp], s_main[j, 1, cp] = turn(jnp.concatenate([ref[2 * cp + core], ref[2 * cp + 1 - core]], axis=0))

    s_rem[0], s_rem[1] = turn(jnp.concatenate([se_ref[c] for c in range(4)] + [jnp.zeros((HALF, N_GRID), F32)], axis=0))

    for h in halos:
        h.wait()
    lane = lax.broadcasted_iota(jnp.int32, (LANES, LANES), 1)
    low = lane < HALF
    t0s, t9s = [], []
    for j in range(5):
        rows = slice(LANES * j, LANES * (j + 1))
        add_first = pltpu.roll(halo[1], (HALF - HW * j) % LANES, axis=1)
        add_last = pltpu.roll(halo[0], (HALF - HW - HW * j) % LANES, axis=1)
        e = edge_ref[rows, :] + jnp.where(low, jnp.where(lane >= HALF - HW, add_last, 0.0), jnp.where(lane < HALF + HW, add_first, 0.0))
        t0s.append(jnp.where(low, tb_ref[0, rows, :].astype(F32), e).astype(BF))
        t9s.append(jnp.where(low, e, tb_ref[9, rows, :].astype(F32)).astype(BF))
    lane = lax.broadcasted_iota(jnp.int32, (PB, LANES), 1)
    low = lane < HALF
    to_rows(4 * LANES, QTR, jnp.concatenate(t0s, axis=0), jnp.concatenate(t9s, axis=0))
    columns(1)

    for cp in swaps[:1]:
        cp.wait_recv()
    n0 = 4 * GROUPS[0][1]

    def block_of(grp, j):
        return jnp.concatenate([hms[grp][(x + j) % 2, cp].reshape(4 * GROUPS[grp][1], LANES) for cp in range(2)], axis=1)

    def ends_of(grp, c):
        v = hrs[grp][2 * c:2 * c + 2].reshape(2 * GROUPS[grp][1], LANES)
        return jnp.concatenate([v, pltpu.roll(v.astype(F32), HALF, axis=1).astype(BF)], axis=0)

    for j in (1, 0):
        acc_m[j] = jnp.dot(eu_ref[x, :, :n0], block_of(0, j), preferred_element_type=F32)
    turn_main(1, sx_ref)
    turn_main(0, so_ref)

    for cp in swaps[1:]:
        cp.wait_recv()

    def rows_dft(half, acc, rhs):
        rows = pl.ds(pl.multiple_of(half * N_IMG, WIN), N_IMG)
        total = acc[rows, :] + jnp.dot(eu_ref[x, rows, n0:], rhs, preferred_element_type=F32)
        return total[:PB], total[PB:]

    quarter = lax.broadcasted_iota(jnp.int32, (PB // 4, LANES), 1) >> 5

    def piece(half, j):
        i_re, i_im = rows_dft(half, acc_m.at[j], block_of(1, j))
        rows = pl.ds(pl.multiple_of(half * PB, SUB), PB)
        re, im = None, None
        for cp in range(2):
            cols = slice(LANES * cp, LANES * (cp + 1))
            s_re, s_im = s_main[j, 0, cp, rows, :], s_main[j, 1, cp, rows, :]
            a = s_re * i_re[:, cols] + s_im * i_im[:, cols]
            b = s_re * i_im[:, cols] - s_im * i_re[:, cols]
            re, im = (a, b) if re is None else (re + a, im + b)
        return jnp.where(low, re + pltpu.roll(re, HALF, axis=1), im + pltpu.roll(im, HALF, axis=1))

    def rest(half):
        i_re, i_im = (acc_r[pl.ds(pl.multiple_of(half * N_IMG + PB * o, WIN), PB), :] for o in range(2))
        rows = pl.ds(pl.multiple_of(half * PB, SUB), PB)
        s_re, s_im = s_rem[0, rows, :], s_rem[1, rows, :]
        w = s_re * i_re + s_im * i_im + pltpu.roll(s_re * i_im - s_im * i_re, HALF, axis=1)
        w = w + pltpu.roll(w, LANES - QTR, axis=1)
        w = w + pltpu.roll(w, LANES - WIN, axis=1)
        w = jnp.where(lane < WIN, w, pltpu.roll(w, LANES - HALF + WIN, axis=1))
        out = w[:PB // 4]
        for g in range(1, 4):
            out = jnp.where(quarter == g, pltpu.roll(w[PB // 4 * g:PB // 4 * (g + 1)], QTR * g, axis=1), out)
        return out

    first, other = pl.ds(0, HALF), pl.ds(HALF, PB - HALF)
    pieces[0] = piece(1 - k, 1)
    joined = remote(pieces.at[0, first], recvs.at[0, first], red_ss, red_rs, 0, homes[1])
    sends = [remote(pieces.at[0, other], recvs.at[0, other], red_ss, red_rs, 1, homes[0])]
    pieces[1] = piece(k, 1)
    sends.append(remote(pieces.at[1], recvs.at[1], red_ss, red_rs, 2, homes[1]))
    across_y = piece(1 - k, 0)
    pieces[2, HALF:] = across_y[HALF:]
    sends.append(remote(pieces.at[2, other], recvs.at[2, other], red_ss, red_rs, 4, homes[2]))
    for cp in trades[:3]:
        cp.wait_recv()
    acc_r[...] = sum(jnp.dot(eu_ref[c, :, :n0], ends_of(0, c), preferred_element_type=F32) for c in range(2))
    for cp in trades[3:]:
        cp.wait_recv()
    acc_r[...] += jnp.dot(jnp.concatenate([eu_ref[c, :, n0:] for c in range(2)], axis=1), jnp.concatenate([ends_of(1, c) for c in range(2)], axis=0), preferred_element_type=F32)
    tails[...] = rest(1 - k)
    tail = remote(tails, recvs_t, red_ss, red_rs, 3, homes[2])
    rem = rest(k)
    joined.wait_recv()
    pieces[2, :HALF] = across_y[:HALF] + recvs[0, :HALF]
    sends.append(remote(pieces.at[2, first], recvs.at[2, first], red_ss, red_rs, 5, homes[2]))
    main = piece(k, 0)
    d8 = jnp.broadcast_to(jnp.concatenate([d_ref[...][None, :], jnp.zeros((1, HALF), F32)], axis=1), (SUB, N_IMG + HALF))
    dq = d8
    for j in range(1, ROWS):
        dq = jnp.where(r == j, pltpu.roll(d8, N_IMG + HALF - QB * j, axis=1), dq)
    dp = jnp.where(k == 0, d8, pltpu.roll(d8, N_IMG + HALF - PB, axis=1))[:, :2 * LANES]
    dd = jnp.concatenate([dp] * WIN, axis=0).T[:PB] * dq[:1, :LANES]

    for cp in sends:
        cp.wait_recv()
    main = main + recvs[1] + recvs[2]
    main = jnp.concatenate([main[:HALF], main[HALF:] + recvs[0, HALF:]], axis=0)
    tail.wait_recv()
    rem = rem + recvs_t[...]
    for o in range(2):
        m = pltpu.roll(main, HALF, axis=1) if o else main
        for j in range(4):
            rows = slice(PB // 4 * j, PB // 4 * (j + 1))
            end = pltpu.roll(rem, (HALF - QTR * j - WIN * o) % LANES, axis=1)
            out_ref[o, rows, :] = (jnp.where(low[rows], m[rows], end) * dd[rows])[:, :QB]

    for cp in sends + swaps + trades + [tail, joined]:
        cp.wait_send()


def solution(mesh):
    sample_spec = ('exam', 'rows', 'cols')
    vm = pl.BlockSpec(memory_space=pltpu.VMEM)
    hbm = pl.BlockSpec(memory_space=pltpu.HBM)
    spread_scratch = ([VMEM((LANES, LANES), F32)] * 4 + [VMEM((LANES * PS, LANES), F32)] * 2
                      + [VMEM((LANES, WIDE * 3), BF), VMEM((NB, LANES), jnp.int32), pltpu.SMEM((NB, LANES), jnp.int32), pltpu.SemaphoreType.DMA])
    acc_shape = [jax.ShapeDtypeStruct((NG * CW, LANES), F32)] * T
    big = 6 * MIB

    def local_fn(kspace, wts_y, wts_x, idx_y, idx_x, coil_maps, deapod):
        own, far, maps, maps_end = pl.pallas_call(
            prep_kernel,
            out_shape=[jax.ShapeDtypeStruct((PAY * NB, LANES), F32)] * 2 + [jax.ShapeDtypeStruct((4, n, N_GRID), F32) for n in (HALF, WIN)],
            in_specs=[hbm] * 6, out_specs=[vm] * 4, name='prep',
            scratch_shapes=[VMEM((2, SUB, NS), F32), VMEM((KW, NS), F32), VMEM((KW, NS), F32), VMEM((NB, LANES), jnp.int32), VMEM((NB, LANES), jnp.int32), VMEM((2, 4, QB, N_IMG), F32), pltpu.SemaphoreType.DMA((6,))],
            compiler_params=pltpu.CompilerParams(vmem_limit_bytes=SUB * MIB),
        )(*[pltpu.with_memory_space_constraint(v, pltpu.HBM) for v in (kspace, wts_y, wts_x, idx_y.reshape(NB, LANES), idx_x.reshape(NB, LANES), jnp.swapaxes(coil_maps, 2, 3))])
        far_in = lax.ppermute(far, 'cols', [(0, 1), (1, 0)])
        half, *accs = pl.pallas_call(
            own_kernel, out_shape=[jax.ShapeDtypeStruct((11, CW, LANES), F32)] + acc_shape, in_specs=[vm], out_specs=[vm] * (T + 1),
            scratch_shapes=spread_scratch, compiler_params=pltpu.CompilerParams(vmem_limit_bytes=big), name='spread_own',
            cost_estimate=pl.CostEstimate(flops=GIGA, bytes_accessed=4 * MIB, transcendentals=0),
        )(own)
        *accs, pack = pl.pallas_call(
            far_kernel, out_shape=acc_shape + [jax.ShapeDtypeStruct((2, LANES, LANES), F32)],
            in_specs=[vm] * (T + 2), out_specs=[vm] * (T + 1), scratch_shapes=[VMEM((N_GRID, LANES), F32)] + spread_scratch,
            input_output_aliases={i + 2: i for i in range(T)},
            compiler_params=pltpu.CompilerParams(vmem_limit_bytes=big), name='spread_far',
            cost_estimate=pl.CostEstimate(flops=GIGA, bytes_accessed=4 * MIB, transcendentals=0),
        )(far_in, half, *accs)
        maps_x = lax.ppermute(maps, 'rows', [(i, (i + 2) % ROWS) for i in range(ROWS)])
        dma = pltpu.SemaphoreType.DMA
        half_bufs = [VMEM((2, 2, 2, n, LANES), BF) for _, n in GROUPS] + [VMEM((ROWS, n, LANES), BF) for _, n in GROUPS]
        full_bufs = [VMEM((2, 2, 2, 2, n, LANES), BF) for _, n in GROUPS] + [VMEM((ROWS, n, LANES), BF) for _, n in GROUPS]
        return pl.pallas_call(
            image_kernel,
            out_shape=jax.ShapeDtypeStruct((2, PB, QB), F32), in_specs=[vm] * (T + 9), out_specs=vm,
            scratch_shapes=[VMEM((TILES, N_GRID, LANES), BF), VMEM((N_GRID, LANES), F32), VMEM((4 * RB, 2 * N_GRID), BF), VMEM((2, LANES, LANES), F32)] + half_bufs + full_bufs + [
                VMEM((2, 2, 2, N_IMG, LANES), F32), VMEM((2, N_IMG, LANES), F32),
                VMEM((2, 2 * N_IMG, 2 * LANES), F32), VMEM((2 * N_IMG, LANES), F32),
                VMEM((3, PB, LANES), F32), VMEM((3, PB, LANES), F32), VMEM((PB // 4, LANES), F32), VMEM((PB // 4, LANES), F32),
                dma((2,)), dma((2,)), dma((8,)), dma((8,)), dma((6,)), dma((6,)),
            ],
            compiler_params=pltpu.CompilerParams(vmem_limit_bytes=11 * MIB, collective_id=0, has_side_effects=True), name='image',
        )(*accs, half, pack, maps, maps_x, maps_end, deapod, col_dft(), row_dft(), unmix())

    return jax.shard_map(
        local_fn,
        mesh=mesh,
        in_specs=(P(None, None, sample_spec), P(None, sample_spec), P(None, sample_spec), P(sample_spec), P(sample_spec), P(None, ('exam', 'cols'), None, 'rows'), P()),
        out_specs=P(None, ('exam', 'cols'), 'rows'),
        check_vma=False,
    )
```

```python
import functools
import math

import jax
import jax.numpy as jnp
import numpy as np
from jax import lax
from jax.experimental import pallas as pl
from jax.experimental.pallas import tpu as pltpu
from jax.sharding import PartitionSpec as P

BF = jnp.bfloat16
F32 = jnp.float32
VMEM = pltpu.VMEM
LANES = 128
MIB = 1 << 20
GIGA = 4000 * MIB
TILES = 10
SUB, WIN, QTR, HALF, WIDE = 8, 16, 32, 64, 256
N_GRID, N_IMG, N_COILS, KW = 640, 320, 8, 6
ROWS, COLS = 4, 2
RB, CB, QB = N_GRID // ROWS, N_GRID // COLS, N_IMG // ROWS
PB = N_IMG // COLS
NS = 4096
NB = NS // LANES
STEP = 11
NG = 15
CW = CB + WIN
T = 7
PS = 9
PAY = 21
CODE = 512
MAPS = 240
HW = 24
ORDER = tuple(range(1, 9)) + (0, 9)
GROUPS = ((0, 128), (128, 32))
MESH_ID = pl.DeviceIdType.MESH


def dft_parts():
    freq = np.arange(N_GRID) - N_GRID // 2
    pos = np.arange(N_IMG) - N_IMG // 2
    ang = ((freq[:, None] * pos[None, :]) % N_GRID).astype(np.float32) * np.float32(2.0 * math.pi / N_GRID)
    norm = np.float32(1.0 / math.sqrt(N_GRID))
    c, s = np.cos(ang) * norm, np.sin(ang) * norm
    return np.stack([np.stack([c, s], 1), np.stack([-s, c], 1)], 0)


def col_dft():
    e = dft_parts()
    out = np.zeros((2 * N_GRID, N_GRID), np.float32)
    for dp in range(2):
        for t in range(2):
            for h in range(2):
                q0 = QB * (2 * dp + h)
                l0 = LANES * (2 * dp + t) + HALF * h
                out[:, l0:l0 + HALF] = e[:, :, t, q0:q0 + HALF].reshape(2 * N_GRID, HALF)
    for t in range(2):
        for d in range(4):
            l0 = 4 * LANES + HALF * t + WIN * d
            out[:, l0:l0 + WIN] = e[:, :, t, QB * d + HALF:QB * (d + 1)].reshape(2 * N_GRID, WIN)
    return jnp.asarray(out, BF)


def row_dft():
    e = dft_parts()
    rows = np.concatenate([np.arange(WIN * l, WIN * (l + 1)) for l in ORDER])
    chips = []
    for x in range(2):
        parts = []
        for start, n in GROUPS:
            for t in range(2):
                for b in range(2):
                    parts.append(e[t, (2 * x + b) * RB + rows[start:start + n]])
        m = np.concatenate(parts, 0)
        chips.append(np.concatenate([m[:, :, PB * h:PB * (h + 1)].reshape(N_GRID, N_IMG).T for h in range(2)], 0))
    return jnp.asarray(np.array(chips), BF)


def unmix():
    m = np.zeros((WIDE, WIDE), np.float32)
    for ch in range(SUB):
        for pp in range(2):
            for i in range(WIN):
                m[ch * QTR + WIN * pp + (i + SUB) % WIN, pp * 128 + i * SUB + ch] = 1.0
    return jnp.asarray(m, BF)


def prep_kernel(ks_hbm, wy_hbm, wx_hbm, iy_hbm, ix_hbm, maps_hbm, own_ref, far_ref, sp_ref, sq_ref, sm_ref, ks_ref, wy_ref, wx_ref, iy_ref, ix_ref, maps_ref, sem):
    k = lax.axis_index('cols')
    r = lax.axis_index('rows')
    loads = []
    for src, dst in ((iy_hbm, iy_ref), (ix_hbm, ix_ref), (wx_hbm, wx_ref), (wy_hbm, wy_ref), (ks_hbm, ks_ref), (maps_hbm.at[:, :, :, WIDE:], maps_ref)):
        cp = pltpu.make_async_copy(src, dst, sem.at[len(loads)])
        cp.start()
        loads.append(cp)
    parts = []
    for c in range(4):
        n = min(HALF, MAPS - HALF * c)
        parts += [(sp_ref.at[pl.ds(HALF * c, n)], c, pl.ds(0, n)), (sq_ref.at[c], c, pl.ds(HALF, WIN))]
    parts.append((sm_ref, 3, pl.ds(HALF - WIN, WIN)))
    for ref, c, q in parts:
        for i in range(2):
            cp = pltpu.make_async_copy(maps_hbm.at[i, c, q, pl.ds(0, WIDE)], ref.at[:, pl.ds(WIDE * i, WIDE)], sem.at[len(loads)])
            cp.start()
            loads.append(cp)
    loads[0].wait()
    loads[1].wait()
    iy = iy_ref[...]
    code = ((iy - r * RB + 5) * CODE + ix_ref[...] - k * CB + 5).astype(F32)
    for i in range(2, 5):
        loads[i].wait()
    lo = jnp.concatenate([ks_ref[0, 0:4, :], ks_ref[1, 0:4, :]], axis=0)
    hi = jnp.concatenate([ks_ref[0, 4:SUB, :], ks_ref[1, 4:SUB, :]], axis=0)
    first = k == 0
    for ref, y in ((own_ref, jnp.where(first, lo, hi)), (far_ref, jnp.where(first, hi, lo))):
        for b in range(NB):
            cols = slice(LANES * b, LANES * (b + 1))
            ref[PAY * b:PAY * b + SUB, :] = y[:, cols]
            ref[PAY * b + SUB:PAY * b + SUB + KW, :] = wx_ref[:, cols]
            ref[PAY * (b + 1) - KW - 1:PAY * (b + 1) - 1, :] = wy_ref[:, cols]
            ref[PAY * (b + 1) - 1:PAY * (b + 1), :] = code[b:b + 1, :]
    loads[5].wait()
    for c in range(4):
        end = jnp.concatenate([maps_ref[i, c] for i in range(2)], axis=1)
        n = min(HALF, MAPS - HALF * c)
        sp_ref[HALF * c:HALF * c + n, 2 * WIDE:] = end[:n]
        sq_ref[c, :, 2 * WIDE:] = end[HALF:]
        if n < HALF:
            sm_ref[:, 2 * WIDE:] = end[n:HALF]
    for cp in loads[KW:]:
        cp.wait()


def split3(x):
    hi = x.astype(BF).astype(F32)
    r = x - hi
    mid = r.astype(BF).astype(F32)
    return hi, mid, r - mid


def accumulate(pay_ref, accs, us, xs, vs, r_ref, int_ref, base_ref, sem):
    row_i = lax.broadcasted_iota(jnp.int32, (WIN, LANES), 0)

    def make_u(blk, k):
        off = jnp.minimum(blk, NB - 1) * PAY
        y8 = pay_ref[pl.ds(off, SUB), :]
        wx = pay_ref[pl.ds(off + SUB, SUB), :]
        wyp = pay_ref[pl.ds(off + PAY - SUB, SUB), :]
        d = (row_i - (wyp[7:, :].astype(jnp.int32) // CODE)) & (WIN - 1)
        p = jnp.zeros((WIN, LANES), F32)
        for a in range(KW):
            p = jnp.where(d == a, wyp[a + 1:a + 2, :], p)
        us[k][...] = jnp.concatenate([y8 * p[i:i + 1, :] for i in range(WIN)], axis=0).T
        x3 = list(split3(wx)) + [jnp.zeros((LANES - HW, LANES), F32)]
        xs[k][...] = jnp.concatenate(x3, axis=0).T

    def make_v(k):
        lhs = xs[k][...].astype(BF)
        u = us[k][...]
        for bp in range(3):
            w = jnp.dot(lhs, r_ref[:, WIDE * bp:WIDE * bp + WIDE], preferred_element_type=F32)
            for c in range(2):
                v = w[:, LANES * c:LANES * (c + 1)] * u
                for g in range(WIN):
                    vs[k][pl.ds(SUB * PS * g + 2 * bp + c, SUB, stride=PS), :] = v[SUB * g:SUB * g + SUB, :]

    def add_tiles(blk, k):
        row = base_ref.at[blk]
        for j in range(LANES):
            acc = accs[j % T]
            b = row[j]
            acc[pl.ds(b, SUB), :] = acc[pl.ds(b, SUB), :] + vs[k][PS * j:PS * j + SUB, :]

    code = jnp.concatenate([pay_ref[PAY * (b + 1) - 1:PAY * (b + 1), :] for b in range(NB)], axis=0).astype(jnp.int32)
    int_ref[...] = (((code // CODE - 5) * 187) >> STEP) * CW + (code & (CODE - 1))
    kk = lax.broadcasted_iota(jnp.int32, (LANES, WIDE * 3), 0)
    ll = lax.broadcasted_iota(jnp.int32, (LANES, WIDE * 3), 1)
    r_ref[...] = jnp.where((kk < HW) & ((kk & 7) == (ll >> 7)), 1.0, 0.0).astype(BF)
    for v in vs:
        v[...] = jnp.zeros_like(v)
    load = pltpu.make_async_copy(int_ref, base_ref, sem)
    load.start()
    make_u(0, 0)
    make_u(1, 1)
    make_v(0)
    load.wait()

    def body(n, _):
        k = 2 * n
        make_v(1)
        add_tiles(k, 0)
        make_u(k + 2, 0)
        make_v(0)
        add_tiles(k + 1, 1)
        make_u(k + 3, 1)
        return 0

    lax.fori_loop(0, NB // 2, body, 0)


def folded(accs, off, n, clear=False):
    def total(g):
        rows = pl.ds(pl.multiple_of(g * CW + off, SUB), n)
        v = accs[0][rows, :]
        for a in accs[1:]:
            v = v + a[rows, :]
        if clear:
            for a in accs:
                a[rows, :] = jnp.zeros((n, LANES), F32)
        return v

    row = lax.broadcasted_iota(jnp.int32, (n, LANES), 1) >> 3
    tiles = [None] * TILES
    for g in range(NG):
        v = total(g)
        if g == 0:
            ghost = v
        first = 5 + STEP * g
        for p in range(TILES):
            lo, hi = max(first, SUB + WIN * p), min(first + WIN, SUB + WIN * (p + 1))
            if lo < hi:
                part = jnp.where((row - lo & (WIN - 1)) < hi - lo, v, 0.0)
                tiles[p] = part if tiles[p] is None else tiles[p] + part
    return tiles + [jnp.where(row >= SUB, v, ghost)]


def own_kernel(pay_ref, out_ref, *refs):
    accs, scr = refs[:T], refs[T:]

    def clear(n, _):
        for a in accs:
            a[pl.ds(pl.multiple_of(n * CW, SUB), CW), :] = jnp.zeros((CW, LANES), F32)
        return 0

    lax.fori_loop(0, NG, clear, 0)
    accumulate(pay_ref, accs, scr[:2], scr[2:4], scr[4:6], *scr[6:])

    def fold(q, _):
        off = pl.multiple_of(q * WIN, WIN)
        for p, t in enumerate(folded(accs, off, WIN, clear=True)):
            out_ref[p, pl.ds(off, WIN), :] = t
        return 0

    lax.fori_loop(0, CW // WIN, fold, 0)


def far_kernel(pay_ref, a_ref, *refs):
    accs, pack_ref, gh_ref, scr = refs[T:2 * T], refs[2 * T], refs[2 * T + 1], refs[2 * T + 2:]
    accumulate(pay_ref, accs, scr[:2], scr[2:4], scr[4:6], *scr[6:])
    own0 = lax.axis_index('cols') * CB
    far0 = CB - own0

    def ghost(off, n):
        high = lax.broadcasted_iota(jnp.int32, (n, LANES), 1) >= HALF
        ends = []
        for g in (0, NG - 1):
            rows = pl.ds(pl.multiple_of(g * CW + off, SUB), n)
            v = accs[0][rows, :]
            for a in accs[1:]:
                v = v + a[rows, :]
            ends.append(v)
        return jnp.where(high, ends[1], ends[0])

    def copy(n, _):
        o = pl.multiple_of(n * QTR, SUB)
        gh_ref[pl.ds(pl.multiple_of(far0 + o, SUB), QTR), :] = ghost(SUB + o, QTR)
        gh_ref[pl.ds(pl.multiple_of(own0 + o, SUB), QTR), :] = a_ref[TILES, pl.ds(pl.multiple_of(SUB + o, SUB), QTR), :]
        return 0

    lax.fori_loop(0, CB // QTR, copy, 0)
    for dst, add in ((own0, ghost(CW - SUB, SUB)), (own0 + CB - SUB, ghost(0, SUB)), (far0, a_ref[TILES, CW - SUB:, :]), (far0 + CB - SUB, a_ref[TILES, :SUB, :])):
        rows = pl.ds(pl.multiple_of(dst, SUB), SUB)
        gh_ref[rows, :] = gh_ref[rows, :] + add

    lane = lax.broadcasted_iota(jnp.int32, (LANES, LANES), 1)
    for side, lane0 in ((0, HALF - HW), (1, HALF)):
        out = jnp.zeros((LANES, LANES), F32)
        for j in range(5):
            piece = pltpu.roll(gh_ref[LANES * j:LANES * (j + 1), :], (HW * j - lane0) % LANES, axis=1)
            out = jnp.where(lane >= HW * j, piece, out)
        pack_ref[side] = out


def image_kernel(*refs):
    accs = refs[:T]
    (a_ref, pack_ref, so_ref, sx_ref, sm_ref, se_ref, d_ref, ev_ref, eu_ref, pm_ref, out_ref,
     tb_ref, edge_ref, g_ref, halo, sm1, sm2, sr1, sr2, hm1, hm2, hr1, hr2, s_main, s_rem, acc_m, acc_r, sx_mid, pieces, recvs, tails, recvs_t,
     halo_ss, halo_rs, swap_ss, swap_rs, red_ss, red_rs) = refs[T:]
    k = lax.axis_index('cols')
    r = lax.axis_index('rows')
    core, x = r % 2, r // 2
    near = r + 1 - 2 * core
    across = (r + 2) % 4
    prev, nxt = (r + 3) % 4, (r + 1) % 4
    homes = ({'rows': across, 'cols': 1 - k}, {'rows': across}, {'cols': 1 - k})

    barrier = pltpu.get_barrier_semaphore()
    for dev in ({'rows': prev}, {'rows': nxt}) + homes:
        pl.semaphore_signal(barrier, inc=1, device_id=dev, device_id_type=MESH_ID)

    own0 = k * CB
    far0 = CB - own0
    high16 = lax.broadcasted_iota(jnp.int32, (WIN, LANES), 1) >= HALF

    def put(v, tiles):
        rows = pl.ds(pl.multiple_of(v, WIN), WIN)
        for p in range(TILES):
            tb_ref[p, rows, :] = tiles[p].astype(BF)
        edge_ref[rows, :] = jnp.where(high16, tiles[0], tiles[9])

    def far_part(n, _):
        put(far0 + WIN * n, folded(accs, pl.multiple_of(SUB + WIN * n, SUB), WIN))
        return 0

    def own_part(n, _):
        put(own0 + WIN * n, [a_ref[p, pl.ds(pl.multiple_of(SUB + WIN * n, SUB), WIN), :] for p in range(TILES)])
        return 0

    last = CB // WIN - 1
    lax.fori_loop(1, last, far_part, 0)
    pl.semaphore_wait(barrier, 5)

    def remote(src, dst, ss, rs, i, dev):
        cp = pltpu.make_async_remote_copy(src_ref=src, dst_ref=dst, send_sem=ss.at[i], recv_sem=rs.at[i], device_id=dev, device_id_type=MESH_ID)
        cp.start()
        return cp

    halos = [remote(pack_ref.at[i], halo.at[i], halo_ss, halo_rs, i, {'rows': dev}) for i, dev in ((0, prev), (1, nxt))]

    lax.fori_loop(1, last, own_part, 0)
    none = jnp.zeros((SUB, LANES), F32)
    for n, side in ((0, CW - SUB), (last, 0)):
        off = SUB + WIN * n
        near_tiles = folded(accs, off, WIN)
        far_ends = folded(accs, side, SUB)
        order = (lambda v: [v, none]) if n == 0 else (lambda v: [none, v])
        put(far0 + WIN * n, [near_tiles[p] + jnp.concatenate(order(a_ref[p, side:side + SUB, :]), axis=0) for p in range(TILES)])
        put(own0 + WIN * n, [a_ref[p, off:off + WIN, :] + jnp.concatenate(order(far_ends[p]), axis=0) for p in range(TILES)])


    def to_rows(row0, n, t0, t1):
        a = jnp.concatenate([t0, t1], axis=1)
        g = lax.dot_general(pm_ref[...], a, (((1,), (1,)), ((), ())), preferred_element_type=F32).astype(BF)
        for ch in range(SUB):
            i, c = ch // 4, ch % 4
            g_ref[row0 + n * c:row0 + n * c + QTR, N_GRID * i:N_GRID * (i + 1)] = g[QTR * ch:QTR * (ch + 1), :]

    for m in range(4):
        to_rows(QTR * m, LANES, tb_ref[2 * m + 1], tb_ref[2 * m + 2])

    mid = remote(sm_ref, sx_mid, halo_ss, halo_rs, 2, {'rows': across})

    sms, srs, hms, hrs = (sm1, sm2), (sr1, sr2), (hm1, hm2), (hr1, hr2)
    swaps, trades = [], []

    def columns(grp):
        start, n = GROUPS[grp]
        lane = lax.broadcasted_iota(jnp.int32, (n, LANES), 1)
        side = lane >> 6
        own_even, far_even = side == core, side != core
        block = (lane & (HALF - 1)) >> 4
        h = jnp.dot(g_ref[4 * start:4 * (start + n), :], ev_ref[...], preferred_element_type=F32)
        hc = [h[n * c:n * (c + 1)] for c in range(4)]
        rems = [v[:, 4 * LANES:] for v in hc]
        for cp in range(2):
            hs = [[v[:, LANES * i:LANES * (i + 1)] for i in range(4)] for v in hc[2 * cp:2 * cp + 2]]
            for i in range(4):
                dp, t = i // 2, i % 2
                odd = pltpu.roll(hs[1][i], HALF, axis=1)
                sms[grp][dp, cp, t] = jnp.where(far_even, hs[0][i], odd).astype(BF)
                hms[grp][dp, cp, t, core] = jnp.where(own_even, hs[0][i], odd).astype(BF)
        for d in range(ROWS):
            out = rems[d]
            for c in range(4):
                if c != d:
                    out = jnp.where(block == c, pltpu.roll(rems[c], (WIN * (c - d)) % LANES, axis=1), out)
            srs[grp][d] = out.astype(BF)
        hrs[grp][r] = srs[grp][r]
        swaps.append(remote(sms[grp], hms[grp].at[:, :, :, core], swap_ss, swap_rs, grp, {'rows': near}))
        for i, dev in enumerate((across, 3 - r, near)):
            trades.append(remote(srs[grp].at[dev], hrs[grp].at[r], swap_ss, swap_rs, 2 + 3 * grp + i, {'rows': dev}))

    columns(0)

    for h in halos:
        h.wait()
    lane = lax.broadcasted_iota(jnp.int32, (LANES, LANES), 1)
    low = lane < HALF
    t0s, t9s = [], []
    for j in range(5):
        rows = slice(LANES * j, LANES * (j + 1))
        add_first = pltpu.roll(halo[1], (HALF - HW * j) % LANES, axis=1)
        add_last = pltpu.roll(halo[0], (HALF - HW - HW * j) % LANES, axis=1)
        e = edge_ref[rows, :] + jnp.where(low, jnp.where(lane >= HALF - HW, add_last, 0.0), jnp.where(lane < HALF + HW, add_first, 0.0))
        t0s.append(jnp.where(low, tb_ref[0, rows, :].astype(F32), e).astype(BF))
        t9s.append(jnp.where(low, e, tb_ref[9, rows, :].astype(F32)).astype(BF))
    lane = lax.broadcasted_iota(jnp.int32, (PB, LANES), 1)
    low = lane < HALF
    to_rows(4 * LANES, QTR, jnp.concatenate(t0s, axis=0), jnp.concatenate(t9s, axis=0))
    columns(1)

    def turn(rows):
        t = [rows[:, LANES * i:LANES * (i + 1)].T for i in range(5)]
        return [jnp.concatenate([t[2 * i], t[2 * i + 1], t[4][HALF * i:HALF * (i + 1)]], axis=0) for i in range(2)]


    for cp in swaps[:1]:
        cp.wait_recv()
    n0 = 4 * GROUPS[0][1]

    def block_of(grp, j):
        return jnp.concatenate([hms[grp][(x + j) % 2, cp].reshape(4 * GROUPS[grp][1], LANES) for cp in range(2)], axis=1)

    mid.wait_recv()
    for j, ref, end in ((1, sx_ref, sx_mid), (0, so_ref, sm_ref)):
        c = [ref[HALF * i:HALF * (i + 1), :] for i in range(3)] + [jnp.concatenate([ref[3 * HALF:, :], end[...]], axis=0)]
        acc_m[j] = jnp.dot(eu_ref[x, :, :n0], block_of(0, j), preferred_element_type=F32)
        for cp in range(2):
            s_main[j, 0, cp], s_main[j, 1, cp] = turn(jnp.concatenate([jnp.where(core == 0, c[2 * cp], c[2 * cp + 1]), jnp.where(core == 0, c[2 * cp + 1], c[2 * cp])], axis=0))

    for cp in swaps[1:]:
        cp.wait_recv()

    def rows_dft(half, acc, rhs):
        rows = pl.ds(pl.multiple_of(half * N_IMG, WIN), N_IMG)
        total = acc[rows, :] + jnp.dot(eu_ref[x, rows, n0:], rhs, preferred_element_type=F32)
        return total[:PB], total[PB:]

    quarter = lax.broadcasted_iota(jnp.int32, (PB // 4, LANES), 1) >> 5

    def piece(half, j):
        i_re, i_im = rows_dft(half, acc_m.at[j], block_of(1, j))
        rows = pl.ds(pl.multiple_of(half * PB, SUB), PB)
        re, im = None, None
        for cp in range(2):
            cols = slice(LANES * cp, LANES * (cp + 1))
            s_re, s_im = s_main[j, 0, cp, rows, :], s_main[j, 1, cp, rows, :]
            a = s_re * i_re[:, cols] + s_im * i_im[:, cols]
            b = s_re * i_im[:, cols] - s_im * i_re[:, cols]
            re, im = (a, b) if re is None else (re + a, im + b)
        return jnp.where(low, re + pltpu.roll(re, HALF, axis=1), im + pltpu.roll(im, HALF, axis=1))

    def rest(half):
        parts = []
        for o in range(2):
            rows = pl.ds(pl.multiple_of(half * N_IMG + PB * o, WIN), PB)
            parts.append(acc_r[0, rows, :] + pltpu.roll(acc_r[1, rows, :], HALF, axis=1))
        i_re, i_im = parts
        rows = pl.ds(pl.multiple_of(half * PB, SUB), PB)
        s_re, s_im = s_rem[0, rows, :], s_rem[1, rows, :]
        w = s_re * i_re + s_im * i_im + pltpu.roll(s_re * i_im - s_im * i_re, HALF, axis=1)
        w = w + pltpu.roll(w, LANES - QTR, axis=1)
        w = w + pltpu.roll(w, LANES - WIN, axis=1)
        w = jnp.where(lane < WIN, w, pltpu.roll(w, LANES - HALF + WIN, axis=1))
        out = w[:PB // 4]
        for g in range(1, 4):
            out = jnp.where(quarter == g, pltpu.roll(w[PB // 4 * g:PB // 4 * (g + 1)], QTR * g, axis=1), out)
        return out

    sends = []
    for i, (half, j) in enumerate(((1 - k, 1), (k, 1), (1 - k, 0))):
        pieces[i] = piece(half, j)
        sends.append(remote(pieces.at[i], recvs.at[i], red_ss, red_rs, i, homes[i]))
    for cp in trades:
        cp.wait_recv()
    for t in range(2):
        total = None
        for grp in range(2):
            kk = 2 * GROUPS[grp][1]
            for c in range(2):
                part = jnp.dot(eu_ref[c, :, n0 * grp + kk * t:n0 * grp + kk * (t + 1)], hrs[grp][2 * c:2 * c + 2].reshape(kk, LANES), preferred_element_type=F32)
                total = part if total is None else total + part
        acc_r[t] = total
    s_rem[0], s_rem[1] = turn(jnp.concatenate([se_ref[c] for c in range(4)] + [jnp.zeros((HALF, N_GRID), F32)], axis=0))
    tails[...] = rest(1 - k)
    tail = remote(tails, recvs_t, red_ss, red_rs, 3, homes[2])
    rem = rest(k)
    main = piece(k, 0)
    d8 = jnp.broadcast_to(jnp.concatenate([d_ref[...][None, :], jnp.zeros((1, HALF), F32)], axis=1), (SUB, N_IMG + HALF))
    dq = d8
    for j in range(1, ROWS):
        dq = jnp.where(r == j, pltpu.roll(d8, N_IMG + HALF - QB * j, axis=1), dq)
    dp = jnp.where(k == 0, d8, pltpu.roll(d8, N_IMG + HALF - PB, axis=1))[:, :2 * LANES]
    dd = jnp.concatenate([dp] * WIN, axis=0).T[:PB] * dq[:1, :LANES]

    for i in (2, 0, 1):
        sends[i].wait_recv()
        main = main + recvs[i]
    tail.wait_recv()
    rem = rem + recvs_t[...]
    for o in range(2):
        m = pltpu.roll(main, HALF, axis=1) if o else main
        for j in range(4):
            rows = slice(PB // 4 * j, PB // 4 * (j + 1))
            end = pltpu.roll(rem, (HALF - QTR * j - WIN * o) % LANES, axis=1)
            out_ref[o, rows, :] = (jnp.where(low[rows], m[rows], end) * dd[rows])[:, :QB]

    for cp in sends + swaps + trades + [mid, tail]:
        cp.wait_send()


def solution(mesh):
    sample_spec = ('exam', 'rows', 'cols')
    vm = pl.BlockSpec(memory_space=pltpu.VMEM)
    hbm = pl.BlockSpec(memory_space=pltpu.HBM)
    spread_scratch = ([VMEM((LANES, LANES), F32)] * 4 + [VMEM((LANES * PS, LANES), F32)] * 2
                      + [VMEM((LANES, WIDE * 3), BF), VMEM((NB, LANES), jnp.int32), pltpu.SMEM((NB, LANES), jnp.int32), pltpu.SemaphoreType.DMA])
    acc_shape = [jax.ShapeDtypeStruct((NG * CW, LANES), F32)] * T
    big = 6 * MIB

    def local_fn(kspace, wts_y, wts_x, idx_y, idx_x, coil_maps, deapod):
        own, far, maps, maps_end, maps_mid = pl.pallas_call(
            prep_kernel,
            out_shape=[jax.ShapeDtypeStruct((PAY * NB, LANES), F32)] * 2 + [jax.ShapeDtypeStruct(d, F32) for d in ((MAPS, N_GRID), (4, WIN, N_GRID), (WIN, N_GRID))],
            in_specs=[hbm] * 6, out_specs=[vm] * 5, name='prep',
            scratch_shapes=[VMEM((2, SUB, NS), F32), VMEM((KW, NS), F32), VMEM((KW, NS), F32), VMEM((NB, LANES), jnp.int32), VMEM((NB, LANES), jnp.int32), VMEM((2, 4, QB, HALF), F32), pltpu.SemaphoreType.DMA((24,))],
            compiler_params=pltpu.CompilerParams(vmem_limit_bytes=SUB * MIB),
        )(*[pltpu.with_memory_space_constraint(v, pltpu.HBM) for v in (kspace, wts_y, wts_x, idx_y.reshape(NB, LANES), idx_x.reshape(NB, LANES), jnp.swapaxes(coil_maps, 2, 3))])
        far_in = lax.ppermute(far, 'cols', [(0, 1), (1, 0)])
        half, *accs = pl.pallas_call(
            own_kernel, out_shape=[jax.ShapeDtypeStruct((11, CW, LANES), F32)] + acc_shape, in_specs=[vm], out_specs=[vm] * (T + 1),
            scratch_shapes=spread_scratch, compiler_params=pltpu.CompilerParams(vmem_limit_bytes=big), name='spread_own',
            cost_estimate=pl.CostEstimate(flops=GIGA, bytes_accessed=4 * MIB, transcendentals=0),
        )(own)
        *accs, pack = pl.pallas_call(
            far_kernel, out_shape=acc_shape + [jax.ShapeDtypeStruct((2, LANES, LANES), F32)],
            in_specs=[vm] * (T + 2), out_specs=[vm] * (T + 1), scratch_shapes=[VMEM((N_GRID, LANES), F32)] + spread_scratch,
            input_output_aliases={i + 2: i for i in range(T)},
            compiler_params=pltpu.CompilerParams(vmem_limit_bytes=big), name='spread_far',
            cost_estimate=pl.CostEstimate(flops=GIGA, bytes_accessed=4 * MIB, transcendentals=0),
        )(far_in, half, *accs)
        maps_x = lax.ppermute(maps, 'rows', [(i, (i + 2) % ROWS) for i in range(ROWS)])
        dma = pltpu.SemaphoreType.DMA
        half_bufs = [VMEM((2, 2, 2, n, LANES), BF) for _, n in GROUPS] + [VMEM((ROWS, n, LANES), BF) for _, n in GROUPS]
        full_bufs = [VMEM((2, 2, 2, 2, n, LANES), BF) for _, n in GROUPS] + [VMEM((ROWS, n, LANES), BF) for _, n in GROUPS]
        return pl.pallas_call(
            image_kernel,
            out_shape=jax.ShapeDtypeStruct((2, PB, QB), F32), in_specs=[vm] * (T + TILES), out_specs=vm,
            scratch_shapes=[VMEM((TILES, N_GRID, LANES), BF), VMEM((N_GRID, LANES), F32), VMEM((4 * RB, 2 * N_GRID), BF), VMEM((2, LANES, LANES), F32)] + half_bufs + full_bufs + [
                VMEM((2, 2, 2, N_IMG, LANES), F32), VMEM((2, N_IMG, LANES), F32),
                VMEM((2, 2 * N_IMG, 2 * LANES), F32), VMEM((2, 2 * N_IMG, LANES), F32), VMEM((WIN, N_GRID), F32),
                VMEM((3, PB, LANES), F32), VMEM((3, PB, LANES), F32), VMEM((PB // 4, LANES), F32), VMEM((PB // 4, LANES), F32),
                dma((3,)), dma((3,)), dma((8,)), dma((8,)), dma((4,)), dma((4,)),
            ],
            compiler_params=pltpu.CompilerParams(vmem_limit_bytes=11 * MIB, collective_id=0, has_side_effects=True), name='image',
        )(*accs, half, pack, maps, maps_x, maps_mid, maps_end, deapod, col_dft(), row_dft(), unmix())

    return jax.shard_map(
        local_fn,
        mesh=mesh,
        in_specs=(P(None, None, sample_spec), P(None, sample_spec), P(None, sample_spec), P(sample_spec), P(sample_spec), P(None, ('exam', 'cols'), None, 'rows'), P()),
        out_specs=P(None, ('exam', 'cols'), 'rows'),
        check_vma=False,
    )
```

```python
import functools
import math

import jax
import jax.numpy as jnp
import numpy as np
from jax import lax
from jax.experimental import pallas as pl
from jax.experimental.pallas import tpu as pltpu
from jax.sharding import PartitionSpec as P

BF = jnp.bfloat16
F32 = jnp.float32
VMEM = pltpu.VMEM
LANES = 128
MIB = 1 << 20
GIGA = 4000 * MIB
TILES = 10
SUB, WIN, QTR, HALF, WIDE = 8, 16, 32, 64, 256
N_GRID, N_IMG, N_COILS, KW = 640, 320, 8, 6
ROWS, COLS = 4, 2
RB, CB, QB = N_GRID // ROWS, N_GRID // COLS, N_IMG // ROWS
PB = N_IMG // COLS
NS = 4096
NB = NS // LANES
STEP = 11
NG = 15
CW = CB + WIN
T = 7
PS = 9
PAY = 21
CODE = 512
MAPS = 240
HW = 24
ORDER = tuple(range(1, 9)) + (0, 9)
GROUPS = ((0, 128), (128, 32))
MESH_ID = pl.DeviceIdType.MESH


def dft_parts():
    freq = np.arange(N_GRID) - N_GRID // 2
    pos = np.arange(N_IMG) - N_IMG // 2
    ang = ((freq[:, None] * pos[None, :]) % N_GRID).astype(np.float32) * np.float32(2.0 * math.pi / N_GRID)
    norm = np.float32(1.0 / math.sqrt(N_GRID))
    c, s = np.cos(ang) * norm, np.sin(ang) * norm
    return np.stack([np.stack([c, s], 1), np.stack([-s, c], 1)], 0)


def col_dft():
    e = dft_parts()
    out = np.zeros((2 * N_GRID, N_GRID), np.float32)
    for dp in range(2):
        for t in range(2):
            for h in range(2):
                q0 = QB * (2 * dp + h)
                l0 = LANES * (2 * dp + t) + HALF * h
                out[:, l0:l0 + HALF] = e[:, :, t, q0:q0 + HALF].reshape(2 * N_GRID, HALF)
    for t in range(2):
        for d in range(4):
            l0 = 4 * LANES + HALF * t + WIN * d
            out[:, l0:l0 + WIN] = e[:, :, t, QB * d + HALF:QB * (d + 1)].reshape(2 * N_GRID, WIN)
    return jnp.asarray(out, BF)


def row_dft():
    e = dft_parts()
    rows = np.concatenate([np.arange(WIN * l, WIN * (l + 1)) for l in ORDER])
    chips = []
    for x in range(2):
        parts = []
        for start, n in GROUPS:
            for t in range(2):
                for b in range(2):
                    parts.append(e[t, (2 * x + b) * RB + rows[start:start + n]])
        m = np.concatenate(parts, 0)
        chips.append(np.concatenate([m[:, :, PB * h:PB * (h + 1)].reshape(N_GRID, N_IMG).T for h in range(2)], 0))
    return jnp.asarray(np.array(chips), BF)


def unmix():
    m = np.zeros((WIDE, WIDE), np.float32)
    for ch in range(SUB):
        for pp in range(2):
            for i in range(WIN):
                m[ch * QTR + WIN * pp + (i + SUB) % WIN, pp * 128 + i * SUB + ch] = 1.0
    return jnp.asarray(m, BF)


def prep_kernel(ks_hbm, wy_hbm, wx_hbm, iy_hbm, ix_hbm, maps_hbm, own_ref, far_ref, sp_ref, sq_ref, sm_ref, r_ref, ks_ref, wy_ref, wx_ref, iy_ref, ix_ref, maps_ref, sem):
    k = lax.axis_index('cols')
    r = lax.axis_index('rows')
    loads = []
    for src, dst in ((iy_hbm, iy_ref), (ix_hbm, ix_ref), (wx_hbm, wx_ref), (wy_hbm, wy_ref), (ks_hbm, ks_ref), (maps_hbm.at[:, :, :, WIDE:], maps_ref)):
        cp = pltpu.make_async_copy(src, dst, sem.at[len(loads)])
        cp.start()
        loads.append(cp)
    parts = []
    for c in range(4):
        n = min(HALF, MAPS - HALF * c)
        parts += [(sp_ref.at[pl.ds(HALF * c, n)], c, pl.ds(0, n)), (sq_ref.at[c], c, pl.ds(HALF, WIN))]
    parts.append((sm_ref, 3, pl.ds(HALF - WIN, WIN)))
    for ref, c, q in parts:
        for i in range(2):
            cp = pltpu.make_async_copy(maps_hbm.at[i, c, q, pl.ds(0, WIDE)], ref.at[:, pl.ds(WIDE * i, WIDE)], sem.at[len(loads)])
            cp.start()
            loads.append(cp)
    kk = lax.broadcasted_iota(jnp.int32, (LANES, WIDE * 3), 0)
    ll = lax.broadcasted_iota(jnp.int32, (LANES, WIDE * 3), 1)
    r_ref[...] = jnp.where((kk < HW) & ((kk & 7) == (ll >> 7)), 1.0, 0.0).astype(BF)
    loads[0].wait()
    loads[1].wait()
    iy = iy_ref[...]
    code = ((iy - r * RB + 5) * CODE + ix_ref[...] - k * CB + 5).astype(F32)
    for i in range(2, 5):
        loads[i].wait()
    lo = jnp.concatenate([ks_ref[0, 0:4, :], ks_ref[1, 0:4, :]], axis=0)
    hi = jnp.concatenate([ks_ref[0, 4:SUB, :], ks_ref[1, 4:SUB, :]], axis=0)
    first = k == 0
    for ref, y in ((own_ref, jnp.where(first, lo, hi)), (far_ref, jnp.where(first, hi, lo))):
        for b in range(NB):
            cols = slice(LANES * b, LANES * (b + 1))
            ref[PAY * b:PAY * b + SUB, :] = y[:, cols]
            ref[PAY * b + SUB:PAY * b + SUB + KW, :] = wx_ref[:, cols]
            ref[PAY * (b + 1) - KW - 1:PAY * (b + 1) - 1, :] = wy_ref[:, cols]
            ref[PAY * (b + 1) - 1:PAY * (b + 1), :] = code[b:b + 1, :]
    loads[5].wait()
    for c in range(4):
        end = jnp.concatenate([maps_ref[i, c] for i in range(2)], axis=1)
        n = min(HALF, MAPS - HALF * c)
        sp_ref[HALF * c:HALF * c + n, 2 * WIDE:] = end[:n]
        sq_ref[c, :, 2 * WIDE:] = end[HALF:]
        if n < HALF:
            sm_ref[:, 2 * WIDE:] = end[n:HALF]
    for cp in loads[KW:]:
        cp.wait()


def split3(x):
    hi = x.astype(BF).astype(F32)
    r = x - hi
    mid = r.astype(BF).astype(F32)
    return hi, mid, r - mid


def accumulate(pay_ref, r_ref, accs, us, xs, vs, int_ref, base_ref, sem):
    row_i = lax.broadcasted_iota(jnp.int32, (WIN, LANES), 0)

    def make_u(blk, k):
        off = jnp.minimum(blk, NB - 1) * PAY
        y8 = pay_ref[pl.ds(off, SUB), :]
        wx = pay_ref[pl.ds(off + SUB, SUB), :]
        wyp = pay_ref[pl.ds(off + PAY - SUB, SUB), :]
        d = (row_i - (wyp[7:, :].astype(jnp.int32) // CODE)) & (WIN - 1)
        p = jnp.zeros((WIN, LANES), F32)
        for a in range(KW):
            p = jnp.where(d == a, wyp[a + 1:a + 2, :], p)
        us[k][...] = jnp.concatenate([y8 * p[i:i + 1, :] for i in range(WIN)], axis=0).T
        x3 = list(split3(wx)) + [jnp.zeros((LANES - HW, LANES), F32)]
        xs[k][...] = jnp.concatenate(x3, axis=0).T

    def make_v(k):
        lhs = xs[k][...].astype(BF)
        u = us[k][...]
        for bp in range(3):
            w = jnp.dot(lhs, r_ref[:, WIDE * bp:WIDE * bp + WIDE], preferred_element_type=F32)
            for c in range(2):
                v = w[:, LANES * c:LANES * (c + 1)] * u
                for g in range(WIN):
                    vs[k][pl.ds(SUB * PS * g + 2 * bp + c, SUB, stride=PS), :] = v[SUB * g:SUB * g + SUB, :]

    def add_tiles(blk, k):
        row = base_ref.at[blk]
        for j in range(LANES):
            acc = accs[j % T]
            b = row[j]
            acc[pl.ds(b, SUB), :] = acc[pl.ds(b, SUB), :] + vs[k][PS * j:PS * j + SUB, :]

    code = jnp.concatenate([pay_ref[PAY * (b + 1) - 1:PAY * (b + 1), :] for b in range(NB)], axis=0).astype(jnp.int32)
    int_ref[...] = (((code // CODE - 5) * 187) >> STEP) * CW + (code & (CODE - 1))
    for v in vs:
        for g in range(WIN):
            for c in range(KW, SUB):
                v[pl.ds(SUB * PS * g + c, SUB, stride=PS), :] = jnp.zeros((SUB, LANES), F32)
    load = pltpu.make_async_copy(int_ref, base_ref, sem)
    load.start()
    make_u(0, 0)
    make_u(1, 1)
    make_v(0)
    load.wait()

    def body(n, _):
        k = 2 * n
        make_v(1)
        add_tiles(k, 0)
        make_u(k + 2, 0)
        make_v(0)
        add_tiles(k + 1, 1)
        make_u(k + 3, 1)
        return 0

    lax.fori_loop(0, NB // 2, body, 0)


def folded(accs, off, n, clear=False):
    def total(g):
        rows = pl.ds(pl.multiple_of(g * CW + off, SUB), n)
        v = accs[0][rows, :]
        for a in accs[1:]:
            v = v + a[rows, :]
        if clear:
            for a in accs:
                a[rows, :] = jnp.zeros((n, LANES), F32)
        return v

    row = lax.broadcasted_iota(jnp.int32, (n, LANES), 1) >> 3
    tiles = [None] * TILES
    for g in range(NG):
        v = total(g)
        if g == 0:
            ghost = v
        first = 5 + STEP * g
        for p in range(TILES):
            lo, hi = max(first, SUB + WIN * p), min(first + WIN, SUB + WIN * (p + 1))
            if lo < hi:
                part = jnp.where((row - lo & (WIN - 1)) < hi - lo, v, 0.0)
                tiles[p] = part if tiles[p] is None else tiles[p] + part
    return tiles + [jnp.where(row >= SUB, v, ghost)]


def own_kernel(pay_ref, r_ref, out_ref, *refs):
    accs, scr = refs[:T], refs[T:]

    def clear(n, _):
        for a in accs:
            a[pl.ds(pl.multiple_of(n * CW, SUB), CW), :] = jnp.zeros((CW, LANES), F32)
        return 0

    lax.fori_loop(0, NG, clear, 0)
    accumulate(pay_ref, r_ref, accs, scr[:2], scr[2:4], scr[4:6], *scr[6:])

    def fold(q, _):
        off = pl.multiple_of(q * WIN, WIN)
        for p, t in enumerate(folded(accs, off, WIN, clear=True)):
            out_ref[p, pl.ds(off, WIN), :] = t
        return 0

    lax.fori_loop(0, CW // WIN, fold, 0)


def far_kernel(pay_ref, r_ref, a_ref, *refs):
    accs, pack_ref, gh_ref, scr = refs[T:2 * T], refs[2 * T], refs[2 * T + 1], refs[2 * T + 2:]
    accumulate(pay_ref, r_ref, accs, scr[:2], scr[2:4], scr[4:6], *scr[6:])
    own0 = lax.axis_index('cols') * CB
    far0 = CB - own0

    def ghost(off, n):
        high = lax.broadcasted_iota(jnp.int32, (n, LANES), 1) >= HALF
        ends = []
        for g in (0, NG - 1):
            rows = pl.ds(pl.multiple_of(g * CW + off, SUB), n)
            v = accs[0][rows, :]
            for a in accs[1:]:
                v = v + a[rows, :]
            ends.append(v)
        return jnp.where(high, ends[1], ends[0])

    def copy(n, _):
        o = pl.multiple_of(n * QTR, SUB)
        gh_ref[pl.ds(pl.multiple_of(far0 + o, SUB), QTR), :] = ghost(SUB + o, QTR)
        gh_ref[pl.ds(pl.multiple_of(own0 + o, SUB), QTR), :] = a_ref[TILES, pl.ds(pl.multiple_of(SUB + o, SUB), QTR), :]
        return 0

    lax.fori_loop(0, CB // QTR, copy, 0)
    for dst, add in ((own0, ghost(CW - SUB, SUB)), (own0 + CB - SUB, ghost(0, SUB)), (far0, a_ref[TILES, CW - SUB:, :]), (far0 + CB - SUB, a_ref[TILES, :SUB, :])):
        rows = pl.ds(pl.multiple_of(dst, SUB), SUB)
        gh_ref[rows, :] = gh_ref[rows, :] + add

    lane = lax.broadcasted_iota(jnp.int32, (LANES, LANES), 1)
    for side, lane0 in ((0, HALF - HW), (1, HALF)):
        out = jnp.zeros((LANES, LANES), F32)
        for j in range(5):
            piece = pltpu.roll(gh_ref[LANES * j:LANES * (j + 1), :], (HW * j - lane0) % LANES, axis=1)
            out = jnp.where(lane >= HW * j, piece, out)
        pack_ref[side] = out


def image_kernel(*refs):
    accs = refs[:T]
    (a_ref, pack_ref, so_ref, sx_ref, sm_ref, se_ref, d_ref, ev_ref, eu_ref, pm_ref, out_ref,
     tb_ref, edge_ref, g_ref, halo, sm1, sm2, sr1, sr2, hm1, hm2, hr1, hr2, s_main, s_rem, acc_m, acc_r, sx_mid, pieces, recvs, tails, recvs_t,
     halo_ss, halo_rs, swap_ss, swap_rs, red_ss, red_rs) = refs[T:]
    k = lax.axis_index('cols')
    r = lax.axis_index('rows')
    core, x = r % 2, r // 2
    near = r + 1 - 2 * core
    across = (r + 2) % 4
    prev, nxt = (r + 3) % 4, (r + 1) % 4
    homes = ({'rows': across, 'cols': 1 - k}, {'rows': across}, {'cols': 1 - k})

    barrier = pltpu.get_barrier_semaphore()
    for dev in ({'rows': prev}, {'rows': nxt}) + homes:
        pl.semaphore_signal(barrier, inc=1, device_id=dev, device_id_type=MESH_ID)

    own0 = k * CB
    far0 = CB - own0
    high16 = lax.broadcasted_iota(jnp.int32, (WIN, LANES), 1) >= HALF

    def put(v, tiles):
        rows = pl.ds(pl.multiple_of(v, WIN), WIN)
        for p in range(TILES):
            tb_ref[p, rows, :] = tiles[p].astype(BF)
        edge_ref[rows, :] = jnp.where(high16, tiles[0], tiles[9])

    def far_part(n, _):
        put(far0 + WIN * n, folded(accs, pl.multiple_of(SUB + WIN * n, SUB), WIN))
        return 0

    def own_part(n, _):
        put(own0 + WIN * n, [a_ref[p, pl.ds(pl.multiple_of(SUB + WIN * n, SUB), WIN), :] for p in range(TILES)])
        return 0

    last = CB // WIN - 1
    lax.fori_loop(1, last, far_part, 0)
    pl.semaphore_wait(barrier, 5)

    def remote(src, dst, ss, rs, i, dev):
        cp = pltpu.make_async_remote_copy(src_ref=src, dst_ref=dst, send_sem=ss.at[i], recv_sem=rs.at[i], device_id=dev, device_id_type=MESH_ID)
        cp.start()
        return cp

    halos = [remote(pack_ref.at[i], halo.at[i], halo_ss, halo_rs, i, {'rows': dev}) for i, dev in ((0, prev), (1, nxt))]

    lax.fori_loop(1, last, own_part, 0)
    none = jnp.zeros((SUB, LANES), F32)
    for n, side in ((0, CW - SUB), (last, 0)):
        off = SUB + WIN * n
        near_tiles = folded(accs, off, WIN)
        far_ends = folded(accs, side, SUB)
        order = (lambda v: [v, none]) if n == 0 else (lambda v: [none, v])
        put(far0 + WIN * n, [near_tiles[p] + jnp.concatenate(order(a_ref[p, side:side + SUB, :]), axis=0) for p in range(TILES)])
        put(own0 + WIN * n, [a_ref[p, off:off + WIN, :] + jnp.concatenate(order(far_ends[p]), axis=0) for p in range(TILES)])


    def to_rows(row0, n, t0, t1):
        a = jnp.concatenate([t0, t1], axis=1)
        g = lax.dot_general(pm_ref[...], a, (((1,), (1,)), ((), ())), preferred_element_type=F32).astype(BF)
        for ch in range(SUB):
            i, c = ch // 4, ch % 4
            g_ref[row0 + n * c:row0 + n * c + QTR, N_GRID * i:N_GRID * (i + 1)] = g[QTR * ch:QTR * (ch + 1), :]

    for m in range(4):
        to_rows(QTR * m, LANES, tb_ref[2 * m + 1], tb_ref[2 * m + 2])

    mid = remote(sm_ref, sx_mid, halo_ss, halo_rs, 2, {'rows': across})

    sms, srs, hms, hrs = (sm1, sm2), (sr1, sr2), (hm1, hm2), (hr1, hr2)
    swaps, trades = [], []

    def columns(grp):
        start, n = GROUPS[grp]
        lane = lax.broadcasted_iota(jnp.int32, (n, LANES), 1)
        side = lane >> 6
        own_even, far_even = side == core, side != core
        block = (lane & (HALF - 1)) >> 4
        h = jnp.dot(g_ref[4 * start:4 * (start + n), :], ev_ref[...], preferred_element_type=F32)
        hc = [h[n * c:n * (c + 1)] for c in range(4)]
        rems = [v[:, 4 * LANES:] for v in hc]
        for cp in range(2):
            hs = [[v[:, LANES * i:LANES * (i + 1)] for i in range(4)] for v in hc[2 * cp:2 * cp + 2]]
            for i in range(4):
                dp, t = i // 2, i % 2
                odd = pltpu.roll(hs[1][i], HALF, axis=1)
                sms[grp][dp, cp, t] = jnp.where(far_even, hs[0][i], odd).astype(BF)
                hms[grp][dp, cp, t, core] = jnp.where(own_even, hs[0][i], odd).astype(BF)
        for d in range(ROWS):
            out = rems[d]
            for c in range(4):
                if c != d:
                    out = jnp.where(block == c, pltpu.roll(rems[c], (WIN * (c - d)) % LANES, axis=1), out)
            srs[grp][d] = out.astype(BF)
        hrs[grp][r] = srs[grp][r]
        swaps.append(remote(sms[grp], hms[grp].at[:, :, :, core], swap_ss, swap_rs, grp, {'rows': near}))
        for i, dev in enumerate((across, 3 - r, near)):
            trades.append(remote(srs[grp].at[dev], hrs[grp].at[r], swap_ss, swap_rs, 2 + 3 * grp + i, {'rows': dev}))

    columns(0)

    for h in halos:
        h.wait()
    lane = lax.broadcasted_iota(jnp.int32, (LANES, LANES), 1)
    low = lane < HALF
    t0s, t9s = [], []
    for j in range(5):
        rows = slice(LANES * j, LANES * (j + 1))
        add_first = pltpu.roll(halo[1], (HALF - HW * j) % LANES, axis=1)
        add_last = pltpu.roll(halo[0], (HALF - HW - HW * j) % LANES, axis=1)
        e = edge_ref[rows, :] + jnp.where(low, jnp.where(lane >= HALF - HW, add_last, 0.0), jnp.where(lane < HALF + HW, add_first, 0.0))
        t0s.append(jnp.where(low, tb_ref[0, rows, :].astype(F32), e).astype(BF))
        t9s.append(jnp.where(low, e, tb_ref[9, rows, :].astype(F32)).astype(BF))
    lane = lax.broadcasted_iota(jnp.int32, (PB, LANES), 1)
    low = lane < HALF
    to_rows(4 * LANES, QTR, jnp.concatenate(t0s, axis=0), jnp.concatenate(t9s, axis=0))
    columns(1)

    def turn(rows):
        t = [rows[:, LANES * i:LANES * (i + 1)].T for i in range(5)]
        return [jnp.concatenate([t[2 * i], t[2 * i + 1], t[4][HALF * i:HALF * (i + 1)]], axis=0) for i in range(2)]


    for cp in swaps[:1]:
        cp.wait_recv()
    n0 = 4 * GROUPS[0][1]

    def block_of(grp, j):
        return jnp.concatenate([hms[grp][(x + j) % 2, cp].reshape(4 * GROUPS[grp][1], LANES) for cp in range(2)], axis=1)

    mid.wait_recv()
    for j, ref, end in ((1, sx_ref, sx_mid), (0, so_ref, sm_ref)):
        c = [ref[HALF * i:HALF * (i + 1), :] for i in range(3)] + [jnp.concatenate([ref[3 * HALF:, :], end[...]], axis=0)]
        acc_m[j] = jnp.dot(eu_ref[x, :, :n0], block_of(0, j), preferred_element_type=F32)
        for cp in range(2):
            s_main[j, 0, cp], s_main[j, 1, cp] = turn(jnp.concatenate([jnp.where(core == 0, c[2 * cp], c[2 * cp + 1]), jnp.where(core == 0, c[2 * cp + 1], c[2 * cp])], axis=0))

    for cp in swaps[1:]:
        cp.wait_recv()

    def rows_dft(half, acc, rhs):
        rows = pl.ds(pl.multiple_of(half * N_IMG, WIN), N_IMG)
        total = acc[rows, :] + jnp.dot(eu_ref[x, rows, n0:], rhs, preferred_element_type=F32)
        return total[:PB], total[PB:]

    quarter = lax.broadcasted_iota(jnp.int32, (PB // 4, LANES), 1) >> 5

    def piece(half, j):
        i_re, i_im = rows_dft(half, acc_m.at[j], block_of(1, j))
        rows = pl.ds(pl.multiple_of(half * PB, SUB), PB)
        re, im = None, None
        for cp in range(2):
            cols = slice(LANES * cp, LANES * (cp + 1))
            s_re, s_im = s_main[j, 0, cp, rows, :], s_main[j, 1, cp, rows, :]
            a = s_re * i_re[:, cols] + s_im * i_im[:, cols]
            b = s_re * i_im[:, cols] - s_im * i_re[:, cols]
            re, im = (a, b) if re is None else (re + a, im + b)
        return jnp.where(low, re + pltpu.roll(re, HALF, axis=1), im + pltpu.roll(im, HALF, axis=1))

    def rest(half):
        parts = []
        for o in range(2):
            rows = pl.ds(pl.multiple_of(half * N_IMG + PB * o, WIN), PB)
            parts.append(acc_r[0, rows, :] + pltpu.roll(acc_r[1, rows, :], HALF, axis=1))
        i_re, i_im = parts
        rows = pl.ds(pl.multiple_of(half * PB, SUB), PB)
        s_re, s_im = s_rem[0, rows, :], s_rem[1, rows, :]
        w = s_re * i_re + s_im * i_im + pltpu.roll(s_re * i_im - s_im * i_re, HALF, axis=1)
        w = w + pltpu.roll(w, LANES - QTR, axis=1)
        w = w + pltpu.roll(w, LANES - WIN, axis=1)
        w = jnp.where(lane < WIN, w, pltpu.roll(w, LANES - HALF + WIN, axis=1))
        out = w[:PB // 4]
        for g in range(1, 4):
            out = jnp.where(quarter == g, pltpu.roll(w[PB // 4 * g:PB // 4 * (g + 1)], QTR * g, axis=1), out)
        return out

    sends = []
    for i, (half, j) in enumerate(((1 - k, 1), (k, 1), (1 - k, 0))):
        pieces[i] = piece(half, j)
        sends.append(remote(pieces.at[i], recvs.at[i], red_ss, red_rs, i, homes[i]))
    for cp in trades:
        cp.wait_recv()
    for t in range(2):
        total = None
        for grp in range(2):
            kk = 2 * GROUPS[grp][1]
            for c in range(2):
                part = jnp.dot(eu_ref[c, :, n0 * grp + kk * t:n0 * grp + kk * (t + 1)], hrs[grp][2 * c:2 * c + 2].reshape(kk, LANES), preferred_element_type=F32)
                total = part if total is None else total + part
        acc_r[t] = total
    s_rem[0], s_rem[1] = turn(jnp.concatenate([se_ref[c] for c in range(4)] + [jnp.zeros((HALF, N_GRID), F32)], axis=0))
    tails[...] = rest(1 - k)
    tail = remote(tails, recvs_t, red_ss, red_rs, 3, homes[2])
    rem = rest(k)
    main = piece(k, 0)
    d8 = jnp.broadcast_to(jnp.concatenate([d_ref[...][None, :], jnp.zeros((1, HALF), F32)], axis=1), (SUB, N_IMG + HALF))
    dq = d8
    for j in range(1, ROWS):
        dq = jnp.where(r == j, pltpu.roll(d8, N_IMG + HALF - QB * j, axis=1), dq)
    dp = jnp.where(k == 0, d8, pltpu.roll(d8, N_IMG + HALF - PB, axis=1))[:, :2 * LANES]
    dd = jnp.concatenate([dp] * WIN, axis=0).T[:PB] * dq[:1, :LANES]

    for i in (2, 0, 1):
        sends[i].wait_recv()
        main = main + recvs[i]
    tail.wait_recv()
    rem = rem + recvs_t[...]
    for o in range(2):
        m = pltpu.roll(main, HALF, axis=1) if o else main
        for j in range(4):
            rows = slice(PB // 4 * j, PB // 4 * (j + 1))
            end = pltpu.roll(rem, (HALF - QTR * j - WIN * o) % LANES, axis=1)
            out_ref[o, rows, :] = (jnp.where(low[rows], m[rows], end) * dd[rows])[:, :QB]

    for cp in sends + swaps + trades + [mid, tail]:
        cp.wait_send()


def solution(mesh):
    sample_spec = ('exam', 'rows', 'cols')
    vm = pl.BlockSpec(memory_space=pltpu.VMEM)
    hbm = pl.BlockSpec(memory_space=pltpu.HBM)
    spread_scratch = ([VMEM((LANES, LANES), F32)] * 4 + [VMEM((LANES * PS, LANES), F32)] * 2
                      + [VMEM((NB, LANES), jnp.int32), pltpu.SMEM((NB, LANES), jnp.int32), pltpu.SemaphoreType.DMA])
    acc_shape = [jax.ShapeDtypeStruct((NG * CW, LANES), F32)] * T
    big = 6 * MIB

    def local_fn(kspace, wts_y, wts_x, idx_y, idx_x, coil_maps, deapod):
        own, far, maps, maps_end, maps_mid, spread_mat = pl.pallas_call(
            prep_kernel,
            out_shape=[jax.ShapeDtypeStruct((PAY * NB, LANES), F32)] * 2 + [jax.ShapeDtypeStruct(d, F32) for d in ((MAPS, N_GRID), (4, WIN, N_GRID), (WIN, N_GRID))] + [jax.ShapeDtypeStruct((LANES, WIDE * 3), BF)],
            in_specs=[hbm] * 6, out_specs=[vm] * 6, name='prep',
            scratch_shapes=[VMEM((2, SUB, NS), F32), VMEM((KW, NS), F32), VMEM((KW, NS), F32), VMEM((NB, LANES), jnp.int32), VMEM((NB, LANES), jnp.int32), VMEM((2, 4, QB, HALF), F32), pltpu.SemaphoreType.DMA((24,))],
            compiler_params=pltpu.CompilerParams(vmem_limit_bytes=SUB * MIB),
        )(*[pltpu.with_memory_space_constraint(v, pltpu.HBM) for v in (kspace, wts_y, wts_x, idx_y.reshape(NB, LANES), idx_x.reshape(NB, LANES), jnp.swapaxes(coil_maps, 2, 3))])
        far_in = lax.ppermute(far, 'cols', [(0, 1), (1, 0)])
        half, *accs = pl.pallas_call(
            own_kernel, out_shape=[jax.ShapeDtypeStruct((11, CW, LANES), F32)] + acc_shape, in_specs=[vm] * 2, out_specs=[vm] * (T + 1),
            scratch_shapes=spread_scratch, compiler_params=pltpu.CompilerParams(vmem_limit_bytes=big), name='spread_own',
            cost_estimate=pl.CostEstimate(flops=GIGA, bytes_accessed=4 * MIB, transcendentals=0),
        )(own, spread_mat)
        *accs, pack = pl.pallas_call(
            far_kernel, out_shape=acc_shape + [jax.ShapeDtypeStruct((2, LANES, LANES), F32)],
            in_specs=[vm] * (T + 3), out_specs=[vm] * (T + 1), scratch_shapes=[VMEM((N_GRID, LANES), F32)] + spread_scratch,
            input_output_aliases={i + 3: i for i in range(T)},
            compiler_params=pltpu.CompilerParams(vmem_limit_bytes=big), name='spread_far',
            cost_estimate=pl.CostEstimate(flops=GIGA, bytes_accessed=4 * MIB, transcendentals=0),
        )(far_in, spread_mat, half, *accs)
        maps_x = lax.ppermute(maps, 'rows', [(i, (i + 2) % ROWS) for i in range(ROWS)])
        dma = pltpu.SemaphoreType.DMA
        half_bufs = [VMEM((2, 2, 2, n, LANES), BF) for _, n in GROUPS] + [VMEM((ROWS, n, LANES), BF) for _, n in GROUPS]
        full_bufs = [VMEM((2, 2, 2, 2, n, LANES), BF) for _, n in GROUPS] + [VMEM((ROWS, n, LANES), BF) for _, n in GROUPS]
        return pl.pallas_call(
            image_kernel,
            out_shape=jax.ShapeDtypeStruct((2, PB, QB), F32), in_specs=[vm] * (T + TILES), out_specs=vm,
            scratch_shapes=[VMEM((TILES, N_GRID, LANES), BF), VMEM((N_GRID, LANES), F32), VMEM((4 * RB, 2 * N_GRID), BF), VMEM((2, LANES, LANES), F32)] + half_bufs + full_bufs + [
                VMEM((2, 2, 2, N_IMG, LANES), F32), VMEM((2, N_IMG, LANES), F32),
                VMEM((2, 2 * N_IMG, 2 * LANES), F32), VMEM((2, 2 * N_IMG, LANES), F32), VMEM((WIN, N_GRID), F32),
                VMEM((3, PB, LANES), F32), VMEM((3, PB, LANES), F32), VMEM((PB // 4, LANES), F32), VMEM((PB // 4, LANES), F32),
                dma((3,)), dma((3,)), dma((8,)), dma((8,)), dma((4,)), dma((4,)),
            ],
            compiler_params=pltpu.CompilerParams(vmem_limit_bytes=11 * MIB, collective_id=0, has_side_effects=True), name='image',
        )(*accs, half, pack, maps, maps_x, maps_mid, maps_end, deapod, col_dft(), row_dft(), unmix())

    return jax.shard_map(
        local_fn,
        mesh=mesh,
        in_specs=(P(None, None, sample_spec), P(None, sample_spec), P(None, sample_spec), P(sample_spec), P(sample_spec), P(None, ('exam', 'cols'), None, 'rows'), P()),
        out_specs=P(None, ('exam', 'cols'), 'rows'),
        check_vma=False,
    )
```

```python
import functools
import math

import jax
import jax.numpy as jnp
import numpy as np
from jax import lax
from jax.experimental import pallas as pl
from jax.experimental.pallas import tpu as pltpu
from jax.sharding import PartitionSpec as P

BF = jnp.bfloat16
F32 = jnp.float32
VMEM = pltpu.VMEM
LANES = 128
MIB = 1 << 20
GIGA = 4000 * MIB
TILES = 10
SUB, WIN, QTR, HALF, WIDE = 8, 16, 32, 64, 256
N_GRID, N_IMG, N_COILS, KW = 640, 320, 8, 6
ROWS, COLS = 4, 2
RB, CB, QB = N_GRID // ROWS, N_GRID // COLS, N_IMG // ROWS
PB = N_IMG // COLS
NS = 4096
NB = NS // LANES
STEP = 11
NG = 15
CW = CB + WIN
T = 7
PS = 9
PAY = 21
CODE = 512
MAPS = 240
HW = 24
ORDER = tuple(range(1, 9)) + (0, 9)
GROUPS = ((0, 128), (128, 32))
MESH_ID = pl.DeviceIdType.MESH


def dft_parts():
    freq = np.arange(N_GRID) - N_GRID // 2
    pos = np.arange(N_IMG) - N_IMG // 2
    ang = ((freq[:, None] * pos[None, :]) % N_GRID).astype(np.float32) * np.float32(2.0 * math.pi / N_GRID)
    norm = np.float32(1.0 / math.sqrt(N_GRID))
    c, s = np.cos(ang) * norm, np.sin(ang) * norm
    return np.stack([np.stack([c, s], 1), np.stack([-s, c], 1)], 0)


def col_dft():
    e = dft_parts()
    out = np.zeros((2 * N_GRID, N_GRID), np.float32)
    for dp in range(2):
        for t in range(2):
            for h in range(2):
                q0 = QB * (2 * dp + h)
                l0 = LANES * (2 * dp + t) + HALF * h
                out[:, l0:l0 + HALF] = e[:, :, t, q0:q0 + HALF].reshape(2 * N_GRID, HALF)
    for t in range(2):
        for d in range(4):
            l0 = 4 * LANES + HALF * t + WIN * d
            out[:, l0:l0 + WIN] = e[:, :, t, QB * d + HALF:QB * (d + 1)].reshape(2 * N_GRID, WIN)
    return jnp.asarray(out, BF)


def row_dft():
    e = dft_parts()
    rows = np.concatenate([np.arange(WIN * l, WIN * (l + 1)) for l in ORDER])
    chips = []
    for x in range(2):
        parts = []
        for start, n in GROUPS:
            for t in range(2):
                for b in range(2):
                    parts.append(e[t, (2 * x + b) * RB + rows[start:start + n]])
        m = np.concatenate(parts, 0)
        chips.append(np.concatenate([m[:, :, PB * h:PB * (h + 1)].reshape(N_GRID, N_IMG).T for h in range(2)], 0))
    return jnp.asarray(np.array(chips), BF)


def unmix():
    m = np.zeros((WIDE, WIDE), np.float32)
    for ch in range(SUB):
        for pp in range(2):
            for i in range(WIN):
                m[ch * QTR + WIN * pp + (i + SUB) % WIN, pp * 128 + i * SUB + ch] = 1.0
    return jnp.asarray(m, BF)


def prep_kernel(ks_hbm, wy_hbm, wx_hbm, iy_hbm, ix_hbm, maps_hbm, own_ref, far_ref, sp_ref, sq_ref, sm_ref, ks_ref, wy_ref, wx_ref, iy_ref, ix_ref, maps_ref, sem):
    k = lax.axis_index('cols')
    r = lax.axis_index('rows')
    loads = []
    for src, dst in ((iy_hbm, iy_ref), (ix_hbm, ix_ref), (wx_hbm, wx_ref), (wy_hbm, wy_ref), (ks_hbm, ks_ref), (maps_hbm.at[:, :, :, WIDE:], maps_ref)):
        cp = pltpu.make_async_copy(src, dst, sem.at[len(loads)])
        cp.start()
        loads.append(cp)
    parts = []
    for c in range(4):
        n = min(HALF, MAPS - HALF * c)
        parts += [(sp_ref.at[pl.ds(HALF * c, n)], c, pl.ds(0, n)), (sq_ref.at[c], c, pl.ds(HALF, WIN))]
    parts.append((sm_ref, 3, pl.ds(HALF - WIN, WIN)))
    for ref, c, q in parts:
        for i in range(2):
            cp = pltpu.make_async_copy(maps_hbm.at[i, c, q, pl.ds(0, WIDE)], ref.at[:, pl.ds(WIDE * i, WIDE)], sem.at[len(loads)])
            cp.start()
            loads.append(cp)
    loads[0].wait()
    loads[1].wait()
    iy = iy_ref[...]
    code = ((iy - r * RB + 5) * CODE + ix_ref[...] - k * CB + 5).astype(F32)
    for i in range(2, 5):
        loads[i].wait()
    lo = jnp.concatenate([ks_ref[0, 0:4, :], ks_ref[1, 0:4, :]], axis=0)
    hi = jnp.concatenate([ks_ref[0, 4:SUB, :], ks_ref[1, 4:SUB, :]], axis=0)
    first = k == 0
    for ref, y in ((own_ref, jnp.where(first, lo, hi)), (far_ref, jnp.where(first, hi, lo))):
        for b in range(NB):
            cols = slice(LANES * b, LANES * (b + 1))
            ref[PAY * b:PAY * b + SUB, :] = y[:, cols]
            ref[PAY * b + SUB:PAY * b + SUB + KW, :] = wx_ref[:, cols]
            ref[PAY * (b + 1) - KW - 1:PAY * (b + 1) - 1, :] = wy_ref[:, cols]
            ref[PAY * (b + 1) - 1:PAY * (b + 1), :] = code[b:b + 1, :]
    loads[5].wait()
    for c in range(4):
        end = jnp.concatenate([maps_ref[i, c] for i in range(2)], axis=1)
        n = min(HALF, MAPS - HALF * c)
        sp_ref[HALF * c:HALF * c + n, 2 * WIDE:] = end[:n]
        sq_ref[c, :, 2 * WIDE:] = end[HALF:]
        if n < HALF:
            sm_ref[:, 2 * WIDE:] = end[n:HALF]
    for cp in loads[KW:]:
        cp.wait()


def split3(x):
    hi = x.astype(BF).astype(F32)
    r = x - hi
    mid = r.astype(BF).astype(F32)
    return hi, mid, r - mid


def accumulate(pay_ref, accs, us, xs, vs, r_ref, int_ref, base_ref, sem):
    row_i = lax.broadcasted_iota(jnp.int32, (WIN, LANES), 0)

    def make_u(blk, k):
        off = jnp.minimum(blk, NB - 1) * PAY
        y8 = pay_ref[pl.ds(off, SUB), :]
        wx = pay_ref[pl.ds(off + SUB, SUB), :]
        wyp = pay_ref[pl.ds(off + PAY - SUB, SUB), :]
        d = (row_i - (wyp[7:, :].astype(jnp.int32) // CODE)) & (WIN - 1)
        p = jnp.zeros((WIN, LANES), F32)
        for a in range(KW):
            p = jnp.where(d == a, wyp[a + 1:a + 2, :], p)
        us[k][...] = jnp.concatenate([y8 * p[i:i + 1, :] for i in range(WIN)], axis=0).T
        x3 = list(split3(wx)) + [jnp.zeros((LANES - HW, LANES), F32)]
        xs[k][...] = jnp.concatenate(x3, axis=0).T

    def make_v(k):
        lhs = xs[k][...].astype(BF)
        u = us[k][...]
        for bp in range(3):
            w = jnp.dot(lhs, r_ref[:, WIDE * bp:WIDE * bp + WIDE], preferred_element_type=F32)
            for c in range(2):
                v = w[:, LANES * c:LANES * (c + 1)] * u
                for g in range(WIN):
                    vs[k][pl.ds(SUB * PS * g + 2 * bp + c, SUB, stride=PS), :] = v[SUB * g:SUB * g + SUB, :]

    def add_tiles(blk, k):
        row = base_ref.at[blk]
        for j in range(LANES):
            acc = accs[j % T]
            b = row[j]
            acc[pl.ds(b, SUB), :] = acc[pl.ds(b, SUB), :] + vs[k][PS * j:PS * j + SUB, :]

    code = jnp.concatenate([pay_ref[PAY * (b + 1) - 1:PAY * (b + 1), :] for b in range(NB)], axis=0).astype(jnp.int32)
    int_ref[...] = (((code // CODE - 5) * 187) >> STEP) * CW + (code & (CODE - 1))
    kk = lax.broadcasted_iota(jnp.int32, (LANES, WIDE * 3), 0)
    ll = lax.broadcasted_iota(jnp.int32, (LANES, WIDE * 3), 1)
    r_ref[...] = jnp.where((kk < HW) & ((kk & 7) == (ll >> 7)), 1.0, 0.0).astype(BF)
    for v in vs:
        v[...] = jnp.zeros_like(v)
    load = pltpu.make_async_copy(int_ref, base_ref, sem)
    load.start()
    make_u(0, 0)
    make_u(1, 1)
    make_v(0)
    load.wait()

    def body(n, _):
        k = 2 * n
        make_v(1)
        add_tiles(k, 0)
        make_u(k + 2, 0)
        make_v(0)
        add_tiles(k + 1, 1)
        make_u(k + 3, 1)
        return 0

    lax.fori_loop(0, NB // 2, body, 0)


def folded(accs, off, n, clear=False):
    def total(g):
        rows = pl.ds(pl.multiple_of(g * CW + off, SUB), n)
        v = accs[0][rows, :]
        for a in accs[1:]:
            v = v + a[rows, :]
        if clear:
            for a in accs:
                a[rows, :] = jnp.zeros((n, LANES), F32)
        return v

    row = lax.broadcasted_iota(jnp.int32, (n, LANES), 1) >> 3
    tiles = [None] * TILES
    for g in range(NG):
        v = total(g)
        if g == 0:
            ghost = v
        first = 5 + STEP * g
        for p in range(TILES):
            lo, hi = max(first, SUB + WIN * p), min(first + WIN, SUB + WIN * (p + 1))
            if lo < hi:
                part = jnp.where((row - lo & (WIN - 1)) < hi - lo, v, 0.0)
                tiles[p] = part if tiles[p] is None else tiles[p] + part
    return tiles + [jnp.where(row >= SUB, v, ghost)]


def own_kernel(pay_ref, out_ref, *refs):
    accs, scr = refs[:T], refs[T:]

    def clear(n, _):
        for a in accs:
            a[pl.ds(pl.multiple_of(n * CW, SUB), CW), :] = jnp.zeros((CW, LANES), F32)
        return 0

    lax.fori_loop(0, NG, clear, 0)
    accumulate(pay_ref, accs, scr[:2], scr[2:4], scr[4:6], *scr[6:])

    def fold(q, _):
        off = pl.multiple_of(q * WIN, WIN)
        for p, t in enumerate(folded(accs, off, WIN, clear=True)):
            out_ref[p, pl.ds(off, WIN), :] = t
        return 0

    lax.fori_loop(0, CW // WIN, fold, 0)


def far_kernel(pay_ref, a_ref, *refs):
    accs, pack_ref, gh_ref, scr = refs[T:2 * T], refs[2 * T], refs[2 * T + 1], refs[2 * T + 2:]
    accumulate(pay_ref, accs, scr[:2], scr[2:4], scr[4:6], *scr[6:])
    own0 = lax.axis_index('cols') * CB
    far0 = CB - own0

    def ghost(off, n):
        high = lax.broadcasted_iota(jnp.int32, (n, LANES), 1) >= HALF
        ends = []
        for g in (0, NG - 1):
            rows = pl.ds(pl.multiple_of(g * CW + off, SUB), n)
            v = accs[0][rows, :]
            for a in accs[1:]:
                v = v + a[rows, :]
            ends.append(v)
        return jnp.where(high, ends[1], ends[0])

    def copy(n, _):
        o = pl.multiple_of(n * QTR, SUB)
        gh_ref[pl.ds(pl.multiple_of(far0 + o, SUB), QTR), :] = ghost(SUB + o, QTR)
        gh_ref[pl.ds(pl.multiple_of(own0 + o, SUB), QTR), :] = a_ref[TILES, pl.ds(pl.multiple_of(SUB + o, SUB), QTR), :]
        return 0

    lax.fori_loop(0, CB // QTR, copy, 0)
    for dst, add in ((own0, ghost(CW - SUB, SUB)), (own0 + CB - SUB, ghost(0, SUB)), (far0, a_ref[TILES, CW - SUB:, :]), (far0 + CB - SUB, a_ref[TILES, :SUB, :])):
        rows = pl.ds(pl.multiple_of(dst, SUB), SUB)
        gh_ref[rows, :] = gh_ref[rows, :] + add

    lane = lax.broadcasted_iota(jnp.int32, (LANES, LANES), 1)
    for side, lane0 in ((0, HALF - HW), (1, HALF)):
        out = jnp.zeros((LANES, LANES), F32)
        for j in range(5):
            piece = pltpu.roll(gh_ref[LANES * j:LANES * (j + 1), :], (HW * j - lane0) % LANES, axis=1)
            out = jnp.where(lane >= HW * j, piece, out)
        pack_ref[side] = out


def image_kernel(*refs):
    accs = refs[:T]
    (a_ref, pack_ref, so_ref, sx_ref, sm_ref, se_ref, d_ref, ev_ref, eu_ref, pm_ref, out_ref,
     tb_ref, edge_ref, g_ref, halo, sm1, sm2, sr1, sr2, hm1, hm2, hr1, hr2, s_main, s_rem, acc_m, acc_r, sx_mid, pieces, recvs, tails, recvs_t,
     halo_ss, halo_rs, swap_ss, swap_rs, red_ss, red_rs) = refs[T:]
    k = lax.axis_index('cols')
    r = lax.axis_index('rows')
    core, x = r % 2, r // 2
    near = r + 1 - 2 * core
    across = (r + 2) % 4
    prev, nxt = (r + 3) % 4, (r + 1) % 4
    homes = ({'rows': across, 'cols': 1 - k}, {'rows': across}, {'cols': 1 - k})

    barrier = pltpu.get_barrier_semaphore()
    for dev in ({'rows': prev}, {'rows': nxt}) + homes:
        pl.semaphore_signal(barrier, inc=1, device_id=dev, device_id_type=MESH_ID)

    own0 = k * CB
    far0 = CB - own0
    high16 = lax.broadcasted_iota(jnp.int32, (WIN, LANES), 1) >= HALF

    def put(v, tiles):
        rows = pl.ds(pl.multiple_of(v, WIN), WIN)
        for p in range(TILES):
            tb_ref[p, rows, :] = tiles[p].astype(BF)
        edge_ref[rows, :] = jnp.where(high16, tiles[0], tiles[9])

    def far_part(n, _):
        put(far0 + WIN * n, folded(accs, pl.multiple_of(SUB + WIN * n, SUB), WIN))
        return 0

    def own_part(n, _):
        put(own0 + WIN * n, [a_ref[p, pl.ds(pl.multiple_of(SUB + WIN * n, SUB), WIN), :] for p in range(TILES)])
        return 0

    last = CB // WIN - 1
    lax.fori_loop(1, last, far_part, 0)
    pl.semaphore_wait(barrier, 5)

    def remote(src, dst, ss, rs, i, dev):
        cp = pltpu.make_async_remote_copy(src_ref=src, dst_ref=dst, send_sem=ss.at[i], recv_sem=rs.at[i], device_id=dev, device_id_type=MESH_ID)
        cp.start()
        return cp

    halos = [remote(pack_ref.at[i], halo.at[i], halo_ss, halo_rs, i, {'rows': dev}) for i, dev in ((0, prev), (1, nxt))]

    lax.fori_loop(1, last, own_part, 0)
    none = jnp.zeros((SUB, LANES), F32)
    for n, side in ((0, CW - SUB), (last, 0)):
        off = SUB + WIN * n
        near_tiles = folded(accs, off, WIN)
        far_ends = folded(accs, side, SUB)
        order = (lambda v: [v, none]) if n == 0 else (lambda v: [none, v])
        put(far0 + WIN * n, [near_tiles[p] + jnp.concatenate(order(a_ref[p, side:side + SUB, :]), axis=0) for p in range(TILES)])
        put(own0 + WIN * n, [a_ref[p, off:off + WIN, :] + jnp.concatenate(order(far_ends[p]), axis=0) for p in range(TILES)])


    def to_rows(row0, n, t0, t1):
        a = jnp.concatenate([t0, t1], axis=1)
        g = lax.dot_general(pm_ref[...], a, (((1,), (1,)), ((), ())), preferred_element_type=F32).astype(BF)
        for ch in range(SUB):
            i, c = ch // 4, ch % 4
            g_ref[row0 + n * c:row0 + n * c + QTR, N_GRID * i:N_GRID * (i + 1)] = g[QTR * ch:QTR * (ch + 1), :]

    for m in range(4):
        to_rows(QTR * m, LANES, tb_ref[2 * m + 1], tb_ref[2 * m + 2])

    mid = remote(sm_ref, sx_mid, halo_ss, halo_rs, 2, {'rows': across})

    sms, srs, hms, hrs = (sm1, sm2), (sr1, sr2), (hm1, hm2), (hr1, hr2)
    swaps, trades = [], []

    def columns(grp):
        start, n = GROUPS[grp]
        lane = lax.broadcasted_iota(jnp.int32, (n, LANES), 1)
        side = lane >> 6
        own_even, far_even = side == core, side != core
        block = (lane & (HALF - 1)) >> 4
        h = jnp.dot(g_ref[4 * start:4 * (start + n), :], ev_ref[...], preferred_element_type=F32)
        hc = [h[n * c:n * (c + 1)] for c in range(4)]
        rems = [v[:, 4 * LANES:] for v in hc]
        for cp in range(2):
            hs = [[v[:, LANES * i:LANES * (i + 1)] for i in range(4)] for v in hc[2 * cp:2 * cp + 2]]
            for i in range(4):
                dp, t = i // 2, i % 2
                odd = pltpu.roll(hs[1][i], HALF, axis=1)
                sms[grp][dp, cp, t] = jnp.where(far_even, hs[0][i], odd).astype(BF)
                hms[grp][dp, cp, t, core] = jnp.where(own_even, hs[0][i], odd).astype(BF)
        for d in range(ROWS):
            out = rems[d]
            for c in range(4):
                if c != d:
                    out = jnp.where(block == c, pltpu.roll(rems[c], (WIN * (c - d)) % LANES, axis=1), out)
            srs[grp][d] = out.astype(BF)
        hrs[grp][r] = srs[grp][r]
        swaps.append(remote(sms[grp], hms[grp].at[:, :, :, core], swap_ss, swap_rs, grp, {'rows': near}))
        for i, dev in enumerate((across, 3 - r, near)):
            trades.append(remote(srs[grp].at[dev], hrs[grp].at[r], swap_ss, swap_rs, 2 + 3 * grp + i, {'rows': dev}))

    columns(0)

    for h in halos:
        h.wait()
    lane = lax.broadcasted_iota(jnp.int32, (LANES, LANES), 1)
    low = lane < HALF
    t0s, t9s = [], []
    for j in range(5):
        rows = slice(LANES * j, LANES * (j + 1))
        add_first = pltpu.roll(halo[1], (HALF - HW * j) % LANES, axis=1)
        add_last = pltpu.roll(halo[0], (HALF - HW - HW * j) % LANES, axis=1)
        e = edge_ref[rows, :] + jnp.where(low, jnp.where(lane >= HALF - HW, add_last, 0.0), jnp.where(lane < HALF + HW, add_first, 0.0))
        t0s.append(jnp.where(low, tb_ref[0, rows, :].astype(F32), e).astype(BF))
        t9s.append(jnp.where(low, e, tb_ref[9, rows, :].astype(F32)).astype(BF))
    lane = lax.broadcasted_iota(jnp.int32, (PB, LANES), 1)
    low = lane < HALF
    to_rows(4 * LANES, QTR, jnp.concatenate(t0s, axis=0), jnp.concatenate(t9s, axis=0))
    columns(1)

    def turn(rows):
        t = [rows[:, LANES * i:LANES * (i + 1)].T for i in range(5)]
        return [jnp.concatenate([t[2 * i], t[2 * i + 1], t[4][HALF * i:HALF * (i + 1)]], axis=0) for i in range(2)]


    for cp in swaps[:1]:
        cp.wait_recv()
    n0 = 4 * GROUPS[0][1]

    def block_of(grp, j):
        return jnp.concatenate([hms[grp][(x + j) % 2, cp].reshape(4 * GROUPS[grp][1], LANES) for cp in range(2)], axis=1)

    mid.wait_recv()
    for j, ref, end in ((1, sx_ref, sx_mid), (0, so_ref, sm_ref)):
        c = [ref[HALF * i:HALF * (i + 1), :] for i in range(3)] + [jnp.concatenate([ref[3 * HALF:, :], end[...]], axis=0)]
        acc_m[j] = jnp.dot(eu_ref[x, :, :n0], block_of(0, j), preferred_element_type=F32)
        for cp in range(2):
            s_main[j, 0, cp], s_main[j, 1, cp] = turn(jnp.concatenate([jnp.where(core == 0, c[2 * cp], c[2 * cp + 1]), jnp.where(core == 0, c[2 * cp + 1], c[2 * cp])], axis=0))

    for cp in swaps[1:]:
        cp.wait_recv()

    def rows_dft(half, acc, rhs):
        rows = pl.ds(pl.multiple_of(half * N_IMG, WIN), N_IMG)
        total = acc[rows, :] + jnp.dot(eu_ref[x, rows, n0:], rhs, preferred_element_type=F32)
        return total[:PB], total[PB:]

    quarter = lax.broadcasted_iota(jnp.int32, (PB // 4, LANES), 1) >> 5

    def piece(half, j):
        i_re, i_im = rows_dft(half, acc_m.at[j], block_of(1, j))
        rows = pl.ds(pl.multiple_of(half * PB, SUB), PB)
        re, im = None, None
        for cp in range(2):
            cols = slice(LANES * cp, LANES * (cp + 1))
            s_re, s_im = s_main[j, 0, cp, rows, :], s_main[j, 1, cp, rows, :]
            a = s_re * i_re[:, cols] + s_im * i_im[:, cols]
            b = s_re * i_im[:, cols] - s_im * i_re[:, cols]
            re, im = (a, b) if re is None else (re + a, im + b)
        return jnp.where(low, re + pltpu.roll(re, HALF, axis=1), im + pltpu.roll(im, HALF, axis=1))

    def rest(half):
        parts = []
        for o in range(2):
            rows = pl.ds(pl.multiple_of(half * N_IMG + PB * o, WIN), PB)
            parts.append(acc_r[0, rows, :] + pltpu.roll(acc_r[1, rows, :], HALF, axis=1))
        i_re, i_im = parts
        rows = pl.ds(pl.multiple_of(half * PB, SUB), PB)
        s_re, s_im = s_rem[0, rows, :], s_rem[1, rows, :]
        w = s_re * i_re + s_im * i_im + pltpu.roll(s_re * i_im - s_im * i_re, HALF, axis=1)
        w = w + pltpu.roll(w, LANES - QTR, axis=1)
        w = w + pltpu.roll(w, LANES - WIN, axis=1)
        w = jnp.where(lane < WIN, w, pltpu.roll(w, LANES - HALF + WIN, axis=1))
        out = w[:PB // 4]
        for g in range(1, 4):
            out = jnp.where(quarter == g, pltpu.roll(w[PB // 4 * g:PB // 4 * (g + 1)], QTR * g, axis=1), out)
        return out

    first, other = pl.ds(0, (QTR + WIN)), pl.ds((QTR + WIN), PB - (QTR + WIN))
    pieces[0] = piece(1 - k, 1)
    joined = remote(pieces.at[0, first], recvs.at[0, first], red_ss, red_rs, 0, homes[1])
    sends = [remote(pieces.at[0, other], recvs.at[0, other], red_ss, red_rs, 1, homes[0])]
    pieces[1] = piece(k, 1)
    sends.append(remote(pieces.at[1], recvs.at[1], red_ss, red_rs, 2, homes[1]))
    across_y = piece(1 - k, 0)
    pieces[2, (QTR + WIN):] = across_y[(QTR + WIN):]
    sends.append(remote(pieces.at[2, other], recvs.at[2, other], red_ss, red_rs, 4, homes[2]))
    for cp in trades:
        cp.wait_recv()
    for t in range(2):
        total = None
        for grp in range(2):
            kk = 2 * GROUPS[grp][1]
            for c in range(2):
                part = jnp.dot(eu_ref[c, :, n0 * grp + kk * t:n0 * grp + kk * (t + 1)], hrs[grp][2 * c:2 * c + 2].reshape(kk, LANES), preferred_element_type=F32)
                total = part if total is None else total + part
        acc_r[t] = total
    s_rem[0], s_rem[1] = turn(jnp.concatenate([se_ref[c] for c in range(4)] + [jnp.zeros((HALF, N_GRID), F32)], axis=0))
    tails[...] = rest(1 - k)
    tail = remote(tails, recvs_t, red_ss, red_rs, 3, homes[2])
    rem = rest(k)
    joined.wait_recv()
    pieces[2, :(QTR + WIN)] = across_y[:(QTR + WIN)] + recvs[0, :(QTR + WIN)]
    sends.append(remote(pieces.at[2, first], recvs.at[2, first], red_ss, red_rs, 5, homes[2]))
    main = piece(k, 0)
    d8 = jnp.broadcast_to(jnp.concatenate([d_ref[...][None, :], jnp.zeros((1, HALF), F32)], axis=1), (SUB, N_IMG + HALF))
    dq = d8
    for j in range(1, ROWS):
        dq = jnp.where(r == j, pltpu.roll(d8, N_IMG + HALF - QB * j, axis=1), dq)
    dp = jnp.where(k == 0, d8, pltpu.roll(d8, N_IMG + HALF - PB, axis=1))[:, :2 * LANES]
    dd = jnp.concatenate([dp] * WIN, axis=0).T[:PB] * dq[:1, :LANES]

    for cp in sends:
        cp.wait_recv()
    main = main + recvs[1] + recvs[2]
    main = jnp.concatenate([main[:(QTR + WIN)], main[(QTR + WIN):] + recvs[0, (QTR + WIN):]], axis=0)
    tail.wait_recv()
    rem = rem + recvs_t[...]
    for o in range(2):
        m = pltpu.roll(main, HALF, axis=1) if o else main
        for j in range(4):
            rows = slice(PB // 4 * j, PB // 4 * (j + 1))
            end = pltpu.roll(rem, (HALF - QTR * j - WIN * o) % LANES, axis=1)
            out_ref[o, rows, :] = (jnp.where(low[rows], m[rows], end) * dd[rows])[:, :QB]

    for cp in sends + swaps + trades + [mid, tail, joined]:
        cp.wait_send()


def solution(mesh):
    sample_spec = ('exam', 'rows', 'cols')
    vm = pl.BlockSpec(memory_space=pltpu.VMEM)
    hbm = pl.BlockSpec(memory_space=pltpu.HBM)
    spread_scratch = ([VMEM((LANES, LANES), F32)] * 4 + [VMEM((LANES * PS, LANES), F32)] * 2
                      + [VMEM((LANES, WIDE * 3), BF), VMEM((NB, LANES), jnp.int32), pltpu.SMEM((NB, LANES), jnp.int32), pltpu.SemaphoreType.DMA])
    acc_shape = [jax.ShapeDtypeStruct((NG * CW, LANES), F32)] * T
    big = 6 * MIB

    def local_fn(kspace, wts_y, wts_x, idx_y, idx_x, coil_maps, deapod):
        own, far, maps, maps_end, maps_mid = pl.pallas_call(
            prep_kernel,
            out_shape=[jax.ShapeDtypeStruct((PAY * NB, LANES), F32)] * 2 + [jax.ShapeDtypeStruct(d, F32) for d in ((MAPS, N_GRID), (4, WIN, N_GRID), (WIN, N_GRID))],
            in_specs=[hbm] * 6, out_specs=[vm] * 5, name='prep',
            scratch_shapes=[VMEM((2, SUB, NS), F32), VMEM((KW, NS), F32), VMEM((KW, NS), F32), VMEM((NB, LANES), jnp.int32), VMEM((NB, LANES), jnp.int32), VMEM((2, 4, QB, HALF), F32), pltpu.SemaphoreType.DMA((24,))],
            compiler_params=pltpu.CompilerParams(vmem_limit_bytes=SUB * MIB),
        )(*[pltpu.with_memory_space_constraint(v, pltpu.HBM) for v in (kspace, wts_y, wts_x, idx_y.reshape(NB, LANES), idx_x.reshape(NB, LANES), jnp.swapaxes(coil_maps, 2, 3))])
        far_in = lax.ppermute(far, 'cols', [(0, 1), (1, 0)])
        half, *accs = pl.pallas_call(
            own_kernel, out_shape=[jax.ShapeDtypeStruct((11, CW, LANES), F32)] + acc_shape, in_specs=[vm], out_specs=[vm] * (T + 1),
            scratch_shapes=spread_scratch, compiler_params=pltpu.CompilerParams(vmem_limit_bytes=big), name='spread_own',
            cost_estimate=pl.CostEstimate(flops=GIGA, bytes_accessed=4 * MIB, transcendentals=0),
        )(own)
        *accs, pack = pl.pallas_call(
            far_kernel, out_shape=acc_shape + [jax.ShapeDtypeStruct((2, LANES, LANES), F32)],
            in_specs=[vm] * (T + 2), out_specs=[vm] * (T + 1), scratch_shapes=[VMEM((N_GRID, LANES), F32)] + spread_scratch,
            input_output_aliases={i + 2: i for i in range(T)},
            compiler_params=pltpu.CompilerParams(vmem_limit_bytes=big), name='spread_far',
            cost_estimate=pl.CostEstimate(flops=GIGA, bytes_accessed=4 * MIB, transcendentals=0),
        )(far_in, half, *accs)
        maps_x = lax.ppermute(maps, 'rows', [(i, (i + 2) % ROWS) for i in range(ROWS)])
        dma = pltpu.SemaphoreType.DMA
        half_bufs = [VMEM((2, 2, 2, n, LANES), BF) for _, n in GROUPS] + [VMEM((ROWS, n, LANES), BF) for _, n in GROUPS]
        full_bufs = [VMEM((2, 2, 2, 2, n, LANES), BF) for _, n in GROUPS] + [VMEM((ROWS, n, LANES), BF) for _, n in GROUPS]
        return pl.pallas_call(
            image_kernel,
            out_shape=jax.ShapeDtypeStruct((2, PB, QB), F32), in_specs=[vm] * (T + TILES), out_specs=vm,
            scratch_shapes=[VMEM((TILES, N_GRID, LANES), BF), VMEM((N_GRID, LANES), F32), VMEM((4 * RB, 2 * N_GRID), BF), VMEM((2, LANES, LANES), F32)] + half_bufs + full_bufs + [
                VMEM((2, 2, 2, N_IMG, LANES), F32), VMEM((2, N_IMG, LANES), F32),
                VMEM((2, 2 * N_IMG, 2 * LANES), F32), VMEM((2, 2 * N_IMG, LANES), F32), VMEM((WIN, N_GRID), F32),
                VMEM((3, PB, LANES), F32), VMEM((3, PB, LANES), F32), VMEM((PB // 4, LANES), F32), VMEM((PB // 4, LANES), F32),
                dma((3,)), dma((3,)), dma((8,)), dma((8,)), dma((6,)), dma((6,)),
            ],
            compiler_params=pltpu.CompilerParams(vmem_limit_bytes=11 * MIB, collective_id=0, has_side_effects=True), name='image',
        )(*accs, half, pack, maps, maps_x, maps_mid, maps_end, deapod, col_dft(), row_dft(), unmix())

    return jax.shard_map(
        local_fn,
        mesh=mesh,
        in_specs=(P(None, None, sample_spec), P(None, sample_spec), P(None, sample_spec), P(sample_spec), P(sample_spec), P(None, ('exam', 'cols'), None, 'rows'), P()),
        out_specs=P(None, ('exam', 'cols'), 'rows'),
        check_vma=False,
    )
```

```python
import functools
import math

import jax
import jax.numpy as jnp
import numpy as np
from jax import lax
from jax.experimental import pallas as pl
from jax.experimental.pallas import tpu as pltpu
from jax.sharding import PartitionSpec as P

BF = jnp.bfloat16
F32 = jnp.float32
VMEM = pltpu.VMEM
LANES = 128
MIB = 1 << 20
GIGA = 4000 * MIB
TILES = 10
SUB, WIN, QTR, HALF, WIDE = 8, 16, 32, 64, 256
N_GRID, N_IMG, N_COILS, KW = 640, 320, 8, 6
ROWS, COLS = 4, 2
RB, CB, QB = N_GRID // ROWS, N_GRID // COLS, N_IMG // ROWS
PB = N_IMG // COLS
NS = 4096
NB = NS // LANES
STEP = 11
NG = 15
CW = CB + WIN
T = 7
PS = 9
PAY = 21
CODE = 512
JOIN = 56
CG = 4
MAPS = 240
HW = 24
ORDER = tuple(range(1, 9)) + (0, 9)
GROUPS = ((0, 128), (128, 32))
MESH_ID = pl.DeviceIdType.MESH


def dft_parts():
    freq = np.arange(N_GRID) - N_GRID // 2
    pos = np.arange(N_IMG) - N_IMG // 2
    ang = ((freq[:, None] * pos[None, :]) % N_GRID).astype(np.float32) * np.float32(2.0 * math.pi / N_GRID)
    norm = np.float32(1.0 / math.sqrt(N_GRID))
    c, s = np.cos(ang) * norm, np.sin(ang) * norm
    return np.stack([np.stack([c, s], 1), np.stack([-s, c], 1)], 0)


def col_dft():
    e = dft_parts()
    out = np.zeros((2 * N_GRID, N_GRID), np.float32)
    for dp in range(2):
        for t in range(2):
            for h in range(2):
                q0 = QB * (2 * dp + h)
                l0 = LANES * (2 * dp + t) + HALF * h
                out[:, l0:l0 + HALF] = e[:, :, t, q0:q0 + HALF].reshape(2 * N_GRID, HALF)
    for t in range(2):
        for d in range(CG):
            l0 = 4 * LANES + HALF * t + WIN * d
            out[:, l0:l0 + WIN] = e[:, :, t, QB * d + HALF:QB * (d + 1)].reshape(2 * N_GRID, WIN)
    return jnp.asarray(out, BF)


def row_dft():
    e = dft_parts()
    rows = np.concatenate([np.arange(WIN * l, WIN * (l + 1)) for l in ORDER])
    chips = []
    for x in range(2):
        parts = []
        for start, n in GROUPS:
            for t in range(2):
                for b in range(2):
                    parts.append(e[t, (2 * x + b) * RB + rows[start:start + n]])
        m = np.concatenate(parts, 0)
        chips.append(np.concatenate([m[:, :, PB * h:PB * (h + 1)].reshape(N_GRID, N_IMG).T for h in range(2)], 0))
    return jnp.asarray(np.array(chips), BF)


def unmix():
    m = np.zeros((WIDE, WIDE), np.float32)
    for ch in range(SUB):
        for pp in range(2):
            for i in range(WIN):
                m[ch * QTR + WIN * pp + (i + SUB) % WIN, pp * 128 + i * SUB + ch] = 1.0
    return jnp.asarray(m, BF)


def prep_kernel(ks_hbm, wy_hbm, wx_hbm, iy_hbm, ix_hbm, maps_hbm, own_ref, far_ref, sp_ref, sq_ref, sm_ref, ks_ref, wy_ref, wx_ref, iy_ref, ix_ref, maps_ref, sem):
    k = lax.axis_index('cols')
    r = lax.axis_index('rows')
    loads = []
    for src, dst in ((iy_hbm, iy_ref), (ix_hbm, ix_ref), (wx_hbm, wx_ref), (wy_hbm, wy_ref), (ks_hbm, ks_ref), (maps_hbm.at[:, :, :, WIDE:], maps_ref)):
        cp = pltpu.make_async_copy(src, dst, sem.at[len(loads)])
        cp.start()
        loads.append(cp)
    parts = []
    for c in range(CG):
        n = min(HALF, MAPS - HALF * c)
        parts += [(sp_ref.at[pl.ds(HALF * c, n)], c, pl.ds(0, n)), (sq_ref.at[c], c, pl.ds(HALF, WIN))]
    parts.append((sm_ref, 3, pl.ds(HALF - WIN, WIN)))
    for ref, c, q in parts:
        for i in range(2):
            cp = pltpu.make_async_copy(maps_hbm.at[i, c, q, pl.ds(0, WIDE)], ref.at[:, pl.ds(WIDE * i, WIDE)], sem.at[len(loads)])
            cp.start()
            loads.append(cp)
    loads[0].wait()
    loads[1].wait()
    iy = iy_ref[...]
    code = ((iy - r * RB + 5) * CODE + ix_ref[...] - k * CB + 5).astype(F32)
    for i in range(2, 5):
        loads[i].wait()
    lo = jnp.concatenate([ks_ref[0, 0:4, :], ks_ref[1, 0:4, :]], axis=0)
    hi = jnp.concatenate([ks_ref[0, 4:SUB, :], ks_ref[1, 4:SUB, :]], axis=0)
    first = k == 0
    for ref, y in ((own_ref, jnp.where(first, lo, hi)), (far_ref, jnp.where(first, hi, lo))):
        for b in range(NB):
            cols = slice(LANES * b, LANES * (b + 1))
            ref[PAY * b:PAY * b + SUB, :] = y[:, cols]
            ref[PAY * b + SUB:PAY * b + SUB + KW, :] = wx_ref[:, cols]
            ref[PAY * (b + 1) - KW - 1:PAY * (b + 1) - 1, :] = wy_ref[:, cols]
            ref[PAY * (b + 1) - 1:PAY * (b + 1), :] = code[b:b + 1, :]
    loads[5].wait()
    for c in range(CG):
        end = jnp.concatenate([maps_ref[i, c] for i in range(2)], axis=1)
        n = min(HALF, MAPS - HALF * c)
        sp_ref[HALF * c:HALF * c + n, 2 * WIDE:] = end[:n]
        sq_ref[c, :, 2 * WIDE:] = end[HALF:]
        if n < HALF:
            sm_ref[:, 2 * WIDE:] = end[n:HALF]
    for cp in loads[KW:]:
        cp.wait()


def split3(x):
    hi = x.astype(BF).astype(F32)
    r = x - hi
    mid = r.astype(BF).astype(F32)
    return hi, mid, r - mid


def accumulate(pay_ref, accs, us, xs, vs, r_ref, int_ref, base_ref, sem):
    row_i = lax.broadcasted_iota(jnp.int32, (WIN, LANES), 0)

    def make_u(blk, k):
        off = jnp.minimum(blk, NB - 1) * PAY
        y8 = pay_ref[pl.ds(off, SUB), :]
        wx = pay_ref[pl.ds(off + SUB, SUB), :]
        wyp = pay_ref[pl.ds(off + PAY - SUB, SUB), :]
        d = (row_i - (wyp[7:, :].astype(jnp.int32) // CODE)) & (WIN - 1)
        p = jnp.zeros((WIN, LANES), F32)
        for a in range(KW):
            p = jnp.where(d == a, wyp[a + 1:a + 2, :], p)
        us[k][...] = jnp.concatenate([y8 * p[i:i + 1, :] for i in range(WIN)], axis=0).T
        x3 = list(split3(wx)) + [jnp.zeros((LANES - HW, LANES), F32)]
        xs[k][...] = jnp.concatenate(x3, axis=0).T

    def make_v(k):
        lhs = xs[k][...].astype(BF)
        u = us[k][...]
        for bp in range(3):
            w = jnp.dot(lhs, r_ref[:, WIDE * bp:WIDE * bp + WIDE], preferred_element_type=F32)
            for c in range(2):
                v = w[:, LANES * c:LANES * (c + 1)] * u
                for g in range(WIN):
                    vs[k][pl.ds(SUB * PS * g + 2 * bp + c, SUB, stride=PS), :] = v[SUB * g:SUB * g + SUB, :]

    def add_tiles(blk, k):
        row = base_ref.at[blk]
        for j in range(LANES):
            acc = accs[j % T]
            b = row[j]
            acc[pl.ds(b, SUB), :] = acc[pl.ds(b, SUB), :] + vs[k][PS * j:PS * j + SUB, :]

    code = jnp.concatenate([pay_ref[PAY * (b + 1) - 1:PAY * (b + 1), :] for b in range(NB)], axis=0).astype(jnp.int32)
    int_ref[...] = (((code // CODE - 5) * 187) >> STEP) * CW + (code & (CODE - 1))
    kk = lax.broadcasted_iota(jnp.int32, (LANES, WIDE * 3), 0)
    ll = lax.broadcasted_iota(jnp.int32, (LANES, WIDE * 3), 1)
    r_ref[...] = jnp.where((kk < HW) & ((kk & 7) == (ll >> 7)), 1.0, 0.0).astype(BF)
    for v in vs:
        v[...] = jnp.zeros_like(v)
    load = pltpu.make_async_copy(int_ref, base_ref, sem)
    load.start()
    make_u(0, 0)
    make_u(1, 1)
    make_v(0)
    load.wait()

    def body(n, _):
        k = 2 * n
        make_v(1)
        add_tiles(k, 0)
        make_u(k + 2, 0)
        make_v(0)
        add_tiles(k + 1, 1)
        make_u(k + 3, 1)
        return 0

    lax.fori_loop(0, NB // 2, body, 0)


def folded(accs, off, n, clear=False):
    def total(g):
        rows = pl.ds(pl.multiple_of(g * CW + off, SUB), n)
        v = accs[0][rows, :]
        for a in accs[1:]:
            v = v + a[rows, :]
        if clear:
            for a in accs:
                a[rows, :] = jnp.zeros((n, LANES), F32)
        return v

    row = lax.broadcasted_iota(jnp.int32, (n, LANES), 1) >> 3
    tiles = [None] * TILES
    for g in range(NG):
        v = total(g)
        if g == 0:
            ghost = v
        first = 5 + STEP * g
        for p in range(TILES):
            lo, hi = max(first, SUB + WIN * p), min(first + WIN, SUB + WIN * (p + 1))
            if lo < hi:
                part = jnp.where((row - lo & (WIN - 1)) < hi - lo, v, 0.0)
                tiles[p] = part if tiles[p] is None else tiles[p] + part
    return tiles + [jnp.where(row >= SUB, v, ghost)]


def own_kernel(pay_ref, out_ref, *refs):
    accs, scr = refs[:T], refs[T:]

    def clear(n, _):
        for a in accs:
            a[pl.ds(pl.multiple_of(n * CW, SUB), CW), :] = jnp.zeros((CW, LANES), F32)
        return 0

    lax.fori_loop(0, NG, clear, 0)
    accumulate(pay_ref, accs, scr[:2], scr[2:4], scr[4:6], *scr[6:])

    def fold(q, _):
        off = pl.multiple_of(q * WIN, WIN)
        for p, t in enumerate(folded(accs, off, WIN, clear=True)):
            out_ref[p, pl.ds(off, WIN), :] = t
        return 0

    lax.fori_loop(0, CW // WIN, fold, 0)


def far_kernel(pay_ref, a_ref, *refs):
    accs, pack_ref, gh_ref, scr = refs[T:2 * T], refs[2 * T], refs[2 * T + 1], refs[2 * T + 2:]
    accumulate(pay_ref, accs, scr[:2], scr[2:4], scr[4:6], *scr[6:])
    own0 = lax.axis_index('cols') * CB
    far0 = CB - own0

    def ghost(off, n):
        high = lax.broadcasted_iota(jnp.int32, (n, LANES), 1) >= HALF
        ends = []
        for g in (0, NG - 1):
            rows = pl.ds(pl.multiple_of(g * CW + off, SUB), n)
            v = accs[0][rows, :]
            for a in accs[1:]:
                v = v + a[rows, :]
            ends.append(v)
        return jnp.where(high, ends[1], ends[0])

    def copy(n, _):
        o = pl.multiple_of(n * QTR, SUB)
        gh_ref[pl.ds(pl.multiple_of(far0 + o, SUB), QTR), :] = ghost(SUB + o, QTR)
        gh_ref[pl.ds(pl.multiple_of(own0 + o, SUB), QTR), :] = a_ref[TILES, pl.ds(pl.multiple_of(SUB + o, SUB), QTR), :]
        return 0

    lax.fori_loop(0, CB // QTR, copy, 0)
    for dst, add in ((own0, ghost(CW - SUB, SUB)), (own0 + CB - SUB, ghost(0, SUB)), (far0, a_ref[TILES, CW - SUB:, :]), (far0 + CB - SUB, a_ref[TILES, :SUB, :])):
        rows = pl.ds(pl.multiple_of(dst, SUB), SUB)
        gh_ref[rows, :] = gh_ref[rows, :] + add

    lane = lax.broadcasted_iota(jnp.int32, (LANES, LANES), 1)
    for side, lane0 in ((0, HALF - HW), (1, HALF)):
        out = jnp.zeros((LANES, LANES), F32)
        for j in range(5):
            piece = pltpu.roll(gh_ref[LANES * j:LANES * (j + 1), :], (HW * j - lane0) % LANES, axis=1)
            out = jnp.where(lane >= HW * j, piece, out)
        pack_ref[side] = out


def image_kernel(*refs):
    accs = refs[:T]
    (a_ref, pack_ref, so_ref, sx_ref, sm_ref, se_ref, d_ref, ev_ref, eu_ref, pm_ref, out_ref,
     tb_ref, edge_ref, g_ref, halo, sm1, sm2, sr1, sr2, hm1, hm2, hr1, hr2, s_main, s_rem, acc_m, acc_r, sx_mid, pieces, recvs, tails, recvs_t,
     halo_ss, halo_rs, swap_ss, swap_rs, red_ss, red_rs) = refs[T:]
    k = lax.axis_index('cols')
    r = lax.axis_index('rows')
    core, x = r % 2, r // 2
    near = r + 1 - 2 * core
    across = (r + 2) % 4
    prev, nxt = (r + 3) % 4, (r + 1) % 4
    homes = ({'rows': across, 'cols': 1 - k}, {'rows': across}, {'cols': 1 - k})

    barrier = pltpu.get_barrier_semaphore()
    for dev in ({'rows': prev}, {'rows': nxt}) + homes:
        pl.semaphore_signal(barrier, inc=1, device_id=dev, device_id_type=MESH_ID)

    own0 = k * CB
    far0 = CB - own0
    high16 = lax.broadcasted_iota(jnp.int32, (WIN, LANES), 1) >= HALF

    def put(v, tiles):
        rows = pl.ds(pl.multiple_of(v, WIN), WIN)
        for p in range(TILES):
            tb_ref[p, rows, :] = tiles[p].astype(BF)
        edge_ref[rows, :] = jnp.where(high16, tiles[0], tiles[9])

    def far_part(n, _):
        put(far0 + WIN * n, folded(accs, pl.multiple_of(SUB + WIN * n, SUB), WIN))
        return 0

    def own_part(n, _):
        put(own0 + WIN * n, [a_ref[p, pl.ds(pl.multiple_of(SUB + WIN * n, SUB), WIN), :] for p in range(TILES)])
        return 0

    last = CB // WIN - 1
    lax.fori_loop(1, last, far_part, 0)
    pl.semaphore_wait(barrier, 5)

    def remote(src, dst, ss, rs, i, dev):
        cp = pltpu.make_async_remote_copy(src_ref=src, dst_ref=dst, send_sem=ss.at[i], recv_sem=rs.at[i], device_id=dev, device_id_type=MESH_ID)
        cp.start()
        return cp

    halos = [remote(pack_ref.at[i], halo.at[i], halo_ss, halo_rs, i, {'rows': dev}) for i, dev in ((0, prev), (1, nxt))]

    lax.fori_loop(1, last, own_part, 0)
    none = jnp.zeros((SUB, LANES), F32)
    for n, side in ((0, CW - SUB), (last, 0)):
        off = SUB + WIN * n
        near_tiles = folded(accs, off, WIN)
        far_ends = folded(accs, side, SUB)
        order = (lambda v: [v, none]) if n == 0 else (lambda v: [none, v])
        put(far0 + WIN * n, [near_tiles[p] + jnp.concatenate(order(a_ref[p, side:side + SUB, :]), axis=0) for p in range(TILES)])
        put(own0 + WIN * n, [a_ref[p, off:off + WIN, :] + jnp.concatenate(order(far_ends[p]), axis=0) for p in range(TILES)])


    def to_rows(row0, n, t0, t1):
        a = jnp.concatenate([t0, t1], axis=1)
        g = lax.dot_general(pm_ref[...], a, (((1,), (1,)), ((), ())), preferred_element_type=F32).astype(BF)
        for ch in range(SUB):
            i, c = ch // 4, ch % 4
            g_ref[row0 + n * c:row0 + n * c + QTR, N_GRID * i:N_GRID * (i + 1)] = g[QTR * ch:QTR * (ch + 1), :]

    for m in range(CG):
        to_rows(QTR * m, LANES, tb_ref[2 * m + 1], tb_ref[2 * m + 2])

    mid = remote(sm_ref, sx_mid, halo_ss, halo_rs, 2, {'rows': across})

    sms, srs, hms, hrs = (sm1, sm2), (sr1, sr2), (hm1, hm2), (hr1, hr2)
    swaps, trades = [], []

    def columns(grp):
        start, n = GROUPS[grp]
        lane = lax.broadcasted_iota(jnp.int32, (n, LANES), 1)
        side = lane >> 6
        own_even, far_even = side == core, side != core
        block = (lane & (HALF - 1)) >> 4
        h = jnp.dot(g_ref[4 * start:4 * (start + n), :], ev_ref[...], preferred_element_type=F32)
        hc = [h[n * c:n * (c + 1)] for c in range(CG)]
        rems = [v[:, 4 * LANES:] for v in hc]
        for cp in range(2):
            hs = [[v[:, LANES * i:LANES * (i + 1)] for i in range(CG)] for v in hc[2 * cp:2 * cp + 2]]
            for i in range(CG):
                dp, t = i // 2, i % 2
                odd = pltpu.roll(hs[1][i], HALF, axis=1)
                sms[grp][dp, cp, t] = jnp.where(far_even, hs[0][i], odd).astype(BF)
                hms[grp][dp, cp, t, core] = jnp.where(own_even, hs[0][i], odd).astype(BF)
        for d in range(ROWS):
            out = rems[d]
            for c in range(CG):
                if c != d:
                    out = jnp.where(block == c, pltpu.roll(rems[c], (WIN * (c - d)) % LANES, axis=1), out)
            srs[grp][d] = out.astype(BF)
        hrs[grp][r] = srs[grp][r]
        swaps.append(remote(sms[grp], hms[grp].at[:, :, :, core], swap_ss, swap_rs, grp, {'rows': near}))
        for i, dev in enumerate((across, 3 - r, near)):
            trades.append(remote(srs[grp].at[dev], hrs[grp].at[r], swap_ss, swap_rs, 2 + 3 * grp + i, {'rows': dev}))

    columns(0)

    for h in halos:
        h.wait()
    lane = lax.broadcasted_iota(jnp.int32, (LANES, LANES), 1)
    low = lane < HALF
    t0s, t9s = [], []
    for j in range(5):
        rows = slice(LANES * j, LANES * (j + 1))
        add_first = pltpu.roll(halo[1], (HALF - HW * j) % LANES, axis=1)
        add_last = pltpu.roll(halo[0], (HALF - HW - HW * j) % LANES, axis=1)
        e = edge_ref[rows, :] + jnp.where(low, jnp.where(lane >= HALF - HW, add_last, 0.0), jnp.where(lane < HALF + HW, add_first, 0.0))
        t0s.append(jnp.where(low, tb_ref[0, rows, :].astype(F32), e).astype(BF))
        t9s.append(jnp.where(low, e, tb_ref[9, rows, :].astype(F32)).astype(BF))
    lane = lax.broadcasted_iota(jnp.int32, (PB, LANES), 1)
    low = lane < HALF
    to_rows(4 * LANES, QTR, jnp.concatenate(t0s, axis=0), jnp.concatenate(t9s, axis=0))
    columns(1)

    def turn(rows):
        t = [rows[:, LANES * i:LANES * (i + 1)].T for i in range(5)]
        return [jnp.concatenate([t[2 * i], t[2 * i + 1], t[4][HALF * i:HALF * (i + 1)]], axis=0) for i in range(2)]


    for cp in swaps[:1]:
        cp.wait_recv()
    n0 = 4 * GROUPS[0][1]

    def block_of(grp, j):
        return jnp.concatenate([hms[grp][(x + j) % 2, cp].reshape(4 * GROUPS[grp][1], LANES) for cp in range(2)], axis=1)

    mid.wait_recv()
    for j, ref, end in ((1, sx_ref, sx_mid), (0, so_ref, sm_ref)):
        c = [ref[HALF * i:HALF * (i + 1), :] for i in range(3)] + [jnp.concatenate([ref[3 * HALF:, :], end[...]], axis=0)]
        acc_m[j] = jnp.dot(eu_ref[x, :, :n0], block_of(0, j), preferred_element_type=F32)
        for cp in range(2):
            s_main[j, 0, cp], s_main[j, 1, cp] = turn(jnp.concatenate([jnp.where(core == 0, c[2 * cp], c[2 * cp + 1]), jnp.where(core == 0, c[2 * cp + 1], c[2 * cp])], axis=0))

    for cp in swaps[1:]:
        cp.wait_recv()

    def rows_dft(half, acc, rhs):
        rows = pl.ds(pl.multiple_of(half * N_IMG, WIN), N_IMG)
        total = acc[rows, :] + jnp.dot(eu_ref[x, rows, n0:], rhs, preferred_element_type=F32)
        return total[:PB], total[PB:]

    quarter = lax.broadcasted_iota(jnp.int32, (PB // 4, LANES), 1) >> 5

    def piece(half, j):
        i_re, i_im = rows_dft(half, acc_m.at[j], block_of(1, j))
        rows = pl.ds(pl.multiple_of(half * PB, SUB), PB)
        re, im = None, None
        for cp in range(2):
            cols = slice(LANES * cp, LANES * (cp + 1))
            s_re, s_im = s_main[j, 0, cp, rows, :], s_main[j, 1, cp, rows, :]
            a = s_re * i_re[:, cols] + s_im * i_im[:, cols]
            b = s_re * i_im[:, cols] - s_im * i_re[:, cols]
            re, im = (a, b) if re is None else (re + a, im + b)
        return jnp.where(low, re + pltpu.roll(re, HALF, axis=1), im + pltpu.roll(im, HALF, axis=1))

    def rest(half):
        parts = []
        for o in range(2):
            rows = pl.ds(pl.multiple_of(half * N_IMG + PB * o, WIN), PB)
            parts.append(acc_r[0, rows, :] + pltpu.roll(acc_r[1, rows, :], HALF, axis=1))
        i_re, i_im = parts
        rows = pl.ds(pl.multiple_of(half * PB, SUB), PB)
        s_re, s_im = s_rem[0, rows, :], s_rem[1, rows, :]
        w = s_re * i_re + s_im * i_im + pltpu.roll(s_re * i_im - s_im * i_re, HALF, axis=1)
        w = w + pltpu.roll(w, LANES - QTR, axis=1)
        w = w + pltpu.roll(w, LANES - WIN, axis=1)
        w = jnp.where(lane < WIN, w, pltpu.roll(w, LANES - HALF + WIN, axis=1))
        out = w[:PB // 4]
        for g in range(1, 4):
            out = jnp.where(quarter == g, pltpu.roll(w[PB // 4 * g:PB // 4 * (g + 1)], QTR * g, axis=1), out)
        return out

    first, other = pl.ds(0, JOIN), pl.ds(JOIN, PB - JOIN)
    pieces[0] = piece(1 - k, 1)
    joined = remote(pieces.at[0, first], recvs.at[0, first], red_ss, red_rs, 0, homes[1])
    sends = [remote(pieces.at[0, other], recvs.at[0, other], red_ss, red_rs, 1, homes[0])]
    pieces[1] = piece(k, 1)
    sends.append(remote(pieces.at[1], recvs.at[1], red_ss, red_rs, 2, homes[1]))
    across_y = piece(1 - k, 0)
    pieces[2, JOIN:] = across_y[JOIN:]
    sends.append(remote(pieces.at[2, other], recvs.at[2, other], red_ss, red_rs, 4, homes[2]))
    for cp in trades:
        cp.wait_recv()
    for t in range(2):
        total = None
        for grp in range(2):
            kk = 2 * GROUPS[grp][1]
            for c in range(2):
                part = jnp.dot(eu_ref[c, :, n0 * grp + kk * t:n0 * grp + kk * (t + 1)], hrs[grp][2 * c:2 * c + 2].reshape(kk, LANES), preferred_element_type=F32)
                total = part if total is None else total + part
        acc_r[t] = total
    s_rem[0], s_rem[1] = turn(jnp.concatenate([se_ref[c] for c in range(CG)] + [jnp.zeros((HALF, N_GRID), F32)], axis=0))
    tails[...] = rest(1 - k)
    tail = remote(tails, recvs_t, red_ss, red_rs, 3, homes[2])
    rem = rest(k)
    joined.wait_recv()
    pieces[2, :JOIN] = across_y[:JOIN] + recvs[0, :JOIN]
    sends.append(remote(pieces.at[2, first], recvs.at[2, first], red_ss, red_rs, 5, homes[2]))
    main = piece(k, 0)
    d8 = jnp.broadcast_to(jnp.concatenate([d_ref[...][None, :], jnp.zeros((1, HALF), F32)], axis=1), (SUB, N_IMG + HALF))
    dq = d8
    for j in range(1, ROWS):
        dq = jnp.where(r == j, pltpu.roll(d8, N_IMG + HALF - QB * j, axis=1), dq)
    dp = jnp.where(k == 0, d8, pltpu.roll(d8, N_IMG + HALF - PB, axis=1))[:, :2 * LANES]
    dd = jnp.concatenate([dp] * WIN, axis=0).T[:PB] * dq[:1, :LANES]

    for cp in sends:
        cp.wait_recv()
    main = main + recvs[1] + recvs[2]
    main = jnp.concatenate([main[:JOIN], main[JOIN:] + recvs[0, JOIN:]], axis=0)
    tail.wait_recv()
    rem = rem + recvs_t[...]
    for o in range(2):
        m = pltpu.roll(main, HALF, axis=1) if o else main
        for j in range(CG):
            rows = slice(PB // 4 * j, PB // 4 * (j + 1))
            end = pltpu.roll(rem, (HALF - QTR * j - WIN * o) % LANES, axis=1)
            out_ref[o, rows, :] = (jnp.where(low[rows], m[rows], end) * dd[rows])[:, :QB]

    for cp in sends + swaps + trades + [mid, tail, joined]:
        cp.wait_send()


def solution(mesh):
    sample_spec = ('exam', 'rows', 'cols')
    vm = pl.BlockSpec(memory_space=pltpu.VMEM)
    hbm = pl.BlockSpec(memory_space=pltpu.HBM)
    spread_scratch = ([VMEM((LANES, LANES), F32)] * 4 + [VMEM((LANES * PS, LANES), F32)] * 2
                      + [VMEM((LANES, WIDE * 3), BF), VMEM((NB, LANES), jnp.int32), pltpu.SMEM((NB, LANES), jnp.int32), pltpu.SemaphoreType.DMA])
    acc_shape = [jax.ShapeDtypeStruct((NG * CW, LANES), F32)] * T
    big = 6 * MIB

    def local_fn(kspace, wts_y, wts_x, idx_y, idx_x, coil_maps, deapod):
        own, far, maps, maps_end, maps_mid = pl.pallas_call(
            prep_kernel,
            out_shape=[jax.ShapeDtypeStruct((PAY * NB, LANES), F32)] * 2 + [jax.ShapeDtypeStruct(d, F32) for d in ((MAPS, N_GRID), (4, WIN, N_GRID), (WIN, N_GRID))],
            in_specs=[hbm] * 6, out_specs=[vm] * 5, name='prep',
            scratch_shapes=[VMEM((2, SUB, NS), F32), VMEM((KW, NS), F32), VMEM((KW, NS), F32), VMEM((NB, LANES), jnp.int32), VMEM((NB, LANES), jnp.int32), VMEM((2, 4, QB, HALF), F32), pltpu.SemaphoreType.DMA((24,))],
            compiler_params=pltpu.CompilerParams(vmem_limit_bytes=SUB * MIB),
        )(*[pltpu.with_memory_space_constraint(v, pltpu.HBM) for v in (kspace, wts_y, wts_x, idx_y.reshape(NB, LANES), idx_x.reshape(NB, LANES), jnp.swapaxes(coil_maps, 2, 3))])
        far_in = lax.ppermute(far, 'cols', [(0, 1), (1, 0)])
        half, *accs = pl.pallas_call(
            own_kernel, out_shape=[jax.ShapeDtypeStruct((11, CW, LANES), F32)] + acc_shape, in_specs=[vm], out_specs=[vm] * (T + 1),
            scratch_shapes=spread_scratch, compiler_params=pltpu.CompilerParams(vmem_limit_bytes=big), name='spread_own',
            cost_estimate=pl.CostEstimate(flops=GIGA, bytes_accessed=4 * MIB, transcendentals=0),
        )(own)
        *accs, pack = pl.pallas_call(
            far_kernel, out_shape=acc_shape + [jax.ShapeDtypeStruct((2, LANES, LANES), F32)],
            in_specs=[vm] * (T + 2), out_specs=[vm] * (T + 1), scratch_shapes=[VMEM((N_GRID, LANES), F32)] + spread_scratch,
            input_output_aliases={i + 2: i for i in range(T)},
            compiler_params=pltpu.CompilerParams(vmem_limit_bytes=big), name='spread_far',
            cost_estimate=pl.CostEstimate(flops=GIGA, bytes_accessed=4 * MIB, transcendentals=0),
        )(far_in, half, *accs)
        maps_x = lax.ppermute(maps, 'rows', [(i, (i + 2) % ROWS) for i in range(ROWS)])
        dma = pltpu.SemaphoreType.DMA
        half_bufs = [VMEM((2, 2, 2, n, LANES), BF) for _, n in GROUPS] + [VMEM((ROWS, n, LANES), BF) for _, n in GROUPS]
        full_bufs = [VMEM((2, 2, 2, 2, n, LANES), BF) for _, n in GROUPS] + [VMEM((ROWS, n, LANES), BF) for _, n in GROUPS]
        return pl.pallas_call(
            image_kernel,
            out_shape=jax.ShapeDtypeStruct((2, PB, QB), F32), in_specs=[vm] * (T + TILES), out_specs=vm,
            scratch_shapes=[VMEM((TILES, N_GRID, LANES), BF), VMEM((N_GRID, LANES), F32), VMEM((4 * RB, 2 * N_GRID), BF), VMEM((2, LANES, LANES), F32)] + half_bufs + full_bufs + [
                VMEM((2, 2, 2, N_IMG, LANES), F32), VMEM((2, N_IMG, LANES), F32),
                VMEM((2, 2 * N_IMG, 2 * LANES), F32), VMEM((2, 2 * N_IMG, LANES), F32), VMEM((WIN, N_GRID), F32),
                VMEM((3, PB, LANES), F32), VMEM((3, PB, LANES), F32), VMEM((PB // 4, LANES), F32), VMEM((PB // 4, LANES), F32),
                dma((3,)), dma((3,)), dma((8,)), dma((8,)), dma((6,)), dma((6,)),
            ],
            compiler_params=pltpu.CompilerParams(vmem_limit_bytes=11 * MIB, collective_id=0, has_side_effects=True), name='image',
        )(*accs, half, pack, maps, maps_x, maps_mid, maps_end, deapod, col_dft(), row_dft(), unmix())

    return jax.shard_map(
        local_fn,
        mesh=mesh,
        in_specs=(P(None, None, sample_spec), P(None, sample_spec), P(None, sample_spec), P(sample_spec), P(sample_spec), P(None, ('exam', 'cols'), None, 'rows'), P()),
        out_specs=P(None, ('exam', 'cols'), 'rows'),
        check_vma=False,
    )
```

```python
import functools
import math

import jax
import jax.numpy as jnp
import numpy as np
from jax import lax
from jax.experimental import pallas as pl
from jax.experimental.pallas import tpu as pltpu
from jax.sharding import PartitionSpec as P

BF = jnp.bfloat16
F32 = jnp.float32
VMEM = pltpu.VMEM
LANES = 128
MIB = 1 << 20
GIGA = 4000 * MIB
TILES = 10
SUB, WIN, QTR, HALF, WIDE = 8, 16, 32, 64, 256
N_GRID, N_IMG, N_COILS, KW = 640, 320, 8, 6
ROWS, COLS = 4, 2
RB, CB, QB = N_GRID // ROWS, N_GRID // COLS, N_IMG // ROWS
PB = N_IMG // COLS
NS = 4096
NB = NS // LANES
STEP = 11
NG = 15
CW = CB + WIN
T = 7
PS = 9
PAY = 21
CODE = 512
JOIN = 56
CG = 4
MAPS = 240
HW = 24
ORDER = tuple(range(1, 9)) + (0, 9)
GROUPS = ((0, 128), (128, 32))
MESH_ID = pl.DeviceIdType.MESH


def dft_parts():
    freq = np.arange(N_GRID) - N_GRID // 2
    pos = np.arange(N_IMG) - N_IMG // 2
    ang = ((freq[:, None] * pos[None, :]) % N_GRID).astype(np.float32) * np.float32(2.0 * math.pi / N_GRID)
    norm = np.float32(1.0 / math.sqrt(N_GRID))
    c, s = np.cos(ang) * norm, np.sin(ang) * norm
    return np.stack([np.stack([c, s], 1), np.stack([-s, c], 1)], 0)


def col_dft():
    e = dft_parts()
    out = np.zeros((2 * N_GRID, N_GRID), np.float32)
    for dp in range(2):
        for t in range(2):
            for h in range(2):
                q0 = QB * (2 * dp + h)
                l0 = LANES * (2 * dp + t) + HALF * h
                out[:, l0:l0 + HALF] = e[:, :, t, q0:q0 + HALF].reshape(2 * N_GRID, HALF)
    for t in range(2):
        for d in range(CG):
            l0 = 4 * LANES + HALF * t + WIN * d
            out[:, l0:l0 + WIN] = e[:, :, t, QB * d + HALF:QB * (d + 1)].reshape(2 * N_GRID, WIN)
    return jnp.asarray(out, BF)


def row_dft():
    e = dft_parts()
    rows = np.concatenate([np.arange(WIN * l, WIN * (l + 1)) for l in ORDER])
    chips = []
    for x in range(2):
        parts = []
        for start, n in GROUPS:
            for t in range(2):
                for b in range(2):
                    parts.append(e[t, (2 * x + b) * RB + rows[start:start + n]])
        m = np.concatenate(parts, 0)
        chips.append(np.concatenate([m[:, :, PB * h:PB * (h + 1)].reshape(N_GRID, N_IMG).T for h in range(2)], 0))
    return jnp.asarray(np.array(chips), BF)


def unmix():
    m = np.zeros((WIDE, WIDE), np.float32)
    for ch in range(SUB):
        for pp in range(2):
            for i in range(WIN):
                m[ch * QTR + WIN * pp + (i + SUB) % WIN, pp * 128 + i * SUB + ch] = 1.0
    return jnp.asarray(m, BF)


def prep_kernel(ks_hbm, wy_hbm, wx_hbm, iy_hbm, ix_hbm, maps_hbm, own_ref, far_ref, sp_ref, sq_ref, sm_ref, ks_ref, wy_ref, wx_ref, iy_ref, ix_ref, maps_ref, sem):
    k = lax.axis_index('cols')
    r = lax.axis_index('rows')
    loads = []
    for src, dst in ((iy_hbm, iy_ref), (ix_hbm, ix_ref), (wx_hbm, wx_ref), (wy_hbm, wy_ref), (ks_hbm, ks_ref), (maps_hbm.at[:, :, :, WIDE:], maps_ref)):
        cp = pltpu.make_async_copy(src, dst, sem.at[len(loads)])
        cp.start()
        loads.append(cp)
    parts = []
    for c in range(CG):
        n = min(HALF, MAPS - HALF * c)
        parts += [(sp_ref.at[pl.ds(HALF * c, n)], c, pl.ds(0, n)), (sq_ref.at[c], c, pl.ds(HALF, WIN))]
    parts.append((sm_ref, 3, pl.ds(HALF - WIN, WIN)))
    for ref, c, q in parts:
        for i in range(2):
            cp = pltpu.make_async_copy(maps_hbm.at[i, c, q, pl.ds(0, WIDE)], ref.at[:, pl.ds(WIDE * i, WIDE)], sem.at[len(loads)])
            cp.start()
            loads.append(cp)
    loads[0].wait()
    loads[1].wait()
    iy = iy_ref[...]
    code = ((iy - r * RB + 5) * CODE + ix_ref[...] - k * CB + 5).astype(F32)
    for i in range(2, 5):
        loads[i].wait()
    lo = jnp.concatenate([ks_ref[0, 0:4, :], ks_ref[1, 0:4, :]], axis=0)
    hi = jnp.concatenate([ks_ref[0, 4:SUB, :], ks_ref[1, 4:SUB, :]], axis=0)
    first = k == 0
    for ref, y in ((own_ref, jnp.where(first, lo, hi)), (far_ref, jnp.where(first, hi, lo))):
        for b in range(NB):
            cols = slice(LANES * b, LANES * (b + 1))
            ref[PAY * b:PAY * b + SUB, :] = y[:, cols]
            ref[PAY * b + SUB:PAY * b + SUB + KW, :] = wx_ref[:, cols]
            ref[PAY * (b + 1) - KW - 1:PAY * (b + 1) - 1, :] = wy_ref[:, cols]
            ref[PAY * (b + 1) - 1:PAY * (b + 1), :] = code[b:b + 1, :]
    loads[5].wait()
    for c in range(CG):
        end = jnp.concatenate([maps_ref[i, c] for i in range(2)], axis=1)
        n = min(HALF, MAPS - HALF * c)
        sp_ref[HALF * c:HALF * c + n, 2 * WIDE:] = end[:n]
        sq_ref[c, :, 2 * WIDE:] = end[HALF:]
        if n < HALF:
            sm_ref[:, 2 * WIDE:] = end[n:HALF]
    for cp in loads[KW:]:
        cp.wait()


def split3(x):
    hi = x.astype(BF).astype(F32)
    r = x - hi
    mid = r.astype(BF).astype(F32)
    return hi, mid, r - mid


def accumulate(pay_ref, accs, us, xs, vs, r_ref, int_ref, base_ref, sem):
    row_i = lax.broadcasted_iota(jnp.int32, (WIN, LANES), 0)

    def make_u(blk, k):
        off = jnp.minimum(blk, NB - 1) * PAY
        y8 = pay_ref[pl.ds(off, SUB), :]
        wx = pay_ref[pl.ds(off + SUB, SUB), :]
        wyp = pay_ref[pl.ds(off + PAY - SUB, SUB), :]
        d = (row_i - (wyp[7:, :].astype(jnp.int32) // CODE)) & (WIN - 1)
        p = jnp.zeros((WIN, LANES), F32)
        for a in range(KW):
            p = jnp.where(d == a, wyp[a + 1:a + 2, :], p)
        us[k][...] = jnp.concatenate([y8 * p[i:i + 1, :] for i in range(WIN)], axis=0).T
        x3 = list(split3(wx)) + [jnp.zeros((LANES - HW, LANES), F32)]
        xs[k][...] = jnp.concatenate(x3, axis=0).T

    def make_v(k):
        lhs = xs[k][...].astype(BF)
        u = us[k][...]
        for bp in range(3):
            w = jnp.dot(lhs, r_ref[:, WIDE * bp:WIDE * bp + WIDE], preferred_element_type=F32)
            for c in range(2):
                v = w[:, LANES * c:LANES * (c + 1)] * u
                for g in range(WIN):
                    vs[k][pl.ds(SUB * PS * g + 2 * bp + c, SUB, stride=PS), :] = v[SUB * g:SUB * g + SUB, :]

    def add_tiles(blk, k):
        row = base_ref.at[blk]
        for j in range(LANES):
            acc = accs[j % T]
            b = row[j]
            acc[pl.ds(b, SUB), :] = acc[pl.ds(b, SUB), :] + vs[k][PS * j:PS * j + SUB, :]

    code = jnp.concatenate([pay_ref[PAY * (b + 1) - 1:PAY * (b + 1), :] for b in range(NB)], axis=0).astype(jnp.int32)
    int_ref[...] = (((code // CODE - 5) * 187) >> STEP) * CW + (code & (CODE - 1))
    kk = lax.broadcasted_iota(jnp.int32, (LANES, WIDE * 3), 0)
    ll = lax.broadcasted_iota(jnp.int32, (LANES, WIDE * 3), 1)
    r_ref[...] = jnp.where((kk < HW) & ((kk & 7) == (ll >> 7)), 1.0, 0.0).astype(BF)
    for v in vs:
        v[...] = jnp.zeros_like(v)
    load = pltpu.make_async_copy(int_ref, base_ref, sem)
    load.start()
    make_u(0, 0)
    make_u(1, 1)
    make_v(0)
    load.wait()

    def body(n, _):
        k = 2 * n
        make_v(1)
        add_tiles(k, 0)
        make_u(k + 2, 0)
        make_v(0)
        add_tiles(k + 1, 1)
        make_u(k + 3, 1)
        return 0

    lax.fori_loop(0, NB // 2, body, 0)


def folded(accs, off, n, clear=False):
    def total(g):
        rows = pl.ds(pl.multiple_of(g * CW + off, SUB), n)
        v = accs[0][rows, :]
        for a in accs[1:]:
            v = v + a[rows, :]
        if clear:
            for a in accs:
                a[rows, :] = jnp.zeros((n, LANES), F32)
        return v

    row = lax.broadcasted_iota(jnp.int32, (n, LANES), 1) >> 3
    tiles = [None] * TILES
    for g in range(NG):
        v = total(g)
        if g == 0:
            ghost = v
        first = 5 + STEP * g
        for p in range(TILES):
            lo, hi = max(first, SUB + WIN * p), min(first + WIN, SUB + WIN * (p + 1))
            if lo < hi:
                part = jnp.where((row - lo & (WIN - 1)) < hi - lo, v, 0.0)
                tiles[p] = part if tiles[p] is None else tiles[p] + part
    return tiles + [jnp.where(row >= SUB, v, ghost)]


def own_kernel(pay_ref, out_ref, *refs):
    accs, scr = refs[:T], refs[T:]

    def clear(n, _):
        for a in accs:
            a[pl.ds(pl.multiple_of(n * CW, SUB), CW), :] = jnp.zeros((CW, LANES), F32)
        return 0

    lax.fori_loop(0, NG, clear, 0)
    accumulate(pay_ref, accs, scr[:2], scr[2:4], scr[4:6], *scr[6:])

    def fold(q, _):
        off = pl.multiple_of(q * WIN, WIN)
        for p, t in enumerate(folded(accs, off, WIN, clear=True)):
            out_ref[p, pl.ds(off, WIN), :] = t
        return 0

    lax.fori_loop(0, CW // WIN, fold, 0)


def far_kernel(pay_ref, a_ref, *refs):
    accs, pack_ref, gh_ref, scr = refs[T:2 * T], refs[2 * T], refs[2 * T + 1], refs[2 * T + 2:]
    accumulate(pay_ref, accs, scr[:2], scr[2:4], scr[4:6], *scr[6:])
    own0 = lax.axis_index('cols') * CB
    far0 = CB - own0

    def ghost(off, n):
        high = lax.broadcasted_iota(jnp.int32, (n, LANES), 1) >= HALF
        ends = []
        for g in (0, NG - 1):
            rows = pl.ds(pl.multiple_of(g * CW + off, SUB), n)
            v = accs[0][rows, :]
            for a in accs[1:]:
                v = v + a[rows, :]
            ends.append(v)
        return jnp.where(high, ends[1], ends[0])

    def copy(n, _):
        o = pl.multiple_of(n * QTR, SUB)
        gh_ref[pl.ds(pl.multiple_of(far0 + o, SUB), QTR), :] = ghost(SUB + o, QTR)
        gh_ref[pl.ds(pl.multiple_of(own0 + o, SUB), QTR), :] = a_ref[TILES, pl.ds(pl.multiple_of(SUB + o, SUB), QTR), :]
        return 0

    lax.fori_loop(0, CB // QTR, copy, 0)
    for dst, add in ((own0, ghost(CW - SUB, SUB)), (own0 + CB - SUB, ghost(0, SUB)), (far0, a_ref[TILES, CW - SUB:, :]), (far0 + CB - SUB, a_ref[TILES, :SUB, :])):
        rows = pl.ds(pl.multiple_of(dst, SUB), SUB)
        gh_ref[rows, :] = gh_ref[rows, :] + add

    lane = lax.broadcasted_iota(jnp.int32, (LANES, LANES), 1)
    for side, lane0 in ((0, HALF - HW), (1, HALF)):
        out = jnp.zeros((LANES, LANES), F32)
        for j in range(5):
            piece = pltpu.roll(gh_ref[LANES * j:LANES * (j + 1), :], (HW * j - lane0) % LANES, axis=1)
            out = jnp.where(lane >= HW * j, piece, out)
        pack_ref[side] = out


def image_kernel(*refs):
    accs = refs[:T]
    (a_ref, pack_ref, so_ref, sx_ref, sm_ref, se_ref, d_ref, ev_ref, eu_ref, pm_ref, out_ref,
     tb_ref, edge_ref, g_ref, halo, sm1, sm2, sr1, sr2, hm1, hm2, hr1, hr2, s_main, s_rem, acc_m, acc_r, sx_mid, pieces, recvs, tails, recvs_t,
     halo_ss, halo_rs, swap_ss, swap_rs, red_ss, red_rs) = refs[T:]
    k = lax.axis_index('cols')
    r = lax.axis_index('rows')
    core, x = r % 2, r // 2
    near = r + 1 - 2 * core
    across = (r + 2) % 4
    prev, nxt = (r + 3) % 4, (r + 1) % 4
    homes = ({'rows': across, 'cols': 1 - k}, {'rows': across}, {'cols': 1 - k})

    barrier = pltpu.get_barrier_semaphore()
    for dev in ({'rows': prev}, {'rows': nxt}) + homes:
        pl.semaphore_signal(barrier, inc=1, device_id=dev, device_id_type=MESH_ID)

    own0 = k * CB
    far0 = CB - own0
    high16 = lax.broadcasted_iota(jnp.int32, (WIN, LANES), 1) >= HALF

    def put(v, tiles):
        rows = pl.ds(pl.multiple_of(v, WIN), WIN)
        for p in range(TILES):
            tb_ref[p, rows, :] = tiles[p].astype(BF)
        edge_ref[rows, :] = jnp.where(high16, tiles[0], tiles[9])

    def far_part(n, _):
        put(far0 + WIN * n, folded(accs, pl.multiple_of(SUB + WIN * n, SUB), WIN))
        return 0

    def own_part(n, _):
        put(own0 + WIN * n, [a_ref[p, pl.ds(pl.multiple_of(SUB + WIN * n, SUB), WIN), :] for p in range(TILES)])
        return 0

    last = CB // WIN - 1
    lax.fori_loop(1, last, far_part, 0)
    pl.semaphore_wait(barrier, 5)

    def remote(src, dst, ss, rs, i, dev):
        cp = pltpu.make_async_remote_copy(src_ref=src, dst_ref=dst, send_sem=ss.at[i], recv_sem=rs.at[i], device_id=dev, device_id_type=MESH_ID)
        cp.start()
        return cp

    halos = [remote(pack_ref.at[i], halo.at[i], halo_ss, halo_rs, i, {'rows': dev}) for i, dev in ((0, prev), (1, nxt))]

    lax.fori_loop(1, last, own_part, 0)
    none = jnp.zeros((SUB, LANES), F32)
    for n, side in ((0, CW - SUB), (last, 0)):
        off = SUB + WIN * n
        near_tiles = folded(accs, off, WIN)
        far_ends = folded(accs, side, SUB)
        order = (lambda v: [v, none]) if n == 0 else (lambda v: [none, v])
        put(far0 + WIN * n, [near_tiles[p] + jnp.concatenate(order(a_ref[p, side:side + SUB, :]), axis=0) for p in range(TILES)])
        put(own0 + WIN * n, [a_ref[p, off:off + WIN, :] + jnp.concatenate(order(far_ends[p]), axis=0) for p in range(TILES)])


    def to_rows(row0, n, t0, t1):
        a = jnp.concatenate([t0, t1], axis=1)
        g = lax.dot_general(pm_ref[...], a, (((1,), (1,)), ((), ())), preferred_element_type=F32).astype(BF)
        for ch in range(SUB):
            i, c = ch // 4, ch % 4
            g_ref[row0 + n * c:row0 + n * c + QTR, N_GRID * i:N_GRID * (i + 1)] = g[QTR * ch:QTR * (ch + 1), :]

    for m in range(CG):
        to_rows(QTR * m, LANES, tb_ref[2 * m + 1], tb_ref[2 * m + 2])

    mid = remote(sm_ref, sx_mid, halo_ss, halo_rs, 2, {'rows': across})

    sms, srs, hms, hrs = (sm1, sm2), (sr1, sr2), (hm1, hm2), (hr1, hr2)
    swaps, trades = [], []

    def columns(grp):
        start, n = GROUPS[grp]
        lane = lax.broadcasted_iota(jnp.int32, (n, LANES), 1)
        side = lane >> 6
        own_even, far_even = side == core, side != core
        block = (lane & (HALF - 1)) >> 4
        h = jnp.dot(g_ref[4 * start:4 * (start + n), :], ev_ref[...], preferred_element_type=F32)
        hc = [h[n * c:n * (c + 1)] for c in range(CG)]
        rems = [v[:, 4 * LANES:] for v in hc]
        for cp in range(2):
            hs = [[v[:, LANES * i:LANES * (i + 1)] for i in range(CG)] for v in hc[2 * cp:2 * cp + 2]]
            for i in range(CG):
                dp, t = i // 2, i % 2
                odd = pltpu.roll(hs[1][i], HALF, axis=1)
                sms[grp][dp, cp, t] = jnp.where(far_even, hs[0][i], odd).astype(BF)
                hms[grp][dp, cp, t, core] = jnp.where(own_even, hs[0][i], odd).astype(BF)
        for d in range(ROWS):
            out = rems[d]
            for c in range(CG):
                if c != d:
                    out = jnp.where(block == c, pltpu.roll(rems[c], (WIN * (c - d)) % LANES, axis=1), out)
            srs[grp][d] = out.astype(BF)
        hrs[grp][r] = srs[grp][r]
        swaps.append(remote(sms[grp], hms[grp].at[:, :, :, core], swap_ss, swap_rs, grp, {'rows': near}))
        for i, dev in enumerate((across, 3 - r, near)):
            trades.append(remote(srs[grp].at[dev], hrs[grp].at[r], swap_ss, swap_rs, 2 + 3 * grp + i, {'rows': dev}))

    columns(0)

    for h in halos:
        h.wait()
    lane = lax.broadcasted_iota(jnp.int32, (LANES, LANES), 1)
    low = lane < HALF
    t0s, t9s = [], []
    for j in range(5):
        rows = slice(LANES * j, LANES * (j + 1))
        add_first = pltpu.roll(halo[1], (HALF - HW * j) % LANES, axis=1)
        add_last = pltpu.roll(halo[0], (HALF - HW - HW * j) % LANES, axis=1)
        e = edge_ref[rows, :] + jnp.where(low, jnp.where(lane >= HALF - HW, add_last, 0.0), jnp.where(lane < HALF + HW, add_first, 0.0))
        t0s.append(jnp.where(low, tb_ref[0, rows, :].astype(F32), e).astype(BF))
        t9s.append(jnp.where(low, e, tb_ref[9, rows, :].astype(F32)).astype(BF))
    lane = lax.broadcasted_iota(jnp.int32, (PB, LANES), 1)
    low = lane < HALF
    to_rows(4 * LANES, QTR, jnp.concatenate(t0s, axis=0), jnp.concatenate(t9s, axis=0))
    columns(1)

    def turn(rows):
        t = [rows[:, LANES * i:LANES * (i + 1)].T for i in range(5)]
        return [jnp.concatenate([t[2 * i], t[2 * i + 1], t[4][HALF * i:HALF * (i + 1)]], axis=0) for i in range(2)]


    for cp in swaps[:1]:
        cp.wait_recv()
    n0 = 4 * GROUPS[0][1]

    def block_of(grp, j):
        return jnp.concatenate([hms[grp][(x + j) % 2, cp].reshape(4 * GROUPS[grp][1], LANES) for cp in range(2)], axis=1)

    mid.wait_recv()
    for j, ref, end in ((1, sx_ref, sx_mid), (0, so_ref, sm_ref)):
        c = [ref[HALF * i:HALF * (i + 1), :] for i in range(3)] + [jnp.concatenate([ref[3 * HALF:, :], end[...]], axis=0)]
        acc_m[j] = jnp.dot(eu_ref[x, :, :n0], block_of(0, j), preferred_element_type=F32)
        for cp in range(2):
            s_main[j, 0, cp], s_main[j, 1, cp] = turn(jnp.concatenate([jnp.where(core == 0, c[2 * cp], c[2 * cp + 1]), jnp.where(core == 0, c[2 * cp + 1], c[2 * cp])], axis=0))

    for cp in swaps[1:]:
        cp.wait_recv()

    def rows_dft(half, acc, rhs):
        rows = pl.ds(pl.multiple_of(half * N_IMG, WIN), N_IMG)
        total = acc[rows, :] + jnp.dot(eu_ref[x, rows, n0:], rhs, preferred_element_type=F32)
        return total[:PB], total[PB:]

    quarter = lax.broadcasted_iota(jnp.int32, (PB // 4, LANES), 1) >> 5

    def piece(half, j):
        i_re, i_im = rows_dft(half, acc_m.at[j], block_of(1, j))
        rows = pl.ds(pl.multiple_of(half * PB, SUB), PB)
        re, im = None, None
        for cp in range(2):
            cols = slice(LANES * cp, LANES * (cp + 1))
            s_re, s_im = s_main[j, 0, cp, rows, :], s_main[j, 1, cp, rows, :]
            a = s_re * i_re[:, cols] + s_im * i_im[:, cols]
            b = s_re * i_im[:, cols] - s_im * i_re[:, cols]
            re, im = (a, b) if re is None else (re + a, im + b)
        return jnp.where(low, re + pltpu.roll(re, HALF, axis=1), im + pltpu.roll(im, HALF, axis=1))

    def rest(half):
        parts = []
        for o in range(2):
            rows = pl.ds(pl.multiple_of(half * N_IMG + PB * o, WIN), PB)
            parts.append(acc_r[0, rows, :] + pltpu.roll(acc_r[1, rows, :], HALF, axis=1))
        i_re, i_im = parts
        rows = pl.ds(pl.multiple_of(half * PB, SUB), PB)
        s_re, s_im = s_rem[0, rows, :], s_rem[1, rows, :]
        w = s_re * i_re + s_im * i_im + pltpu.roll(s_re * i_im - s_im * i_re, HALF, axis=1)
        w = w + pltpu.roll(w, LANES - QTR, axis=1)
        w = w + pltpu.roll(w, LANES - WIN, axis=1)
        w = jnp.where(lane < WIN, w, pltpu.roll(w, LANES - HALF + WIN, axis=1))
        out = w[:PB // 4]
        for g in range(1, 4):
            out = jnp.where(quarter == g, pltpu.roll(w[PB // 4 * g:PB // 4 * (g + 1)], QTR * g, axis=1), out)
        return out

    first, other = pl.ds(0, JOIN), pl.ds(JOIN, PB - JOIN)
    pieces[0] = piece(1 - k, 1)
    joined = remote(pieces.at[0, first], recvs.at[0, first], red_ss, red_rs, 0, homes[1])
    sends = [remote(pieces.at[0, other], recvs.at[0, other], red_ss, red_rs, 1, homes[0])]
    across_y = piece(1 - k, 0)
    pieces[2, JOIN:] = across_y[JOIN:]
    sends.append(remote(pieces.at[2, other], recvs.at[2, other], red_ss, red_rs, 4, homes[2]))
    pieces[1] = piece(k, 1)
    sends.append(remote(pieces.at[1], recvs.at[1], red_ss, red_rs, 2, homes[1]))
    for cp in trades:
        cp.wait_recv()
    for t in range(2):
        total = None
        for grp in range(2):
            kk = 2 * GROUPS[grp][1]
            for c in range(2):
                part = jnp.dot(eu_ref[c, :, n0 * grp + kk * t:n0 * grp + kk * (t + 1)], hrs[grp][2 * c:2 * c + 2].reshape(kk, LANES), preferred_element_type=F32)
                total = part if total is None else total + part
        acc_r[t] = total
    s_rem[0], s_rem[1] = turn(jnp.concatenate([se_ref[c] for c in range(CG)] + [jnp.zeros((HALF, N_GRID), F32)], axis=0))
    tails[...] = rest(1 - k)
    tail = remote(tails, recvs_t, red_ss, red_rs, 3, homes[2])
    rem = rest(k)
    joined.wait_recv()
    pieces[2, :JOIN] = across_y[:JOIN] + recvs[0, :JOIN]
    sends.append(remote(pieces.at[2, first], recvs.at[2, first], red_ss, red_rs, 5, homes[2]))
    main = piece(k, 0)
    d8 = jnp.broadcast_to(jnp.concatenate([d_ref[...][None, :], jnp.zeros((1, HALF), F32)], axis=1), (SUB, N_IMG + HALF))
    dq = d8
    for j in range(1, ROWS):
        dq = jnp.where(r == j, pltpu.roll(d8, N_IMG + HALF - QB * j, axis=1), dq)
    dp = jnp.where(k == 0, d8, pltpu.roll(d8, N_IMG + HALF - PB, axis=1))[:, :2 * LANES]
    dd = jnp.concatenate([dp] * WIN, axis=0).T[:PB] * dq[:1, :LANES]

    for cp in sends:
        cp.wait_recv()
    main = main + recvs[1] + recvs[2]
    main = jnp.concatenate([main[:JOIN], main[JOIN:] + recvs[0, JOIN:]], axis=0)
    tail.wait_recv()
    rem = rem + recvs_t[...]
    for o in range(2):
        m = pltpu.roll(main, HALF, axis=1) if o else main
        for j in range(CG):
            rows = slice(PB // 4 * j, PB // 4 * (j + 1))
            end = pltpu.roll(rem, (HALF - QTR * j - WIN * o) % LANES, axis=1)
            out_ref[o, rows, :] = (jnp.where(low[rows], m[rows], end) * dd[rows])[:, :QB]

    for cp in sends + swaps + trades + [mid, tail, joined]:
        cp.wait_send()


def solution(mesh):
    sample_spec = ('exam', 'rows', 'cols')
    vm = pl.BlockSpec(memory_space=pltpu.VMEM)
    hbm = pl.BlockSpec(memory_space=pltpu.HBM)
    spread_scratch = ([VMEM((LANES, LANES), F32)] * 4 + [VMEM((LANES * PS, LANES), F32)] * 2
                      + [VMEM((LANES, WIDE * 3), BF), VMEM((NB, LANES), jnp.int32), pltpu.SMEM((NB, LANES), jnp.int32), pltpu.SemaphoreType.DMA])
    acc_shape = [jax.ShapeDtypeStruct((NG * CW, LANES), F32)] * T
    big = 6 * MIB

    def local_fn(kspace, wts_y, wts_x, idx_y, idx_x, coil_maps, deapod):
        own, far, maps, maps_end, maps_mid = pl.pallas_call(
            prep_kernel,
            out_shape=[jax.ShapeDtypeStruct((PAY * NB, LANES), F32)] * 2 + [jax.ShapeDtypeStruct(d, F32) for d in ((MAPS, N_GRID), (4, WIN, N_GRID), (WIN, N_GRID))],
            in_specs=[hbm] * 6, out_specs=[vm] * 5, name='prep',
            scratch_shapes=[VMEM((2, SUB, NS), F32), VMEM((KW, NS), F32), VMEM((KW, NS), F32), VMEM((NB, LANES), jnp.int32), VMEM((NB, LANES), jnp.int32), VMEM((2, 4, QB, HALF), F32), pltpu.SemaphoreType.DMA((24,))],
            compiler_params=pltpu.CompilerParams(vmem_limit_bytes=SUB * MIB),
        )(*[pltpu.with_memory_space_constraint(v, pltpu.HBM) for v in (kspace, wts_y, wts_x, idx_y.reshape(NB, LANES), idx_x.reshape(NB, LANES), jnp.swapaxes(coil_maps, 2, 3))])
        far_in = lax.ppermute(far, 'cols', [(0, 1), (1, 0)])
        half, *accs = pl.pallas_call(
            own_kernel, out_shape=[jax.ShapeDtypeStruct((11, CW, LANES), F32)] + acc_shape, in_specs=[vm], out_specs=[vm] * (T + 1),
            scratch_shapes=spread_scratch, compiler_params=pltpu.CompilerParams(vmem_limit_bytes=big), name='spread_own',
            cost_estimate=pl.CostEstimate(flops=GIGA, bytes_accessed=4 * MIB, transcendentals=0),
        )(own)
        *accs, pack = pl.pallas_call(
            far_kernel, out_shape=acc_shape + [jax.ShapeDtypeStruct((2, LANES, LANES), F32)],
            in_specs=[vm] * (T + 2), out_specs=[vm] * (T + 1), scratch_shapes=[VMEM((N_GRID, LANES), F32)] + spread_scratch,
            input_output_aliases={i + 2: i for i in range(T)},
            compiler_params=pltpu.CompilerParams(vmem_limit_bytes=big), name='spread_far',
            cost_estimate=pl.CostEstimate(flops=GIGA, bytes_accessed=4 * MIB, transcendentals=0),
        )(far_in, half, *accs)
        maps_x = lax.ppermute(maps, 'rows', [(i, (i + 2) % ROWS) for i in range(ROWS)])
        dma = pltpu.SemaphoreType.DMA
        half_bufs = [VMEM((2, 2, 2, n, LANES), BF) for _, n in GROUPS] + [VMEM((ROWS, n, LANES), BF) for _, n in GROUPS]
        full_bufs = [VMEM((2, 2, 2, 2, n, LANES), BF) for _, n in GROUPS] + [VMEM((ROWS, n, LANES), BF) for _, n in GROUPS]
        return pl.pallas_call(
            image_kernel,
            out_shape=jax.ShapeDtypeStruct((2, PB, QB), F32), in_specs=[vm] * (T + TILES), out_specs=vm,
            scratch_shapes=[VMEM((TILES, N_GRID, LANES), BF), VMEM((N_GRID, LANES), F32), VMEM((4 * RB, 2 * N_GRID), BF), VMEM((2, LANES, LANES), F32)] + half_bufs + full_bufs + [
                VMEM((2, 2, 2, N_IMG, LANES), F32), VMEM((2, N_IMG, LANES), F32),
                VMEM((2, 2 * N_IMG, 2 * LANES), F32), VMEM((2, 2 * N_IMG, LANES), F32), VMEM((WIN, N_GRID), F32),
                VMEM((3, PB, LANES), F32), VMEM((3, PB, LANES), F32), VMEM((PB // 4, LANES), F32), VMEM((PB // 4, LANES), F32),
                dma((3,)), dma((3,)), dma((8,)), dma((8,)), dma((6,)), dma((6,)),
            ],
            compiler_params=pltpu.CompilerParams(vmem_limit_bytes=11 * MIB, collective_id=0, has_side_effects=True), name='image',
        )(*accs, half, pack, maps, maps_x, maps_mid, maps_end, deapod, col_dft(), row_dft(), unmix())

    return jax.shard_map(
        local_fn,
        mesh=mesh,
        in_specs=(P(None, None, sample_spec), P(None, sample_spec), P(None, sample_spec), P(sample_spec), P(sample_spec), P(None, ('exam', 'cols'), None, 'rows'), P()),
        out_specs=P(None, ('exam', 'cols'), 'rows'),
        check_vma=False,
    )
```

```python
import functools
import math

import jax
import jax.numpy as jnp
import numpy as np
from jax import lax
from jax.experimental import pallas as pl
from jax.experimental.pallas import tpu as pltpu
from jax.sharding import PartitionSpec as P

BF = jnp.bfloat16
F32 = jnp.float32
VMEM = pltpu.VMEM
LANES = 128
MIB = 1 << 20
GIGA = 4000 * MIB
TILES = 10
SUB, WIN, QTR, HALF, WIDE = 8, 16, 32, 64, 256
N_GRID, N_IMG, N_COILS, KW = 640, 320, 8, 6
ROWS, COLS = 4, 2
RB, CB, QB = N_GRID // ROWS, N_GRID // COLS, N_IMG // ROWS
PB = N_IMG // COLS
NS = 4096
NB = NS // LANES
STEP = 11
NG = 15
CW = CB + WIN
T = 7
PS = 9
PAY = 21
CODE = 512
JOIN = 64
CG = 4
MAPS = 240
HW = 24
ORDER = tuple(range(1, 9)) + (0, 9)
GROUPS = ((0, 128), (128, 32))
MESH_ID = pl.DeviceIdType.MESH


def dft_parts():
    freq = np.arange(N_GRID) - N_GRID // 2
    pos = np.arange(N_IMG) - N_IMG // 2
    ang = ((freq[:, None] * pos[None, :]) % N_GRID).astype(np.float32) * np.float32(2.0 * math.pi / N_GRID)
    norm = np.float32(1.0 / math.sqrt(N_GRID))
    c, s = np.cos(ang) * norm, np.sin(ang) * norm
    return np.stack([np.stack([c, s], 1), np.stack([-s, c], 1)], 0)


def col_dft():
    e = dft_parts()
    out = np.zeros((2 * N_GRID, N_GRID), np.float32)
    for dp in range(2):
        for t in range(2):
            for h in range(2):
                q0 = QB * (2 * dp + h)
                l0 = LANES * (2 * dp + t) + HALF * h
                out[:, l0:l0 + HALF] = e[:, :, t, q0:q0 + HALF].reshape(2 * N_GRID, HALF)
    for t in range(2):
        for d in range(CG):
            l0 = 4 * LANES + HALF * t + WIN * d
            out[:, l0:l0 + WIN] = e[:, :, t, QB * d + HALF:QB * (d + 1)].reshape(2 * N_GRID, WIN)
    return jnp.asarray(out, BF)


def row_dft():
    e = dft_parts()
    rows = np.concatenate([np.arange(WIN * l, WIN * (l + 1)) for l in ORDER])
    chips = []
    for x in range(2):
        parts = []
        for start, n in GROUPS:
            for t in range(2):
                for b in range(2):
                    parts.append(e[t, (2 * x + b) * RB + rows[start:start + n]])
        m = np.concatenate(parts, 0)
        chips.append(np.concatenate([m[:, :, PB * h:PB * (h + 1)].reshape(N_GRID, N_IMG).T for h in range(2)], 0))
    return jnp.asarray(np.array(chips), BF)


def unmix():
    m = np.zeros((WIDE, WIDE), np.float32)
    for ch in range(SUB):
        for pp in range(2):
            for i in range(WIN):
                m[ch * QTR + WIN * pp + (i + SUB) % WIN, pp * 128 + i * SUB + ch] = 1.0
    return jnp.asarray(m, BF)


def prep_kernel(ks_hbm, wy_hbm, wx_hbm, iy_hbm, ix_hbm, maps_hbm, own_ref, far_ref, sp_ref, sq_ref, sm_ref, ks_ref, wy_ref, wx_ref, iy_ref, ix_ref, maps_ref, sem):
    k = lax.axis_index('cols')
    r = lax.axis_index('rows')
    loads = []
    for src, dst in ((iy_hbm, iy_ref), (ix_hbm, ix_ref), (wx_hbm, wx_ref), (wy_hbm, wy_ref), (ks_hbm, ks_ref), (maps_hbm.at[:, :, :, WIDE:], maps_ref)):
        cp = pltpu.make_async_copy(src, dst, sem.at[len(loads)])
        cp.start()
        loads.append(cp)
    parts = []
    for c in range(CG):
        n = min(HALF, MAPS - HALF * c)
        parts += [(sp_ref.at[pl.ds(HALF * c, n)], c, pl.ds(0, n)), (sq_ref.at[c], c, pl.ds(HALF, WIN))]
    parts.append((sm_ref, 3, pl.ds(HALF - WIN, WIN)))
    for ref, c, q in parts:
        for i in range(2):
            cp = pltpu.make_async_copy(maps_hbm.at[i, c, q, pl.ds(0, WIDE)], ref.at[:, pl.ds(WIDE * i, WIDE)], sem.at[len(loads)])
            cp.start()
            loads.append(cp)
    loads[0].wait()
    loads[1].wait()
    iy = iy_ref[...]
    code = ((iy - r * RB + 5) * CODE + ix_ref[...] - k * CB + 5).astype(F32)
    for i in range(2, 5):
        loads[i].wait()
    lo = jnp.concatenate([ks_ref[0, 0:4, :], ks_ref[1, 0:4, :]], axis=0)
    hi = jnp.concatenate([ks_ref[0, 4:SUB, :], ks_ref[1, 4:SUB, :]], axis=0)
    first = k == 0
    for ref, y in ((own_ref, jnp.where(first, lo, hi)), (far_ref, jnp.where(first, hi, lo))):
        for b in range(NB):
            cols = slice(LANES * b, LANES * (b + 1))
            ref[PAY * b:PAY * b + SUB, :] = y[:, cols]
            ref[PAY * b + SUB:PAY * b + SUB + KW, :] = wx_ref[:, cols]
            ref[PAY * (b + 1) - KW - 1:PAY * (b + 1) - 1, :] = wy_ref[:, cols]
            ref[PAY * (b + 1) - 1:PAY * (b + 1), :] = code[b:b + 1, :]
    loads[5].wait()
    for c in range(CG):
        end = jnp.concatenate([maps_ref[i, c] for i in range(2)], axis=1)
        n = min(HALF, MAPS - HALF * c)
        sp_ref[HALF * c:HALF * c + n, 2 * WIDE:] = end[:n]
        sq_ref[c, :, 2 * WIDE:] = end[HALF:]
        if n < HALF:
            sm_ref[:, 2 * WIDE:] = end[n:HALF]
    for cp in loads[KW:]:
        cp.wait()


def split3(x):
    hi = x.astype(BF).astype(F32)
    r = x - hi
    mid = r.astype(BF).astype(F32)
    return hi, mid, r - mid


def accumulate(pay_ref, accs, us, xs, vs, r_ref, int_ref, base_ref, sem):
    row_i = lax.broadcasted_iota(jnp.int32, (WIN, LANES), 0)

    def make_u(blk, k):
        off = jnp.minimum(blk, NB - 1) * PAY
        y8 = pay_ref[pl.ds(off, SUB), :]
        wx = pay_ref[pl.ds(off + SUB, SUB), :]
        wyp = pay_ref[pl.ds(off + PAY - SUB, SUB), :]
        d = (row_i - (wyp[7:, :].astype(jnp.int32) // CODE)) & (WIN - 1)
        p = jnp.zeros((WIN, LANES), F32)
        for a in range(KW):
            p = jnp.where(d == a, wyp[a + 1:a + 2, :], p)
        us[k][...] = jnp.concatenate([y8 * p[i:i + 1, :] for i in range(WIN)], axis=0).T
        x3 = list(split3(wx)) + [jnp.zeros((LANES - HW, LANES), F32)]
        xs[k][...] = jnp.concatenate(x3, axis=0).T

    def make_v(k):
        lhs = xs[k][...].astype(BF)
        u = us[k][...]
        for bp in range(3):
            w = jnp.dot(lhs, r_ref[:, WIDE * bp:WIDE * bp + WIDE], preferred_element_type=F32)
            for c in range(2):
                v = w[:, LANES * c:LANES * (c + 1)] * u
                for g in range(WIN):
                    vs[k][pl.ds(SUB * PS * g + 2 * bp + c, SUB, stride=PS), :] = v[SUB * g:SUB * g + SUB, :]

    def add_tiles(blk, k):
        row = base_ref.at[blk]
        for j in range(LANES):
            acc = accs[j % T]
            b = row[j]
            acc[pl.ds(b, SUB), :] = acc[pl.ds(b, SUB), :] + vs[k][PS * j:PS * j + SUB, :]

    code = jnp.concatenate([pay_ref[PAY * (b + 1) - 1:PAY * (b + 1), :] for b in range(NB)], axis=0).astype(jnp.int32)
    int_ref[...] = (((code // CODE - 5) * 187) >> STEP) * CW + (code & (CODE - 1))
    kk = lax.broadcasted_iota(jnp.int32, (LANES, WIDE * 3), 0)
    ll = lax.broadcasted_iota(jnp.int32, (LANES, WIDE * 3), 1)
    r_ref[...] = jnp.where((kk < HW) & ((kk & 7) == (ll >> 7)), 1.0, 0.0).astype(BF)
    for v in vs:
        v[...] = jnp.zeros_like(v)
    load = pltpu.make_async_copy(int_ref, base_ref, sem)
    load.start()
    make_u(0, 0)
    make_u(1, 1)
    make_v(0)
    load.wait()

    def body(n, _):
        k = 2 * n
        make_v(1)
        add_tiles(k, 0)
        make_u(k + 2, 0)
        make_v(0)
        add_tiles(k + 1, 1)
        make_u(k + 3, 1)
        return 0

    lax.fori_loop(0, NB // 2, body, 0)


def folded(accs, off, n, clear=False):
    def total(g):
        rows = pl.ds(pl.multiple_of(g * CW + off, SUB), n)
        v = accs[0][rows, :]
        for a in accs[1:]:
            v = v + a[rows, :]
        if clear:
            for a in accs:
                a[rows, :] = jnp.zeros((n, LANES), F32)
        return v

    row = lax.broadcasted_iota(jnp.int32, (n, LANES), 1) >> 3
    tiles = [None] * TILES
    for g in range(NG):
        v = total(g)
        if g == 0:
            ghost = v
        first = 5 + STEP * g
        for p in range(TILES):
            lo, hi = max(first, SUB + WIN * p), min(first + WIN, SUB + WIN * (p + 1))
            if lo < hi:
                part = jnp.where((row - lo & (WIN - 1)) < hi - lo, v, 0.0)
                tiles[p] = part if tiles[p] is None else tiles[p] + part
    return tiles + [jnp.where(row >= SUB, v, ghost)]


def own_kernel(pay_ref, out_ref, *refs):
    accs, scr = refs[:T], refs[T:]

    def clear(n, _):
        for a in accs:
            a[pl.ds(pl.multiple_of(n * CW, SUB), CW), :] = jnp.zeros((CW, LANES), F32)
        return 0

    lax.fori_loop(0, NG, clear, 0)
    accumulate(pay_ref, accs, scr[:2], scr[2:4], scr[4:6], *scr[6:])

    def fold(q, _):
        off = pl.multiple_of(q * WIN, WIN)
        for p, t in enumerate(folded(accs, off, WIN, clear=True)):
            out_ref[p, pl.ds(off, WIN), :] = t
        return 0

    lax.fori_loop(0, CW // WIN, fold, 0)


def far_kernel(pay_ref, a_ref, *refs):
    accs, pack_ref, gh_ref, scr = refs[T:2 * T], refs[2 * T], refs[2 * T + 1], refs[2 * T + 2:]
    accumulate(pay_ref, accs, scr[:2], scr[2:4], scr[4:6], *scr[6:])
    own0 = lax.axis_index('cols') * CB
    far0 = CB - own0

    def ghost(off, n):
        high = lax.broadcasted_iota(jnp.int32, (n, LANES), 1) >= HALF
        ends = []
        for g in (0, NG - 1):
            rows = pl.ds(pl.multiple_of(g * CW + off, SUB), n)
            v = accs[0][rows, :]
            for a in accs[1:]:
                v = v + a[rows, :]
            ends.append(v)
        return jnp.where(high, ends[1], ends[0])

    def copy(n, _):
        o = pl.multiple_of(n * QTR, SUB)
        gh_ref[pl.ds(pl.multiple_of(far0 + o, SUB), QTR), :] = ghost(SUB + o, QTR)
        gh_ref[pl.ds(pl.multiple_of(own0 + o, SUB), QTR), :] = a_ref[TILES, pl.ds(pl.multiple_of(SUB + o, SUB), QTR), :]
        return 0

    lax.fori_loop(0, CB // QTR, copy, 0)
    for dst, add in ((own0, ghost(CW - SUB, SUB)), (own0 + CB - SUB, ghost(0, SUB)), (far0, a_ref[TILES, CW - SUB:, :]), (far0 + CB - SUB, a_ref[TILES, :SUB, :])):
        rows = pl.ds(pl.multiple_of(dst, SUB), SUB)
        gh_ref[rows, :] = gh_ref[rows, :] + add

    lane = lax.broadcasted_iota(jnp.int32, (LANES, LANES), 1)
    for side, lane0 in ((0, HALF - HW), (1, HALF)):
        out = jnp.zeros((LANES, LANES), F32)
        for j in range(5):
            piece = pltpu.roll(gh_ref[LANES * j:LANES * (j + 1), :], (HW * j - lane0) % LANES, axis=1)
            out = jnp.where(lane >= HW * j, piece, out)
        pack_ref[side] = out


def image_kernel(*refs):
    accs = refs[:T]
    (a_ref, pack_ref, so_ref, sx_ref, sm_ref, se_ref, d_ref, ev_ref, eu_ref, pm_ref, out_ref,
     tb_ref, edge_ref, g_ref, halo, sm1, sm2, sr1, sr2, hm1, hm2, hr1, hr2, s_main, s_rem, acc_m, acc_r, sx_mid, pieces, recvs, tails, recvs_t,
     halo_ss, halo_rs, swap_ss, swap_rs, red_ss, red_rs) = refs[T:]
    k = lax.axis_index('cols')
    r = lax.axis_index('rows')
    core, x = r % 2, r // 2
    near = r + 1 - 2 * core
    across = (r + 2) % 4
    prev, nxt = (r + 3) % 4, (r + 1) % 4
    homes = ({'rows': across, 'cols': 1 - k}, {'rows': across}, {'cols': 1 - k})

    barrier = pltpu.get_barrier_semaphore()
    for dev in ({'rows': prev}, {'rows': nxt}) + homes:
        pl.semaphore_signal(barrier, inc=1, device_id=dev, device_id_type=MESH_ID)

    own0 = k * CB
    far0 = CB - own0
    high16 = lax.broadcasted_iota(jnp.int32, (WIN, LANES), 1) >= HALF

    def put(v, tiles):
        rows = pl.ds(pl.multiple_of(v, WIN), WIN)
        for p in range(TILES):
            tb_ref[p, rows, :] = tiles[p].astype(BF)
        edge_ref[rows, :] = jnp.where(high16, tiles[0], tiles[9])

    def far_part(n, _):
        put(far0 + WIN * n, folded(accs, pl.multiple_of(SUB + WIN * n, SUB), WIN))
        return 0

    def own_part(n, _):
        put(own0 + WIN * n, [a_ref[p, pl.ds(pl.multiple_of(SUB + WIN * n, SUB), WIN), :] for p in range(TILES)])
        return 0

    last = CB // WIN - 1
    lax.fori_loop(1, last, far_part, 0)
    pl.semaphore_wait(barrier, 5)

    def remote(src, dst, ss, rs, i, dev):
        cp = pltpu.make_async_remote_copy(src_ref=src, dst_ref=dst, send_sem=ss.at[i], recv_sem=rs.at[i], device_id=dev, device_id_type=MESH_ID)
        cp.start()
        return cp

    halos = [remote(pack_ref.at[i], halo.at[i], halo_ss, halo_rs, i, {'rows': dev}) for i, dev in ((0, prev), (1, nxt))]

    lax.fori_loop(1, last, own_part, 0)
    none = jnp.zeros((SUB, LANES), F32)
    for n, side in ((0, CW - SUB), (last, 0)):
        off = SUB + WIN * n
        near_tiles = folded(accs, off, WIN)
        far_ends = folded(accs, side, SUB)
        order = (lambda v: [v, none]) if n == 0 else (lambda v: [none, v])
        put(far0 + WIN * n, [near_tiles[p] + jnp.concatenate(order(a_ref[p, side:side + SUB, :]), axis=0) for p in range(TILES)])
        put(own0 + WIN * n, [a_ref[p, off:off + WIN, :] + jnp.concatenate(order(far_ends[p]), axis=0) for p in range(TILES)])


    def to_rows(row0, n, t0, t1):
        a = jnp.concatenate([t0, t1], axis=1)
        g = lax.dot_general(pm_ref[...], a, (((1,), (1,)), ((), ())), preferred_element_type=F32).astype(BF)
        for ch in range(SUB):
            i, c = ch // 4, ch % 4
            g_ref[row0 + n * c:row0 + n * c + QTR, N_GRID * i:N_GRID * (i + 1)] = g[QTR * ch:QTR * (ch + 1), :]

    for m in range(CG):
        to_rows(QTR * m, LANES, tb_ref[2 * m + 1], tb_ref[2 * m + 2])

    mid = remote(sm_ref, sx_mid, halo_ss, halo_rs, 2, {'rows': across})

    sms, srs, hms, hrs = (sm1, sm2), (sr1, sr2), (hm1, hm2), (hr1, hr2)
    swaps, trades = [], []

    def columns(grp):
        start, n = GROUPS[grp]
        lane = lax.broadcasted_iota(jnp.int32, (n, LANES), 1)
        side = lane >> 6
        own_even, far_even = side == core, side != core
        block = (lane & (HALF - 1)) >> 4
        h = jnp.dot(g_ref[4 * start:4 * (start + n), :], ev_ref[...], preferred_element_type=F32)
        hc = [h[n * c:n * (c + 1)] for c in range(CG)]
        rems = [v[:, 4 * LANES:] for v in hc]
        for cp in range(2):
            hs = [[v[:, LANES * i:LANES * (i + 1)] for i in range(CG)] for v in hc[2 * cp:2 * cp + 2]]
            for i in range(CG):
                dp, t = i // 2, i % 2
                odd = pltpu.roll(hs[1][i], HALF, axis=1)
                sms[grp][dp, cp, t] = jnp.where(far_even, hs[0][i], odd).astype(BF)
                hms[grp][dp, cp, t, core] = jnp.where(own_even, hs[0][i], odd).astype(BF)
        for d in range(ROWS):
            out = rems[d]
            for c in range(CG):
                if c != d:
                    out = jnp.where(block == c, pltpu.roll(rems[c], (WIN * (c - d)) % LANES, axis=1), out)
            srs[grp][d] = out.astype(BF)
        hrs[grp][r] = srs[grp][r]
        swaps.append(remote(sms[grp], hms[grp].at[:, :, :, core], swap_ss, swap_rs, grp, {'rows': near}))
        for i, dev in enumerate((across, 3 - r, near)):
            trades.append(remote(srs[grp].at[dev], hrs[grp].at[r], swap_ss, swap_rs, 2 + 3 * grp + i, {'rows': dev}))

    columns(0)

    for h in halos:
        h.wait()
    lane = lax.broadcasted_iota(jnp.int32, (LANES, LANES), 1)
    low = lane < HALF
    t0s, t9s = [], []
    for j in range(5):
        rows = slice(LANES * j, LANES * (j + 1))
        add_first = pltpu.roll(halo[1], (HALF - HW * j) % LANES, axis=1)
        add_last = pltpu.roll(halo[0], (HALF - HW - HW * j) % LANES, axis=1)
        e = edge_ref[rows, :] + jnp.where(low, jnp.where(lane >= HALF - HW, add_last, 0.0), jnp.where(lane < HALF + HW, add_first, 0.0))
        t0s.append(jnp.where(low, tb_ref[0, rows, :].astype(F32), e).astype(BF))
        t9s.append(jnp.where(low, e, tb_ref[9, rows, :].astype(F32)).astype(BF))
    lane = lax.broadcasted_iota(jnp.int32, (PB, LANES), 1)
    low = lane < HALF
    to_rows(4 * LANES, QTR, jnp.concatenate(t0s, axis=0), jnp.concatenate(t9s, axis=0))
    columns(1)

    def turn(rows):
        t = [rows[:, LANES * i:LANES * (i + 1)].T for i in range(5)]
        return [jnp.concatenate([t[2 * i], t[2 * i + 1], t[4][HALF * i:HALF * (i + 1)]], axis=0) for i in range(2)]


    for cp in swaps[:1]:
        cp.wait_recv()
    n0 = 4 * GROUPS[0][1]

    def block_of(grp, j):
        return jnp.concatenate([hms[grp][(x + j) % 2, cp].reshape(4 * GROUPS[grp][1], LANES) for cp in range(2)], axis=1)

    mid.wait_recv()
    for j, ref, end in ((1, sx_ref, sx_mid), (0, so_ref, sm_ref)):
        c = [ref[HALF * i:HALF * (i + 1), :] for i in range(3)] + [jnp.concatenate([ref[3 * HALF:, :], end[...]], axis=0)]
        acc_m[j] = jnp.dot(eu_ref[x, :, :n0], block_of(0, j), preferred_element_type=F32)
        for cp in range(2):
            s_main[j, 0, cp], s_main[j, 1, cp] = turn(jnp.concatenate([jnp.where(core == 0, c[2 * cp], c[2 * cp + 1]), jnp.where(core == 0, c[2 * cp + 1], c[2 * cp])], axis=0))

    for cp in swaps[1:]:
        cp.wait_recv()

    def rows_dft(half, acc, rhs):
        rows = pl.ds(pl.multiple_of(half * N_IMG, WIN), N_IMG)
        total = acc[rows, :] + jnp.dot(eu_ref[x, rows, n0:], rhs, preferred_element_type=F32)
        return total[:PB], total[PB:]

    quarter = lax.broadcasted_iota(jnp.int32, (PB // 4, LANES), 1) >> 5

    def piece(half, j):
        i_re, i_im = rows_dft(half, acc_m.at[j], block_of(1, j))
        rows = pl.ds(pl.multiple_of(half * PB, SUB), PB)
        re, im = None, None
        for cp in range(2):
            cols = slice(LANES * cp, LANES * (cp + 1))
            s_re, s_im = s_main[j, 0, cp, rows, :], s_main[j, 1, cp, rows, :]
            a = s_re * i_re[:, cols] + s_im * i_im[:, cols]
            b = s_re * i_im[:, cols] - s_im * i_re[:, cols]
            re, im = (a, b) if re is None else (re + a, im + b)
        return jnp.where(low, re + pltpu.roll(re, HALF, axis=1), im + pltpu.roll(im, HALF, axis=1))

    def rest(half):
        parts = []
        for o in range(2):
            rows = pl.ds(pl.multiple_of(half * N_IMG + PB * o, WIN), PB)
            parts.append(acc_r[0, rows, :] + pltpu.roll(acc_r[1, rows, :], HALF, axis=1))
        i_re, i_im = parts
        rows = pl.ds(pl.multiple_of(half * PB, SUB), PB)
        s_re, s_im = s_rem[0, rows, :], s_rem[1, rows, :]
        w = s_re * i_re + s_im * i_im + pltpu.roll(s_re * i_im - s_im * i_re, HALF, axis=1)
        w = w + pltpu.roll(w, LANES - QTR, axis=1)
        w = w + pltpu.roll(w, LANES - WIN, axis=1)
        w = jnp.where(lane < WIN, w, pltpu.roll(w, LANES - HALF + WIN, axis=1))
        out = w[:PB // 4]
        for g in range(1, 4):
            out = jnp.where(quarter == g, pltpu.roll(w[PB // 4 * g:PB // 4 * (g + 1)], QTR * g, axis=1), out)
        return out

    first, other = pl.ds(0, JOIN), pl.ds(JOIN, PB - JOIN)
    pieces[0] = piece(1 - k, 1)
    joined = remote(pieces.at[0, first], recvs.at[0, first], red_ss, red_rs, 0, homes[1])
    sends = [remote(pieces.at[0, other], recvs.at[0, other], red_ss, red_rs, 1, homes[0])]
    across_y = piece(1 - k, 0)
    pieces[2, JOIN:] = across_y[JOIN:]
    sends.append(remote(pieces.at[2, other], recvs.at[2, other], red_ss, red_rs, 4, homes[2]))
    pieces[1] = piece(k, 1)
    sends.append(remote(pieces.at[1], recvs.at[1], red_ss, red_rs, 2, homes[1]))
    for cp in trades:
        cp.wait_recv()
    for t in range(2):
        total = None
        for grp in range(2):
            kk = 2 * GROUPS[grp][1]
            for c in range(2):
                part = jnp.dot(eu_ref[c, :, n0 * grp + kk * t:n0 * grp + kk * (t + 1)], hrs[grp][2 * c:2 * c + 2].reshape(kk, LANES), preferred_element_type=F32)
                total = part if total is None else total + part
        acc_r[t] = total
    s_rem[0], s_rem[1] = turn(jnp.concatenate([se_ref[c] for c in range(CG)] + [jnp.zeros((HALF, N_GRID), F32)], axis=0))
    tails[...] = rest(1 - k)
    tail = remote(tails, recvs_t, red_ss, red_rs, 3, homes[2])
    rem = rest(k)
    joined.wait_recv()
    pieces[2, :JOIN] = across_y[:JOIN] + recvs[0, :JOIN]
    sends.append(remote(pieces.at[2, first], recvs.at[2, first], red_ss, red_rs, 5, homes[2]))
    main = piece(k, 0)
    d8 = jnp.broadcast_to(jnp.concatenate([d_ref[...][None, :], jnp.zeros((1, HALF), F32)], axis=1), (SUB, N_IMG + HALF))
    dq = d8
    for j in range(1, ROWS):
        dq = jnp.where(r == j, pltpu.roll(d8, N_IMG + HALF - QB * j, axis=1), dq)
    dp = jnp.where(k == 0, d8, pltpu.roll(d8, N_IMG + HALF - PB, axis=1))[:, :2 * LANES]
    dd = jnp.concatenate([dp] * WIN, axis=0).T[:PB] * dq[:1, :LANES]

    for cp in sends:
        cp.wait_recv()
    main = main + recvs[1] + recvs[2]
    main = jnp.concatenate([main[:JOIN], main[JOIN:] + recvs[0, JOIN:]], axis=0)
    tail.wait_recv()
    rem = rem + recvs_t[...]
    for o in range(2):
        m = pltpu.roll(main, HALF, axis=1) if o else main
        for j in range(CG):
            rows = slice(PB // 4 * j, PB // 4 * (j + 1))
            end = pltpu.roll(rem, (HALF - QTR * j - WIN * o) % LANES, axis=1)
            out_ref[o, rows, :] = (jnp.where(low[rows], m[rows], end) * dd[rows])[:, :QB]

    for cp in sends + swaps + trades + [mid, tail, joined]:
        cp.wait_send()


def solution(mesh):
    sample_spec = ('exam', 'rows', 'cols')
    vm = pl.BlockSpec(memory_space=pltpu.VMEM)
    hbm = pl.BlockSpec(memory_space=pltpu.HBM)
    spread_scratch = ([VMEM((LANES, LANES), F32)] * 4 + [VMEM((LANES * PS, LANES), F32)] * 2
                      + [VMEM((LANES, WIDE * 3), BF), VMEM((NB, LANES), jnp.int32), pltpu.SMEM((NB, LANES), jnp.int32), pltpu.SemaphoreType.DMA])
    acc_shape = [jax.ShapeDtypeStruct((NG * CW, LANES), F32)] * T
    big = 6 * MIB

    def local_fn(kspace, wts_y, wts_x, idx_y, idx_x, coil_maps, deapod):
        own, far, maps, maps_end, maps_mid = pl.pallas_call(
            prep_kernel,
            out_shape=[jax.ShapeDtypeStruct((PAY * NB, LANES), F32)] * 2 + [jax.ShapeDtypeStruct(d, F32) for d in ((MAPS, N_GRID), (4, WIN, N_GRID), (WIN, N_GRID))],
            in_specs=[hbm] * 6, out_specs=[vm] * 5, name='prep',
            scratch_shapes=[VMEM((2, SUB, NS), F32), VMEM((KW, NS), F32), VMEM((KW, NS), F32), VMEM((NB, LANES), jnp.int32), VMEM((NB, LANES), jnp.int32), VMEM((2, 4, QB, HALF), F32), pltpu.SemaphoreType.DMA((24,))],
            compiler_params=pltpu.CompilerParams(vmem_limit_bytes=SUB * MIB),
        )(*[pltpu.with_memory_space_constraint(v, pltpu.HBM) for v in (kspace, wts_y, wts_x, idx_y.reshape(NB, LANES), idx_x.reshape(NB, LANES), jnp.swapaxes(coil_maps, 2, 3))])
        far_in = lax.ppermute(far, 'cols', [(0, 1), (1, 0)])
        half, *accs = pl.pallas_call(
            own_kernel, out_shape=[jax.ShapeDtypeStruct((11, CW, LANES), F32)] + acc_shape, in_specs=[vm], out_specs=[vm] * (T + 1),
            scratch_shapes=spread_scratch, compiler_params=pltpu.CompilerParams(vmem_limit_bytes=big), name='spread_own',
            cost_estimate=pl.CostEstimate(flops=GIGA, bytes_accessed=4 * MIB, transcendentals=0),
        )(own)
        *accs, pack = pl.pallas_call(
            far_kernel, out_shape=acc_shape + [jax.ShapeDtypeStruct((2, LANES, LANES), F32)],
            in_specs=[vm] * (T + 2), out_specs=[vm] * (T + 1), scratch_shapes=[VMEM((N_GRID, LANES), F32)] + spread_scratch,
            input_output_aliases={i + 2: i for i in range(T)},
            compiler_params=pltpu.CompilerParams(vmem_limit_bytes=big), name='spread_far',
            cost_estimate=pl.CostEstimate(flops=GIGA, bytes_accessed=4 * MIB, transcendentals=0),
        )(far_in, half, *accs)
        maps_x = lax.ppermute(maps, 'rows', [(i, (i + 2) % ROWS) for i in range(ROWS)])
        dma = pltpu.SemaphoreType.DMA
        half_bufs = [VMEM((2, 2, 2, n, LANES), BF) for _, n in GROUPS] + [VMEM((ROWS, n, LANES), BF) for _, n in GROUPS]
        full_bufs = [VMEM((2, 2, 2, 2, n, LANES), BF) for _, n in GROUPS] + [VMEM((ROWS, n, LANES), BF) for _, n in GROUPS]
        return pl.pallas_call(
            image_kernel,
            out_shape=jax.ShapeDtypeStruct((2, PB, QB), F32), in_specs=[vm] * (T + TILES), out_specs=vm,
            scratch_shapes=[VMEM((TILES, N_GRID, LANES), BF), VMEM((N_GRID, LANES), F32), VMEM((4 * RB, 2 * N_GRID), BF), VMEM((2, LANES, LANES), F32)] + half_bufs + full_bufs + [
                VMEM((2, 2, 2, N_IMG, LANES), F32), VMEM((2, N_IMG, LANES), F32),
                VMEM((2, 2 * N_IMG, 2 * LANES), F32), VMEM((2, 2 * N_IMG, LANES), F32), VMEM((WIN, N_GRID), F32),
                VMEM((3, PB, LANES), F32), VMEM((3, PB, LANES), F32), VMEM((PB // 4, LANES), F32), VMEM((PB // 4, LANES), F32),
                dma((3,)), dma((3,)), dma((8,)), dma((8,)), dma((6,)), dma((6,)),
            ],
            compiler_params=pltpu.CompilerParams(vmem_limit_bytes=11 * MIB, collective_id=0, has_side_effects=True), name='image',
        )(*accs, half, pack, maps, maps_x, maps_mid, maps_end, deapod, col_dft(), row_dft(), unmix())

    return jax.shard_map(
        local_fn,
        mesh=mesh,
        in_specs=(P(None, None, sample_spec), P(None, sample_spec), P(None, sample_spec), P(sample_spec), P(sample_spec), P(None, ('exam', 'cols'), None, 'rows'), P()),
        out_specs=P(None, ('exam', 'cols'), 'rows'),
        check_vma=False,
    )
```
